32 devices in a mesh: dp: 1 (over z), sp: 32 (over y, x, core).
Axes of the slice: x: 4, y: 4, z: 1, core: 2. Of those that a mesh axis runs over, the one named last changes fastest.
The devices are a block of a 4x4x8 slice.
Arguments:
- x_in: bfloat16 [3, 2048, 2560], P('dp', 'sp')
- positions: int32 [3, 2048], P('dp', 'sp')
- keep_mask: int32 [3, 2048], P('dp', 'sp')
- ln_gain: float32 [2560], replicated
- ln_bias: float32 [2560], replicated
- w_qkv: bfloat16 [2560, 32, 3, 80], replicated
- b_qkv: float32 [32, 3, 80], replicated
- w_out: bfloat16 [2560, 2560], replicated
- b_out: float32 [2560], replicated
- grad_y: bfloat16 [3, 2048, 2560], P('dp', 'sp')
Outputs:
- output 1: bfloat16 [3, 2048, 2560], P('dp', 'sp')
- output 2: bfloat16 [3, 2048, 2560], P('dp', 'sp')
- output 3: float32 [2560, 32, 3, 80], P('dp')
- output 4: float32 [32, 3, 80], P('dp')
- output 5: float32 [2560, 2560], P('dp')
- output 6: float32 [2560], P('dp')
- output 7: float32 [2560], P('dp')
- output 8: float32 [2560], P('dp')
All inputs are finite; a program needn't handle non-finite values.
Results may differ from the reference program's by a relative error of at most 0.00985173.
Values are sent between devices in bfloat16 or wider.
A program may use at most 768 MiB of HBM per device.

```python
import jax
import jax.numpy as jnp
import numpy as np
from jax import lax

BATCH_SEQS = 3
SEQ_LEN = 2048
HIDDEN = 2560
NUM_HEADS = 32
HEAD_DIM = HIDDEN // NUM_HEADS
NORM_EPS = 1e-5
MASK_FILL = -1e30
QK_SCALE = HEAD_DIM ** -0.5
SLOPES = 2.0 ** (-8.0 * (np.arange(NUM_HEADS) + 1) / NUM_HEADS)


def setup_inputs(seed: int = 0, part: int = 0) -> dict:
    part_key = jax.random.fold_in(jax.random.key(seed), part)
    k_x, k_dy, k_len, k_gap = jax.random.split(part_key, 4)
    k_g, k_b, k_wq, k_bq, k_wo, k_bo = jax.random.split(jax.random.key(seed + 1), 6)
    shape_act = (BATCH_SEQS, SEQ_LEN, HIDDEN)
    x_in = jax.random.normal(k_x, shape_act, jnp.float32).astype(jnp.bfloat16)
    grad_y = jax.random.normal(k_dy, shape_act, jnp.float32).astype(jnp.bfloat16)
    lengths = jax.random.randint(k_len, (BATCH_SEQS,), SEQ_LEN // 8, SEQ_LEN + 1)
    lengths = lengths.at[0].set(SEQ_LEN)
    keep_mask = (jnp.arange(SEQ_LEN)[None, :] < lengths[:, None]).astype(jnp.int32)
    pos_steps = jax.random.randint(k_gap, (BATCH_SEQS, SEQ_LEN), 1, 3)
    positions = (jnp.cumsum(pos_steps, axis=1) - pos_steps[:, :1]).astype(jnp.int32)
    w_scale = HIDDEN ** -0.5
    return {
        "x_in": x_in,
        "positions": positions,
        "keep_mask": keep_mask,
        "ln_gain": 1.0 + 0.5 * jax.random.normal(k_g, (HIDDEN,), jnp.float32),
        "ln_bias": 0.5 * jax.random.normal(k_b, (HIDDEN,), jnp.float32),
        "w_qkv": (w_scale * jax.random.normal(k_wq, (HIDDEN, NUM_HEADS, 3, HEAD_DIM), jnp.float32)).astype(jnp.bfloat16),
        "b_qkv": 0.5 * jax.random.normal(k_bq, (NUM_HEADS, 3, HEAD_DIM), jnp.float32),
        "w_out": (w_scale * jax.random.normal(k_wo, (HIDDEN, HIDDEN), jnp.float32)).astype(jnp.bfloat16),
        "b_out": 0.5 * jax.random.normal(k_bo, (HIDDEN,), jnp.float32),
        "grad_y": grad_y,
    }


def head_probs(q_head, k_head, pos_row, keep_row, head_slope):
    scores = jnp.dot(q_head, k_head.T, preferred_element_type=jnp.float32) * QK_SCALE
    pos_gap = (pos_row[:, None] - pos_row[None, :]).astype(jnp.float32)
    scores = scores - head_slope * pos_gap
    tok_index = jnp.arange(SEQ_LEN)
    allowed = (tok_index[None, :] <= tok_index[:, None]) & (keep_row[None, :] > 0)
    return jax.nn.softmax(jnp.where(allowed, scores, MASK_FILL), axis=-1)


def head_forward(head_item):
    q_head, k_head, v_head, pos_row, keep_row, head_slope = head_item
    attn_prob = head_probs(q_head, k_head, pos_row, keep_row, head_slope)
    return jnp.dot(attn_prob.astype(jnp.bfloat16), v_head, preferred_element_type=jnp.float32).astype(jnp.bfloat16)


def head_backward(head_item):
    q_head, k_head, v_head, o_head, do_head, pos_row, keep_row, head_slope = head_item
    attn_prob = head_probs(q_head, k_head, pos_row, keep_row, head_slope)
    prob_lo = attn_prob.astype(jnp.bfloat16)
    dv_head = jnp.dot(prob_lo.T, do_head, preferred_element_type=jnp.float32).astype(jnp.bfloat16)
    grad_prob = jnp.dot(do_head, v_head.T, preferred_element_type=jnp.float32)
    row_dot = jnp.sum(do_head.astype(jnp.float32) * o_head.astype(jnp.float32), axis=-1)
    ds_lo = (attn_prob * (grad_prob - row_dot[:, None])).astype(jnp.bfloat16)
    dq_head = (jnp.dot(ds_lo, k_head, preferred_element_type=jnp.float32) * QK_SCALE).astype(jnp.bfloat16)
    dk_head = (jnp.dot(ds_lo.T, q_head, preferred_element_type=jnp.float32) * QK_SCALE).astype(jnp.bfloat16)
    return dq_head, dk_head, dv_head


def reference(x_in, positions, keep_mask, ln_gain, ln_bias, w_qkv, b_qkv, w_out, b_out, grad_y):
    tokens = BATCH_SEQS * SEQ_LEN
    x_f32 = x_in.astype(jnp.float32)
    centered = x_f32 - jnp.mean(x_f32, axis=-1, keepdims=True)
    inv_std = lax.rsqrt(jnp.mean(centered * centered, axis=-1, keepdims=True) + NORM_EPS)
    x_hat = centered * inv_std
    x_norm = (x_hat * ln_gain + ln_bias).astype(jnp.bfloat16).reshape(tokens, HIDDEN)
    w_flat = w_qkv.reshape(HIDDEN, 3 * HIDDEN)
    qkv_flat = (jnp.dot(x_norm, w_flat, preferred_element_type=jnp.float32) + b_qkv.reshape(3 * HIDDEN)).astype(jnp.bfloat16)
    qkv_heads = jnp.transpose(qkv_flat.reshape(BATCH_SEQS, SEQ_LEN, NUM_HEADS, 3, HEAD_DIM), (3, 0, 2, 1, 4))
    qkv_heads = qkv_heads.reshape(3, BATCH_SEQS * NUM_HEADS, SEQ_LEN, HEAD_DIM)
    pos_rows = jnp.repeat(positions, NUM_HEADS, axis=0)
    keep_rows = jnp.repeat(keep_mask, NUM_HEADS, axis=0)
    slope_rows = jnp.tile(jnp.asarray(SLOPES, jnp.float32), BATCH_SEQS)
    o_heads = lax.map(head_forward, (qkv_heads[0], qkv_heads[1], qkv_heads[2], pos_rows, keep_rows, slope_rows))
    o_flat = jnp.transpose(o_heads.reshape(BATCH_SEQS, NUM_HEADS, SEQ_LEN, HEAD_DIM), (0, 2, 1, 3)).reshape(tokens, HIDDEN)
    y_out = (x_f32.reshape(tokens, HIDDEN) + jnp.dot(o_flat, w_out, preferred_element_type=jnp.float32) + b_out).astype(jnp.bfloat16)
    dy_flat = grad_y.reshape(tokens, HIDDEN)
    grad_b_out = jnp.sum(dy_flat.astype(jnp.float32), axis=0)
    grad_w_out = jnp.dot(o_flat.T, dy_flat, preferred_element_type=jnp.float32)
    do_flat = jnp.dot(dy_flat, w_out.T, preferred_element_type=jnp.float32).astype(jnp.bfloat16)
    do_heads = jnp.transpose(do_flat.reshape(BATCH_SEQS, SEQ_LEN, NUM_HEADS, HEAD_DIM), (0, 2, 1, 3)).reshape(BATCH_SEQS * NUM_HEADS, SEQ_LEN, HEAD_DIM)
    dq_heads, dk_heads, dv_heads = lax.map(head_backward, (qkv_heads[0], qkv_heads[1], qkv_heads[2], o_heads, do_heads, pos_rows, keep_rows, slope_rows))
    d_qkv = jnp.stack([dq_heads, dk_heads, dv_heads], axis=0).reshape(3, BATCH_SEQS, NUM_HEADS, SEQ_LEN, HEAD_DIM)
    d_qkv = jnp.transpose(d_qkv, (1, 3, 2, 0, 4)).reshape(tokens, 3 * HIDDEN)
    grad_b_qkv = jnp.sum(d_qkv.astype(jnp.float32), axis=0).reshape(NUM_HEADS, 3, HEAD_DIM)
    grad_w_qkv = jnp.dot(x_norm.T, d_qkv, preferred_element_type=jnp.float32).reshape(HIDDEN, NUM_HEADS, 3, HEAD_DIM)
    d_norm = jnp.dot(d_qkv, w_flat.T, preferred_element_type=jnp.float32).reshape(BATCH_SEQS, SEQ_LEN, HIDDEN)
    grad_gain = jnp.sum(d_norm * x_hat, axis=(0, 1))
    grad_bias = jnp.sum(d_norm, axis=(0, 1))
    d_hat = d_norm * ln_gain
    d_ln = inv_std * (d_hat - jnp.mean(d_hat, axis=-1, keepdims=True) - x_hat * jnp.mean(d_hat * x_hat, axis=-1, keepdims=True))
    grad_x = (grad_y.astype(jnp.float32) + d_ln).astype(jnp.bfloat16)
    return (y_out.reshape(BATCH_SEQS, SEQ_LEN, HIDDEN), grad_x, grad_w_qkv, grad_b_qkv, grad_w_out, grad_b_out, grad_gain, grad_bias)
```

```python
import functools

import jax
import jax.numpy as jnp
from jax import lax
from jax.experimental import pallas as pl
from jax.experimental.pallas import tpu as pltpu
from jax.sharding import PartitionSpec as P

NORM_EPS = 1e-5
MASK_FILL = -1e30
LANES = 128
MESH = pl.DeviceIdType.MESH
VMEM_LIMIT = 60 * 1024 * 1024


def dot(a, b, ca, cb):
    return lax.dot_general(a, b, (((ca,), (cb,)), ((), ())), preferred_element_type=jnp.float32)


def norm_forward(x_blk, ln_gain, ln_bias):
    x_f32 = x_blk.astype(jnp.float32)
    centered = x_f32 - jnp.mean(x_f32, axis=-1, keepdims=True)
    inv_std = lax.rsqrt(jnp.mean(centered * centered, axis=-1, keepdims=True) + NORM_EPS)
    return (centered * inv_std * ln_gain + ln_bias).astype(jnp.bfloat16)


def exchange_kernel(size, gather, in_ref, out_ref, send_sems, recv_sems, local_sem):
    me = lax.axis_index("sp")
    barrier = pltpu.get_barrier_semaphore()

    def greet(d, carry):
        pl.semaphore_signal(barrier, inc=1, device_id={"sp": lax.rem(me + d, size)}, device_id_type=MESH)
        return carry

    lax.fori_loop(1, size, greet, 0)
    pl.semaphore_wait(barrier, size - 1)

    def block(j):
        return in_ref if gather else in_ref.at[j]

    own = pltpu.make_async_copy(block(me), out_ref.at[me], local_sem)
    own.start()

    def copy_to(d):
        peer = lax.rem(me + d, size)
        return pltpu.make_async_remote_copy(
            src_ref=block(peer), dst_ref=out_ref.at[me], send_sem=send_sems.at[d], recv_sem=recv_sems.at[d],
            device_id={"sp": peer}, device_id_type=MESH)

    def send(d, carry):
        copy_to(d).start()
        return carry

    def arrive(d, carry):
        peer = lax.rem(me + size - d, size)
        pltpu.make_async_remote_copy(
            src_ref=block(peer), dst_ref=out_ref.at[peer], send_sem=send_sems.at[d], recv_sem=recv_sems.at[d],
            device_id={"sp": peer}, device_id_type=MESH).wait_recv()
        return carry

    def sent(d, carry):
        copy_to(d).wait_send()
        return carry

    lax.fori_loop(1, size, send, 0)
    own.wait()
    lax.fori_loop(1, size, arrive, 0)
    lax.fori_loop(1, size, sent, 0)


def exchange(x, size, collective_id, gather=False):
    out_shape = (size, *x.shape) if gather else x.shape
    nbytes = x.size * x.dtype.itemsize
    return pl.pallas_call(
        functools.partial(exchange_kernel, size, gather),
        out_shape=jax.ShapeDtypeStruct(out_shape, x.dtype),
        in_specs=[pl.BlockSpec(memory_space=pl.ANY)],
        out_specs=pl.BlockSpec(memory_space=pl.ANY),
        scratch_shapes=[pltpu.SemaphoreType.DMA((size,)), pltpu.SemaphoreType.DMA((size,)), pltpu.SemaphoreType.DMA],
        compiler_params=pltpu.CompilerParams(collective_id=collective_id, has_side_effects=True),
        cost_estimate=pl.CostEstimate(flops=10_000_000_000, bytes_accessed=2 * nbytes, transcendentals=0),
        name="gather_small" if gather else "all_to_all",
    )(x)


def attn_kernel(head_dim, q_block, slope_ref, qkv_ref, do_ref, pos_ref, keep_ref, out_ref, dk_acc, dv_acc):
    seq_len, pad_dim = dk_acc.shape
    blocks, _, tok, _ = qkv_ref.shape
    scale = head_dim ** -0.5
    slope = slope_ref[0]
    pos_row = pos_ref[0]
    keep_row = keep_ref[0]
    per = q_block // tok
    dk_acc[...] = jnp.zeros_like(dk_acc)
    dv_acc[...] = jnp.zeros_like(dv_acc)

    def rows(ref, lo, hi, part):
        return ref[lo * per:hi * per, 0, :, part * pad_dim:(part + 1) * pad_dim].reshape((hi - lo) * q_block, pad_dim)

    for i in range(seq_len // q_block):
        span = (i + 1) * q_block
        q = rows(qkv_ref, i, i + 1, 0)
        k = rows(qkv_ref, 0, i + 1, 1)
        v = rows(qkv_ref, 0, i + 1, 2)
        do = rows(do_ref, i, i + 1, 0)
        gap = (pos_row[:, span - 1:span] - pos_row[:, :span]).astype(jnp.float32)
        bias = jnp.where(keep_row[:, :span] > 0, -slope * gap, MASK_FILL)
        scores = dot(q, k, 1, 1) * scale + bias
        row_id = lax.broadcasted_iota(jnp.int32, (q_block, span), 0) + i * q_block
        col_id = lax.broadcasted_iota(jnp.int32, (q_block, span), 1)
        scores = jnp.where(col_id <= row_id, scores, MASK_FILL)
        expo = jnp.exp(scores - jnp.max(scores, axis=-1, keepdims=True))
        prob = expo * (1.0 / jnp.sum(expo, axis=-1, keepdims=True))
        prob_lo = prob.astype(jnp.bfloat16)
        o = dot(prob_lo, v, 1, 0).astype(jnp.bfloat16)
        row_dot = jnp.sum(do.astype(jnp.float32) * o.astype(jnp.float32), axis=-1, keepdims=True)
        ds_lo = (prob * (dot(do, v, 1, 1) - row_dot)).astype(jnp.bfloat16)
        dq = (dot(ds_lo, k, 1, 0) * scale).astype(jnp.bfloat16)
        dv_acc[:span, :] += dot(prob_lo, do, 0, 0)
        dk_acc[:span, :] += dot(ds_lo, q, 0, 0)
        both = jnp.concatenate([o[:, :head_dim], dq[:, :head_dim]], axis=1)
        out_ref[i * per:(i + 1) * per, 0, :, 0:2 * head_dim] = both.reshape(per, tok, 2 * head_dim)
    dk = (dk_acc[...] * scale).astype(jnp.bfloat16)
    dv = dv_acc[...].astype(jnp.bfloat16)
    both = jnp.concatenate([dk[:, :head_dim], dv[:, :head_dim]], axis=1)
    out_ref[:, 0, :, 2 * head_dim:4 * head_dim] = both.reshape(blocks, tok, 2 * head_dim)


def attention(slope, qkv, do, pos, keep, head_dim, q_block):
    blocks, batch, tok, wide = qkv.shape
    pad_dim = wide // 3
    seq_len = blocks * tok
    flops = 6 * batch * seq_len * seq_len * 256
    return pl.pallas_call(
        functools.partial(attn_kernel, head_dim, q_block),
        grid=(batch,),
        out_shape=jax.ShapeDtypeStruct((blocks, batch, tok, 4 * head_dim), jnp.bfloat16),
        in_specs=[
            pl.BlockSpec(memory_space=pltpu.SMEM),
            pl.BlockSpec((blocks, 1, tok, wide), lambda b: (0, b, 0, 0)),
            pl.BlockSpec((blocks, 1, tok, pad_dim), lambda b: (0, b, 0, 0)),
            pl.BlockSpec((1, 1, seq_len), lambda b: (b, 0, 0)),
            pl.BlockSpec((1, 1, seq_len), lambda b: (b, 0, 0)),
        ],
        out_specs=pl.BlockSpec((blocks, 1, tok, 4 * head_dim), lambda b: (0, b, 0, 0)),
        scratch_shapes=[pltpu.VMEM((seq_len, pad_dim), jnp.float32)] * 2,
        compiler_params=pltpu.CompilerParams(vmem_limit_bytes=VMEM_LIMIT),
        cost_estimate=pl.CostEstimate(flops=flops, bytes_accessed=20_000_000, transcendentals=batch * seq_len * seq_len // 2),
        name="attention",
    )(slope, qkv, do, pos, keep)


def token_kernel(head_dim, chunk, parts_ref, wq_ref, wo_ref, x_ref, dy_ref, gain_ref, bout_ref,
                 y_ref, gx_ref, bq_ref, sums_ref, dn_acc, y_acc):
    n = pl.program_id(0)
    parts = parts_ref[0]
    o = parts[:, :head_dim]
    dqkv = parts[:, head_dim:]
    bq_ref[0] = jnp.sum(dqkv.astype(jnp.float32), axis=0, keepdims=True)
    dn_term = dot(dqkv, wq_ref[0], 1, 0)
    y_term = dot(o, wo_ref[0], 1, 0)

    @pl.when(n == 0)
    def _():
        dn_acc[...] = dn_term
        y_acc[...] = y_term

    @pl.when(n > 0)
    def _():
        dn_acc[...] += dn_term
        y_acc[...] += y_term

    @pl.when(n == pl.num_programs(0) - 1)
    def _():
        sums_ref[...] = jnp.zeros_like(sums_ref)
        gain = gain_ref[...]
        bout = bout_ref[...]

        def body(c, carry):
            at = pl.ds(pl.multiple_of(c * chunk, chunk), chunk)
            x = x_ref[at, :].astype(jnp.float32)
            dy = dy_ref[at, :].astype(jnp.float32)
            centered = x - jnp.mean(x, axis=-1, keepdims=True)
            inv_std = lax.rsqrt(jnp.mean(centered * centered, axis=-1, keepdims=True) + NORM_EPS)
            x_hat = centered * inv_std
            d_norm = dn_acc[at, :]
            d_hat = d_norm * gain
            d_mean = jnp.mean(d_hat, axis=-1, keepdims=True)
            d_proj = jnp.mean(d_hat * x_hat, axis=-1, keepdims=True)
            gx_ref[at, :] = (dy + inv_std * (d_hat - d_mean - x_hat * d_proj)).astype(jnp.bfloat16)
            y_ref[at, :] = (x + y_acc[at, :] + bout).astype(jnp.bfloat16)
            sums_ref[0:1, :] += jnp.sum(d_norm * x_hat, axis=0, keepdims=True)
            sums_ref[1:2, :] += jnp.sum(d_norm, axis=0, keepdims=True)
            sums_ref[2:3, :] += jnp.sum(dy, axis=0, keepdims=True)
            return carry

        lax.fori_loop(0, x_ref.shape[0] // chunk, body, 0)


def token_side(parts, wq, wo, x, dy, gain, bout, head_dim):
    heads, tokens, _ = parts.shape
    hidden = x.shape[1]
    whole = lambda n: (0, 0)
    per_head = lambda n: (n, 0, 0)
    return pl.pallas_call(
        functools.partial(token_kernel, head_dim, 16),
        grid=(heads,),
        out_shape=(
            jax.ShapeDtypeStruct((tokens, hidden), jnp.bfloat16),
            jax.ShapeDtypeStruct((tokens, hidden), jnp.bfloat16),
            jax.ShapeDtypeStruct((heads, 1, 3 * head_dim), jnp.float32),
            jax.ShapeDtypeStruct((8, hidden), jnp.float32),
        ),
        in_specs=[
            pl.BlockSpec((1, tokens, 4 * head_dim), per_head),
            pl.BlockSpec((1, 3 * head_dim, hidden), per_head),
            pl.BlockSpec((1, head_dim, hidden), per_head),
            pl.BlockSpec((tokens, hidden), whole),
            pl.BlockSpec((tokens, hidden), whole),
            pl.BlockSpec((1, hidden), whole),
            pl.BlockSpec((1, hidden), whole),
        ],
        out_specs=(
            pl.BlockSpec((tokens, hidden), whole),
            pl.BlockSpec((tokens, hidden), whole),
            pl.BlockSpec((1, 1, 3 * head_dim), per_head),
            pl.BlockSpec((8, hidden), whole),
        ),
        scratch_shapes=[pltpu.VMEM((tokens, hidden), jnp.float32)] * 2,
        compiler_params=pltpu.CompilerParams(vmem_limit_bytes=VMEM_LIMIT),
        cost_estimate=pl.CostEstimate(
            flops=2 * tokens * hidden * 4 * heads * head_dim, bytes_accessed=8 * hidden * heads * head_dim, transcendentals=0),
        name="token_side",
    )(parts, wq, wo, x, dy, gain, bout)


def place_kernel(piece_ref, *refs):
    refs[-1][0, 0] = piece_ref[0]


def place(piece, slot, slots, into=None):
    heads, rows, cols = piece.shape
    shape = jax.ShapeDtypeStruct((heads, slots, rows, cols), piece.dtype)
    old = [] if into is None else [into]
    return pl.pallas_call(
        place_kernel,
        grid=(heads,),
        out_shape=shape,
        in_specs=[pl.BlockSpec((1, rows, cols), lambda n: (n, 0, 0))] + [pl.BlockSpec(memory_space=pl.ANY)] * len(old),
        out_specs=pl.BlockSpec((1, 1, rows, cols), lambda n: (n, slot, 0, 0)),
        input_output_aliases={} if into is None else {1: 0},
        cost_estimate=pl.CostEstimate(flops=5_000_000_000, bytes_accessed=8 * heads * rows * cols, transcendentals=0),
        name="place",
    )(piece, *old)


def solution(mesh):
    size = mesh.shape["sp"]

    def block_fn(x_blk, pos_blk, keep_blk, ln_gain, ln_bias, w_qkv, b_qkv, w_out, b_out, dy_blk):
        batch, tok, hidden = x_blk.shape
        heads, head_dim = w_qkv.shape[1], w_qkv.shape[3]
        tokens, seq_len = batch * tok, size * tok
        pad_dim = -(-head_dim // LANES) * LANES
        rank = lax.axis_index("sp")
        wq = jnp.transpose(w_qkv, (1, 2, 3, 0))
        wo = w_out.reshape(heads, head_dim, hidden)
        dy_flat = dy_blk.reshape(tokens, hidden)

        def gather(a):
            return lax.all_gather(a, "sp", axis=0, tiled=True)

        x_norm = norm_forward(x_blk, ln_gain, ln_bias).reshape(tokens, hidden)
        x_all = gather(x_norm)
        dy_all = gather(dy_flat)

        do_out = jnp.einsum("sk,nck->nsc", dy_flat, wo, preferred_element_type=jnp.float32).astype(jnp.bfloat16)
        do_in = exchange(do_out.reshape(heads, tokens * head_dim // LANES, LANES), size, 0)
        do_head = jnp.pad(do_in.reshape(size, batch, tok, head_dim), ((0, 0), (0, 0), (0, 0), (0, pad_dim - head_dim)))

        meta = jnp.pad(jnp.concatenate([pos_blk, keep_blk], axis=0), ((0, 8 - 2 * batch), (0, LANES - tok)))
        meta_all = jnp.transpose(exchange(meta, size, 1, gather=True)[:, :2 * batch, :tok], (1, 0, 2)).reshape(2 * batch, 1, seq_len)

        w_head = jnp.pad(lax.dynamic_slice_in_dim(wq, rank, 1, 0)[0], ((0, 0), (0, pad_dim - head_dim), (0, 0)))
        b_head = jnp.pad(lax.dynamic_slice_in_dim(b_qkv, rank, 1, 0)[0], ((0, 0), (0, pad_dim - head_dim)))
        qkv = (dot(x_all, w_head.reshape(3 * pad_dim, hidden), 1, 1) + b_head.reshape(-1)).astype(jnp.bfloat16)
        slope = jnp.exp2(-8.0 * (rank + 1).astype(jnp.float32) / heads).reshape(1)
        parts = attention(slope, qkv.reshape(size, batch, tok, 3 * pad_dim), do_head, meta_all[:batch], meta_all[batch:],
                          head_dim, min(256, seq_len))

        parts_flat = parts.reshape(size * tokens, 4 * head_dim)
        grad_head = dot(parts_flat, x_all, 0, 0)
        pieces = [grad_head[(c + 1) * head_dim:(c + 2) * head_dim] for c in range(3)]
        grad_wq = None
        for c in range(3):
            grad_wq = place(gather(pieces[c]).reshape(heads, head_dim, hidden), c, 3, grad_wq)
        grad_wo_head = dot(parts_flat[:, :head_dim], dy_all, 0, 0)
        grad_wo = place(gather(grad_wo_head).reshape(heads, head_dim, hidden), 0, 1)

        flat = parts.reshape(size, tokens * 4 * head_dim // LANES, LANES)
        parts_tok = exchange(flat, size, 2).reshape(heads, tokens, 4 * head_dim)
        y, grad_x, bq_part, sums = token_side(
            parts_tok, wq.reshape(heads, 3 * head_dim, hidden), wo, x_blk.reshape(tokens, hidden), dy_flat,
            ln_gain.reshape(1, hidden), b_out.reshape(1, hidden), head_dim)
        bq, gain, bias, bo = lax.psum((bq_part.reshape(-1), sums[0], sums[1], sums[2]), "sp")
        return (y.reshape(x_blk.shape), grad_x.reshape(x_blk.shape), jnp.transpose(grad_wq, (3, 0, 1, 2)),
                bq.reshape(heads, 3, head_dim), grad_wo.reshape(heads * head_dim, hidden), bo, gain, bias)

    act_spec = P("dp", "sp", None)
    tok_spec = P("dp", "sp")
    in_specs = (act_spec, tok_spec, tok_spec, P(), P(), P(), P(), P(), P(), act_spec)
    out_specs = (act_spec, act_spec, P("dp", None, None, None), P("dp", None, None), P("dp", None), P("dp"), P("dp"), P("dp"))
    return jax.shard_map(block_fn, mesh=mesh, in_specs=in_specs, out_specs=out_specs, check_vma=False)
```

```python
import functools
import math

import jax
import jax.numpy as jnp
from jax import lax
from jax.experimental import pallas as pl
from jax.experimental.pallas import tpu as pltpu
from jax.sharding import PartitionSpec as P

NORM_EPS = 1e-5
MASK_FILL = -1e30
LANES = 128
MESH = pl.DeviceIdType.MESH
VMEM_LIMIT = 61 * 1024 * 1024


def dot(a, b, ca, cb):
    return lax.dot_general(a, b, (((ca,), (cb,)), ((), ())), preferred_element_type=jnp.float32)


def norm_forward(x_blk, ln_gain, ln_bias):
    x_f32 = x_blk.astype(jnp.float32)
    centered = x_f32 - jnp.mean(x_f32, axis=-1, keepdims=True)
    inv_std = lax.rsqrt(jnp.mean(centered * centered, axis=-1, keepdims=True) + NORM_EPS)
    return (centered * inv_std * ln_gain + ln_bias).astype(jnp.bfloat16)


def greet_all(me, size):
    barrier = pltpu.get_barrier_semaphore()

    def greet(d, carry):
        pl.semaphore_signal(barrier, inc=1, device_id={"sp": lax.rem(me + d, size)}, device_id_type=MESH)
        return carry

    lax.fori_loop(1, size, greet, 0)
    pl.semaphore_wait(barrier, size - 1)


class Direct:
    def __init__(self, me, size, src, dst, send_sems, recv_sems):
        self.me, self.size, self.src, self.dst, self.send_sems, self.recv_sems = me, size, src, dst, send_sems, recv_sems

    def copy(self, d, peer, slot):
        return pltpu.make_async_remote_copy(
            src_ref=self.src(peer), dst_ref=self.dst(slot), send_sem=self.send_sems.at[d], recv_sem=self.recv_sems.at[d],
            device_id={"sp": peer}, device_id_type=MESH)

    def loop(self, step):
        def body(d, carry):
            step(d)
            return carry

        lax.fori_loop(1, self.size, body, 0)

    def start(self):
        self.loop(lambda d: self.copy(d, lax.rem(self.me + d, self.size), self.me).start())

    def wait_recv(self):
        def one(d):
            peer = lax.rem(self.me + self.size - d, self.size)
            self.copy(d, peer, peer).wait_recv()

        self.loop(one)

    def wait_send(self):
        self.loop(lambda d: self.copy(d, lax.rem(self.me + d, self.size), self.me).wait_send())


def exchange_kernel(size, in_ref, out_ref, send_sems, recv_sems, local_sem):
    me = lax.axis_index("sp")
    greet_all(me, size)
    own = pltpu.make_async_copy(in_ref.at[me], out_ref.at[me], local_sem)
    own.start()
    direct = Direct(me, size, lambda j: in_ref.at[j], lambda j: out_ref.at[j], send_sems, recv_sems)
    direct.start()
    own.wait()
    direct.wait_recv()
    direct.wait_send()


def exchange(x, size, collective_id):
    nbytes = x.size * x.dtype.itemsize
    return pl.pallas_call(
        functools.partial(exchange_kernel, size),
        out_shape=jax.ShapeDtypeStruct(x.shape, x.dtype),
        in_specs=[pl.BlockSpec(memory_space=pl.ANY)],
        out_specs=pl.BlockSpec(memory_space=pl.ANY),
        scratch_shapes=[pltpu.SemaphoreType.DMA((size,)), pltpu.SemaphoreType.DMA((size,)), pltpu.SemaphoreType.DMA],
        compiler_params=pltpu.CompilerParams(collective_id=collective_id, has_side_effects=True),
        cost_estimate=pl.CostEstimate(flops=40_000_000_000, bytes_accessed=2 * nbytes, transcendentals=0),
        name="all_to_all",
    )(x)


FIRST_OF = (2, 3, 0, 1)
SENDS = (("P", 0), ("Q", 0, 0), ("P", 1), ("Q", 0, 1), ("P", 2), ("Q", 1, 0), ("Q", 0, 2), ("Q", 1, 1),
         ("Q", 2, 0), ("Q", 3, 0), ("Q", 1, 2), ("Q", 2, 1), ("Q", 3, 1), ("Q", 2, 2), ("Q", 3, 2))
LAG = 2
COLOURS = 4
HEADS_STEP = 4


def gather_kernel(size, side, dims, xn_ref, dy_ref, wq_ref, bias_ref, wo_ref, meta_ref,
                  xall_ref, qkv_ref, do_ref, metaall_ref,
                  xbuf, wbuf, wobuf, dybuf, dosend, dorecv,
                  load_sems, wo_sems, out_sems, meta_sem, ici_send, ici_recv, d2d_send, d2d_recv, do_send, do_recv, meta_send, meta_recv):
    batch, tok, head_dim, pad_dim = dims
    me = lax.axis_index("sp")
    core = lax.rem(me, 2)
    chip = me // 2
    cx, cy = lax.rem(chip, side), chip // side
    sibling = me + 1 - 2 * core

    def chip_at(dx, dy):
        return lax.rem(cy + dy + side, side) * side + lax.rem(cx + dx + side, side)

    def device_at(dx, dy):
        return chip_at(dx, dy) * 2 + core

    step_of = ((1, 0), (-1, 0), (0, 1), (0, -1))

    def back_on(link, n, other=None, m=0):
        dx, dy = step_of[link][0] * -n, step_of[link][1] * -n
        if other is not None:
            dx, dy = dx - step_of[other][0] * m, dy - step_of[other][1] * m
        return device_at(dx, dy)

    def sent_chunk(link, slot, ahead=0):
        what = SENDS[slot]
        if what[0] == "P":
            return back_on(link, what[1] + ahead), link
        first = FIRST_OF[link]
        return back_on(link, what[2] + ahead, first, what[1]), first

    def ici_copy(link, slot, arriving):
        block, colour = sent_chunk(link, slot, 1 if arriving else 0)
        ref = xbuf.at[block, colour]
        return pltpu.make_async_remote_copy(
            src_ref=ref, dst_ref=ref, send_sem=ici_send.at[link, slot], recv_sem=ici_recv.at[link, slot],
            device_id={"sp": device_at(*step_of[link])}, device_id_type=MESH)

    def d2d_copy(link, slot, from_sibling):
        block, colour = sent_chunk(link, slot, 1)
        ref = xbuf.at[block + ((1 - 2 * core) if from_sibling else 0), colour]
        return pltpu.make_async_remote_copy(
            src_ref=ref, dst_ref=ref, send_sem=d2d_send.at[slot + 1, link], recv_sem=d2d_recv.at[slot + 1, link],
            device_id={"sp": sibling}, device_id_type=MESH)

    def d2d_own(block):
        return pltpu.make_async_remote_copy(
            src_ref=xbuf.at[block], dst_ref=xbuf.at[block], send_sem=d2d_send.at[0, 0], recv_sem=d2d_recv.at[0, 0],
            device_id={"sp": sibling}, device_id_type=MESH)

    rows = xbuf.shape[2]
    loads = [pltpu.make_async_copy(xn_ref.at[pl.ds(c * rows, rows)], xbuf.at[me, c], load_sems.at[c]) for c in range(COLOURS)]
    load_dy = pltpu.make_async_copy(dy_ref, dybuf, load_sems.at[COLOURS])
    load_w = pltpu.make_async_copy(wq_ref.at[me], wbuf, load_sems.at[COLOURS + 1])
    for load in loads:
        load.start()
    load_dy.start()
    load_w.start()
    heads = wo_ref.shape[0]
    groups = heads // HEADS_STEP

    def load_wo(g):
        return pltpu.make_async_copy(wo_ref.at[pl.ds(g * HEADS_STEP, HEADS_STEP)], wobuf.at[lax.rem(g, 2)], wo_sems.at[lax.rem(g, 2)])

    load_wo(0).start()
    meta = Direct(me, size, lambda j: meta_ref, lambda j: metaall_ref.at[j], meta_send, meta_recv)
    exch = Direct(me, size, lambda j: dosend.at[j], lambda j: dorecv.at[j], do_send, do_recv)
    greet_all(me, size)
    for load in loads:
        load.wait()
    for slot in range(LAG):
        for link in range(4):
            ici_copy(link, slot, False).start()
    d2d_own(me).start()
    own_meta = pltpu.make_async_copy(meta_ref, metaall_ref.at[me], meta_sem)
    own_meta.start()
    meta.start()
    load_dy.wait()

    def do_group(g, carry):
        @pl.when(g + 1 < groups)
        def _():
            load_wo(g + 1).start()

        load_wo(g).wait()
        w = wobuf[lax.rem(g, 2)].reshape(HEADS_STEP * head_dim, -1)
        d = dot(dybuf[...], w, 1, 1).astype(jnp.bfloat16)
        for h in range(HEADS_STEP):
            pieces = [d[b * tok:(b + 1) * tok, h * head_dim:(h + 1) * head_dim] for b in range(batch)]
            fill = dosend.shape[2] - batch * head_dim
            if fill:
                pieces.append(jnp.zeros((tok, fill), jnp.bfloat16))
            dosend[g * HEADS_STEP + h] = jnp.concatenate(pieces, axis=1)
        return carry

    lax.fori_loop(0, groups, do_group, 0)
    exch.start()
    dorecv[me] = dosend[me]
    load_w.wait()

    def store_out(pair):
        return pltpu.make_async_copy(
            xbuf.at[pl.ds(pair * 2, 2)], xall_ref.at[pl.ds(pair * 2, 2)], out_sems.at[pair])

    def multiply(pair):
        store_out(pair).start()
        x = xbuf[pl.ds(pair * 2, 2)].reshape(2 * COLOURS * rows, -1)
        r = (dot(x, wbuf[...], 1, 1) + bias_ref[...]).astype(jnp.bfloat16)
        zero = jnp.zeros((r.shape[0], pad_dim - head_dim), jnp.bfloat16)
        pieces = []
        for c in range(3):
            pieces += [r[:, c * head_dim:(c + 1) * head_dim], zero]
        qkv_ref[pl.ds(pair * 2, 2)] = jnp.concatenate(pieces, axis=1).reshape(2, COLOURS * rows, 3 * pad_dim)

    slots = len(SENDS)
    for step in range(LAG, slots + LAG + 1):
        for link in range(4):
            if step - LAG < slots:
                ici_copy(link, step - LAG, True).wait_recv()
                d2d_copy(link, step - LAG, False).start()
                if step < slots:
                    ici_copy(link, step, False).start()
        for link in range(4):
            if step == LAG:
                if link == 0:
                    d2d_own(sibling).wait_recv()
            else:
                d2d_copy(link, step - LAG - 1, True).wait_recv()
        if step == 12:
            def straight(i, carry):
                multiply(chip_at(jnp.where(i < side, i, 0), jnp.where(i < side, 0, i - side + 1)))
                return carry

            lax.fori_loop(0, 2 * side - 1, straight, 0)

    def cornered(i, carry):
        multiply(chip_at(1 + i // (side - 1), 1 + lax.rem(i, side - 1)))
        return carry

    lax.fori_loop(0, (side - 1) * (side - 1), cornered, 0)
    exch.wait_recv()

    def unpack(j, carry):
        d = dorecv[j]
        for b in range(batch):
            do_ref[j, b] = jnp.concatenate(
                [d[:, b * head_dim:(b + 1) * head_dim], jnp.zeros((tok, pad_dim - head_dim), jnp.bfloat16)], axis=1)
        return carry

    lax.fori_loop(0, size, unpack, 0)
    own_meta.wait()
    meta.wait_recv()
    meta.wait_send()
    exch.wait_send()
    d2d_own(me).wait_send()
    for slot in range(slots):
        for link in range(4):
            ici_copy(link, slot, False).wait_send()
            d2d_copy(link, slot, False).wait_send()

    def stored(i, carry):
        store_out(i).wait()
        return carry

    lax.fori_loop(0, side * side, stored, 0)


def gather_qkv(x_norm, dy, wq, bias, wo, meta, size, batch, collective_id):
    tokens, hidden = x_norm.shape
    heads, head_dim, _ = wo.shape
    pad_dim = -(-head_dim // LANES) * LANES
    tok = tokens // batch
    side = math.isqrt(size // 2)
    pack = -(-batch * head_dim // LANES) * LANES
    slots = len(SENDS)
    anywhere = pl.BlockSpec(memory_space=pl.ANY)
    vmem = pl.BlockSpec(memory_space=pltpu.VMEM)
    sem = pltpu.SemaphoreType.DMA
    xall, qkv, do, metaall = pl.pallas_call(
        functools.partial(gather_kernel, size, side, (batch, tok, head_dim, pad_dim)),
        out_shape=(
            jax.ShapeDtypeStruct((size, COLOURS, tokens // COLOURS, hidden), jnp.bfloat16),
            jax.ShapeDtypeStruct((size, tokens, 3 * pad_dim), jnp.bfloat16),
            jax.ShapeDtypeStruct((size, batch, tok, pad_dim), jnp.bfloat16),
            jax.ShapeDtypeStruct((size, *meta.shape), meta.dtype),
        ),
        in_specs=[anywhere, anywhere, anywhere, vmem, anywhere, anywhere],
        out_specs=(anywhere, vmem, vmem, anywhere),
        scratch_shapes=[
            pltpu.VMEM((size, COLOURS, tokens // COLOURS, hidden), jnp.bfloat16),
            pltpu.VMEM((3 * head_dim, hidden), jnp.bfloat16),
            pltpu.VMEM((2, HEADS_STEP, head_dim, hidden), jnp.bfloat16),
            pltpu.VMEM((tokens, hidden), jnp.bfloat16),
            pltpu.VMEM((size, tok, pack), jnp.bfloat16),
            pltpu.VMEM((size, tok, pack), jnp.bfloat16),
            sem((COLOURS + 2,)), sem((2,)), sem((side * side,)), sem,
            sem((4, slots)), sem((4, slots)), sem((slots + 1, 4)), sem((slots + 1, 4)),
            sem((size,)), sem((size,)), sem((size,)), sem((size,)),
        ],
        compiler_params=pltpu.CompilerParams(collective_id=collective_id, has_side_effects=True, vmem_limit_bytes=VMEM_LIMIT),
        cost_estimate=pl.CostEstimate(flops=80_000_000_000, bytes_accessed=60_000_000, transcendentals=0),
        name="gather_qkv",
    )(x_norm, dy, wq, bias, wo, meta)
    return xall.reshape(size, batch, tok, hidden), qkv.reshape(size, batch, tok, 3 * pad_dim), do, metaall


def attn_kernel(head_dim, q_block, slope_ref, qkv_ref, do_ref, pos_ref, keep_ref, x_ref, out_ref, gw_ref,
                dk_acc, dv_acc, dq_all, o_all, d_all, x_buf, x_sems):
    seq_len, pad_dim = dk_acc.shape
    blocks, _, tok, _ = qkv_ref.shape
    b = pl.program_id(0)
    batch = x_buf.shape[0]
    scale = head_dim ** -0.5
    slope = slope_ref[0]
    pos_row = pos_ref[0]
    keep_row = keep_ref[0]
    per = q_block // tok

    def load_x(i):
        return pltpu.make_async_copy(x_ref.at[:, i], x_buf.at[i], x_sems.at[i])

    @pl.when(b == 0)
    def _():
        for i in range(batch):
            load_x(i).start()

    dk_acc[...] = jnp.zeros_like(dk_acc)
    dv_acc[...] = jnp.zeros_like(dv_acc)

    def rows(ref, lo, hi, part):
        return ref[lo * per:hi * per, 0, :, part * pad_dim:(part + 1) * pad_dim].reshape((hi - lo) * q_block, pad_dim)

    for i in range(seq_len // q_block):
        span = (i + 1) * q_block
        q = rows(qkv_ref, i, i + 1, 0)
        k = rows(qkv_ref, 0, i + 1, 1)
        v = rows(qkv_ref, 0, i + 1, 2)
        do = rows(do_ref, i, i + 1, 0)
        gap = (pos_row[:, span - 1:span] - pos_row[:, :span]).astype(jnp.float32)
        bias = jnp.where(keep_row[:, :span] > 0, -slope * gap, MASK_FILL)
        scores = dot(q, k, 1, 1) * scale + bias
        row_id = lax.broadcasted_iota(jnp.int32, (q_block, span), 0) + i * q_block
        col_id = lax.broadcasted_iota(jnp.int32, (q_block, span), 1)
        scores = jnp.where(col_id <= row_id, scores, MASK_FILL)
        expo = jnp.exp(scores - jnp.max(scores, axis=-1, keepdims=True))
        prob = expo * (1.0 / jnp.sum(expo, axis=-1, keepdims=True))
        prob_lo = prob.astype(jnp.bfloat16)
        o = dot(prob_lo, v, 1, 0).astype(jnp.bfloat16)
        row_dot = jnp.sum(do.astype(jnp.float32) * o.astype(jnp.float32), axis=-1, keepdims=True)
        ds_lo = (prob * (dot(do, v, 1, 1) - row_dot)).astype(jnp.bfloat16)
        o_all[i * q_block:span, :] = o
        dq_all[i * q_block:span, :] = (dot(ds_lo, k, 1, 0) * scale).astype(jnp.bfloat16)
        dv_acc[:span, :] += dot(prob_lo, do, 0, 0)
        dk_acc[:span, :] += dot(ds_lo, q, 0, 0)
    dk = (dk_acc[...] * scale).astype(jnp.bfloat16)
    dv = dv_acc[...].astype(jnp.bfloat16)
    d_all[...] = jnp.concatenate([dq_all[:, :head_dim], dk[:, :head_dim], dv[:, :head_dim]], axis=1)
    whole = jnp.concatenate([d_all[...], o_all[:, :head_dim]], axis=1)
    out_ref[:, 0] = whole.reshape(blocks, tok, 4 * head_dim)
    load_x(b).wait()
    width = 512

    def columns(n, carry):
        at = pl.ds(pl.multiple_of(n * width, width), width)
        term = dot(d_all[...], x_buf[b, :, :, at].reshape(seq_len, width), 0, 0)

        @pl.when(b == 0)
        def _():
            gw_ref[:, at] = term

        @pl.when(b > 0)
        def _():
            gw_ref[:, at] += term

        return carry

    hidden = gw_ref.shape[1]
    if hidden % width:
        term = dot(d_all[...], x_buf[b].reshape(seq_len, hidden), 0, 0)
        gw_ref[...] = jnp.where(b == 0, term, gw_ref[...] + term)
    else:
        lax.fori_loop(0, hidden // width, columns, 0)


def attention(slope, qkv, do, pos, keep, x_all, head_dim, q_block):
    blocks, batch, tok, wide = qkv.shape
    hidden = x_all.shape[-1]
    pad_dim = wide // 3
    seq_len = blocks * tok
    flops = 6 * batch * seq_len * seq_len * 256 + 2 * batch * seq_len * 3 * head_dim * hidden
    return pl.pallas_call(
        functools.partial(attn_kernel, head_dim, q_block),
        grid=(batch,),
        out_shape=(jax.ShapeDtypeStruct((blocks, batch, tok, 4 * head_dim), jnp.bfloat16),
                   jax.ShapeDtypeStruct((3 * head_dim, hidden), jnp.float32)),
        in_specs=[
            pl.BlockSpec(memory_space=pltpu.SMEM),
            pl.BlockSpec((blocks, 1, tok, wide), lambda b: (0, b, 0, 0)),
            pl.BlockSpec((blocks, 1, tok, pad_dim), lambda b: (0, b, 0, 0)),
            pl.BlockSpec((1, 1, seq_len), lambda b: (b, 0, 0)),
            pl.BlockSpec((1, 1, seq_len), lambda b: (b, 0, 0)),
            pl.BlockSpec(memory_space=pl.ANY),
        ],
        out_specs=(pl.BlockSpec((blocks, 1, tok, 4 * head_dim), lambda b: (0, b, 0, 0)),
                   pl.BlockSpec((3 * head_dim, hidden), lambda b: (0, 0))),
        scratch_shapes=[pltpu.VMEM((seq_len, pad_dim), jnp.float32)] * 2 + [pltpu.VMEM((seq_len, pad_dim), jnp.bfloat16)] * 2 + [
            pltpu.VMEM((seq_len, 3 * head_dim), jnp.bfloat16),
            pltpu.VMEM((batch, blocks, tok, hidden), jnp.bfloat16),
            pltpu.SemaphoreType.DMA((batch,)),
        ],
        compiler_params=pltpu.CompilerParams(vmem_limit_bytes=VMEM_LIMIT),
        cost_estimate=pl.CostEstimate(flops=flops, bytes_accessed=50_000_000, transcendentals=batch * seq_len * seq_len // 2),
        name="attention",
    )(slope, qkv, do, pos, keep, x_all)


def outgrad_kernel(head_dim, parts_ref, dy_ref, after_ref, gw_ref):
    blocks, tokens, wide = parts_ref.shape
    o = parts_ref[...].reshape(blocks * tokens, wide)[:, wide - head_dim:]
    term = dot(o, dy_ref[...].reshape(blocks * tokens, -1), 0, 0)

    @pl.when(pl.program_id(0) == 0)
    def _():
        gw_ref[...] = term

    @pl.when(pl.program_id(0) > 0)
    def _():
        gw_ref[...] += term


def outgrad(parts, dy_all, after, head_dim):
    size, tokens, wide = parts.shape
    hidden = dy_all.shape[-1]
    step = 2
    return pl.pallas_call(
        functools.partial(outgrad_kernel, head_dim),
        grid=(size // step,),
        out_shape=jax.ShapeDtypeStruct((head_dim, hidden), jnp.float32),
        in_specs=[pl.BlockSpec((step, tokens, wide), lambda i: (i, 0, 0)),
                  pl.BlockSpec((step, tokens, hidden), lambda i: (i, 0, 0)),
                  pl.BlockSpec(memory_space=pl.ANY)],
        out_specs=pl.BlockSpec((head_dim, hidden), lambda i: (0, 0)),
        compiler_params=pltpu.CompilerParams(vmem_limit_bytes=VMEM_LIMIT),
        cost_estimate=pl.CostEstimate(flops=10_000_000_000, bytes_accessed=40_000_000, transcendentals=0),
        name="outgrad",
    )(parts, dy_all, after)


def token_kernel(head_dim, chunk, parts_ref, wq_ref, wo_ref, x_ref, dy_ref, gain_ref, bout_ref,
                 y_ref, gx_ref, bq_ref, sums_ref, dn_acc, y_acc):
    n = pl.program_id(0)
    parts = parts_ref[0]
    dqkv = parts[:, :3 * head_dim]
    o = parts[:, 3 * head_dim:]
    bq_ref[0] = jnp.sum(dqkv.astype(jnp.float32), axis=0, keepdims=True)
    dn_term = dot(dqkv, wq_ref[0], 1, 0)
    y_term = dot(o, wo_ref[0], 1, 0)

    @pl.when(n == 0)
    def _():
        dn_acc[...] = dn_term
        y_acc[...] = y_term

    @pl.when(n > 0)
    def _():
        dn_acc[...] += dn_term
        y_acc[...] += y_term

    @pl.when(n == pl.num_programs(0) - 1)
    def _():
        sums_ref[...] = jnp.zeros_like(sums_ref)
        gain = gain_ref[...]
        bout = bout_ref[...]

        def body(c, carry):
            at = pl.ds(pl.multiple_of(c * chunk, chunk), chunk)
            x = x_ref[at, :].astype(jnp.float32)
            dy = dy_ref[at, :].astype(jnp.float32)
            centered = x - jnp.mean(x, axis=-1, keepdims=True)
            inv_std = lax.rsqrt(jnp.mean(centered * centered, axis=-1, keepdims=True) + NORM_EPS)
            x_hat = centered * inv_std
            d_norm = dn_acc[at, :]
            d_hat = d_norm * gain
            d_mean = jnp.mean(d_hat, axis=-1, keepdims=True)
            d_proj = jnp.mean(d_hat * x_hat, axis=-1, keepdims=True)
            gx_ref[at, :] = (dy + inv_std * (d_hat - d_mean - x_hat * d_proj)).astype(jnp.bfloat16)
            y_ref[at, :] = (x + y_acc[at, :] + bout).astype(jnp.bfloat16)
            sums_ref[0:1, :] += jnp.sum(d_norm * x_hat, axis=0, keepdims=True)
            sums_ref[1:2, :] += jnp.sum(d_norm, axis=0, keepdims=True)
            sums_ref[2:3, :] += jnp.sum(dy, axis=0, keepdims=True)
            return carry

        lax.fori_loop(0, x_ref.shape[0] // chunk, body, 0)


def token_side(parts, wq, wo, x, dy, gain, bout, head_dim):
    heads, tokens, _ = parts.shape
    hidden = x.shape[1]
    whole = lambda n: (0, 0)
    per_head = lambda n: (n, 0, 0)
    return pl.pallas_call(
        functools.partial(token_kernel, head_dim, 16),
        grid=(heads,),
        out_shape=(
            jax.ShapeDtypeStruct((tokens, hidden), jnp.bfloat16),
            jax.ShapeDtypeStruct((tokens, hidden), jnp.bfloat16),
            jax.ShapeDtypeStruct((heads, 1, 3 * head_dim), jnp.float32),
            jax.ShapeDtypeStruct((8, hidden), jnp.float32),
        ),
        in_specs=[
            pl.BlockSpec((1, tokens, 4 * head_dim), per_head),
            pl.BlockSpec((1, 3 * head_dim, hidden), per_head),
            pl.BlockSpec((1, head_dim, hidden), per_head),
            pl.BlockSpec((tokens, hidden), whole),
            pl.BlockSpec((tokens, hidden), whole),
            pl.BlockSpec((1, hidden), whole),
            pl.BlockSpec((1, hidden), whole),
        ],
        out_specs=(
            pl.BlockSpec((tokens, hidden), whole),
            pl.BlockSpec((tokens, hidden), whole),
            pl.BlockSpec((1, 1, 3 * head_dim), per_head),
            pl.BlockSpec((8, hidden), whole),
        ),
        scratch_shapes=[pltpu.VMEM((tokens, hidden), jnp.float32)] * 2,
        compiler_params=pltpu.CompilerParams(vmem_limit_bytes=VMEM_LIMIT),
        cost_estimate=pl.CostEstimate(
            flops=2 * tokens * hidden * 4 * heads * head_dim, bytes_accessed=8 * hidden * heads * head_dim, transcendentals=0),
        name="token_side",
    )(parts, wq, wo, x, dy, gain, bout)


def settle_kernel(block, depth, ahead, src_ref, *refs):
    dst_ref, buf, read_sems, write_sems = refs[-4:]
    count = src_ref.shape[0] // block

    def at(i):
        return pl.ds(pl.multiple_of(i * block, block), block)

    def read(i):
        return pltpu.make_async_copy(src_ref.at[at(i)], buf.at[lax.rem(i, depth)], read_sems.at[lax.rem(i, depth)])

    def write(i):
        return pltpu.make_async_copy(buf.at[lax.rem(i, depth)], dst_ref.at[at(i)], write_sems.at[lax.rem(i, depth)])

    def step(i, carry):
        @pl.when(jnp.logical_and(i >= depth, i < count))
        def _():
            write(i - depth).wait()

        @pl.when(i < count)
        def _():
            read(i).start()

        @pl.when(i >= ahead)
        def _():
            read(i - ahead).wait()
            write(i - ahead).start()

        return carry

    lax.fori_loop(0, count + ahead, step, 0)

    def drain(i, carry):
        write(i).wait()
        return carry

    lax.fori_loop(max(0, count - depth), count, drain, 0)


def settle(x, block, after=()):
    depth, ahead = 12, 6
    rows, cols = x.shape
    sem = pltpu.SemaphoreType.DMA((depth,))
    return pl.pallas_call(
        functools.partial(settle_kernel, block, depth, ahead),
        out_shape=jax.ShapeDtypeStruct(x.shape, x.dtype),
        in_specs=[pl.BlockSpec(memory_space=pl.ANY)] * (1 + len(after)),
        out_specs=pl.BlockSpec(memory_space=pl.ANY),
        scratch_shapes=[pltpu.VMEM((depth, block, cols), x.dtype), sem, sem],
        cost_estimate=pl.CostEstimate(flops=10_000_000_000, bytes_accessed=8 * rows * cols, transcendentals=0),
        name="settle",
    )(x, *after)


def solution(mesh):
    size = mesh.shape["sp"]

    def block_fn(x_blk, pos_blk, keep_blk, ln_gain, ln_bias, w_qkv, b_qkv, w_out, b_out, dy_blk):
        batch, tok, hidden = x_blk.shape
        heads, head_dim = w_qkv.shape[1], w_qkv.shape[3]
        tokens, seq_len = batch * tok, size * tok
        rank = lax.axis_index("sp")
        wq = jnp.transpose(w_qkv, (1, 2, 3, 0)).reshape(heads, 3 * head_dim, hidden)
        wo = w_out.reshape(heads, head_dim, hidden)
        dy_flat = dy_blk.reshape(tokens, hidden)

        def gather(a):
            return lax.all_gather(a, "sp", axis=0, tiled=True)

        x_norm = norm_forward(x_blk, ln_gain, ln_bias).reshape(tokens, hidden)
        meta = jnp.pad(jnp.concatenate([pos_blk, keep_blk], axis=0), ((0, 8 - 2 * batch), (0, LANES - tok)))
        bias = lax.dynamic_slice_in_dim(b_qkv, rank, 1, 0).reshape(1, 3 * head_dim)
        x_all, qkv, do_head, meta_all = gather_qkv(x_norm, dy_flat, wq, bias, wo, meta, size, batch, 0)
        dy_later, meta_all = lax.optimization_barrier((dy_flat, meta_all))
        dy_all = gather(dy_later)

        meta_all = jnp.transpose(meta_all[:, :2 * batch, :tok], (1, 0, 2)).reshape(2 * batch, 1, seq_len)
        slope = jnp.exp2(-8.0 * (rank + 1).astype(jnp.float32) / heads).reshape(1)
        parts, grad_head = attention(slope, qkv, do_head, meta_all[:batch], meta_all[batch:], x_all, head_dim, min(256, seq_len))

        flat = parts.reshape(size, tokens * 4 * head_dim // LANES, LANES)
        parts_tok = exchange(flat, size, 1).reshape(heads, tokens, 4 * head_dim)
        y, grad_x, bq_part, sums = token_side(
            parts_tok, wq, wo, x_blk.reshape(tokens, hidden), dy_flat, ln_gain.reshape(1, hidden), b_out.reshape(1, hidden), head_dim)
        grad_wq = settle(gather(grad_head), head_dim)
        grad_out = outgrad(parts.reshape(size, tokens, 4 * head_dim), dy_all.reshape(size, tokens, hidden), parts_tok, head_dim)
        grad_wo = settle(gather(grad_out), head_dim, after=(grad_wq,))
        bq, gain, bias_sum, bo = lax.psum((bq_part.reshape(-1), sums[0], sums[1], sums[2]), "sp")
        grad_wq = jnp.transpose(grad_wq.reshape(heads, 3, head_dim, hidden), (3, 0, 1, 2))
        return (y.reshape(x_blk.shape), grad_x.reshape(x_blk.shape), grad_wq, bq.reshape(heads, 3, head_dim), grad_wo,
                bo, gain, bias_sum)

    act_spec = P("dp", "sp", None)
    tok_spec = P("dp", "sp")
    in_specs = (act_spec, tok_spec, tok_spec, P(), P(), P(), P(), P(), P(), act_spec)
    out_specs = (act_spec, act_spec, P("dp", None, None, None), P("dp", None, None), P("dp", None), P("dp"), P("dp"), P("dp"))
    return jax.shard_map(block_fn, mesh=mesh, in_specs=in_specs, out_specs=out_specs, check_vma=False)
```

```python
import functools
import math

import jax
import jax.numpy as jnp
from jax import lax
from jax.experimental import pallas as pl
from jax.experimental.pallas import tpu as pltpu
from jax.sharding import PartitionSpec as P

NORM_EPS = 1e-5
MASK_FILL = -1e30
LANES = 128
MESH = pl.DeviceIdType.MESH
VMEM_LIMIT = 61 * 1024 * 1024


def dot(a, b, ca, cb):
    return lax.dot_general(a, b, (((ca,), (cb,)), ((), ())), preferred_element_type=jnp.float32)


def norm_forward(x_blk, ln_gain, ln_bias):
    x_f32 = x_blk.astype(jnp.float32)
    centered = x_f32 - jnp.mean(x_f32, axis=-1, keepdims=True)
    inv_std = lax.rsqrt(jnp.mean(centered * centered, axis=-1, keepdims=True) + NORM_EPS)
    return (centered * inv_std * ln_gain + ln_bias).astype(jnp.bfloat16)


def greet_all(me, size):
    barrier = pltpu.get_barrier_semaphore()

    def greet(d, carry):
        pl.semaphore_signal(barrier, inc=1, device_id={"sp": lax.rem(me + d, size)}, device_id_type=MESH)
        return carry

    lax.fori_loop(1, size, greet, 0)
    pl.semaphore_wait(barrier, size - 1)


class Direct:
    def __init__(self, me, size, src, dst, send_sems, recv_sems):
        self.me, self.size, self.src, self.dst, self.send_sems, self.recv_sems = me, size, src, dst, send_sems, recv_sems

    def copy(self, d, peer, slot):
        return pltpu.make_async_remote_copy(
            src_ref=self.src(peer), dst_ref=self.dst(slot), send_sem=self.send_sems.at[d], recv_sem=self.recv_sems.at[d],
            device_id={"sp": peer}, device_id_type=MESH)

    def loop(self, step):
        def body(d, carry):
            step(d)
            return carry

        lax.fori_loop(1, self.size, body, 0)

    def start(self):
        self.loop(lambda d: self.copy(d, lax.rem(self.me + d, self.size), self.me).start())

    def wait_recv(self):
        def one(d):
            peer = lax.rem(self.me + self.size - d, self.size)
            self.copy(d, peer, peer).wait_recv()

        self.loop(one)

    def wait_send(self):
        self.loop(lambda d: self.copy(d, lax.rem(self.me + d, self.size), self.me).wait_send())


def exchange_kernel(size, in_ref, out_ref, send_sems, recv_sems, local_sem):
    me = lax.axis_index("sp")
    greet_all(me, size)
    own = pltpu.make_async_copy(in_ref.at[me], out_ref.at[me], local_sem)
    own.start()
    direct = Direct(me, size, lambda j: in_ref.at[j], lambda j: out_ref.at[j], send_sems, recv_sems)
    direct.start()
    own.wait()
    direct.wait_recv()
    direct.wait_send()


def exchange(x, size, collective_id):
    nbytes = x.size * x.dtype.itemsize
    return pl.pallas_call(
        functools.partial(exchange_kernel, size),
        out_shape=jax.ShapeDtypeStruct(x.shape, x.dtype),
        in_specs=[pl.BlockSpec(memory_space=pl.ANY)],
        out_specs=pl.BlockSpec(memory_space=pl.ANY),
        scratch_shapes=[pltpu.SemaphoreType.DMA((size,)), pltpu.SemaphoreType.DMA((size,)), pltpu.SemaphoreType.DMA],
        compiler_params=pltpu.CompilerParams(collective_id=collective_id, has_side_effects=True),
        cost_estimate=pl.CostEstimate(flops=40_000_000_000, bytes_accessed=2 * nbytes, transcendentals=0),
        name="all_to_all",
    )(x)


FIRST_OF = (2, 3, 0, 1)
CYCLE = (("P", 0), ("Q", 0, 0), ("Q", 3, 2), ("P", 1), ("Q", 0, 1), ("Q", 1, 0), ("Q", 2, 0), ("P", 2), ("Q", 1, 1),
         ("Q", 2, 1), ("Q", 3, 0), ("Q", 1, 2), ("Q", 2, 2), ("Q", 3, 1), ("Q", 0, 2))
LATE = 2
LAG = 3
COLOURS = 4
READY = 6
STEP_OF = ((1, 0), (-1, 0), (0, 1), (0, -1))


def block_kernel(size, side, dims, own_ref, wq_ref, bias_ref, wo_ref, meta_ref, slope_ref,
                 gat_ref, parts_ref, partstok_ref, gwq_ref, gwo_ref,
                 stage, wbuf, wobuf, metabuf, rowbuf, sbuf, qkvb, dob, dk_acc, dv_acc, dq_all, o_all, d_all, pbuf,
                 load_sems, own_sems, piece_sems, parts_sem, ici_send, ici_recv, d2d_send, d2d_recv, own_send, own_recv,
                 meta_send, meta_recv, part_send, part_recv):
    batch, tok, head_dim, pad_dim, hidden, q_block = dims
    seq_len = size * tok
    me = lax.axis_index("sp")
    core = lax.rem(me, 2)
    chip = me // 2
    cx, cy = lax.rem(chip, side), chip // side
    flip = 1 - 2 * core
    sibling = me + flip
    places = len(CYCLE)
    scale = head_dim ** -0.5
    slope = slope_ref[0]

    def device_at(dx, dy):
        return (lax.rem(cy + dy + side, side) * side + lax.rem(cx + dx + side, side)) * 2 + core

    def chunk(link, place, ahead):
        what = CYCLE[place]
        if what[0] == "P":
            first, n, m = link, what[1] + ahead, 0
        else:
            first, n, m = FIRST_OF[link], what[2] + ahead, what[1]
        dx = -STEP_OF[link][0] * n - STEP_OF[first][0] * m
        dy = -STEP_OF[link][1] * n - STEP_OF[first][1] * m
        return device_at(dx, dy), first

    def send(b, link, place):
        block, colour = chunk(link, place, 0)
        dst = gat_ref.at[b, block, colour]
        return pltpu.make_async_remote_copy(
            src_ref=stage.at[b, colour] if CYCLE[place] in (("P", 0), ("Q", 0, 0)) else dst, dst_ref=dst,
            send_sem=ici_send.at[b, link, place], recv_sem=ici_recv.at[b, link, place],
            device_id={"sp": device_at(*STEP_OF[link])}, device_id_type=MESH)

    def arrival(b, link, place):
        block, colour = chunk(link, place, 1)
        ref = gat_ref.at[b, block, colour]
        return pltpu.make_async_remote_copy(
            src_ref=ref, dst_ref=ref, send_sem=ici_send.at[b, link, place], recv_sem=ici_recv.at[b, link, place],
            device_id={"sp": me}, device_id_type=MESH)

    def share(b, link, place, shift):
        block, colour = chunk(link, place, 1)
        ref = gat_ref.at[b, block + shift, colour]
        return pltpu.make_async_remote_copy(
            src_ref=ref, dst_ref=ref, send_sem=d2d_send.at[b, link, place], recv_sem=d2d_recv.at[b, link, place],
            device_id={"sp": sibling}, device_id_type=MESH)

    def share_own(b, block):
        return pltpu.make_async_remote_copy(
            src_ref=stage.at[b], dst_ref=gat_ref.at[b, block], send_sem=own_send.at[b], recv_sem=own_recv.at[b],
            device_id={"sp": sibling}, device_id_type=MESH)

    def keep_own(b):
        return pltpu.make_async_copy(stage.at[b], gat_ref.at[b, me], own_sems.at[b])

    load_own = pltpu.make_async_copy(own_ref, stage, load_sems.at[0])
    load_wq = pltpu.make_async_copy(wq_ref.at[me], wbuf, load_sems.at[1])
    load_wo = pltpu.make_async_copy(wo_ref.at[me], wobuf, load_sems.at[2])
    own_meta = pltpu.make_async_copy(meta_ref, metabuf.at[me], load_sems.at[3])
    for load in (load_own, load_wq, load_wo, own_meta):
        load.start()
    meta = Direct(me, size, lambda j: meta_ref, lambda j: metabuf.at[j], meta_send, meta_recv)
    early = batch - 1
    trades = [Direct(me, size, lambda j, b=b: parts_ref.at[b, j], lambda j, b=b: partstok_ref.at[j, b], part_send.at[b], part_recv.at[b])
              for b in range(early)]
    own_parts = [pltpu.make_async_copy(parts_ref.at[b, me], partstok_ref.at[me, b], load_sems.at[4 + b]) for b in range(early)]
    greet_all(me, size)
    load_own.wait()

    group = sbuf.shape[1]
    pieces = size // group
    piece_rows = group * tok

    def load_piece(b, p):
        return pltpu.make_async_copy(gat_ref.at[b, pl.ds(p * group, group)], sbuf.at[lax.rem(p, 2)], piece_sems.at[lax.rem(p, 2)])

    def rows_of(p, which, at=slice(None)):
        return sbuf[lax.rem(p, 2), :, :, which, :, at].reshape(piece_rows, -1)

    def stream(b, lo, hi, use):
        def body(p, carry):
            @pl.when(p + 1 < pieces)
            def _():
                load_piece(b, p + 1).start()

            load_piece(b, p).wait()
            use(p)
            return carry

        lax.fori_loop(lo, hi, body, 0)

    def pad_lanes(a):
        return jnp.concatenate([a, jnp.zeros((a.shape[0], pad_dim - head_dim), a.dtype)], axis=1)

    def project(p):
        at = pl.ds(pl.multiple_of(p * piece_rows, piece_rows), piece_rows)
        r = (dot(rows_of(p, 1), wbuf[...], 1, 1) + bias_ref[...]).astype(jnp.bfloat16)
        for c in range(3):
            qkvb[at, c * pad_dim:(c + 1) * pad_dim] = pad_lanes(r[:, c * head_dim:(c + 1) * head_dim])
        dob[at, :] = pad_lanes(dot(rows_of(p, 0), wobuf[...], 1, 1).astype(jnp.bfloat16))

    def attend(b, i):
        span = (i + 1) * q_block
        mine = slice(i * q_block, span)
        q, k, v = qkvb[mine, :pad_dim], qkvb[:span, pad_dim:2 * pad_dim], qkvb[:span, 2 * pad_dim:]
        do = dob[mine, :]
        pos = rowbuf[pl.ds(b, 1), :span]
        keep = rowbuf[pl.ds(b + batch, 1), :span]
        bias = jnp.where(keep > 0, -slope * (pos[:, span - 1:] - pos).astype(jnp.float32), MASK_FILL)
        scores = dot(q, k, 1, 1) * scale + bias
        row_id = lax.broadcasted_iota(jnp.int32, (q_block, span), 0) + i * q_block
        col_id = lax.broadcasted_iota(jnp.int32, (q_block, span), 1)
        scores = jnp.where(col_id <= row_id, scores, MASK_FILL)
        expo = jnp.exp(scores - jnp.max(scores, axis=-1, keepdims=True))
        prob = expo * (1.0 / jnp.sum(expo, axis=-1, keepdims=True))
        prob_lo = prob.astype(jnp.bfloat16)
        o = dot(prob_lo, v, 1, 0).astype(jnp.bfloat16)
        row_dot = jnp.sum(do.astype(jnp.float32) * o.astype(jnp.float32), axis=-1, keepdims=True)
        ds_lo = (prob * (dot(do, v, 1, 1) - row_dot)).astype(jnp.bfloat16)
        o_all[mine, :] = o
        dq_all[mine, :] = (dot(ds_lo, k, 1, 0) * scale).astype(jnp.bfloat16)
        dv_acc[:span, :] += dot(prob_lo, do, 0, 0)
        dk_acc[:span, :] += dot(ds_lo, q, 0, 0)

    def store_parts(b):
        return pltpu.make_async_copy(pbuf, parts_ref.at[b], parts_sem)

    def finish(b):
        dk = (dk_acc[...] * scale).astype(jnp.bfloat16)
        dv = dv_acc[...].astype(jnp.bfloat16)
        d_all[...] = jnp.concatenate([dq_all[:, :head_dim], dk[:, :head_dim], dv[:, :head_dim]], axis=1)
        whole = jnp.concatenate([d_all[...], o_all[:, :head_dim]], axis=1).reshape(size, tok, 4 * head_dim)
        pbuf[...] = jnp.concatenate([whole[:, :tok // 2], whole[:, tok // 2:]], axis=2)
        store_parts(b).start()

    width = min(512, hidden)

    def gradient(p):
        rows = pl.ds(pl.multiple_of(p * piece_rows, piece_rows), piece_rows)

        def columns(n, carry):
            at = pl.ds(pl.multiple_of(n * width, width), width)
            gwq_ref[:, at] += dot(d_all[rows, :], rows_of(p, 1, at), 0, 0)
            gwo_ref[:, at] += dot(o_all[rows, :head_dim], rows_of(p, 0, at), 0, 0)
            return carry

        lax.fori_loop(0, hidden // width, columns, 0)

    count = seq_len // q_block
    todo = [list(range(min(3, count)))] + [[i] for i in range(3, count)]

    def work_front(b, place):
        place -= READY + 1
        if place == 0:
            load_piece(b, 0).start()
            dk_acc[...] = jnp.zeros_like(dk_acc)
            dv_acc[...] = jnp.zeros_like(dv_acc)
            stream(b, 0, pieces // 2, project)
        elif place == 1:
            stream(b, pieces // 2, pieces, project)
        elif place - 2 < len(todo):
            for i in todo[place - 2]:
                attend(b, i)

    def work_back(b, place):
        if place == 0:
            load_piece(b, 0).start()
            finish(b)
        elif place == 2:
            stream(b, 0, pieces // 2, gradient)
        elif place == 4:
            stream(b, pieces // 2, pieces, gradient)
            store_parts(b).wait()

    gwq_ref[...] = jnp.zeros_like(gwq_ref)
    gwo_ref[...] = jnp.zeros_like(gwo_ref)

    def phase_of(i, place):
        return i - 1 if place == LATE else i

    def among(b):
        return jnp.logical_and(b >= 0, b < batch)

    def turn(i, carry):
        for place in range(places):
            came = (place - LAG) % places
            b_came = phase_of(i if place >= LAG else i - 1, came)

            @pl.when(among(b_came))
            def _():
                for link in range(4):
                    arrival(b_came, link, came).wait_recv()
                    share(b_came, link, came, 0).start()

            b_send = phase_of(i, place)

            @pl.when(among(b_send))
            def _():
                for link in range(4):
                    send(b_send, link, place).start()

            shared = (place - LAG - 1) % places
            b_shared = phase_of(i if place >= LAG + 1 else i - 1, shared)

            @pl.when(among(b_shared))
            def _():
                for link in range(4):
                    share(b_shared, link, shared, flip).wait_recv()

            if place == 1:
                @pl.when(i == 0)
                def _():
                    for b in range(batch):
                        share_own(b, me).start()
                        keep_own(b).start()
                    meta.start()

            if place == READY:
                @pl.when(i == 1)
                def _():
                    for load in (load_wq, load_wo, own_meta):
                        load.wait()
                    meta.wait_recv()
                    for j in range(size):
                        rowbuf[:, j * tok:(j + 1) * tok] = metabuf[j, :, :tok]
                    for b in range(batch):
                        share_own(b, sibling).wait_recv()
                        keep_own(b).wait()

                @pl.when(i == batch)
                def _():
                    for b in range(early):
                        own_parts[b].start()
                        trades[b].start()

            if place > READY:
                @pl.when(among(i - 1))
                def _():
                    work_front(i - 1, place)
            else:
                @pl.when(among(i - 2))
                def _():
                    work_back(i - 2, place)
        return carry

    lax.fori_loop(0, batch + 2, turn, 0)
    for b in range(early):
        own_parts[b].wait()
        trades[b].wait_recv()
        trades[b].wait_send()
    meta.wait_send()

    def sent(n, carry):
        b = n // (4 * places)
        link = lax.rem(n, 4 * places) // places
        place = lax.rem(n, places)
        ref = gat_ref.at[0, 0, 0]
        for sem in (ici_send, d2d_send):
            pltpu.make_async_remote_copy(
                src_ref=ref, dst_ref=ref, send_sem=sem.at[b, link, place], recv_sem=ici_recv.at[b, link, place],
                device_id={"sp": sibling}, device_id_type=MESH).wait_send()
        return carry

    lax.fori_loop(0, batch * 4 * places, sent, 0)
    for b in range(batch):
        share_own(b, me).wait_send()


def block_call(own, wq, bias, wo, meta, slope, size, q_block, collective_id):
    batch, _, _, rows, hidden = own.shape
    tok = COLOURS * rows
    heads, head_dim, _ = wo.shape
    pad_dim = -(-head_dim // LANES) * LANES
    seq_len = size * tok
    side = math.isqrt(size // 2)
    group = size // 4
    places = len(CYCLE)
    anywhere = pl.BlockSpec(memory_space=pl.ANY)
    vmem = pl.BlockSpec(memory_space=pltpu.VMEM)
    sem = pltpu.SemaphoreType.DMA
    bf16, f32 = jnp.bfloat16, jnp.float32
    flops = batch * (6 * seq_len * seq_len * 256 + 4 * seq_len * 4 * head_dim * hidden) + 80_000_000_000
    return pl.pallas_call(
        functools.partial(block_kernel, size, side, (batch, tok, head_dim, pad_dim, hidden, min(q_block, seq_len))),
        out_shape=(
            jax.ShapeDtypeStruct((batch, size, COLOURS, 2, rows, hidden), bf16),
            jax.ShapeDtypeStruct((batch, size, tok // 2, 8 * head_dim), bf16),
            jax.ShapeDtypeStruct((size, batch - 1, tok // 2, 8 * head_dim), bf16),
            jax.ShapeDtypeStruct((3 * head_dim, hidden), f32),
            jax.ShapeDtypeStruct((head_dim, hidden), f32),
        ),
        in_specs=[anywhere, anywhere, vmem, anywhere, anywhere, pl.BlockSpec(memory_space=pltpu.SMEM)],
        out_specs=(anywhere, anywhere, anywhere, vmem, vmem),
        scratch_shapes=[
            pltpu.VMEM((batch, COLOURS, 2, rows, hidden), bf16),
            pltpu.VMEM((3 * head_dim, hidden), bf16),
            pltpu.VMEM((head_dim, hidden), bf16),
            pltpu.VMEM((size, *meta.shape), meta.dtype),
            pltpu.VMEM((meta.shape[0], seq_len), meta.dtype),
            pltpu.VMEM((2, group, COLOURS, 2, rows, hidden), bf16),
            pltpu.VMEM((seq_len, 3 * pad_dim), bf16),
            pltpu.VMEM((seq_len, pad_dim), bf16),
            pltpu.VMEM((seq_len, pad_dim), f32),
            pltpu.VMEM((seq_len, pad_dim), f32),
            pltpu.VMEM((seq_len, pad_dim), bf16),
            pltpu.VMEM((seq_len, pad_dim), bf16),
            pltpu.VMEM((seq_len, 3 * head_dim), bf16),
            pltpu.VMEM((size, tok // 2, 8 * head_dim), bf16),
            sem((4 + batch,)), sem((batch,)), sem((2,)), sem,
            sem((batch, 4, places)), sem((batch, 4, places)), sem((batch, 4, places)), sem((batch, 4, places)),
            sem((batch,)), sem((batch,)), sem((size,)), sem((size,)), sem((batch - 1, size)), sem((batch - 1, size)),
        ],
        compiler_params=pltpu.CompilerParams(collective_id=collective_id, has_side_effects=True, vmem_limit_bytes=VMEM_LIMIT),
        cost_estimate=pl.CostEstimate(flops=flops, bytes_accessed=60_000_000, transcendentals=batch * seq_len * seq_len // 2),
        name="block",
    )(own, wq, bias, wo, meta, slope)


def token_kernel(head_dim, chunk, early_ref, last_ref, wq_ref, wo_ref, x_ref, dy_ref, gain_ref, bout_ref,
                 y_ref, gx_ref, bq_ref, sums_ref, dn_acc, y_acc):
    n = pl.program_id(0)
    parts = []
    for b in range(early_ref.shape[1] + 1):
        pair = early_ref[0, b] if b < early_ref.shape[1] else last_ref[0]
        parts += [pair[:, :4 * head_dim], pair[:, 4 * head_dim:]]
    parts = jnp.concatenate(parts, axis=0)
    dqkv = parts[:, :3 * head_dim]
    o = parts[:, 3 * head_dim:]
    bq_ref[0] = jnp.sum(dqkv.astype(jnp.float32), axis=0, keepdims=True)
    dn_term = dot(dqkv, wq_ref[0], 1, 0)
    y_term = dot(o, wo_ref[0], 1, 0)

    @pl.when(n == 0)
    def _():
        dn_acc[...] = dn_term
        y_acc[...] = y_term

    @pl.when(n > 0)
    def _():
        dn_acc[...] += dn_term
        y_acc[...] += y_term

    @pl.when(n == pl.num_programs(0) - 1)
    def _():
        sums_ref[...] = jnp.zeros_like(sums_ref)
        gain = gain_ref[...]
        bout = bout_ref[...]

        def body(c, carry):
            at = pl.ds(pl.multiple_of(c * chunk, chunk), chunk)
            x = x_ref[at, :].astype(jnp.float32)
            dy = dy_ref[at, :].astype(jnp.float32)
            centered = x - jnp.mean(x, axis=-1, keepdims=True)
            inv_std = lax.rsqrt(jnp.mean(centered * centered, axis=-1, keepdims=True) + NORM_EPS)
            x_hat = centered * inv_std
            d_norm = dn_acc[at, :]
            d_hat = d_norm * gain
            d_mean = jnp.mean(d_hat, axis=-1, keepdims=True)
            d_proj = jnp.mean(d_hat * x_hat, axis=-1, keepdims=True)
            gx_ref[at, :] = (dy + inv_std * (d_hat - d_mean - x_hat * d_proj)).astype(jnp.bfloat16)
            y_ref[at, :] = (x + y_acc[at, :] + bout).astype(jnp.bfloat16)
            sums_ref[0:1, :] += jnp.sum(d_norm * x_hat, axis=0, keepdims=True)
            sums_ref[1:2, :] += jnp.sum(d_norm, axis=0, keepdims=True)
            sums_ref[2:3, :] += jnp.sum(dy, axis=0, keepdims=True)
            return carry

        lax.fori_loop(0, x_ref.shape[0] // chunk, body, 0)


def token_side(early, last, wq, wo, x, dy, gain, bout, head_dim):
    heads = early.shape[0]
    tokens, hidden = x.shape
    whole = lambda n: (0, 0)
    per_head = lambda n: (n, 0, 0)
    return pl.pallas_call(
        functools.partial(token_kernel, head_dim, 16),
        grid=(heads,),
        out_shape=(
            jax.ShapeDtypeStruct((tokens, hidden), jnp.bfloat16),
            jax.ShapeDtypeStruct((tokens, hidden), jnp.bfloat16),
            jax.ShapeDtypeStruct((heads, 1, 3 * head_dim), jnp.float32),
            jax.ShapeDtypeStruct((8, hidden), jnp.float32),
        ),
        in_specs=[
            pl.BlockSpec((1, *early.shape[1:]), lambda n: (n, 0, 0, 0)),
            pl.BlockSpec((1, *last.shape[1:]), per_head),
            pl.BlockSpec((1, 3 * head_dim, hidden), per_head),
            pl.BlockSpec((1, head_dim, hidden), per_head),
            pl.BlockSpec((tokens, hidden), whole),
            pl.BlockSpec((tokens, hidden), whole),
            pl.BlockSpec((1, hidden), whole),
            pl.BlockSpec((1, hidden), whole),
        ],
        out_specs=(
            pl.BlockSpec((tokens, hidden), whole),
            pl.BlockSpec((tokens, hidden), whole),
            pl.BlockSpec((1, 1, 3 * head_dim), per_head),
            pl.BlockSpec((8, hidden), whole),
        ),
        scratch_shapes=[pltpu.VMEM((tokens, hidden), jnp.float32)] * 2,
        compiler_params=pltpu.CompilerParams(vmem_limit_bytes=VMEM_LIMIT),
        cost_estimate=pl.CostEstimate(
            flops=2 * tokens * hidden * 4 * heads * head_dim, bytes_accessed=8 * hidden * heads * head_dim, transcendentals=0),
        name="token_side",
    )(early, last, wq, wo, x, dy, gain, bout)


def settle_kernel(block, depth, ahead, src_ref, *refs):
    dst_ref, buf, read_sems, write_sems = refs[-4:]
    count = src_ref.shape[0] // block

    def at(i):
        return pl.ds(pl.multiple_of(i * block, block), block)

    def read(i):
        return pltpu.make_async_copy(src_ref.at[at(i)], buf.at[lax.rem(i, depth)], read_sems.at[lax.rem(i, depth)])

    def write(i):
        return pltpu.make_async_copy(buf.at[lax.rem(i, depth)], dst_ref.at[at(i)], write_sems.at[lax.rem(i, depth)])

    def step(i, carry):
        @pl.when(jnp.logical_and(i >= depth, i < count))
        def _():
            write(i - depth).wait()

        @pl.when(i < count)
        def _():
            read(i).start()

        @pl.when(i >= ahead)
        def _():
            read(i - ahead).wait()
            write(i - ahead).start()

        return carry

    lax.fori_loop(0, count + ahead, step, 0)

    def drain(i, carry):
        write(i).wait()
        return carry

    lax.fori_loop(max(0, count - depth), count, drain, 0)


def settle(x, block, after=()):
    depth, ahead = 12, 6
    rows, cols = x.shape
    sem = pltpu.SemaphoreType.DMA((depth,))
    return pl.pallas_call(
        functools.partial(settle_kernel, block, depth, ahead),
        out_shape=jax.ShapeDtypeStruct(x.shape, x.dtype),
        in_specs=[pl.BlockSpec(memory_space=pl.ANY)] * (1 + len(after)),
        out_specs=pl.BlockSpec(memory_space=pl.ANY),
        scratch_shapes=[pltpu.VMEM((depth, block, cols), x.dtype), sem, sem],
        cost_estimate=pl.CostEstimate(flops=10_000_000_000, bytes_accessed=8 * rows * cols, transcendentals=0),
        name="settle",
    )(x, *after)


def solution(mesh):
    size = mesh.shape["sp"]

    def block_fn(x_blk, pos_blk, keep_blk, ln_gain, ln_bias, w_qkv, b_qkv, w_out, b_out, dy_blk):
        batch, tok, hidden = x_blk.shape
        heads, head_dim = w_qkv.shape[1], w_qkv.shape[3]
        tokens = batch * tok
        rank = lax.axis_index("sp")
        wq = jnp.transpose(w_qkv, (1, 2, 3, 0)).reshape(heads, 3 * head_dim, hidden)
        wo = w_out.reshape(heads, head_dim, hidden)
        dy_flat = dy_blk.reshape(tokens, hidden)

        def gather(a):
            return lax.all_gather(a, "sp", axis=0, tiled=True)

        x_norm = norm_forward(x_blk, ln_gain, ln_bias)
        own = jnp.stack([dy_blk, x_norm], axis=0).reshape(2, batch, COLOURS, tok // COLOURS, hidden).transpose(1, 2, 0, 3, 4)
        meta = jnp.pad(jnp.concatenate([pos_blk, keep_blk], axis=0), ((0, 8 - 2 * batch), (0, LANES - tok)))
        bias = lax.dynamic_slice_in_dim(b_qkv, rank, 1, 0).reshape(1, 3 * head_dim)
        slope = jnp.exp2(-8.0 * (rank + 1).astype(jnp.float32) / heads).reshape(1)
        _, parts, early, grad_head, grad_out = block_call(own, wq, bias, wo, meta, slope, size, 256, 0)

        grad_wq = settle(gather(grad_head), head_dim)
        grad_wo = settle(gather(grad_out), head_dim, after=(grad_wq,))

        last = exchange(parts[batch - 1], size, 1)
        y, grad_x, bq_part, sums = token_side(
            early, last, wq, wo, x_blk.reshape(tokens, hidden), dy_flat, ln_gain.reshape(1, hidden), b_out.reshape(1, hidden), head_dim)
        bq, gain, bias_sum, bo = lax.psum((bq_part.reshape(-1), sums[0], sums[1], sums[2]), "sp")
        grad_wq = jnp.transpose(grad_wq.reshape(heads, 3, head_dim, hidden), (3, 0, 1, 2))
        return (y.reshape(x_blk.shape), grad_x.reshape(x_blk.shape), grad_wq, bq.reshape(heads, 3, head_dim), grad_wo,
                bo, gain, bias_sum)

    act_spec = P("dp", "sp", None)
    tok_spec = P("dp", "sp")
    in_specs = (act_spec, tok_spec, tok_spec, P(), P(), P(), P(), P(), P(), act_spec)
    out_specs = (act_spec, act_spec, P("dp", None, None, None), P("dp", None, None), P("dp", None), P("dp"), P("dp"), P("dp"))
    return jax.shard_map(block_fn, mesh=mesh, in_specs=in_specs, out_specs=out_specs, check_vma=False)
```

```python
import functools
import math

import jax
import jax.numpy as jnp
from jax import lax
from jax.experimental import pallas as pl
from jax.experimental.pallas import tpu as pltpu
from jax.sharding import PartitionSpec as P

NORM_EPS = 1e-5
MASK_FILL = -1e30
LANES = 128
MESH = pl.DeviceIdType.MESH
VMEM_LIMIT = 61 * 1024 * 1024


def dot(a, b, ca, cb):
    return lax.dot_general(a, b, (((ca,), (cb,)), ((), ())), preferred_element_type=jnp.float32)


def norm_forward(x_blk, ln_gain, ln_bias):
    x_f32 = x_blk.astype(jnp.float32)
    centered = x_f32 - jnp.mean(x_f32, axis=-1, keepdims=True)
    inv_std = lax.rsqrt(jnp.mean(centered * centered, axis=-1, keepdims=True) + NORM_EPS)
    return (centered * inv_std * ln_gain + ln_bias).astype(jnp.bfloat16)


def greet_all(me, size):
    barrier = pltpu.get_barrier_semaphore()

    def greet(d, carry):
        pl.semaphore_signal(barrier, inc=1, device_id={"sp": lax.rem(me + d, size)}, device_id_type=MESH)
        return carry

    lax.fori_loop(1, size, greet, 0)
    pl.semaphore_wait(barrier, size - 1)


class Direct:
    def __init__(self, me, size, src, dst, send_sems, recv_sems):
        self.me, self.size, self.src, self.dst, self.send_sems, self.recv_sems = me, size, src, dst, send_sems, recv_sems

    def copy(self, d, peer, slot):
        return pltpu.make_async_remote_copy(
            src_ref=self.src(peer), dst_ref=self.dst(slot), send_sem=self.send_sems.at[d], recv_sem=self.recv_sems.at[d],
            device_id={"sp": peer}, device_id_type=MESH)

    def loop(self, step):
        def body(d, carry):
            step(d)
            return carry

        lax.fori_loop(1, self.size, body, 0)

    def start(self):
        self.loop(lambda d: self.copy(d, lax.rem(self.me + d, self.size), self.me).start())

    def wait_recv(self):
        def one(d):
            peer = lax.rem(self.me + self.size - d, self.size)
            self.copy(d, peer, peer).wait_recv()

        self.loop(one)

    def wait_send(self):
        self.loop(lambda d: self.copy(d, lax.rem(self.me + d, self.size), self.me).wait_send())


FIRST_OF = (2, 3, 0, 1)
CYCLE = (("P", 0), ("Q", 0, 0), ("Q", 3, 2), ("P", 1), ("Q", 0, 1), ("Q", 1, 0), ("Q", 2, 0), ("P", 2), ("Q", 1, 1),
         ("Q", 2, 1), ("Q", 3, 0), ("Q", 1, 2), ("Q", 2, 2), ("Q", 3, 1), ("Q", 0, 2))
LATE = 2
LAG = 3
COLOURS = 4
READY = 6
TAIL_ROWS = 32
STEP_OF = ((1, 0), (-1, 0), (0, 1), (0, -1))
PLACES = len(CYCLE)


class Torus:
    def __init__(self, size):
        self.side = math.isqrt(size // 2)
        self.me = lax.axis_index("sp")
        self.core = lax.rem(self.me, 2)
        chip = self.me // 2
        self.cx, self.cy = lax.rem(chip, self.side), chip // self.side
        self.flip = 1 - 2 * self.core
        self.sibling = self.me + self.flip

    def device_at(self, dx, dy):
        side = self.side
        return (lax.rem(self.cy + dy + side, side) * side + lax.rem(self.cx + dx + side, side)) * 2 + self.core

    def neighbour(self, link):
        return self.device_at(*STEP_OF[link])

    def chunk(self, link, place, ahead):
        what = CYCLE[place]
        if what[0] == "P":
            first, n, m = link, what[1] + ahead, 0
        else:
            first, n, m = FIRST_OF[link], what[2] + ahead, what[1]
        dx = -STEP_OF[link][0] * n - STEP_OF[first][0] * m
        dy = -STEP_OF[link][1] * n - STEP_OF[first][1] * m
        return self.device_at(dx, dy), first


def is_own(place):
    return CYCLE[place] in (("P", 0), ("Q", 0, 0))


def block_kernel(size, dims, own_ref, wq_ref, bias_ref, wo_ref, meta_ref, slope_ref,
                 gat_ref, parts_ref, partstok_ref, gwq_ref, gwtail_ref, gwo_ref,
                 stage, wbuf, wobuf, metabuf, rowbuf, sbuf, qkvb, dob, dk_acc, dv_acc, dq_all, o_all, d_all, pbuf,
                 load_sems, own_sems, piece_sems, parts_sem, ici_send, ici_recv, d2d_send, d2d_recv, own_send, own_recv,
                 meta_send, meta_recv, part_send, part_recv):
    batch, tok, head_dim, pad_dim, hidden, q_block = dims
    seq_len = size * tok
    torus = Torus(size)
    me, flip, sibling = torus.me, torus.flip, torus.sibling
    places = PLACES
    scale = head_dim ** -0.5
    slope = slope_ref[0]

    def send(b, link, place):
        block, colour = torus.chunk(link, place, 0)
        dst = gat_ref.at[b, block, colour]
        return pltpu.make_async_remote_copy(
            src_ref=stage.at[b, colour] if is_own(place) else dst, dst_ref=dst,
            send_sem=ici_send.at[b, link, place], recv_sem=ici_recv.at[b, link, place],
            device_id={"sp": torus.neighbour(link)}, device_id_type=MESH)

    def arrival(b, link, place):
        block, colour = torus.chunk(link, place, 1)
        ref = gat_ref.at[b, block, colour]
        return pltpu.make_async_remote_copy(
            src_ref=ref, dst_ref=ref, send_sem=ici_send.at[b, link, place], recv_sem=ici_recv.at[b, link, place],
            device_id={"sp": me}, device_id_type=MESH)

    def share(b, link, place, shift):
        block, colour = torus.chunk(link, place, 1)
        ref = gat_ref.at[b, block + shift, colour]
        return pltpu.make_async_remote_copy(
            src_ref=ref, dst_ref=ref, send_sem=d2d_send.at[b, link, place], recv_sem=d2d_recv.at[b, link, place],
            device_id={"sp": sibling}, device_id_type=MESH)

    def share_own(b, block):
        return pltpu.make_async_remote_copy(
            src_ref=stage.at[b], dst_ref=gat_ref.at[b, block], send_sem=own_send.at[b], recv_sem=own_recv.at[b],
            device_id={"sp": sibling}, device_id_type=MESH)

    def keep_own(b):
        return pltpu.make_async_copy(stage.at[b], gat_ref.at[b, me], own_sems.at[b])

    load_own = pltpu.make_async_copy(own_ref, stage, load_sems.at[0])
    load_wq = pltpu.make_async_copy(wq_ref.at[me], wbuf, load_sems.at[1])
    load_wo = pltpu.make_async_copy(wo_ref.at[me], wobuf, load_sems.at[2])
    own_meta = pltpu.make_async_copy(meta_ref, metabuf.at[me], load_sems.at[3])
    for load in (load_own, load_wq, load_wo, own_meta):
        load.start()
    meta = Direct(me, size, lambda j: meta_ref, lambda j: metabuf.at[j], meta_send, meta_recv)
    early = batch - 1
    trades = [Direct(me, size, lambda j, b=b: parts_ref.at[b, j], lambda j, b=b: partstok_ref.at[j, b], part_send.at[b], part_recv.at[b])
              for b in range(early)]
    own_parts = [pltpu.make_async_copy(parts_ref.at[b, me], partstok_ref.at[me, b], load_sems.at[4 + b]) for b in range(early)]
    greet_all(me, size)
    load_own.wait()

    pieces, group = sbuf.shape[0], sbuf.shape[1]
    piece_rows = group * tok

    def load_piece(b, p):
        return pltpu.make_async_copy(gat_ref.at[b, pl.ds(p * group, group)], sbuf.at[p], piece_sems.at[p])

    def rows_of(p, which, at=slice(None)):
        return sbuf[p, :, :, which, :, at].reshape(piece_rows, -1)

    def each(lo, hi, use):
        def body(p, carry):
            use(p)
            return carry

        lax.fori_loop(lo, hi, body, 0)

    def pad_lanes(a):
        return jnp.concatenate([a, jnp.zeros((a.shape[0], pad_dim - head_dim), a.dtype)], axis=1)

    def project(b, p):
        load_piece(b, p).wait()
        at = pl.ds(pl.multiple_of(p * piece_rows, piece_rows), piece_rows)
        r = (dot(rows_of(p, 1), wbuf[...], 1, 1) + bias_ref[...]).astype(jnp.bfloat16)
        for c in range(3):
            qkvb[at, c * pad_dim:(c + 1) * pad_dim] = pad_lanes(r[:, c * head_dim:(c + 1) * head_dim])
        dob[at, :] = pad_lanes(dot(rows_of(p, 0), wobuf[...], 1, 1).astype(jnp.bfloat16))

    def attend(b, i):
        span = (i + 1) * q_block
        mine = slice(i * q_block, span)
        if i == 0:
            dk_acc[...] = jnp.zeros_like(dk_acc)
            dv_acc[...] = jnp.zeros_like(dv_acc)
        q, k, v = qkvb[mine, :pad_dim], qkvb[:span, pad_dim:2 * pad_dim], qkvb[:span, 2 * pad_dim:]
        do = dob[mine, :]
        pos = rowbuf[pl.ds(b, 1), :span]
        keep = rowbuf[pl.ds(b + batch, 1), :span]
        bias = jnp.where(keep > 0, -slope * (pos[:, span - 1:] - pos).astype(jnp.float32), MASK_FILL)
        scores = dot(q, k, 1, 1) * scale + bias
        row_id = lax.broadcasted_iota(jnp.int32, (q_block, span), 0) + i * q_block
        col_id = lax.broadcasted_iota(jnp.int32, (q_block, span), 1)
        scores = jnp.where(col_id <= row_id, scores, MASK_FILL)
        expo = jnp.exp(scores - jnp.max(scores, axis=-1, keepdims=True))
        prob = expo * (1.0 / jnp.sum(expo, axis=-1, keepdims=True))
        prob_lo = prob.astype(jnp.bfloat16)
        o = dot(prob_lo, v, 1, 0).astype(jnp.bfloat16)
        row_dot = jnp.sum(do.astype(jnp.float32) * o.astype(jnp.float32), axis=-1, keepdims=True)
        ds_lo = (prob * (dot(do, v, 1, 1) - row_dot)).astype(jnp.bfloat16)
        o_all[mine, :] = o
        dq_all[mine, :] = (dot(ds_lo, k, 1, 0) * scale).astype(jnp.bfloat16)
        dv_acc[:span, :] += dot(prob_lo, do, 0, 0)
        dk_acc[:span, :] += dot(ds_lo, q, 0, 0)

    def store_parts(b):
        return pltpu.make_async_copy(pbuf, parts_ref.at[b], parts_sem)

    def finish(b):
        dk = (dk_acc[...] * scale).astype(jnp.bfloat16)
        dv = dv_acc[...].astype(jnp.bfloat16)
        d_all[...] = jnp.concatenate([dq_all[:, :head_dim], dk[:, :head_dim], dv[:, :head_dim]], axis=1)
        whole = jnp.concatenate([d_all[...], o_all[:, :head_dim]], axis=1).reshape(size, tok, 4 * head_dim)
        pbuf[...] = jnp.concatenate([whole[:, :tok // 2], whole[:, tok // 2:]], axis=2)
        store_parts(b).start()

    width = min(512, hidden)

    def gradient(p):
        rows = pl.ds(pl.multiple_of(p * piece_rows, piece_rows), piece_rows)

        def columns(n, carry):
            at = pl.ds(pl.multiple_of(n * width, width), width)
            term = dot(d_all[rows, :], rows_of(p, 1, at), 0, 0)
            gwq_ref[:, at] += term[:gwq_ref.shape[0]]
            gwtail_ref[:, at] += term[gwq_ref.shape[0]:]
            gwo_ref[:, at] += dot(o_all[rows, :head_dim], rows_of(p, 0, at), 0, 0)
            return carry

        lax.fori_loop(0, hidden // width, columns, 0)

    count = seq_len // q_block
    half = pieces // 2
    tasks = {(0, READY): [lambda b: each(0, pieces, lambda p: load_piece(b, p).start())],
             (0, READY + 2): [lambda b: each(0, half, lambda p: project(b, p))],
             (0, READY + 3): [lambda b: each(half, pieces, lambda p: project(b, p))],
             (1, 1): [finish],
             (1, 3): [lambda b: each(0, half, gradient)],
             (1, 5): [lambda b: each(half, pieces, gradient), lambda b: store_parts(b).wait()]}
    spots = [(0, place) for place in range(READY + 4, places)] + [(1, 0)]
    for i in range(count):
        tasks.setdefault(spots[min(max(0, i - 2), len(spots) - 1)], []).append(lambda b, i=i: attend(b, i))

    for ref in (gwq_ref, gwtail_ref, gwo_ref):
        ref[...] = jnp.zeros_like(ref)

    def phase_of(i, place):
        return i - 1 if place == LATE else i

    def among(b):
        return jnp.logical_and(b >= 0, b < batch)

    def turn(i, carry):
        for place in range(places):
            came = (place - LAG) % places
            b_came = phase_of(i if place >= LAG else i - 1, came)

            @pl.when(among(b_came))
            def _():
                for link in range(4):
                    arrival(b_came, link, came).wait_recv()
                    share(b_came, link, came, 0).start()

            b_send = phase_of(i, place)

            @pl.when(among(b_send))
            def _():
                for link in range(4):
                    send(b_send, link, place).start()

            shared = (place - LAG - 1) % places
            b_shared = phase_of(i if place >= LAG + 1 else i - 1, shared)

            @pl.when(among(b_shared))
            def _():
                for link in range(4):
                    share(b_shared, link, shared, flip).wait_recv()

            if place == 1:
                @pl.when(i == 0)
                def _():
                    for b in range(batch):
                        share_own(b, me).start()
                        keep_own(b).start()
                    meta.start()

            if place == READY:
                @pl.when(i == 1)
                def _():
                    for load in (load_wq, load_wo, own_meta):
                        load.wait()
                    meta.wait_recv()
                    for j in range(size):
                        rowbuf[:, j * tok:(j + 1) * tok] = metabuf[j, :, :tok]
                    for b in range(batch):
                        share_own(b, sibling).wait_recv()
                        keep_own(b).wait()

                @pl.when(i == batch)
                def _():
                    for b in range(early):
                        own_parts[b].start()
                        trades[b].start()

            for later in (0, 1):
                if (later, place) in tasks:
                    @pl.when(among(i - 1 - later))
                    def _():
                        for task in tasks[later, place]:
                            task(i - 1 - later)
        return carry

    lax.fori_loop(0, batch + 2, turn, 0)
    for b in range(early):
        own_parts[b].wait()
        trades[b].wait_recv()
        trades[b].wait_send()
    meta.wait_send()

    def sent(n, carry):
        b = n // (4 * places)
        link = lax.rem(n, 4 * places) // places
        place = lax.rem(n, places)
        ref = gat_ref.at[0, 0, 0]
        for sem in (ici_send, d2d_send):
            pltpu.make_async_remote_copy(
                src_ref=ref, dst_ref=ref, send_sem=sem.at[b, link, place], recv_sem=ici_recv.at[b, link, place],
                device_id={"sp": sibling}, device_id_type=MESH).wait_send()
        return carry

    lax.fori_loop(0, batch * 4 * places, sent, 0)
    for b in range(batch):
        share_own(b, me).wait_send()


def block_call(own, wq, bias, wo, meta, slope, size, q_block, collective_id):
    batch, _, _, rows, hidden = own.shape
    tok = COLOURS * rows
    heads, head_dim, _ = wo.shape
    pad_dim = -(-head_dim // LANES) * LANES
    seq_len = size * tok
    pieces = 4
    places = PLACES
    anywhere = pl.BlockSpec(memory_space=pl.ANY)
    vmem = pl.BlockSpec(memory_space=pltpu.VMEM)
    sem = pltpu.SemaphoreType.DMA
    bf16, f32 = jnp.bfloat16, jnp.float32
    flops = batch * (6 * seq_len * seq_len * 256 + 4 * seq_len * 4 * head_dim * hidden) + 80_000_000_000
    return pl.pallas_call(
        functools.partial(block_kernel, size, (batch, tok, head_dim, pad_dim, hidden, min(q_block, seq_len))),
        out_shape=(
            jax.ShapeDtypeStruct((batch, size, COLOURS, 2, rows, hidden), bf16),
            jax.ShapeDtypeStruct((batch, size, tok // 2, 8 * head_dim), bf16),
            jax.ShapeDtypeStruct((size, batch - 1, tok // 2, 8 * head_dim), bf16),
            jax.ShapeDtypeStruct((3 * head_dim - TAIL_ROWS, hidden), f32),
            jax.ShapeDtypeStruct((TAIL_ROWS, hidden), f32),
            jax.ShapeDtypeStruct((head_dim, hidden), f32),
        ),
        in_specs=[anywhere, anywhere, vmem, anywhere, anywhere, pl.BlockSpec(memory_space=pltpu.SMEM)],
        out_specs=(anywhere, anywhere, anywhere, vmem, vmem, vmem),
        scratch_shapes=[
            pltpu.VMEM((batch, COLOURS, 2, rows, hidden), bf16),
            pltpu.VMEM((3 * head_dim, hidden), bf16),
            pltpu.VMEM((head_dim, hidden), bf16),
            pltpu.VMEM((size, *meta.shape), meta.dtype),
            pltpu.VMEM((meta.shape[0], seq_len), meta.dtype),
            pltpu.VMEM((pieces, size // pieces, COLOURS, 2, rows, hidden), bf16),
            pltpu.VMEM((seq_len, 3 * pad_dim), bf16),
            pltpu.VMEM((seq_len, pad_dim), bf16),
            pltpu.VMEM((seq_len, pad_dim), f32),
            pltpu.VMEM((seq_len, pad_dim), f32),
            pltpu.VMEM((seq_len, pad_dim), bf16),
            pltpu.VMEM((seq_len, pad_dim), bf16),
            pltpu.VMEM((seq_len, 3 * head_dim), bf16),
            pltpu.VMEM((size, tok // 2, 8 * head_dim), bf16),
            sem((4 + batch,)), sem((batch,)), sem((pieces,)), sem,
            sem((batch, 4, places)), sem((batch, 4, places)), sem((batch, 4, places)), sem((batch, 4, places)),
            sem((batch,)), sem((batch,)), sem((size,)), sem((size,)), sem((batch - 1, size)), sem((batch - 1, size)),
        ],
        compiler_params=pltpu.CompilerParams(collective_id=collective_id, has_side_effects=True, vmem_limit_bytes=VMEM_LIMIT),
        cost_estimate=pl.CostEstimate(flops=flops, bytes_accessed=60_000_000, transcendentals=batch * seq_len * seq_len // 2),
        name="block",
    )(own, wq, bias, wo, meta, slope)


def spread_kernel(size, own_ref, parts_ref, gat_ref, last_ref, stage, load_sem, keep_sem, part_sem,
                  ici_send, ici_recv, d2d_send, d2d_recv, own_send, own_recv, part_send, part_recv):
    torus = Torus(size)
    me, sibling = torus.me, torus.sibling
    b = parts_ref.shape[0] - 1
    part = own_ref.shape[1] // COLOURS

    def view(block, colour):
        return gat_ref.at[block, :, pl.ds(colour * part, part)]

    def send(link, place):
        block, colour = torus.chunk(link, place, 0)
        dst = view(block, colour)
        return pltpu.make_async_remote_copy(
            src_ref=stage.at[:, pl.ds(colour * part, part)] if is_own(place) else dst, dst_ref=dst,
            send_sem=ici_send.at[link, place], recv_sem=ici_recv.at[link, place],
            device_id={"sp": torus.neighbour(link)}, device_id_type=MESH)

    def arrival(link, place):
        ref = view(*torus.chunk(link, place, 1))
        return pltpu.make_async_remote_copy(
            src_ref=ref, dst_ref=ref, send_sem=ici_send.at[link, place], recv_sem=ici_recv.at[link, place],
            device_id={"sp": me}, device_id_type=MESH)

    def share(link, place, shift):
        block, colour = torus.chunk(link, place, 1)
        ref = view(block + shift, colour)
        return pltpu.make_async_remote_copy(
            src_ref=ref, dst_ref=ref, send_sem=d2d_send.at[link, place], recv_sem=d2d_recv.at[link, place],
            device_id={"sp": sibling}, device_id_type=MESH)

    def share_own(block):
        return pltpu.make_async_remote_copy(
            src_ref=stage, dst_ref=gat_ref.at[block], send_sem=own_send, recv_sem=own_recv,
            device_id={"sp": sibling}, device_id_type=MESH)

    load = pltpu.make_async_copy(own_ref, stage, load_sem)
    load.start()
    keep = pltpu.make_async_copy(stage, gat_ref.at[me], keep_sem)
    trade = Direct(me, size, lambda j: parts_ref.at[b, j], lambda j: last_ref.at[j], part_send, part_recv)
    own_part = pltpu.make_async_copy(parts_ref.at[b, me], last_ref.at[me], part_sem)
    greet_all(me, size)
    load.wait()

    def place_of(g):
        place = g % PLACES
        return place if g >= 0 and g // PLACES == (1 if place == LATE else 0) else None

    for g in range(PLACES + LATE + LAG + 2):
        came, now, shared = place_of(g - LAG), place_of(g), place_of(g - LAG - 1)
        for link in range(4):
            if came is not None:
                arrival(link, came).wait_recv()
                share(link, came, 0).start()
        for link in range(4):
            if now is not None:
                send(link, now).start()
        for link in range(4):
            if shared is not None:
                share(link, shared, torus.flip).wait_recv()
        if g == 1:
            trade.start()
            own_part.start()
            share_own(me).start()
            keep.start()
    share_own(sibling).wait_recv()
    own_part.wait()
    keep.wait()
    trade.wait_recv()
    trade.wait_send()
    share_own(me).wait_send()
    for place in range(PLACES):
        for link in range(4):
            send(link, place).wait_send()
            share(link, place, 0).wait_send()


def spread(block, parts, size, collective_id):
    rows, cols = block.shape
    anywhere = pl.BlockSpec(memory_space=pl.ANY)
    sem = pltpu.SemaphoreType.DMA
    return pl.pallas_call(
        functools.partial(spread_kernel, size),
        out_shape=(jax.ShapeDtypeStruct((size, rows, cols), block.dtype), jax.ShapeDtypeStruct(parts.shape[1:], parts.dtype)),
        in_specs=[anywhere, anywhere],
        out_specs=(anywhere, anywhere),
        scratch_shapes=[
            pltpu.VMEM((rows, cols), block.dtype), sem, sem, sem,
            sem((4, PLACES)), sem((4, PLACES)), sem((4, PLACES)), sem((4, PLACES)), sem, sem, sem((size,)), sem((size,)),
        ],
        compiler_params=pltpu.CompilerParams(collective_id=collective_id, has_side_effects=True),
        cost_estimate=pl.CostEstimate(flops=100_000_000_000, bytes_accessed=8 * size * rows * cols, transcendentals=0),
        name="spread",
    )(block, parts)


def token_kernel(head_dim, chunk, early_ref, last_ref, wq_ref, wo_ref, x_ref, dy_ref, gain_ref, bout_ref,
                 y_ref, gx_ref, bq_ref, sums_ref, dn_acc, y_acc):
    n = pl.program_id(0)
    parts = []
    for b in range(early_ref.shape[1] + 1):
        pair = early_ref[0, b] if b < early_ref.shape[1] else last_ref[0]
        parts += [pair[:, :4 * head_dim], pair[:, 4 * head_dim:]]
    parts = jnp.concatenate(parts, axis=0)
    dqkv = parts[:, :3 * head_dim]
    o = parts[:, 3 * head_dim:]
    bq_ref[0] = jnp.sum(dqkv.astype(jnp.float32), axis=0, keepdims=True)
    dn_term = dot(dqkv, wq_ref[0], 1, 0)
    y_term = dot(o, wo_ref[0], 1, 0)

    @pl.when(n == 0)
    def _():
        dn_acc[...] = dn_term
        y_acc[...] = y_term

    @pl.when(n > 0)
    def _():
        dn_acc[...] += dn_term
        y_acc[...] += y_term

    @pl.when(n == pl.num_programs(0) - 1)
    def _():
        sums_ref[...] = jnp.zeros_like(sums_ref)
        gain = gain_ref[...]
        bout = bout_ref[...]

        def body(c, carry):
            at = pl.ds(pl.multiple_of(c * chunk, chunk), chunk)
            x = x_ref[at, :].astype(jnp.float32)
            dy = dy_ref[at, :].astype(jnp.float32)
            centered = x - jnp.mean(x, axis=-1, keepdims=True)
            inv_std = lax.rsqrt(jnp.mean(centered * centered, axis=-1, keepdims=True) + NORM_EPS)
            x_hat = centered * inv_std
            d_norm = dn_acc[at, :]
            d_hat = d_norm * gain
            d_mean = jnp.mean(d_hat, axis=-1, keepdims=True)
            d_proj = jnp.mean(d_hat * x_hat, axis=-1, keepdims=True)
            gx_ref[at, :] = (dy + inv_std * (d_hat - d_mean - x_hat * d_proj)).astype(jnp.bfloat16)
            y_ref[at, :] = (x + y_acc[at, :] + bout).astype(jnp.bfloat16)
            sums_ref[0:1, :] += jnp.sum(d_norm * x_hat, axis=0, keepdims=True)
            sums_ref[1:2, :] += jnp.sum(d_norm, axis=0, keepdims=True)
            sums_ref[2:3, :] += jnp.sum(dy, axis=0, keepdims=True)
            return carry

        lax.fori_loop(0, x_ref.shape[0] // chunk, body, 0)


def token_side(early, last, wq, wo, x, dy, gain, bout, head_dim):
    heads = early.shape[0]
    tokens, hidden = x.shape
    whole = lambda n: (0, 0)
    per_head = lambda n: (n, 0, 0)
    return pl.pallas_call(
        functools.partial(token_kernel, head_dim, 16),
        grid=(heads,),
        out_shape=(
            jax.ShapeDtypeStruct((tokens, hidden), jnp.bfloat16),
            jax.ShapeDtypeStruct((tokens, hidden), jnp.bfloat16),
            jax.ShapeDtypeStruct((heads, 1, 3 * head_dim), jnp.float32),
            jax.ShapeDtypeStruct((8, hidden), jnp.float32),
        ),
        in_specs=[
            pl.BlockSpec((1, *early.shape[1:]), lambda n: (n, 0, 0, 0)),
            pl.BlockSpec((1, *last.shape[1:]), per_head),
            pl.BlockSpec((1, 3 * head_dim, hidden), per_head),
            pl.BlockSpec((1, head_dim, hidden), per_head),
            pl.BlockSpec((tokens, hidden), whole),
            pl.BlockSpec((tokens, hidden), whole),
            pl.BlockSpec((1, hidden), whole),
            pl.BlockSpec((1, hidden), whole),
        ],
        out_specs=(
            pl.BlockSpec((tokens, hidden), whole),
            pl.BlockSpec((tokens, hidden), whole),
            pl.BlockSpec((1, 1, 3 * head_dim), per_head),
            pl.BlockSpec((8, hidden), whole),
        ),
        scratch_shapes=[pltpu.VMEM((tokens, hidden), jnp.float32)] * 2,
        compiler_params=pltpu.CompilerParams(vmem_limit_bytes=VMEM_LIMIT),
        cost_estimate=pl.CostEstimate(
            flops=2 * tokens * hidden * 4 * heads * head_dim, bytes_accessed=8 * hidden * heads * head_dim, transcendentals=0),
        name="token_side",
    )(early, last, wq, wo, x, dy, gain, bout)


def settle_kernel(block, depth, ahead, first, src_ref, *refs):
    dst_ref, buf, read_sems, write_sems = refs[-4:]
    per = src_ref.shape[1] // block
    count = src_ref.shape[0] * per

    def slab(ref, i, start):
        return ref.at[i // per, pl.ds(pl.multiple_of(start + lax.rem(i, per) * block, 8), block)]

    def read(i):
        return pltpu.make_async_copy(slab(src_ref, i, 0), buf.at[lax.rem(i, depth)], read_sems.at[lax.rem(i, depth)])

    def write(i):
        return pltpu.make_async_copy(buf.at[lax.rem(i, depth)], slab(dst_ref, i, first), write_sems.at[lax.rem(i, depth)])

    def step(i, carry):
        @pl.when(jnp.logical_and(i >= depth, i < count))
        def _():
            write(i - depth).wait()

        @pl.when(i < count)
        def _():
            read(i).start()

        @pl.when(i >= ahead)
        def _():
            read(i - ahead).wait()
            write(i - ahead).start()

        return carry

    lax.fori_loop(0, count + ahead, step, 0)

    def drain(i, carry):
        write(i).wait()
        return carry

    lax.fori_loop(max(0, count - depth), count, drain, 0)


def settle(x, first, total, block, into=None):
    depth, ahead = 12, 6
    count, _, cols = x.shape
    sem = pltpu.SemaphoreType.DMA((depth,))
    old = [] if into is None else [into]
    return pl.pallas_call(
        functools.partial(settle_kernel, block, depth, ahead, first),
        out_shape=jax.ShapeDtypeStruct((count, total, cols), x.dtype),
        in_specs=[pl.BlockSpec(memory_space=pl.ANY)] * (1 + len(old)),
        out_specs=pl.BlockSpec(memory_space=pl.ANY),
        scratch_shapes=[pltpu.VMEM((depth, block, cols), x.dtype), sem, sem],
        input_output_aliases={1: 0} if old else {},
        compiler_params=pltpu.CompilerParams(vmem_limit_bytes=VMEM_LIMIT),
        cost_estimate=pl.CostEstimate(flops=10_000_000_000, bytes_accessed=8 * x.size, transcendentals=0),
        name="settle",
    )(x, *old)


def solution(mesh):
    size = mesh.shape["sp"]

    def block_fn(x_blk, pos_blk, keep_blk, ln_gain, ln_bias, w_qkv, b_qkv, w_out, b_out, dy_blk):
        batch, tok, hidden = x_blk.shape
        heads, head_dim = w_qkv.shape[1], w_qkv.shape[3]
        tokens = batch * tok
        rank = lax.axis_index("sp")
        wq = jnp.transpose(w_qkv, (1, 2, 3, 0)).reshape(heads, 3 * head_dim, hidden)
        wo = w_out.reshape(heads, head_dim, hidden)
        dy_flat = dy_blk.reshape(tokens, hidden)

        def gather(a):
            return lax.all_gather(a, "sp", axis=0, tiled=True)

        x_norm = norm_forward(x_blk, ln_gain, ln_bias)
        own = jnp.stack([dy_blk, x_norm], axis=0).reshape(2, batch, COLOURS, tok // COLOURS, hidden).transpose(1, 2, 0, 3, 4)
        meta = jnp.pad(jnp.concatenate([pos_blk, keep_blk], axis=0), ((0, 8 - 2 * batch), (0, LANES - tok)))
        bias = lax.dynamic_slice_in_dim(b_qkv, rank, 1, 0).reshape(1, 3 * head_dim)
        slope = jnp.exp2(-8.0 * (rank + 1).astype(jnp.float32) / heads).reshape(1)
        _, parts, early, grad_head, grad_tail, grad_out = block_call(own, wq, bias, wo, meta, slope, size, 256, 0)

        rows, split = 3 * head_dim, 3 * head_dim - TAIL_ROWS
        grad_wq = settle(gather(grad_head).reshape(heads, split, hidden), 0, rows, split // 2)
        grad_wq = settle(gather(grad_tail).reshape(heads, TAIL_ROWS, hidden), split, rows, TAIL_ROWS, grad_wq)
        out_all, last = spread(grad_out, parts, size, 1)
        grad_wo = settle(out_all, 0, head_dim, head_dim)

        y, grad_x, bq_part, sums = token_side(
            early, last, wq, wo, x_blk.reshape(tokens, hidden), dy_flat, ln_gain.reshape(1, hidden), b_out.reshape(1, hidden), head_dim)
        bq, gain, bias_sum, bo = lax.psum((bq_part.reshape(-1), sums[0], sums[1], sums[2]), "sp")
        grad_wq = jnp.transpose(grad_wq.reshape(heads, 3, head_dim, hidden), (3, 0, 1, 2))
        return (y.reshape(x_blk.shape), grad_x.reshape(x_blk.shape), grad_wq, bq.reshape(heads, 3, head_dim),
                grad_wo.reshape(heads * head_dim, hidden),
                bo, gain, bias_sum)

    act_spec = P("dp", "sp", None)
    tok_spec = P("dp", "sp")
    in_specs = (act_spec, tok_spec, tok_spec, P(), P(), P(), P(), P(), P(), act_spec)
    out_specs = (act_spec, act_spec, P("dp", None, None, None), P("dp", None, None), P("dp", None), P("dp"), P("dp"), P("dp"))
    return jax.shard_map(block_fn, mesh=mesh, in_specs=in_specs, out_specs=out_specs, check_vma=False)
```

```python
import functools
import math

import jax
import jax.numpy as jnp
from jax import lax
from jax.experimental import pallas as pl
from jax.experimental.pallas import tpu as pltpu
from jax.sharding import PartitionSpec as P

NORM_EPS = 1e-5
MASK_FILL = -1e30
LANES = 128
MESH = pl.DeviceIdType.MESH
VMEM_LIMIT = 61 * 1024 * 1024


def dot(a, b, ca, cb):
    return lax.dot_general(a, b, (((ca,), (cb,)), ((), ())), preferred_element_type=jnp.float32)


def greet_all(me, size, meanwhile=lambda: None):
    barrier = pltpu.get_barrier_semaphore()

    def greet(d, carry):
        pl.semaphore_signal(barrier, inc=1, device_id={"sp": lax.rem(me + d, size)}, device_id_type=MESH)
        return carry

    lax.fori_loop(1, size, greet, 0)
    meanwhile()
    pl.semaphore_wait(barrier, size - 1)


class Direct:
    def __init__(self, me, size, src, dst, send_sems, recv_sems):
        self.me, self.size, self.src, self.dst, self.send_sems, self.recv_sems = me, size, src, dst, send_sems, recv_sems

    def copy(self, d, peer, slot):
        return pltpu.make_async_remote_copy(
            src_ref=self.src(peer), dst_ref=self.dst(slot), send_sem=self.send_sems.at[d], recv_sem=self.recv_sems.at[d],
            device_id={"sp": peer}, device_id_type=MESH)

    def loop(self, step):
        def body(d, carry):
            step(d)
            return carry

        lax.fori_loop(1, self.size, body, 0)

    def start(self):
        self.loop(lambda d: self.copy(d, lax.rem(self.me + d, self.size), self.me).start())

    def wait_recv(self):
        def one(d):
            peer = lax.rem(self.me + self.size - d, self.size)
            self.copy(d, peer, peer).wait_recv()

        self.loop(one)

    def wait_send(self):
        self.loop(lambda d: self.copy(d, lax.rem(self.me + d, self.size), self.me).wait_send())


FIRST_OF = (2, 3, 0, 1)
CYCLE = (("P", 0), ("Q", 0, 0), ("Q", 3, 2), ("P", 1), ("Q", 0, 1), ("Q", 1, 0), ("Q", 2, 0), ("P", 2), ("Q", 1, 1),
         ("Q", 2, 1), ("Q", 3, 0), ("Q", 1, 2), ("Q", 2, 2), ("Q", 3, 1), ("Q", 0, 2))
LATE = 2
LAG = 3
COLOURS = 4
READY = 6
STEP_OF = ((1, 0), (-1, 0), (0, 1), (0, -1))
PLACES = len(CYCLE)


class Torus:
    def __init__(self, size):
        self.side = math.isqrt(size // 2)
        self.me = lax.axis_index("sp")
        self.core = lax.rem(self.me, 2)
        chip = self.me // 2
        self.cx, self.cy = lax.rem(chip, self.side), chip // self.side
        self.flip = 1 - 2 * self.core
        self.sibling = self.me + self.flip

    def device_at(self, dx, dy):
        side = self.side
        return (lax.rem(self.cy + dy + side, side) * side + lax.rem(self.cx + dx + side, side)) * 2 + self.core

    def neighbour(self, link):
        return self.device_at(*STEP_OF[link])

    def chunk(self, link, place, ahead):
        what = CYCLE[place]
        if what[0] == "P":
            first, n, m = link, what[1] + ahead, 0
        else:
            first, n, m = FIRST_OF[link], what[2] + ahead, what[1]
        dx = -STEP_OF[link][0] * n - STEP_OF[first][0] * m
        dy = -STEP_OF[link][1] * n - STEP_OF[first][1] * m
        return self.device_at(dx, dy), first


def is_own(place):
    return CYCLE[place] in (("P", 0), ("Q", 0, 0))


def block_kernel(size, dims, x_ref, dy_ref, gain_ref, shift_ref, pos_ref, keep_ref, wq_ref, bias_ref, wo_ref,
                 gat_ref, parts_ref, partstok_ref, gwa_ref, gwb_ref, gwc_ref, gwo_ref,
                 xin, stage, wbuf, wobuf, metatile, metabuf, rowbuf, sbuf, qkvb, dob, dk_acc, dv_acc, dq_all, o_all, d_all, pbuf,
                 load_sems, own_sems, piece_sems, parts_sem, ici_send, ici_recv, d2d_send, d2d_recv, own_send, own_recv,
                 meta_send, meta_recv, part_send, part_recv):
    batch, tok, head_dim, pad_dim, hidden, q_block = dims
    seq_len = size * tok
    torus = Torus(size)
    me, flip, sibling, side = torus.me, torus.flip, torus.sibling, torus.side
    places = PLACES
    scale = head_dim ** -0.5
    heads = wo_ref.shape[0]
    slope = jnp.exp2(jnp.full((1, 1), -8.0 / heads, jnp.float32) * (me + 1).astype(jnp.float32))

    def send(b, link, place):
        block, colour = torus.chunk(link, place, 0)
        dst = gat_ref.at[b, block, colour]
        return pltpu.make_async_remote_copy(
            src_ref=stage.at[b, colour] if is_own(place) else dst, dst_ref=dst,
            send_sem=ici_send.at[b, link, place], recv_sem=ici_recv.at[b, link, place],
            device_id={"sp": torus.neighbour(link)}, device_id_type=MESH)

    def arrival(b, link, place):
        block, colour = torus.chunk(link, place, 1)
        ref = gat_ref.at[b, block, colour]
        return pltpu.make_async_remote_copy(
            src_ref=ref, dst_ref=ref, send_sem=ici_send.at[b, link, place], recv_sem=ici_recv.at[b, link, place],
            device_id={"sp": me}, device_id_type=MESH)

    def share(b, link, place, shift):
        block, colour = torus.chunk(link, place, 1)
        ref = gat_ref.at[b, block + shift, colour]
        return pltpu.make_async_remote_copy(
            src_ref=ref, dst_ref=ref, send_sem=d2d_send.at[b, link, place], recv_sem=d2d_recv.at[b, link, place],
            device_id={"sp": sibling}, device_id_type=MESH)

    def share_own(b, block):
        return pltpu.make_async_remote_copy(
            src_ref=stage.at[b], dst_ref=gat_ref.at[b, block], send_sem=own_send.at[b], recv_sem=own_recv.at[b],
            device_id={"sp": sibling}, device_id_type=MESH)

    def keep_own(b):
        return pltpu.make_async_copy(stage.at[b], gat_ref.at[b, me], own_sems.at[b])

    load_x = pltpu.make_async_copy(x_ref, xin, load_sems.at[0])
    load_dy = pltpu.make_async_copy(dy_ref, stage.at[:, :, 0], load_sems.at[1])
    load_wq = pltpu.make_async_copy(wq_ref.at[me], wbuf, load_sems.at[2])
    load_wo = pltpu.make_async_copy(wo_ref.at[me], wobuf, load_sems.at[3])
    for load in (load_x, load_dy, load_wq, load_wo):
        load.start()
    meta = Direct(me, size, lambda j: metatile, lambda j: metabuf.at[j], meta_send, meta_recv)
    early = batch - 1
    trades = [Direct(me, size, lambda j, b=b: parts_ref.at[b, j], lambda j, b=b: partstok_ref.at[j, b], part_send.at[b], part_recv.at[b])
              for b in range(early)]
    own_parts = [pltpu.make_async_copy(parts_ref.at[b, me], partstok_ref.at[me, b], load_sems.at[4 + b]) for b in range(early)]

    def prepare():
        metatile[...] = jnp.zeros_like(metatile)
        metatile[0:batch, 0:tok] = pos_ref[...]
        metatile[batch:2 * batch, 0:tok] = keep_ref[...]
        metabuf[me] = metatile[...]
        load_x.wait()

        def normalise(n, carry):
            b, c = n // COLOURS, lax.rem(n, COLOURS)
            x = xin[b, c].astype(jnp.float32)
            centered = x - jnp.mean(x, axis=-1, keepdims=True)
            inv_std = lax.rsqrt(jnp.mean(centered * centered, axis=-1, keepdims=True) + NORM_EPS)
            stage[b, c, 1] = (centered * inv_std * gain_ref[...] + shift_ref[...]).astype(jnp.bfloat16)
            return carry

        lax.fori_loop(0, batch * COLOURS, normalise, 0)
        load_dy.wait()

    greet_all(me, size, prepare)

    pieces = sbuf.shape[0]
    chip_rows = 2 * tok

    def chip_of(p, e):
        return torus.device_at(lax.rem(p + 1 + e, side), e) // 2

    def rows_at(p, e):
        return pl.ds(pl.multiple_of(chip_of(p, e) * chip_rows, chip_rows), chip_rows)

    def load_piece(b, p):
        return [pltpu.make_async_copy(gat_ref.at[b, pl.ds(chip_of(p, e) * 2, 2)], sbuf.at[p, e], piece_sems.at[p, e]) for e in range(side)]

    def start_piece(b, p):
        for load in load_piece(b, p):
            load.start()

    def rows_of(p, which, at=slice(None)):
        return sbuf[p, :, :, :, which, :, at].reshape(side * chip_rows, -1)

    def each(lo, hi, use):
        def body(p, carry):
            use(p)
            return carry

        lax.fori_loop(lo, hi, body, 0)

    def pad_lanes(a):
        return jnp.concatenate([a, jnp.zeros((a.shape[0], pad_dim - head_dim), a.dtype)], axis=1)

    def project(b, p):
        for load in load_piece(b, p):
            load.wait()
        bias = jnp.concatenate([bias_ref[c, pl.ds(me, 1), :] for c in range(3)], axis=1)
        r = (dot(rows_of(p, 1), wbuf[...], 1, 1) + bias).astype(jnp.bfloat16)
        d = pad_lanes(dot(rows_of(p, 0), wobuf[...], 1, 1).astype(jnp.bfloat16))
        q, k, v = (pad_lanes(r[:, c * head_dim:(c + 1) * head_dim]) for c in range(3))
        for e in range(side):
            mine = slice(e * chip_rows, (e + 1) * chip_rows)
            at = rows_at(p, e)
            for c, part in enumerate((q, k, v)):
                qkvb[at, c * pad_dim:(c + 1) * pad_dim] = part[mine]
            dob[at, :] = d[mine]

    def attend(b, i):
        span = (i + 1) * q_block
        mine = slice(i * q_block, span)
        if i == 0:
            dk_acc[...] = jnp.zeros_like(dk_acc)
            dv_acc[...] = jnp.zeros_like(dv_acc)
        q, k, v = qkvb[mine, :pad_dim], qkvb[:span, pad_dim:2 * pad_dim], qkvb[:span, 2 * pad_dim:]
        do = dob[mine, :]
        pos = rowbuf[pl.ds(b, 1), :span]
        keep = rowbuf[pl.ds(b + batch, 1), :span]
        bias = jnp.where(keep > 0, -slope * (pos[:, span - 1:] - pos).astype(jnp.float32), MASK_FILL)
        scores = dot(q, k, 1, 1) * scale + bias
        row_id = lax.broadcasted_iota(jnp.int32, (q_block, span), 0) + i * q_block
        col_id = lax.broadcasted_iota(jnp.int32, (q_block, span), 1)
        scores = jnp.where(col_id <= row_id, scores, MASK_FILL)
        expo = jnp.exp(scores - jnp.max(scores, axis=-1, keepdims=True))
        prob = expo * (1.0 / jnp.sum(expo, axis=-1, keepdims=True))
        prob_lo = prob.astype(jnp.bfloat16)
        o = dot(prob_lo, v, 1, 0).astype(jnp.bfloat16)
        row_dot = jnp.sum(do.astype(jnp.float32) * o.astype(jnp.float32), axis=-1, keepdims=True)
        ds_lo = (prob * (dot(do, v, 1, 1) - row_dot)).astype(jnp.bfloat16)
        o_all[mine, :] = o
        dq_all[mine, :] = (dot(ds_lo, k, 1, 0) * scale).astype(jnp.bfloat16)
        dv_acc[:span, :] += dot(prob_lo, do, 0, 0)
        dk_acc[:span, :] += dot(ds_lo, q, 0, 0)

    def store_parts(b):
        return pltpu.make_async_copy(pbuf, parts_ref.at[b], parts_sem)

    def finish(b):
        dk = (dk_acc[...] * scale).astype(jnp.bfloat16)
        dv = dv_acc[...].astype(jnp.bfloat16)
        d_all[...] = jnp.concatenate([dq_all[:, :head_dim], dk[:, :head_dim], dv[:, :head_dim]], axis=1)
        whole = jnp.concatenate([d_all[...], o_all[:, :head_dim]], axis=1).reshape(size, tok, 4 * head_dim)
        pbuf[...] = jnp.concatenate([whole[:, :tok // 2], whole[:, tok // 2:]], axis=2)
        store_parts(b).start()

    width = min(512, hidden)

    def gradient(p):
        d = jnp.concatenate([d_all[rows_at(p, e), :] for e in range(side)], axis=0)
        o = jnp.concatenate([o_all[rows_at(p, e), :] for e in range(side)], axis=0)[:, :head_dim]

        def columns(n, carry):
            at = pl.ds(pl.multiple_of(n * width, width), width)
            term = dot(d, rows_of(p, 1, at), 0, 0)
            row = 0
            for ref in (gwa_ref, gwb_ref, gwc_ref):
                ref[:, at] += term[row:row + ref.shape[0]]
                row += ref.shape[0]
            gwo_ref[:, at] += dot(o, rows_of(p, 0, at), 0, 0)
            return carry

        lax.fori_loop(0, hidden // width, columns, 0)

    count = seq_len // q_block
    last = pieces - 1
    tasks = {(0, READY - 3): [lambda b: each(0, last, lambda p: start_piece(b, p))],
             (0, READY - 2): [lambda b: each(0, last - 1, lambda p: project(b, p))],
             (0, READY - 1): [lambda b: project(b, last - 1)],
             (0, READY): [lambda b: start_piece(b, last)],
             (0, READY + 1): [lambda b: project(b, last)],
             (0, READY + 7): [finish],
             (0, READY + 8): [lambda b: each(0, pieces // 2, gradient)],
             (1, 0): [lambda b: each(pieces // 2, pieces, gradient)],
             (1, 1): [lambda b: store_parts(b).wait()]}
    spot = (2, 2, 2, 3, 3, 4, 5, 6)
    for i in range(count):
        tasks.setdefault((0, READY + spot[i]), []).append(lambda b, i=i: attend(b, i))

    for ref in (gwa_ref, gwb_ref, gwc_ref, gwo_ref):
        ref[...] = jnp.zeros_like(ref)

    def phase_of(i, place):
        return i - 1 if place == LATE else i

    def among(b):
        return jnp.logical_and(b >= 0, b < batch)

    def turn(i, carry):
        for place in range(places):
            came = (place - LAG) % places
            b_came = phase_of(i if place >= LAG else i - 1, came)

            @pl.when(among(b_came))
            def _():
                for link in range(4):
                    arrival(b_came, link, came).wait_recv()
                    share(b_came, link, came, 0).start()

            b_send = phase_of(i, place)

            @pl.when(among(b_send))
            def _():
                for link in range(4):
                    send(b_send, link, place).start()

            shared = (place - LAG - 1) % places
            b_shared = phase_of(i if place >= LAG + 1 else i - 1, shared)

            @pl.when(among(b_shared))
            def _():
                for link in range(4):
                    share(b_shared, link, shared, flip).wait_recv()
                for link in range(4):
                    share(b_shared, link, shared, 0).wait_send()
                    send(b_shared, link, shared).wait_send()

            if place == 1:
                @pl.when(i == 0)
                def _():
                    for b in range(batch):
                        share_own(b, me).start()
                        keep_own(b).start()
                    meta.start()

            if place == READY - 3:
                @pl.when(i == 1)
                def _():
                    for load in (load_wq, load_wo):
                        load.wait()
                    meta.wait_recv()
                    for j in range(size):
                        rowbuf[:, j * tok:(j + 1) * tok] = metabuf[j, :, :tok]
                    for b in range(batch):
                        share_own(b, sibling).wait_recv()
                        keep_own(b).wait()
                    meta.wait_send()
                    for b in range(batch):
                        share_own(b, me).wait_send()

            if place == READY:
                @pl.when(i == batch)
                def _():
                    for b in range(early):
                        own_parts[b].start()
                        trades[b].start()

            for later in (0, 1):
                if (later, place) in tasks:
                    @pl.when(among(i - 1 - later))
                    def _():
                        for task in tasks[later, place]:
                            task(i - 1 - later)
        return carry

    lax.fori_loop(0, batch + 2, turn, 0)
    for b in range(early):
        own_parts[b].wait()
        trades[b].wait_recv()
        trades[b].wait_send()


def split_rows(rows):
    first = 8 * (rows * 3 // 80)
    return first, rows - first - 8, 8


def block_call(x, dy, gain, shift, pos, keep, wq, bias, wo, size, q_block, collective_id):
    batch, tok, hidden = x.shape
    rows = tok // COLOURS
    heads, head_dim, _ = wo.shape
    pad_dim = -(-head_dim // LANES) * LANES
    seq_len = size * tok
    side = math.isqrt(size // 2)
    places = PLACES
    anywhere = pl.BlockSpec(memory_space=pl.ANY)
    vmem = pl.BlockSpec(memory_space=pltpu.VMEM)
    sem = pltpu.SemaphoreType.DMA
    bf16, f32 = jnp.bfloat16, jnp.float32
    flops = batch * (6 * seq_len * seq_len * 256 + 4 * seq_len * 4 * head_dim * hidden) + 80_000_000_000
    cut = (batch, COLOURS, rows, hidden)
    return pl.pallas_call(
        functools.partial(block_kernel, size, (batch, tok, head_dim, pad_dim, hidden, min(q_block, seq_len))),
        out_shape=(
            jax.ShapeDtypeStruct((batch, size, COLOURS, 2, rows, hidden), bf16),
            jax.ShapeDtypeStruct((batch, size, tok // 2, 8 * head_dim), bf16),
            jax.ShapeDtypeStruct((size, batch - 1, tok // 2, 8 * head_dim), bf16),
            *(jax.ShapeDtypeStruct((n, hidden), f32) for n in split_rows(3 * head_dim)),
            jax.ShapeDtypeStruct((head_dim, hidden), f32),
        ),
        in_specs=[anywhere, anywhere, vmem, vmem, vmem, vmem, anywhere, vmem, anywhere],
        out_specs=(anywhere, anywhere, anywhere, vmem, vmem, vmem, vmem),
        scratch_shapes=[
            pltpu.VMEM(cut, bf16),
            pltpu.VMEM((batch, COLOURS, 2, rows, hidden), bf16),
            pltpu.VMEM((3 * head_dim, hidden), bf16),
            pltpu.VMEM((head_dim, hidden), bf16),
            pltpu.VMEM((8, LANES), jnp.int32),
            pltpu.VMEM((size, 8, LANES), jnp.int32),
            pltpu.VMEM((8, seq_len), jnp.int32),
            pltpu.VMEM((side, side, 2, COLOURS, 2, rows, hidden), bf16),
            pltpu.VMEM((seq_len, 3 * pad_dim), bf16),
            pltpu.VMEM((seq_len, pad_dim), bf16),
            pltpu.VMEM((seq_len, pad_dim), f32),
            pltpu.VMEM((seq_len, pad_dim), f32),
            pltpu.VMEM((seq_len, pad_dim), bf16),
            pltpu.VMEM((seq_len, pad_dim), bf16),
            pltpu.VMEM((seq_len, 3 * head_dim), bf16),
            pltpu.VMEM((size, tok // 2, 8 * head_dim), bf16),
            sem((4 + batch,)), sem((batch,)), sem((side, side)), sem,
            sem((batch, 4, places)), sem((batch, 4, places)), sem((batch, 4, places)), sem((batch, 4, places)),
            sem((batch,)), sem((batch,)), sem((size,)), sem((size,)), sem((batch - 1, size)), sem((batch - 1, size)),
        ],
        compiler_params=pltpu.CompilerParams(collective_id=collective_id, has_side_effects=True, vmem_limit_bytes=VMEM_LIMIT),
        cost_estimate=pl.CostEstimate(flops=flops, bytes_accessed=60_000_000, transcendentals=batch * seq_len * seq_len // 2),
        name="block",
    )(x.reshape(cut), dy.reshape(cut), gain, shift, pos, keep, wq, bias, wo)


def spread_kernel(size, own_ref, parts_ref, gat_ref, last_ref, stage, load_sem, keep_sem, part_sem,
                  ici_send, ici_recv, d2d_send, d2d_recv, own_send, own_recv, part_send, part_recv):
    torus = Torus(size)
    me, sibling = torus.me, torus.sibling
    b = parts_ref.shape[0] - 1
    part = own_ref.shape[1] // COLOURS

    def view(block, colour):
        return gat_ref.at[block, :, pl.ds(colour * part, part)]

    def send(link, place):
        block, colour = torus.chunk(link, place, 0)
        dst = view(block, colour)
        return pltpu.make_async_remote_copy(
            src_ref=stage.at[:, pl.ds(colour * part, part)] if is_own(place) else dst, dst_ref=dst,
            send_sem=ici_send.at[link, place], recv_sem=ici_recv.at[link, place],
            device_id={"sp": torus.neighbour(link)}, device_id_type=MESH)

    def arrival(link, place):
        ref = view(*torus.chunk(link, place, 1))
        return pltpu.make_async_remote_copy(
            src_ref=ref, dst_ref=ref, send_sem=ici_send.at[link, place], recv_sem=ici_recv.at[link, place],
            device_id={"sp": me}, device_id_type=MESH)

    def share(link, place, shift):
        block, colour = torus.chunk(link, place, 1)
        ref = view(block + shift, colour)
        return pltpu.make_async_remote_copy(
            src_ref=ref, dst_ref=ref, send_sem=d2d_send.at[link, place], recv_sem=d2d_recv.at[link, place],
            device_id={"sp": sibling}, device_id_type=MESH)

    def share_own(block):
        return pltpu.make_async_remote_copy(
            src_ref=stage, dst_ref=gat_ref.at[block], send_sem=own_send, recv_sem=own_recv,
            device_id={"sp": sibling}, device_id_type=MESH)

    load = pltpu.make_async_copy(own_ref, stage, load_sem)
    load.start()
    keep = pltpu.make_async_copy(stage, gat_ref.at[me], keep_sem)
    trade = Direct(me, size, lambda j: parts_ref.at[b, j], lambda j: last_ref.at[j], part_send, part_recv)
    own_part = pltpu.make_async_copy(parts_ref.at[b, me], last_ref.at[me], part_sem)
    greet_all(me, size)
    load.wait()

    def place_of(g):
        place = g % PLACES
        return place if g >= 0 and g // PLACES == (1 if place == LATE else 0) else None

    for g in range(PLACES + LATE + LAG + 2):
        came, now, shared = place_of(g - LAG), place_of(g), place_of(g - LAG - 1)
        for link in range(4):
            if came is not None:
                arrival(link, came).wait_recv()
                share(link, came, 0).start()
        for link in range(4):
            if now is not None:
                send(link, now).start()
        for link in range(4):
            if shared is not None:
                share(link, shared, torus.flip).wait_recv()
        if g == 1:
            trade.start()
            own_part.start()
            share_own(me).start()
            keep.start()
    share_own(sibling).wait_recv()
    own_part.wait()
    keep.wait()
    trade.wait_recv()
    trade.wait_send()
    share_own(me).wait_send()
    for place in range(PLACES):
        for link in range(4):
            send(link, place).wait_send()
            share(link, place, 0).wait_send()


def spread(block, parts, size, collective_id):
    rows, cols = block.shape
    anywhere = pl.BlockSpec(memory_space=pl.ANY)
    sem = pltpu.SemaphoreType.DMA
    return pl.pallas_call(
        functools.partial(spread_kernel, size),
        out_shape=(jax.ShapeDtypeStruct((size, rows, cols), block.dtype), jax.ShapeDtypeStruct(parts.shape[1:], parts.dtype)),
        in_specs=[anywhere, anywhere],
        out_specs=(anywhere, anywhere),
        scratch_shapes=[
            pltpu.VMEM((rows, cols), block.dtype), sem, sem, sem,
            sem((4, PLACES)), sem((4, PLACES)), sem((4, PLACES)), sem((4, PLACES)), sem, sem, sem((size,)), sem((size,)),
        ],
        compiler_params=pltpu.CompilerParams(collective_id=collective_id, has_side_effects=True),
        cost_estimate=pl.CostEstimate(flops=100_000_000_000, bytes_accessed=8 * size * rows * cols, transcendentals=0),
        name="spread",
    )(block, parts)


def token_kernel(head_dim, chunk, early_ref, last_ref, wq_ref, wo_ref, x_ref, dy_ref, gain_ref, bout_ref,
                 y_ref, gx_ref, tiles_ref, dn_acc, y_acc, sums):
    n = pl.program_id(0)
    step = wq_ref.shape[0]

    @pl.when(n == 0)
    def _():
        tiles_ref[...] = jnp.zeros_like(tiles_ref)

    dn_term = y_term = 0.0
    for h in range(step):
        parts = []
        for b in range(early_ref.shape[1] + 1):
            pair = early_ref[h, b] if b < early_ref.shape[1] else last_ref[h]
            parts += [pair[:, :4 * head_dim], pair[:, 4 * head_dim:]]
        parts = jnp.concatenate(parts, axis=0)
        dqkv = parts[:, :3 * head_dim]
        total = jnp.sum(dqkv.astype(jnp.float32), axis=0, keepdims=True)
        for c in range(3):
            tiles_ref[n * step + h, 3 + c:4 + c, 0:head_dim] = total[:, c * head_dim:(c + 1) * head_dim]
        dn_term += dot(dqkv, wq_ref[h], 1, 0)
        y_term += dot(parts[:, 3 * head_dim:], wo_ref[h], 1, 0)

    @pl.when(n == 0)
    def _():
        dn_acc[...] = dn_term
        y_acc[...] = y_term

    @pl.when(n > 0)
    def _():
        dn_acc[...] += dn_term
        y_acc[...] += y_term

    @pl.when(n == pl.num_programs(0) - 1)
    def _():
        sums[...] = jnp.zeros_like(sums)
        gain = gain_ref[...]
        bout = bout_ref[...]

        def body(c, carry):
            at = pl.ds(pl.multiple_of(c * chunk, chunk), chunk)
            x = x_ref[at, :].astype(jnp.float32)
            dy = dy_ref[at, :].astype(jnp.float32)
            centered = x - jnp.mean(x, axis=-1, keepdims=True)
            inv_std = lax.rsqrt(jnp.mean(centered * centered, axis=-1, keepdims=True) + NORM_EPS)
            x_hat = centered * inv_std
            d_norm = dn_acc[at, :]
            d_hat = d_norm * gain
            d_mean = jnp.mean(d_hat, axis=-1, keepdims=True)
            d_proj = jnp.mean(d_hat * x_hat, axis=-1, keepdims=True)
            gx_ref[at, :] = (dy + inv_std * (d_hat - d_mean - x_hat * d_proj)).astype(jnp.bfloat16)
            y_ref[at, :] = (x + y_acc[at, :] + bout).astype(jnp.bfloat16)
            sums[0:1, :] += jnp.sum(d_norm * x_hat, axis=0, keepdims=True)
            sums[1:2, :] += jnp.sum(d_norm, axis=0, keepdims=True)
            sums[2:3, :] += jnp.sum(dy, axis=0, keepdims=True)
            return carry

        lax.fori_loop(0, x_ref.shape[0] // chunk, body, 0)
        for j in range(tiles_ref.shape[0]):
            tiles_ref[j, 0:3, 0:head_dim] = sums[0:3, j * head_dim:(j + 1) * head_dim]


def token_side(early, last, wq, wo, x, dy, gain, bout, head_dim):
    heads = early.shape[0]
    tokens, hidden = x.shape
    step = 4
    whole = lambda n: (0, 0)
    per_head = lambda n: (n, 0, 0)
    return pl.pallas_call(
        functools.partial(token_kernel, head_dim, 16),
        grid=(heads // step,),
        out_shape=(
            jax.ShapeDtypeStruct((tokens, hidden), jnp.bfloat16),
            jax.ShapeDtypeStruct((tokens, hidden), jnp.bfloat16),
            jax.ShapeDtypeStruct((heads, 8, LANES), jnp.float32),
        ),
        in_specs=[
            pl.BlockSpec((step, *early.shape[1:]), lambda n: (n, 0, 0, 0)),
            pl.BlockSpec((step, *last.shape[1:]), per_head),
            pl.BlockSpec((step, 3 * head_dim, hidden), per_head),
            pl.BlockSpec((step, head_dim, hidden), per_head),
            pl.BlockSpec((tokens, hidden), whole),
            pl.BlockSpec((tokens, hidden), whole),
            pl.BlockSpec((1, hidden), whole),
            pl.BlockSpec((1, hidden), whole),
        ],
        out_specs=(
            pl.BlockSpec((tokens, hidden), whole),
            pl.BlockSpec((tokens, hidden), whole),
            pl.BlockSpec((heads, 8, LANES), lambda n: (0, 0, 0)),
        ),
        scratch_shapes=[pltpu.VMEM((tokens, hidden), jnp.float32)] * 2 + [pltpu.VMEM((8, hidden), jnp.float32)],
        compiler_params=pltpu.CompilerParams(vmem_limit_bytes=VMEM_LIMIT),
        cost_estimate=pl.CostEstimate(
            flops=2 * tokens * hidden * 4 * heads * head_dim, bytes_accessed=8 * hidden * heads * head_dim, transcendentals=0),
        name="token_side",
    )(early, last, wq, wo, x, dy, gain, bout)


def sums_kernel(size, tiles_ref, all_ref, come, total, own_sem, send_a, recv_a, send_b, recv_b):
    me = lax.axis_index("sp")
    greet_all(me, size)
    own = pltpu.make_async_copy(tiles_ref.at[me], come.at[me], own_sem)
    own.start()
    spread_out = Direct(me, size, lambda j: tiles_ref.at[j], lambda j: come.at[j], send_a, recv_a)
    spread_out.start()
    own.wait()
    spread_out.wait_recv()
    total[...] = jnp.sum(come[...], axis=0)
    all_ref[me] = total[...]
    collect = Direct(me, size, lambda j: total, lambda j: all_ref.at[j], send_b, recv_b)
    collect.start()
    spread_out.wait_send()
    collect.wait_recv()
    collect.wait_send()


def sum_tiles(tiles, size, collective_id):
    sem = pltpu.SemaphoreType.DMA
    return pl.pallas_call(
        functools.partial(sums_kernel, size),
        out_shape=jax.ShapeDtypeStruct(tiles.shape, tiles.dtype),
        in_specs=[pl.BlockSpec(memory_space=pl.ANY)],
        out_specs=pl.BlockSpec(memory_space=pltpu.VMEM),
        scratch_shapes=[pltpu.VMEM(tiles.shape, tiles.dtype), pltpu.VMEM(tiles.shape[1:], tiles.dtype),
                        sem, sem((size,)), sem((size,)), sem((size,)), sem((size,))],
        compiler_params=pltpu.CompilerParams(collective_id=collective_id, has_side_effects=True),
        cost_estimate=pl.CostEstimate(flops=10_000_000_000, bytes_accessed=2 * 4 * tiles.size, transcendentals=0),
        name="sum_tiles",
    )(tiles)


def settle_kernel(block, depth, ahead, first, src_ref, *refs):
    dst_ref, buf, read_sems, write_sems = refs[-4:]
    per = src_ref.shape[1] // block
    count = src_ref.shape[0] * per

    def slab(ref, i, start):
        return ref.at[i // per, pl.ds(pl.multiple_of(start + lax.rem(i, per) * block, 8), block)]

    def read(i):
        return pltpu.make_async_copy(slab(src_ref, i, 0), buf.at[lax.rem(i, depth)], read_sems.at[lax.rem(i, depth)])

    def write(i):
        return pltpu.make_async_copy(buf.at[lax.rem(i, depth)], slab(dst_ref, i, first), write_sems.at[lax.rem(i, depth)])

    def step(i, carry):
        @pl.when(jnp.logical_and(i >= depth, i < count))
        def _():
            write(i - depth).wait()

        @pl.when(i < count)
        def _():
            read(i).start()

        @pl.when(i >= ahead)
        def _():
            read(i - ahead).wait()
            write(i - ahead).start()

        return carry

    lax.fori_loop(0, count + ahead, step, 0)

    def drain(i, carry):
        write(i).wait()
        return carry

    lax.fori_loop(max(0, count - depth), count, drain, 0)


def settle(x, first, total, block, into=None):
    depth, ahead = 12, 6
    count, _, cols = x.shape
    sem = pltpu.SemaphoreType.DMA((depth,))
    old = [] if into is None else [into]
    return pl.pallas_call(
        functools.partial(settle_kernel, block, depth, ahead, first),
        out_shape=jax.ShapeDtypeStruct((count, total, cols), x.dtype),
        in_specs=[pl.BlockSpec(memory_space=pl.ANY)] * (1 + len(old)),
        out_specs=pl.BlockSpec(memory_space=pl.ANY),
        scratch_shapes=[pltpu.VMEM((depth, block, cols), x.dtype), sem, sem],
        input_output_aliases={1: 0} if old else {},
        compiler_params=pltpu.CompilerParams(vmem_limit_bytes=VMEM_LIMIT),
        cost_estimate=pl.CostEstimate(flops=10_000_000_000, bytes_accessed=8 * x.size, transcendentals=0),
        name="settle",
    )(x, *old)


def solution(mesh):
    size = mesh.shape["sp"]

    def block_fn(x_blk, pos_blk, keep_blk, ln_gain, ln_bias, w_qkv, b_qkv, w_out, b_out, dy_blk):
        batch, tok, hidden = x_blk.shape
        heads, head_dim = w_qkv.shape[1], w_qkv.shape[3]
        tokens = batch * tok
        wq = jnp.transpose(w_qkv, (1, 2, 3, 0)).reshape(heads, 3 * head_dim, hidden)
        wo = w_out.reshape(heads, head_dim, hidden)
        row = lambda a: a.reshape(1, hidden)

        def gather(a):
            return lax.all_gather(a, "sp", axis=0, tiled=True).reshape(heads, a.shape[0], hidden)

        _, parts, early, grad_a, grad_b, grad_c, grad_out = block_call(
            x_blk, dy_blk, row(ln_gain), row(ln_bias), pos_blk, keep_blk, wq, jnp.transpose(b_qkv, (1, 0, 2)), wo, size, 256, 0)

        rows = 3 * head_dim
        first, second, third = split_rows(rows)
        grad_wq = settle(gather(grad_a), 0, rows, first)
        grad_wq = settle(gather(grad_b), first, rows, second // 2, grad_wq)
        grad_wq = settle(gather(grad_c), first + second, rows, third, grad_wq)
        out_all, last = spread(grad_out, parts, size, 1)
        grad_wo = settle(out_all, 0, head_dim, head_dim)

        y, grad_x, tiles = token_side(
            early, last, wq, wo, x_blk.reshape(tokens, hidden), dy_blk.reshape(tokens, hidden), row(ln_gain), row(b_out), head_dim)
        totals = sum_tiles(tiles, size, 2)[:, :, :head_dim]
        grad_wq = jnp.transpose(grad_wq.reshape(heads, 3, head_dim, hidden), (3, 0, 1, 2))
        return (y.reshape(x_blk.shape), grad_x.reshape(x_blk.shape), grad_wq, totals[:, 3:6],
                grad_wo.reshape(heads * head_dim, hidden), totals[:, 2].reshape(-1), totals[:, 0].reshape(-1), totals[:, 1].reshape(-1))

    act_spec = P("dp", "sp", None)
    tok_spec = P("dp", "sp")
    in_specs = (act_spec, tok_spec, tok_spec, P(), P(), P(), P(), P(), P(), act_spec)
    out_specs = (act_spec, act_spec, P("dp", None, None, None), P("dp", None, None), P("dp", None), P("dp"), P("dp"), P("dp"))
    return jax.shard_map(block_fn, mesh=mesh, in_specs=in_specs, out_specs=out_specs, check_vma=False)
```

```python
import functools
import math

import jax
import jax.numpy as jnp
from jax import lax
from jax.experimental import pallas as pl
from jax.experimental.pallas import tpu as pltpu
from jax.sharding import PartitionSpec as P

NORM_EPS = 1e-5
MASK_FILL = -1e30
LANES = 128
MESH = pl.DeviceIdType.MESH
VMEM_LIMIT = 61 * 1024 * 1024


def dot(a, b, ca, cb):
    return lax.dot_general(a, b, (((ca,), (cb,)), ((), ())), preferred_element_type=jnp.float32)


def greet_all(me, size, meanwhile=lambda: None):
    barrier = pltpu.get_barrier_semaphore()

    def greet(d, carry):
        pl.semaphore_signal(barrier, inc=1, device_id={"sp": lax.rem(me + d, size)}, device_id_type=MESH)
        return carry

    lax.fori_loop(1, size, greet, 0)
    meanwhile()
    pl.semaphore_wait(barrier, size - 1)


class Direct:
    def __init__(self, me, size, src, dst, whole, send_sem, recv_sem):
        self.me, self.size, self.src, self.dst, self.whole, self.send_sem, self.recv_sem = me, size, src, dst, whole, send_sem, recv_sem

    def start(self):
        def body(d, carry):
            peer = lax.rem(self.me + d, self.size)
            pltpu.make_async_remote_copy(
                src_ref=self.src(peer), dst_ref=self.dst(self.me), send_sem=self.send_sem, recv_sem=self.recv_sem,
                device_id={"sp": peer}, device_id_type=MESH).start()
            return carry

        lax.fori_loop(1, self.size, body, 0)

    def total(self):
        ref = self.whole.at[pl.ds(0, self.size - 1)]
        return pltpu.make_async_remote_copy(
            src_ref=ref, dst_ref=ref, send_sem=self.send_sem, recv_sem=self.recv_sem,
            device_id={"sp": self.me}, device_id_type=MESH)

    def wait_recv(self):
        self.total().wait_recv()

    def wait_send(self):
        self.total().wait_send()


FIRST_OF = (2, 3, 0, 1)
CYCLE = (("P", 0), ("Q", 0, 0), ("Q", 3, 2), ("P", 1), ("Q", 0, 1), ("Q", 1, 0), ("Q", 2, 0), ("P", 2), ("Q", 1, 1),
         ("Q", 2, 1), ("Q", 3, 0), ("Q", 1, 2), ("Q", 2, 2), ("Q", 3, 1), ("Q", 0, 2))
LATE = 2
LAG = 3
COLOURS = 4
READY = 6
STEP_OF = ((1, 0), (-1, 0), (0, 1), (0, -1))
PLACES = len(CYCLE)


class Torus:
    def __init__(self, size):
        self.side = math.isqrt(size // 2)
        self.me = lax.axis_index("sp")
        self.core = lax.rem(self.me, 2)
        chip = self.me // 2
        self.cx, self.cy = lax.rem(chip, self.side), chip // self.side
        self.flip = 1 - 2 * self.core
        self.sibling = self.me + self.flip

    def device_at(self, dx, dy):
        side = self.side
        return (lax.rem(self.cy + dy + side, side) * side + lax.rem(self.cx + dx + side, side)) * 2 + self.core

    def neighbour(self, link):
        return self.device_at(*STEP_OF[link])

    def chunk(self, link, place, ahead):
        what = CYCLE[place]
        if what[0] == "P":
            first, n, m = link, what[1] + ahead, 0
        else:
            first, n, m = FIRST_OF[link], what[2] + ahead, what[1]
        dx = -STEP_OF[link][0] * n - STEP_OF[first][0] * m
        dy = -STEP_OF[link][1] * n - STEP_OF[first][1] * m
        return self.device_at(dx, dy), first


def is_own(place):
    return CYCLE[place] in (("P", 0), ("Q", 0, 0))


def block_kernel(size, dims, x_ref, dy_ref, gain_ref, shift_ref, pos_ref, keep_ref, wq_ref, bias_ref, wo_ref,
                 gat_ref, parts_ref, partstok_ref, gwa_ref, gwb_ref, gwc_ref, gwo_ref,
                 xin, stage, wbuf, wobuf, metatile, metabuf, rowbuf, sbuf, qkvb, dob, dk_acc, dv_acc, dq_all, o_all, d_all, pbuf,
                 load_sems, own_sems, piece_sems, parts_sem, ici_send, ici_recv, d2d_send, d2d_recv, own_send, own_recv,
                 meta_send, meta_recv, part_send, part_recv):
    batch, tok, head_dim, pad_dim, hidden, q_block = dims
    seq_len = size * tok
    torus = Torus(size)
    me, flip, sibling, side = torus.me, torus.flip, torus.sibling, torus.side
    places = PLACES
    scale = head_dim ** -0.5
    heads = wo_ref.shape[0]
    slope = jnp.exp2(jnp.full((1, 1), -8.0 / heads, jnp.float32) * (me + 1).astype(jnp.float32))

    def send(b, link, place):
        block, colour = torus.chunk(link, place, 0)
        dst = gat_ref.at[b, block, colour]
        return pltpu.make_async_remote_copy(
            src_ref=stage.at[b, colour] if is_own(place) else dst, dst_ref=dst,
            send_sem=ici_send.at[link], recv_sem=ici_recv.at[link, place],
            device_id={"sp": torus.neighbour(link)}, device_id_type=MESH)

    def arrival(b, link, place):
        block, colour = torus.chunk(link, place, 1)
        ref = gat_ref.at[b, block, colour]
        return pltpu.make_async_remote_copy(
            src_ref=ref, dst_ref=ref, send_sem=ici_send.at[link], recv_sem=ici_recv.at[link, place],
            device_id={"sp": me}, device_id_type=MESH)

    def share(b, link, place, shift):
        block, colour = torus.chunk(link, place, 1)
        ref = gat_ref.at[b, block + shift, colour]
        return pltpu.make_async_remote_copy(
            src_ref=ref, dst_ref=ref, send_sem=d2d_send.at[link], recv_sem=d2d_recv.at[link, place],
            device_id={"sp": sibling}, device_id_type=MESH)

    def share_own(b, block):
        return pltpu.make_async_remote_copy(
            src_ref=stage.at[b], dst_ref=gat_ref.at[b, block], send_sem=own_send.at[b], recv_sem=own_recv.at[b],
            device_id={"sp": sibling}, device_id_type=MESH)

    def keep_own(b):
        return pltpu.make_async_copy(stage.at[b], gat_ref.at[b, me], own_sems.at[b])

    load_x = pltpu.make_async_copy(x_ref, xin, load_sems.at[0])
    load_dy = pltpu.make_async_copy(dy_ref, stage.at[:, :, 0], load_sems.at[1])
    load_wq = pltpu.make_async_copy(wq_ref.at[me], wbuf, load_sems.at[2])
    load_wo = pltpu.make_async_copy(wo_ref.at[me], wobuf, load_sems.at[3])
    for load in (load_x, load_dy, load_wq, load_wo):
        load.start()
    meta = Direct(me, size, lambda j: metatile, lambda j: metabuf.at[j], metabuf, meta_send, meta_recv)
    trade = Direct(me, size, lambda j: parts_ref.at[0, j], lambda j: partstok_ref.at[j], partstok_ref, part_send, part_recv)
    own_parts = pltpu.make_async_copy(parts_ref.at[0, me], partstok_ref.at[me], load_sems.at[4])

    def prepare():
        metatile[...] = jnp.zeros_like(metatile)
        metatile[0:batch, 0:tok] = pos_ref[...]
        metatile[batch:2 * batch, 0:tok] = keep_ref[...]
        metabuf[me] = metatile[...]
        load_x.wait()

        gain, shift = gain_ref[...].reshape(1, 1, hidden), shift_ref[...].reshape(1, 1, hidden)

        def normalise(b, carry):
            x = xin[b].astype(jnp.float32)
            centered = x - jnp.mean(x, axis=-1, keepdims=True)
            inv_std = lax.rsqrt(jnp.mean(centered * centered, axis=-1, keepdims=True) + NORM_EPS)
            stage[b, :, 1] = (centered * inv_std * gain + shift).astype(jnp.bfloat16)
            return carry

        lax.fori_loop(0, batch, normalise, 0)
        load_dy.wait()

    greet_all(me, size, prepare)

    pieces = sbuf.shape[0]
    chip_rows = 2 * tok

    def chip_of(p, e):
        return torus.device_at(lax.rem(p + 1 + e, side), e) // 2

    def rows_at(p, e):
        return pl.ds(pl.multiple_of(chip_of(p, e) * chip_rows, chip_rows), chip_rows)

    def load_piece(b, p):
        return [pltpu.make_async_copy(gat_ref.at[b, pl.ds(chip_of(p, e) * 2, 2)], sbuf.at[p, e], piece_sems.at[p, e]) for e in range(side)]

    def start_piece(b, p):
        for load in load_piece(b, p):
            load.start()

    def rows_of(p, which, at=slice(None)):
        return sbuf[p, :, :, :, which, :, at].reshape(side * chip_rows, -1)

    def each(lo, hi, use):
        def body(p, carry):
            use(p)
            return carry

        lax.fori_loop(lo, hi, body, 0)

    def pad_lanes(a):
        return jnp.concatenate([a, jnp.zeros((a.shape[0], pad_dim - head_dim), a.dtype)], axis=1)

    def project(b, p):
        for load in load_piece(b, p):
            load.wait()
        bias = jnp.concatenate([bias_ref[c, pl.ds(me, 1), :] for c in range(3)], axis=1)
        r = (dot(rows_of(p, 1), wbuf[...], 1, 1) + bias).astype(jnp.bfloat16)
        d = pad_lanes(dot(rows_of(p, 0), wobuf[...], 1, 1).astype(jnp.bfloat16))
        q, k, v = (pad_lanes(r[:, c * head_dim:(c + 1) * head_dim]) for c in range(3))
        for e in range(side):
            mine = slice(e * chip_rows, (e + 1) * chip_rows)
            at = rows_at(p, e)
            for c, part in enumerate((q, k, v)):
                qkvb[at, c * pad_dim:(c + 1) * pad_dim] = part[mine]
            dob[at, :] = d[mine]

    def attend(b, i):
        span = (i + 1) * q_block
        mine = slice(i * q_block, span)
        if i == 0:
            dk_acc[...] = jnp.zeros_like(dk_acc)
            dv_acc[...] = jnp.zeros_like(dv_acc)
        q, k, v = qkvb[mine, :pad_dim], qkvb[:span, pad_dim:2 * pad_dim], qkvb[:span, 2 * pad_dim:]
        do = dob[mine, :]
        pos = rowbuf[pl.ds(b, 1), :span]
        keep = rowbuf[pl.ds(b + batch, 1), :span]
        bias = jnp.where(keep > 0, -slope * (pos[:, span - 1:] - pos).astype(jnp.float32), MASK_FILL)
        scores = dot(q, k, 1, 1) * scale + bias
        row_id = lax.broadcasted_iota(jnp.int32, (q_block, span), 0) + i * q_block
        col_id = lax.broadcasted_iota(jnp.int32, (q_block, span), 1)
        scores = jnp.where(col_id <= row_id, scores, MASK_FILL)
        expo = jnp.exp(scores - jnp.max(scores, axis=-1, keepdims=True))
        prob = expo * (1.0 / jnp.sum(expo, axis=-1, keepdims=True))
        prob_lo = prob.astype(jnp.bfloat16)
        o = dot(prob_lo, v, 1, 0).astype(jnp.bfloat16)
        row_dot = jnp.sum(do.astype(jnp.float32) * o.astype(jnp.float32), axis=-1, keepdims=True)
        ds_lo = (prob * (dot(do, v, 1, 1) - row_dot)).astype(jnp.bfloat16)
        o_all[mine, :] = o
        dq_all[mine, :] = (dot(ds_lo, k, 1, 0) * scale).astype(jnp.bfloat16)
        dv_acc[:span, :] += dot(prob_lo, do, 0, 0)
        dk_acc[:span, :] += dot(ds_lo, q, 0, 0)

    def store_parts(b):
        return pltpu.make_async_copy(pbuf, parts_ref.at[b], parts_sem)

    def finish(b):
        dk = (dk_acc[...] * scale).astype(jnp.bfloat16)
        dv = dv_acc[...].astype(jnp.bfloat16)
        d_all[...] = jnp.concatenate([dq_all[:, :head_dim], dk[:, :head_dim], dv[:, :head_dim]], axis=1)
        whole = jnp.concatenate([d_all[...], o_all[:, :head_dim]], axis=1).reshape(size, tok, 4 * head_dim)
        pbuf[...] = jnp.concatenate([whole[:, :tok // 2], whole[:, tok // 2:]], axis=2)
        store_parts(b).start()

    width = min(512, hidden)

    def gradient(p):
        d = jnp.concatenate([d_all[rows_at(p, e), :] for e in range(side)], axis=0)
        o = jnp.concatenate([o_all[rows_at(p, e), :] for e in range(side)], axis=0)[:, :head_dim]

        def columns(n, carry):
            at = pl.ds(pl.multiple_of(n * width, width), width)
            term = dot(d, rows_of(p, 1, at), 0, 0)
            row = 0
            for ref in (gwa_ref, gwb_ref, gwc_ref):
                ref[:, at] += term[row:row + ref.shape[0]]
                row += ref.shape[0]
            gwo_ref[:, at] += dot(o, rows_of(p, 0, at), 0, 0)
            return carry

        lax.fori_loop(0, hidden // width, columns, 0)

    count = seq_len // q_block
    last = pieces - 1
    tasks = {(0, READY - 3): [lambda b: each(0, last, lambda p: start_piece(b, p))],
             (0, READY - 2): [lambda b: each(0, last - 1, lambda p: project(b, p))],
             (0, READY - 1): [lambda b: project(b, last - 1)],
             (0, READY): [lambda b: start_piece(b, last)],
             (0, READY + 1): [lambda b: project(b, last)],
             (0, READY + 7): [finish],
             (0, READY + 8): [lambda b: each(0, pieces // 2, gradient)],
             (1, 0): [lambda b: each(pieces // 2, pieces, gradient)],
             (1, 1): [lambda b: store_parts(b).wait()]}
    spot = (2, 2, 2, 3, 3, 4, 5, 6)
    for i in range(count):
        tasks.setdefault((0, READY + spot[i]), []).append(lambda b, i=i: attend(b, i))

    for ref in (gwa_ref, gwb_ref, gwc_ref, gwo_ref):
        ref[...] = jnp.zeros_like(ref)

    def phase_of(i, place):
        return i - 1 if place == LATE else i

    def among(b):
        return jnp.logical_and(b >= 0, b < batch)

    def turn(i, carry):
        for place in range(places):
            came = (place - LAG) % places
            b_came = phase_of(i if place >= LAG else i - 1, came)

            @pl.when(among(b_came))
            def _():
                for link in range(4):
                    arrival(b_came, link, came).wait_recv()
                    share(b_came, link, came, 0).start()

            b_send = phase_of(i, place)

            @pl.when(among(b_send))
            def _():
                for link in range(4):
                    send(b_send, link, place).start()

            shared = (place - LAG - 1) % places
            b_shared = phase_of(i if place >= LAG + 1 else i - 1, shared)

            @pl.when(among(b_shared))
            def _():
                for link in range(4):
                    share(b_shared, link, shared, flip).wait_recv()

            if place == 1:
                @pl.when(i == 0)
                def _():
                    for b in range(batch):
                        share_own(b, me).start()
                        keep_own(b).start()
                    meta.start()

            if place == READY - 3:
                @pl.when(i == 1)
                def _():
                    for load in (load_wq, load_wo):
                        load.wait()
                    meta.wait_recv()
                    for j in range(size):
                        rowbuf[:, j * tok:(j + 1) * tok] = metabuf[j, :, :tok]
                    for b in range(batch):
                        share_own(b, sibling).wait_recv()
                        keep_own(b).wait()
                    meta.wait_send()
                    for b in range(batch):
                        share_own(b, me).wait_send()

            if place == READY:
                @pl.when(i == batch)
                def _():
                    own_parts.start()
                    trade.start()

            for later in (0, 1):
                if (later, place) in tasks:
                    @pl.when(among(i - 1 - later))
                    def _():
                        for task in tasks[later, place]:
                            task(i - 1 - later)
        return carry

    lax.fori_loop(0, batch + 2, turn, 0)
    own_parts.wait()
    trade.wait_recv()
    trade.wait_send()
    sent = gat_ref.at[:, pl.ds(0, places), 0]
    for link in range(4):
        for sem in (ici_send, d2d_send):
            pltpu.make_async_remote_copy(
                src_ref=sent, dst_ref=sent, send_sem=sem.at[link], recv_sem=ici_recv.at[link, 0],
                device_id={"sp": sibling}, device_id_type=MESH).wait_send()


def split_rows(rows):
    own = 8 * (rows // 60)
    first = 16 * (rows // 24)
    return first, rows - first - own, own


def block_call(x, dy, gain, shift, pos, keep, wq, bias, wo, size, q_block, collective_id):
    batch, tok, hidden = x.shape
    rows = tok // COLOURS
    heads, head_dim, _ = wo.shape
    pad_dim = -(-head_dim // LANES) * LANES
    seq_len = size * tok
    side = math.isqrt(size // 2)
    places = PLACES
    anywhere = pl.BlockSpec(memory_space=pl.ANY)
    vmem = pl.BlockSpec(memory_space=pltpu.VMEM)
    sem = pltpu.SemaphoreType.DMA
    bf16, f32 = jnp.bfloat16, jnp.float32
    flops = batch * (6 * seq_len * seq_len * 256 + 4 * seq_len * 4 * head_dim * hidden) + 80_000_000_000
    cut = (batch, COLOURS, rows, hidden)
    return pl.pallas_call(
        functools.partial(block_kernel, size, (batch, tok, head_dim, pad_dim, hidden, min(q_block, seq_len))),
        out_shape=(
            jax.ShapeDtypeStruct((batch, size, COLOURS, 2, rows, hidden), bf16),
            jax.ShapeDtypeStruct((batch, size, tok // 2, 8 * head_dim), bf16),
            jax.ShapeDtypeStruct((size, tok // 2, 8 * head_dim), bf16),
            *(jax.ShapeDtypeStruct((n, hidden), f32) for n in split_rows(3 * head_dim)),
            jax.ShapeDtypeStruct((head_dim, hidden), f32),
        ),
        in_specs=[anywhere, anywhere, vmem, vmem, vmem, vmem, anywhere, vmem, anywhere],
        out_specs=(anywhere, anywhere, anywhere, vmem, vmem, vmem, vmem),
        scratch_shapes=[
            pltpu.VMEM(cut, bf16),
            pltpu.VMEM((batch, COLOURS, 2, rows, hidden), bf16),
            pltpu.VMEM((3 * head_dim, hidden), bf16),
            pltpu.VMEM((head_dim, hidden), bf16),
            pltpu.VMEM((8, LANES), jnp.int32),
            pltpu.VMEM((size, 8, LANES), jnp.int32),
            pltpu.VMEM((8, seq_len), jnp.int32),
            pltpu.VMEM((side, side, 2, COLOURS, 2, rows, hidden), bf16),
            pltpu.VMEM((seq_len, 3 * pad_dim), bf16),
            pltpu.VMEM((seq_len, pad_dim), bf16),
            pltpu.VMEM((seq_len, pad_dim), f32),
            pltpu.VMEM((seq_len, pad_dim), f32),
            pltpu.VMEM((seq_len, pad_dim), bf16),
            pltpu.VMEM((seq_len, pad_dim), bf16),
            pltpu.VMEM((seq_len, 3 * head_dim), bf16),
            pltpu.VMEM((size, tok // 2, 8 * head_dim), bf16),
            sem((5,)), sem((batch,)), sem((side, side)), sem,
            sem((4,)), sem((4, places)), sem((4,)), sem((4, places)), sem((batch,)), sem((batch,)), sem, sem, sem, sem,
        ],
        compiler_params=pltpu.CompilerParams(collective_id=collective_id, has_side_effects=True, vmem_limit_bytes=VMEM_LIMIT),
        cost_estimate=pl.CostEstimate(flops=flops, bytes_accessed=60_000_000, transcendentals=batch * seq_len * seq_len // 2),
        name="block",
    )(x.reshape(cut), dy.reshape(cut), gain, shift, pos, keep, wq, bias, wo)


def spread_kernel(size, begin, own_ref, parts_ref, after_ref, gat_ref, late_ref, stage, load_sem, keep_sem, own_part_sems,
                  ici_send, ici_recv, d2d_send, d2d_recv, own_send, own_recv, part_send, part_recv):
    torus = Torus(size)
    me, sibling = torus.me, torus.sibling
    part = own_ref.shape[1] // COLOURS

    def view(block, colour):
        return gat_ref.at[block, :, pl.ds(colour * part, part)]

    def send(link, place):
        block, colour = torus.chunk(link, place, 0)
        dst = view(block, colour)
        return pltpu.make_async_remote_copy(
            src_ref=stage.at[:, pl.ds(colour * part, part)] if is_own(place) else dst, dst_ref=dst,
            send_sem=ici_send.at[link], recv_sem=ici_recv.at[link, place],
            device_id={"sp": torus.neighbour(link)}, device_id_type=MESH)

    def arrival(link, place):
        ref = view(*torus.chunk(link, place, 1))
        return pltpu.make_async_remote_copy(
            src_ref=ref, dst_ref=ref, send_sem=ici_send.at[link], recv_sem=ici_recv.at[link, place],
            device_id={"sp": me}, device_id_type=MESH)

    def share(link, place, shift):
        block, colour = torus.chunk(link, place, 1)
        ref = view(block + shift, colour)
        return pltpu.make_async_remote_copy(
            src_ref=ref, dst_ref=ref, send_sem=d2d_send.at[link], recv_sem=d2d_recv.at[link, place],
            device_id={"sp": sibling}, device_id_type=MESH)

    def share_own(block):
        return pltpu.make_async_remote_copy(
            src_ref=stage, dst_ref=gat_ref.at[block], send_sem=own_send, recv_sem=own_recv,
            device_id={"sp": sibling}, device_id_type=MESH)

    load = pltpu.make_async_copy(own_ref, stage, load_sem)
    load.start()
    keep = pltpu.make_async_copy(stage, gat_ref.at[me], keep_sem)
    trades, own_parts = [], []
    for n in range(parts_ref.shape[0] - begin):
        b = begin + n
        trades.append(Direct(me, size, lambda j, b=b: parts_ref.at[b, j], lambda j, n=n: late_ref.at[n, j], late_ref.at[n],
                             part_send.at[n], part_recv.at[n]))
        own_parts.append(pltpu.make_async_copy(parts_ref.at[b, me], late_ref.at[n, me], own_part_sems.at[n]))
    greet_all(me, size)
    load.wait()

    def place_of(g):
        place = g % PLACES
        return place if g >= 0 and g // PLACES == (1 if place == LATE else 0) else None

    for g in range(PLACES + LATE + LAG + 2):
        came, now, shared = place_of(g - LAG), place_of(g), place_of(g - LAG - 1)
        for link in range(4):
            if came is not None:
                arrival(link, came).wait_recv()
                share(link, came, 0).start()
        for link in range(4):
            if now is not None:
                send(link, now).start()
        for link in range(4):
            if shared is not None:
                share(link, shared, torus.flip).wait_recv()
        if g == 1:
            for copy in trades + own_parts:
                copy.start()
            share_own(me).start()
            keep.start()
    share_own(sibling).wait_recv()
    keep.wait()
    for copy in own_parts:
        copy.wait()
    for trade in trades:
        trade.wait_recv()
        trade.wait_send()
    share_own(me).wait_send()
    sent = gat_ref.at[pl.ds(0, PLACES), :, pl.ds(0, part)]
    for link in range(4):
        for sem in (ici_send, d2d_send):
            pltpu.make_async_remote_copy(
                src_ref=sent, dst_ref=sent, send_sem=sem.at[link], recv_sem=ici_recv.at[link, 0],
                device_id={"sp": sibling}, device_id_type=MESH).wait_send()


def spread(block, parts, begin, after, size, collective_id):
    rows, cols = block.shape
    late = parts.shape[0] - begin
    anywhere = pl.BlockSpec(memory_space=pl.ANY)
    sem = pltpu.SemaphoreType.DMA
    late_shape = (late, *parts.shape[1:]) if late else (8, LANES)
    return pl.pallas_call(
        functools.partial(spread_kernel, size, begin),
        out_shape=(jax.ShapeDtypeStruct((size, rows, cols), block.dtype), jax.ShapeDtypeStruct(late_shape, parts.dtype)),
        in_specs=[anywhere, anywhere, anywhere],
        out_specs=(anywhere, anywhere),
        scratch_shapes=[
            pltpu.VMEM((rows, cols), block.dtype), sem, sem, sem((max(late, 1),)),
            sem((4,)), sem((4, PLACES)), sem((4,)), sem((4, PLACES)), sem, sem, sem((max(late, 1),)), sem((max(late, 1),)),
        ],
        compiler_params=pltpu.CompilerParams(collective_id=collective_id, has_side_effects=True),
        cost_estimate=pl.CostEstimate(
            flops=100_000_000_000 if late else 30_000_000_000, bytes_accessed=8 * size * rows * cols, transcendentals=0),
        name="spread",
    )(block, parts, after)


def token_kernel(head_dim, chunk, early_ref, late_ref, wq_ref, wo_ref, x_ref, dy_ref, gain_ref, bout_ref,
                 y_ref, gx_ref, tiles_ref, dn_acc, y_acc, sums):
    n = pl.program_id(0)
    step = wq_ref.shape[0]

    @pl.when(n == 0)
    def _():
        tiles_ref[...] = jnp.zeros_like(tiles_ref)

    dn_term = y_term = 0.0
    for h in range(step):
        parts = []
        for pair in [early_ref[h]] + [late_ref[b, h] for b in range(late_ref.shape[0])]:
            parts += [pair[:, :4 * head_dim], pair[:, 4 * head_dim:]]
        parts = jnp.concatenate(parts, axis=0)
        dqkv = parts[:, :3 * head_dim]
        total = jnp.sum(dqkv.astype(jnp.float32), axis=0, keepdims=True)
        for c in range(3):
            tiles_ref[n * step + h, 3 + c:4 + c, 0:head_dim] = total[:, c * head_dim:(c + 1) * head_dim]
        dn_term += dot(dqkv, wq_ref[h], 1, 0)
        y_term += dot(parts[:, 3 * head_dim:], wo_ref[h], 1, 0)

    @pl.when(n == 0)
    def _():
        dn_acc[...] = dn_term
        y_acc[...] = y_term

    @pl.when(n > 0)
    def _():
        dn_acc[...] += dn_term
        y_acc[...] += y_term

    @pl.when(n == pl.num_programs(0) - 1)
    def _():
        sums[...] = jnp.zeros_like(sums)
        gain = gain_ref[...]
        bout = bout_ref[...]

        def body(c, carry):
            at = pl.ds(pl.multiple_of(c * chunk, chunk), chunk)
            x = x_ref[at, :].astype(jnp.float32)
            dy = dy_ref[at, :].astype(jnp.float32)
            centered = x - jnp.mean(x, axis=-1, keepdims=True)
            inv_std = lax.rsqrt(jnp.mean(centered * centered, axis=-1, keepdims=True) + NORM_EPS)
            x_hat = centered * inv_std
            d_norm = dn_acc[at, :]
            d_hat = d_norm * gain
            d_mean = jnp.mean(d_hat, axis=-1, keepdims=True)
            d_proj = jnp.mean(d_hat * x_hat, axis=-1, keepdims=True)
            gx_ref[at, :] = (dy + inv_std * (d_hat - d_mean - x_hat * d_proj)).astype(jnp.bfloat16)
            y_ref[at, :] = (x + y_acc[at, :] + bout).astype(jnp.bfloat16)
            sums[0:1, :] += jnp.sum(d_norm * x_hat, axis=0, keepdims=True)
            sums[1:2, :] += jnp.sum(d_norm, axis=0, keepdims=True)
            sums[2:3, :] += jnp.sum(dy, axis=0, keepdims=True)
            return carry

        lax.fori_loop(0, x_ref.shape[0] // chunk, body, 0)
        for j in range(tiles_ref.shape[0]):
            tiles_ref[j, 0:3, 0:head_dim] = sums[0:3, j * head_dim:(j + 1) * head_dim]


def token_side(early, late, wq, wo, x, dy, gain, bout, head_dim):
    heads = early.shape[0]
    tokens, hidden = x.shape
    step = 4
    whole = lambda n: (0, 0)
    per_head = lambda n: (n, 0, 0)
    return pl.pallas_call(
        functools.partial(token_kernel, head_dim, 16),
        grid=(heads // step,),
        out_shape=(
            jax.ShapeDtypeStruct((tokens, hidden), jnp.bfloat16),
            jax.ShapeDtypeStruct((tokens, hidden), jnp.bfloat16),
            jax.ShapeDtypeStruct((heads, 8, LANES), jnp.float32),
        ),
        in_specs=[
            pl.BlockSpec((step, *early.shape[1:]), per_head),
            pl.BlockSpec((late.shape[0], step, *late.shape[2:]), lambda n: (0, n, 0, 0)),
            pl.BlockSpec((step, 3 * head_dim, hidden), per_head),
            pl.BlockSpec((step, head_dim, hidden), per_head),
            pl.BlockSpec((tokens, hidden), whole),
            pl.BlockSpec((tokens, hidden), whole),
            pl.BlockSpec((1, hidden), whole),
            pl.BlockSpec((1, hidden), whole),
        ],
        out_specs=(
            pl.BlockSpec((tokens, hidden), whole),
            pl.BlockSpec((tokens, hidden), whole),
            pl.BlockSpec((heads, 8, LANES), lambda n: (0, 0, 0)),
        ),
        scratch_shapes=[pltpu.VMEM((tokens, hidden), jnp.float32)] * 2 + [pltpu.VMEM((8, hidden), jnp.float32)],
        compiler_params=pltpu.CompilerParams(vmem_limit_bytes=VMEM_LIMIT),
        cost_estimate=pl.CostEstimate(
            flops=2 * tokens * hidden * 4 * heads * head_dim, bytes_accessed=8 * hidden * heads * head_dim, transcendentals=0),
        name="token_side",
    )(early, late, wq, wo, x, dy, gain, bout)


def sums_kernel(size, tiles_ref, all_ref, come, total, own_sem, send_a, recv_a, send_b, recv_b):
    me = lax.axis_index("sp")
    greet_all(me, size)
    own = pltpu.make_async_copy(tiles_ref.at[me], come.at[me], own_sem)
    own.start()
    deal = Direct(me, size, lambda j: tiles_ref.at[j], lambda j: come.at[j], come, send_a, recv_a)
    deal.start()
    own.wait()
    deal.wait_recv()
    total[...] = jnp.sum(come[...], axis=0)
    all_ref[me] = total[...]
    collect = Direct(me, size, lambda j: total, lambda j: all_ref.at[j], all_ref, send_b, recv_b)
    collect.start()
    deal.wait_send()
    collect.wait_recv()
    collect.wait_send()


def sum_tiles(tiles, size, collective_id):
    sem = pltpu.SemaphoreType.DMA
    return pl.pallas_call(
        functools.partial(sums_kernel, size),
        out_shape=jax.ShapeDtypeStruct(tiles.shape, tiles.dtype),
        in_specs=[pl.BlockSpec(memory_space=pl.ANY)],
        out_specs=pl.BlockSpec(memory_space=pltpu.VMEM),
        scratch_shapes=[pltpu.VMEM(tiles.shape, tiles.dtype), pltpu.VMEM(tiles.shape[1:], tiles.dtype),
                        sem, sem, sem, sem, sem],
        compiler_params=pltpu.CompilerParams(collective_id=collective_id, has_side_effects=True),
        cost_estimate=pl.CostEstimate(flops=10_000_000_000, bytes_accessed=2 * 4 * tiles.size, transcendentals=0),
        name="sum_tiles",
    )(tiles)


def settle_kernel(block, depth, ahead, first, src_ref, *refs):
    dst_ref, buf, read_sems, write_sems = refs[-4:]
    per = src_ref.shape[1] // block
    count = src_ref.shape[0] * per

    def slab(ref, i, start):
        return ref.at[i // per, pl.ds(pl.multiple_of(start + lax.rem(i, per) * block, 8), block)]

    def read(i):
        return pltpu.make_async_copy(slab(src_ref, i, 0), buf.at[lax.rem(i, depth)], read_sems.at[lax.rem(i, depth)])

    def write(i):
        return pltpu.make_async_copy(buf.at[lax.rem(i, depth)], slab(dst_ref, i, first), write_sems.at[lax.rem(i, depth)])

    def step(i, carry):
        @pl.when(jnp.logical_and(i >= depth, i < count))
        def _():
            write(i - depth).wait()

        @pl.when(i < count)
        def _():
            read(i).start()

        @pl.when(i >= ahead)
        def _():
            read(i - ahead).wait()
            write(i - ahead).start()

        return carry

    lax.fori_loop(0, count + ahead, step, 0)

    def drain(i, carry):
        write(i).wait()
        return carry

    lax.fori_loop(max(0, count - depth), count, drain, 0)


def settle(x, first, total, block, into=None, after=()):
    depth, ahead = 12, 6
    count, _, cols = x.shape
    sem = pltpu.SemaphoreType.DMA((depth,))
    old = [] if into is None else [into]
    return pl.pallas_call(
        functools.partial(settle_kernel, block, depth, ahead, first),
        out_shape=jax.ShapeDtypeStruct((count, total, cols), x.dtype),
        in_specs=[pl.BlockSpec(memory_space=pl.ANY)] * (1 + len(old) + len(after)),
        out_specs=pl.BlockSpec(memory_space=pl.ANY),
        scratch_shapes=[pltpu.VMEM((depth, block, cols), x.dtype), sem, sem],
        input_output_aliases={1: 0} if old else {},
        compiler_params=pltpu.CompilerParams(vmem_limit_bytes=VMEM_LIMIT),
        cost_estimate=pl.CostEstimate(flops=10_000_000_000, bytes_accessed=8 * x.size, transcendentals=0),
        name="settle",
    )(x, *old, *after)


def solution(mesh):
    size = mesh.shape["sp"]

    def block_fn(x_blk, pos_blk, keep_blk, ln_gain, ln_bias, w_qkv, b_qkv, w_out, b_out, dy_blk):
        batch, tok, hidden = x_blk.shape
        heads, head_dim = w_qkv.shape[1], w_qkv.shape[3]
        tokens = batch * tok
        wq = jnp.transpose(w_qkv, (1, 2, 3, 0)).reshape(heads, 3 * head_dim, hidden)
        wo = w_out.reshape(heads, head_dim, hidden)
        row = lambda a: a.reshape(1, hidden)

        def gather(a):
            return lax.all_gather(a, "sp", axis=0, tiled=True).reshape(heads, a.shape[0], hidden)

        _, parts, early, grad_a, grad_b, grad_c, grad_out = block_call(
            x_blk, dy_blk, ln_gain, ln_bias, pos_blk, keep_blk, wq, jnp.transpose(b_qkv, (1, 0, 2)), wo, size, 256, 0)

        all_out, late = spread(grad_out, parts, 1, grad_a, size, 1)
        y, grad_x, tiles = token_side(
            early, late, wq, wo, x_blk.reshape(tokens, hidden), dy_blk.reshape(tokens, hidden), row(ln_gain), row(b_out), head_dim)
        totals = sum_tiles(tiles, size, 2)
        grad_wo = settle(all_out, 0, head_dim, head_dim, after=(totals,))

        rows = 3 * head_dim
        first, second, own = split_rows(rows)
        all_c, _ = spread(grad_c, parts, batch, grad_wo, size, 3)
        grad_wq = settle(gather(grad_a), 0, rows, first // 2, after=(all_c,))
        grad_wq = settle(all_c, first + second, rows, own, grad_wq)
        grad_wq = settle(gather(grad_b), first, rows, second, grad_wq)
        totals = totals[:, :, :head_dim]
        grad_wq = jnp.transpose(grad_wq.reshape(heads, 3, head_dim, hidden), (3, 0, 1, 2))
        return (y.reshape(x_blk.shape), grad_x.reshape(x_blk.shape), grad_wq, totals[:, 3:6],
                grad_wo.reshape(heads * head_dim, hidden), totals[:, 2].reshape(-1), totals[:, 0].reshape(-1), totals[:, 1].reshape(-1))

    act_spec = P("dp", "sp", None)
    tok_spec = P("dp", "sp")
    in_specs = (act_spec, tok_spec, tok_spec, P(), P(), P(), P(), P(), P(), act_spec)
    out_specs = (act_spec, act_spec, P("dp", None, None, None), P("dp", None, None), P("dp", None), P("dp"), P("dp"), P("dp"))
    return jax.shard_map(block_fn, mesh=mesh, in_specs=in_specs, out_specs=out_specs, check_vma=False)
```

```python
import functools
import math

import jax
import jax.numpy as jnp
from jax import lax
from jax.experimental import pallas as pl
from jax.experimental.pallas import tpu as pltpu
from jax.sharding import PartitionSpec as P

NORM_EPS = 1e-5
MASK_FILL = -1e30
LANES = 128
LOG2E = 1.4426950408889634
MESH = pl.DeviceIdType.MESH
VMEM_LIMIT = 61 * 1024 * 1024


def dot(a, b, ca, cb):
    return lax.dot_general(a, b, (((ca,), (cb,)), ((), ())), preferred_element_type=jnp.float32)


def greet_all(me, size, meanwhile=lambda: None):
    barrier = pltpu.get_barrier_semaphore()

    def greet(d, carry):
        pl.semaphore_signal(barrier, inc=1, device_id={"sp": lax.rem(me + d, size)}, device_id_type=MESH)
        return carry

    lax.fori_loop(1, size, greet, 0)
    meanwhile()
    pl.semaphore_wait(barrier, size - 1)


class Direct:
    def __init__(self, me, size, src, dst, whole, send_sem, recv_sem):
        self.me, self.size, self.src, self.dst, self.whole, self.send_sem, self.recv_sem = me, size, src, dst, whole, send_sem, recv_sem

    def start(self):
        def body(d, carry):
            peer = lax.rem(self.me + d, self.size)
            pltpu.make_async_remote_copy(
                src_ref=self.src(peer), dst_ref=self.dst(self.me), send_sem=self.send_sem, recv_sem=self.recv_sem,
                device_id={"sp": peer}, device_id_type=MESH).start()
            return carry

        lax.fori_loop(1, self.size, body, 0)

    def total(self):
        ref = self.whole.at[pl.ds(0, self.size - 1)]
        return pltpu.make_async_remote_copy(
            src_ref=ref, dst_ref=ref, send_sem=self.send_sem, recv_sem=self.recv_sem,
            device_id={"sp": self.me}, device_id_type=MESH)

    def wait_recv(self):
        self.total().wait_recv()

    def wait_send(self):
        self.total().wait_send()


FIRST_OF = (2, 3, 0, 1)
CYCLE = (("P", 0), ("Q", 0, 0), ("Q", 3, 2), ("P", 1), ("Q", 0, 1), ("Q", 1, 0), ("Q", 2, 0), ("P", 2), ("Q", 1, 1),
         ("Q", 2, 1), ("Q", 3, 0), ("Q", 1, 2), ("Q", 2, 2), ("Q", 3, 1), ("Q", 0, 2))
LATE = 2
LAG = 3
COLOURS = 4
READY = 6
STEP_OF = ((1, 0), (-1, 0), (0, 1), (0, -1))
PLACES = len(CYCLE)


class Torus:
    def __init__(self, size):
        self.side = math.isqrt(size // 2)
        self.me = lax.axis_index("sp")
        self.core = lax.rem(self.me, 2)
        chip = self.me // 2
        self.cx, self.cy = lax.rem(chip, self.side), chip // self.side
        self.flip = 1 - 2 * self.core
        self.sibling = self.me + self.flip

    def device_at(self, dx, dy):
        side = self.side
        return (lax.rem(self.cy + dy + side, side) * side + lax.rem(self.cx + dx + side, side)) * 2 + self.core

    def neighbour(self, link):
        return self.device_at(*STEP_OF[link])

    def chunk(self, link, place, ahead):
        what = CYCLE[place]
        if what[0] == "P":
            first, n, m = link, what[1] + ahead, 0
        else:
            first, n, m = FIRST_OF[link], what[2] + ahead, what[1]
        dx = -STEP_OF[link][0] * n - STEP_OF[first][0] * m
        dy = -STEP_OF[link][1] * n - STEP_OF[first][1] * m
        return self.device_at(dx, dy), first


def is_own(place):
    return CYCLE[place] in (("P", 0), ("Q", 0, 0))


def block_kernel(size, dims, x_ref, dy_ref, gain_ref, shift_ref, pos_ref, keep_ref, wq_ref, bias_ref, wo_ref,
                 gat_ref, parts_ref, partstok_ref, gwa_ref, gwb_ref, gwc_ref, gwd_ref, gwo_ref,
                 xin, stage, wbuf, wobuf, metatile, metabuf, rowbuf, sbuf, qkvb, dob, dk_acc, dv_acc, dq_all, o_all, d_all, pbuf,
                 load_sems, own_sems, piece_sems, parts_sem, ici_send, ici_recv, d2d_send, d2d_recv, own_send, own_recv,
                 meta_send, meta_recv, part_send, part_recv):
    batch, tok, head_dim, pad_dim, hidden, q_block = dims
    seq_len = size * tok
    torus = Torus(size)
    me, flip, sibling, side = torus.me, torus.flip, torus.sibling, torus.side
    places = PLACES
    scale = head_dim ** -0.5
    heads = wo_ref.shape[0]
    slope = jnp.exp2(jnp.full((1, 1), -8.0 / heads, jnp.float32) * (me + 1).astype(jnp.float32))

    def send(b, link, place):
        block, colour = torus.chunk(link, place, 0)
        dst = gat_ref.at[b, block, colour]
        return pltpu.make_async_remote_copy(
            src_ref=stage.at[b, colour] if is_own(place) else dst, dst_ref=dst,
            send_sem=ici_send.at[link], recv_sem=ici_recv.at[link, place],
            device_id={"sp": torus.neighbour(link)}, device_id_type=MESH)

    def arrival(b, link, place):
        block, colour = torus.chunk(link, place, 1)
        ref = gat_ref.at[b, block, colour]
        return pltpu.make_async_remote_copy(
            src_ref=ref, dst_ref=ref, send_sem=ici_send.at[link], recv_sem=ici_recv.at[link, place],
            device_id={"sp": me}, device_id_type=MESH)

    def share(b, link, place, shift):
        block, colour = torus.chunk(link, place, 1)
        ref = gat_ref.at[b, block + shift, colour]
        return pltpu.make_async_remote_copy(
            src_ref=ref, dst_ref=ref, send_sem=d2d_send.at[link], recv_sem=d2d_recv.at[link, place],
            device_id={"sp": sibling}, device_id_type=MESH)

    def share_own(b, block):
        return pltpu.make_async_remote_copy(
            src_ref=stage.at[b], dst_ref=gat_ref.at[b, block], send_sem=own_send.at[b], recv_sem=own_recv.at[b],
            device_id={"sp": sibling}, device_id_type=MESH)

    def keep_own(b):
        return pltpu.make_async_copy(stage.at[b], gat_ref.at[b, me], own_sems.at[b])

    load_x = pltpu.make_async_copy(x_ref, xin, load_sems.at[0])
    load_dy = pltpu.make_async_copy(dy_ref, stage.at[:, :, 0], load_sems.at[1])
    load_wq = pltpu.make_async_copy(wq_ref.at[me], wbuf, load_sems.at[2])
    load_wo = pltpu.make_async_copy(wo_ref.at[me], wobuf, load_sems.at[3])
    for load in (load_x, load_dy, load_wq, load_wo):
        load.start()
    meta = Direct(me, size, lambda j: metatile, lambda j: metabuf.at[j], metabuf, meta_send, meta_recv)
    trade = Direct(me, size, lambda j: parts_ref.at[0, j], lambda j: partstok_ref.at[j], partstok_ref, part_send, part_recv)
    own_parts = pltpu.make_async_copy(parts_ref.at[0, me], partstok_ref.at[me], load_sems.at[4])

    def prepare():
        metatile[...] = jnp.zeros_like(metatile)
        metatile[0:batch, 0:tok] = pos_ref[...]
        metatile[batch:2 * batch, 0:tok] = keep_ref[...]
        metabuf[me] = metatile[...]
        load_x.wait()

        gain, shift = gain_ref[...].reshape(1, 1, hidden), shift_ref[...].reshape(1, 1, hidden)

        def normalise(b, carry):
            x = xin[b].astype(jnp.float32)
            centered = x - jnp.mean(x, axis=-1, keepdims=True)
            inv_std = lax.rsqrt(jnp.mean(centered * centered, axis=-1, keepdims=True) + NORM_EPS)
            stage[b, :, 1] = (centered * inv_std * gain + shift).astype(jnp.bfloat16)
            return carry

        lax.fori_loop(0, batch, normalise, 0)
        load_dy.wait()

    greet_all(me, size, prepare)

    pieces = sbuf.shape[0]
    chip_rows = 2 * tok

    def chip_of(p, e):
        return torus.device_at(lax.rem(p + 1 + e, side), e) // 2

    def rows_at(p, e):
        return pl.ds(pl.multiple_of(chip_of(p, e) * chip_rows, chip_rows), chip_rows)

    def load_piece(b, p):
        return [pltpu.make_async_copy(gat_ref.at[b, pl.ds(chip_of(p, e) * 2, 2)], sbuf.at[p, e], piece_sems.at[p, e]) for e in range(side)]

    def start_piece(b, p):
        for load in load_piece(b, p):
            load.start()

    def rows_of(p, which, at=slice(None)):
        return sbuf[p, :, :, :, which, :, at].reshape(side * chip_rows, -1)

    def each(lo, hi, use):
        def body(p, carry):
            use(p)
            return carry

        lax.fori_loop(lo, hi, body, 0)

    def pad_lanes(a):
        return jnp.concatenate([a, jnp.zeros((a.shape[0], pad_dim - head_dim), a.dtype)], axis=1)

    def project(b, p):
        for load in load_piece(b, p):
            load.wait()
        bias = jnp.concatenate([bias_ref[c, pl.ds(me, 1), :] for c in range(3)], axis=1)
        r = (dot(rows_of(p, 1), wbuf[...], 1, 1) + bias).astype(jnp.bfloat16)
        d = pad_lanes(dot(rows_of(p, 0), wobuf[...], 1, 1).astype(jnp.bfloat16))
        q, k, v = (pad_lanes(r[:, c * head_dim:(c + 1) * head_dim]) for c in range(3))
        for e in range(side):
            mine = slice(e * chip_rows, (e + 1) * chip_rows)
            at = rows_at(p, e)
            for c, part in enumerate((q, k, v)):
                qkvb[at, c * pad_dim:(c + 1) * pad_dim] = part[mine]
            dob[at, :] = d[mine]

    def attend(b, i):
        span = (i + 1) * q_block
        mine = slice(i * q_block, span)
        if i == 0:
            dk_acc[...] = jnp.zeros_like(dk_acc)
            dv_acc[...] = jnp.zeros_like(dv_acc)
        q, k, v = qkvb[mine, :pad_dim], qkvb[:span, pad_dim:2 * pad_dim], qkvb[:span, 2 * pad_dim:]
        do = dob[mine, :]
        pos = rowbuf[pl.ds(b, 1), :span]
        keep = rowbuf[pl.ds(b + batch, 1), :span]
        bias = jnp.where(keep > 0, (-slope * LOG2E) * (pos[:, span - 1:] - pos).astype(jnp.float32), MASK_FILL)
        scores = dot(q, k, 1, 1) * (scale * LOG2E) + bias
        row_id = lax.broadcasted_iota(jnp.int32, (q_block, q_block), 0)
        col_id = lax.broadcasted_iota(jnp.int32, (q_block, q_block), 1)
        corner = jnp.where(col_id <= row_id, scores[:, span - q_block:], MASK_FILL)
        scores = jnp.concatenate([scores[:, :span - q_block], corner], axis=1) if i else corner
        expo = jnp.exp2(scores - jnp.max(scores, axis=-1, keepdims=True))
        prob = expo * (1.0 / jnp.sum(expo, axis=-1, keepdims=True))
        prob_lo = prob.astype(jnp.bfloat16)
        o = dot(prob_lo, v, 1, 0).astype(jnp.bfloat16)
        row_dot = jnp.sum(do.astype(jnp.float32) * o.astype(jnp.float32), axis=-1, keepdims=True)
        ds_lo = (prob * (dot(do, v, 1, 1) - row_dot)).astype(jnp.bfloat16)
        o_all[mine, :] = o
        dq_all[mine, :] = (dot(ds_lo, k, 1, 0) * scale).astype(jnp.bfloat16)
        dv_acc[:span, :] += dot(prob_lo, do, 0, 0)
        dk_acc[:span, :] += dot(ds_lo, q, 0, 0)

    def store_parts(b):
        return pltpu.make_async_copy(pbuf, parts_ref.at[b], parts_sem)

    def finish(b):
        dk = (dk_acc[...] * scale).astype(jnp.bfloat16)
        dv = dv_acc[...].astype(jnp.bfloat16)
        d_all[...] = jnp.concatenate([dq_all[:, :head_dim], dk[:, :head_dim], dv[:, :head_dim]], axis=1)
        whole = jnp.concatenate([d_all[...], o_all[:, :head_dim]], axis=1).reshape(size, tok, 4 * head_dim)
        pbuf[...] = jnp.concatenate([whole[:, :tok // 2], whole[:, tok // 2:]], axis=2)
        store_parts(b).start()

    width = min(1280, hidden)

    def gradient(p):
        d = jnp.concatenate([d_all[rows_at(p, e), :] for e in range(side)], axis=0)
        o = jnp.concatenate([o_all[rows_at(p, e), :] for e in range(side)], axis=0)[:, :head_dim]

        def columns(n, carry):
            at = pl.ds(pl.multiple_of(n * width, width), width)
            term = dot(d, rows_of(p, 1, at), 0, 0)
            row = 0
            for ref in (gwa_ref, gwb_ref, gwc_ref, gwd_ref):
                ref[:, at] += term[row:row + ref.shape[0]]
                row += ref.shape[0]
            gwo_ref[:, at] += dot(o, rows_of(p, 0, at), 0, 0)
            return carry

        lax.fori_loop(0, hidden // width, columns, 0)

    count = seq_len // q_block
    last = pieces - 1
    tasks = {(0, READY - 3): [lambda b: each(0, last, lambda p: start_piece(b, p))],
             (0, READY - 2): [lambda b: each(0, last - 1, lambda p: project(b, p))],
             (0, READY - 1): [lambda b: project(b, last - 1)],
             (0, READY): [lambda b: start_piece(b, last)],
             (0, READY + 1): [lambda b: project(b, last)],
             (0, READY + 7): [finish],
             (0, READY + 8): [lambda b: each(0, pieces // 2, gradient)],
             (1, 0): [lambda b: each(pieces // 2, pieces, gradient)],
             (1, 1): [lambda b: store_parts(b).wait()]}
    spot = (2, 2, 2, 3, 3, 4, 5, 6)
    for i in range(count):
        tasks.setdefault((0, READY + spot[i]), []).append(lambda b, i=i: attend(b, i))

    for ref in (gwa_ref, gwb_ref, gwc_ref, gwd_ref, gwo_ref):
        ref[...] = jnp.zeros_like(ref)

    def phase_of(i, place):
        return i - 1 if place == LATE else i

    def among(b):
        return jnp.logical_and(b >= 0, b < batch)

    def turn(i, carry):
        for place in range(places):
            came = (place - LAG) % places
            b_came = phase_of(i if place >= LAG else i - 1, came)

            @pl.when(among(b_came))
            def _():
                for link in range(4):
                    arrival(b_came, link, came).wait_recv()
                    share(b_came, link, came, 0).start()

            b_send = phase_of(i, place)

            @pl.when(among(b_send))
            def _():
                for link in range(4):
                    send(b_send, link, place).start()

            shared = (place - LAG - 1) % places
            b_shared = phase_of(i if place >= LAG + 1 else i - 1, shared)

            @pl.when(among(b_shared))
            def _():
                for link in range(4):
                    share(b_shared, link, shared, flip).wait_recv()

            if place == 1:
                @pl.when(i == 0)
                def _():
                    for b in range(batch):
                        share_own(b, me).start()
                        keep_own(b).start()
                    meta.start()

            if place == READY - 3:
                @pl.when(i == 1)
                def _():
                    for load in (load_wq, load_wo):
                        load.wait()
                    meta.wait_recv()
                    for j in range(size):
                        rowbuf[:, j * tok:(j + 1) * tok] = metabuf[j, :, :tok]
                    for b in range(batch):
                        share_own(b, sibling).wait_recv()
                        keep_own(b).wait()
                    meta.wait_send()
                    for b in range(batch):
                        share_own(b, me).wait_send()

            if place == READY:
                @pl.when(i == batch)
                def _():
                    own_parts.start()
                    trade.start()

            for later in (0, 1):
                if (later, place) in tasks:
                    @pl.when(among(i - 1 - later))
                    def _():
                        for task in tasks[later, place]:
                            task(i - 1 - later)
        return carry

    lax.fori_loop(0, batch + 2, turn, 0)
    own_parts.wait()
    trade.wait_recv()
    trade.wait_send()
    sent = gat_ref.at[:, pl.ds(0, places), 0]
    for link in range(4):
        for sem in (ici_send, d2d_send):
            pltpu.make_async_remote_copy(
                src_ref=sent, dst_ref=sent, send_sem=sem.at[link], recv_sem=ici_recv.at[link, 0],
                device_id={"sp": sibling}, device_id_type=MESH).wait_send()


def split_rows(rows):
    own, third = 8 * (rows // 34), 8 * max(1, rows // 80)
    first = (rows - own - third) // 2
    return first, first, third, own


def block_call(x, dy, gain, shift, pos, keep, wq, bias, wo, size, q_block, collective_id):
    batch, tok, hidden = x.shape
    rows = tok // COLOURS
    heads, head_dim, _ = wo.shape
    pad_dim = -(-head_dim // LANES) * LANES
    seq_len = size * tok
    side = math.isqrt(size // 2)
    places = PLACES
    anywhere = pl.BlockSpec(memory_space=pl.ANY)
    vmem = pl.BlockSpec(memory_space=pltpu.VMEM)
    sem = pltpu.SemaphoreType.DMA
    bf16, f32 = jnp.bfloat16, jnp.float32
    flops = batch * (6 * seq_len * seq_len * 256 + 4 * seq_len * 4 * head_dim * hidden) + 80_000_000_000
    cut = (batch, COLOURS, rows, hidden)
    return pl.pallas_call(
        functools.partial(block_kernel, size, (batch, tok, head_dim, pad_dim, hidden, min(q_block, seq_len))),
        out_shape=(
            jax.ShapeDtypeStruct((batch, size, COLOURS, 2, rows, hidden), bf16),
            jax.ShapeDtypeStruct((batch, size, tok // 2, 8 * head_dim), bf16),
            jax.ShapeDtypeStruct((size, tok // 2, 8 * head_dim), bf16),
            *(jax.ShapeDtypeStruct((n, hidden), f32) for n in split_rows(3 * head_dim)),
            jax.ShapeDtypeStruct((head_dim, hidden), f32),
        ),
        in_specs=[anywhere, anywhere, vmem, vmem, vmem, vmem, anywhere, vmem, anywhere],
        out_specs=(anywhere, anywhere, anywhere, vmem, vmem, vmem, vmem, vmem),
        scratch_shapes=[
            pltpu.VMEM(cut, bf16),
            pltpu.VMEM((batch, COLOURS, 2, rows, hidden), bf16),
            pltpu.VMEM((3 * head_dim, hidden), bf16),
            pltpu.VMEM((head_dim, hidden), bf16),
            pltpu.VMEM((8, LANES), jnp.int32),
            pltpu.VMEM((size, 8, LANES), jnp.int32),
            pltpu.VMEM((8, seq_len), jnp.int32),
            pltpu.VMEM((side, side, 2, COLOURS, 2, rows, hidden), bf16),
            pltpu.VMEM((seq_len, 3 * pad_dim), bf16),
            pltpu.VMEM((seq_len, pad_dim), bf16),
            pltpu.VMEM((seq_len, pad_dim), f32),
            pltpu.VMEM((seq_len, pad_dim), f32),
            pltpu.VMEM((seq_len, pad_dim), bf16),
            pltpu.VMEM((seq_len, pad_dim), bf16),
            pltpu.VMEM((seq_len, 3 * head_dim), bf16),
            pltpu.VMEM((size, tok // 2, 8 * head_dim), bf16),
            sem((5,)), sem((batch,)), sem((side, side)), sem,
            sem((4,)), sem((4, places)), sem((4,)), sem((4, places)), sem((batch,)), sem((batch,)), sem, sem, sem, sem,
        ],
        compiler_params=pltpu.CompilerParams(collective_id=collective_id, has_side_effects=True, vmem_limit_bytes=VMEM_LIMIT),
        cost_estimate=pl.CostEstimate(flops=flops, bytes_accessed=60_000_000, transcendentals=batch * seq_len * seq_len // 2),
        name="block",
    )(x.reshape(cut), dy.reshape(cut), gain, shift, pos, keep, wq, bias, wo)


class Spread:
    def __init__(self, size, own_ref, gat_ref, stage, sems):
        self.torus, self.size, self.gat_ref, self.stage = Torus(size), size, gat_ref, stage
        self.load_sem, self.keep_sem, self.ici_send, self.ici_recv, self.d2d_send, self.d2d_recv, self.own_send, self.own_recv = sems
        self.part = stage.shape[1] // COLOURS
        self.load = pltpu.make_async_copy(own_ref, stage, self.load_sem)
        self.keep = pltpu.make_async_copy(stage, gat_ref.at[self.torus.me], self.keep_sem)

    def columns(self, colour):
        return pl.ds(colour * self.part, self.part)

    def view(self, block, colour):
        return self.gat_ref.at[block, :, self.columns(colour)]

    def remote(self, src, dst, send_sem, recv_sem, device):
        return pltpu.make_async_remote_copy(
            src_ref=src, dst_ref=dst, send_sem=send_sem, recv_sem=recv_sem, device_id={"sp": device}, device_id_type=MESH)

    def send(self, link, place):
        block, colour = self.torus.chunk(link, place, 0)
        dst = self.view(block, colour)
        src = self.stage.at[:, self.columns(colour)] if is_own(place) else dst
        return self.remote(src, dst, self.ici_send.at[link], self.ici_recv.at[link, place], self.torus.neighbour(link))

    def arrival(self, link, place):
        ref = self.view(*self.torus.chunk(link, place, 1))
        return self.remote(ref, ref, self.ici_send.at[link], self.ici_recv.at[link, place], self.torus.me)

    def share(self, link, place, shift):
        block, colour = self.torus.chunk(link, place, 1)
        ref = self.view(block + shift, colour)
        return self.remote(ref, ref, self.d2d_send.at[link], self.d2d_recv.at[link, place], self.torus.sibling)

    def share_own(self, block):
        return self.remote(self.stage, self.gat_ref.at[block], self.own_send, self.own_recv, self.torus.sibling)

    STEPS = PLACES + LATE + LAG + 2

    def step(self, g):
        def place_of(g):
            place = g % PLACES
            return place if g >= 0 and g // PLACES == (1 if place == LATE else 0) else None

        came, now, shared = place_of(g - LAG), place_of(g), place_of(g - LAG - 1)
        for link in range(4):
            if came is not None:
                self.arrival(link, came).wait_recv()
                self.share(link, came, 0).start()
        for link in range(4):
            if now is not None:
                self.send(link, now).start()
        for link in range(4):
            if shared is not None:
                self.share(link, shared, self.torus.flip).wait_recv()
        if g == 1:
            self.share_own(self.torus.me).start()
            self.keep.start()

    def close(self):
        self.share_own(self.torus.sibling).wait_recv()
        self.keep.wait()
        self.share_own(self.torus.me).wait_send()
        sent = self.gat_ref.at[pl.ds(0, PLACES), :, pl.ds(0, self.part)]
        for link in range(4):
            for sem in (self.ici_send, self.d2d_send):
                self.remote(sent, sent, sem.at[link], self.ici_recv.at[link, 0], self.torus.sibling).wait_send()

    @staticmethod
    def scratch(rows, cols, dtype):
        sem = pltpu.SemaphoreType.DMA
        return [pltpu.VMEM((rows, cols), dtype), sem, sem, sem((4,)), sem((4, PLACES)), sem((4,)), sem((4, PLACES)), sem, sem]


def spread_kernel(size, own_ref, after_ref, gat_ref, stage, *sems):
    spread = Spread(size, own_ref, gat_ref, stage, sems)
    spread.load.start()
    greet_all(spread.torus.me, size)
    spread.load.wait()
    for g in range(Spread.STEPS):
        spread.step(g)
    spread.close()


def spread_rows(block, after, size, collective_id):
    rows, cols = block.shape
    anywhere = pl.BlockSpec(memory_space=pl.ANY)
    return pl.pallas_call(
        functools.partial(spread_kernel, size),
        out_shape=jax.ShapeDtypeStruct((size, rows, cols), block.dtype),
        in_specs=[anywhere, anywhere],
        out_specs=anywhere,
        scratch_shapes=Spread.scratch(rows, cols, block.dtype),
        compiler_params=pltpu.CompilerParams(collective_id=collective_id, has_side_effects=True),
        cost_estimate=pl.CostEstimate(flops=50_000_000_000, bytes_accessed=8 * size * rows * cols, transcendentals=0),
        name="spread",
    )(block, after)


TOKEN_AT = 8
TOKEN_STEPS = 8


def token_kernel(size, head_dim, chunk, own_ref, parts_ref, early_ref, wq_ref, wo_ref, x_ref, dy_ref, gain_ref, bout_ref,
                 gat_ref, late_ref, y_ref, gx_ref, totals_ref,
                 stage, load_sem, keep_sem, ici_send, ici_recv, d2d_send, d2d_recv, own_send, own_recv,
                 wqbuf, wobuf, pbuf, dn_acc, y_acc, sums, tiles, come, total,
                 part_send, part_recv, own_part_sems, wq_sems, wo_sems, p_sems, deal_send, deal_recv, collect_send, collect_recv):
    spread = Spread(size, own_ref, gat_ref, stage,
                    (load_sem, keep_sem, ici_send, ici_recv, d2d_send, d2d_recv, own_send, own_recv))
    me = spread.torus.me
    late = late_ref.shape[0]
    heads, hidden = wq_ref.shape[0], wq_ref.shape[2]
    per = heads // TOKEN_STEPS
    trades, own_parts = [], []
    for n in range(late):
        b = parts_ref.shape[0] - late + n
        trades.append(Direct(me, size, lambda j, b=b: parts_ref.at[b, j], lambda j, n=n: late_ref.at[n, j], late_ref.at[n],
                             part_send.at[n], part_recv.at[n]))
        own_parts.append(pltpu.make_async_copy(parts_ref.at[b, me], late_ref.at[n, me], own_part_sems.at[n]))
    deal = Direct(me, size, lambda j: tiles.at[j], lambda j: come.at[j], come, deal_send, deal_recv)
    collect = Direct(me, size, lambda j: total, lambda j: totals_ref.at[j], totals_ref, collect_send, collect_recv)

    def weights(m):
        at, slot = pl.ds(m * per, per), m % 2
        return (pltpu.make_async_copy(wq_ref.at[at], wqbuf.at[slot], wq_sems.at[slot]),
                pltpu.make_async_copy(wo_ref.at[at], wobuf.at[slot], wo_sems.at[slot]))

    def rows(m):
        at, slot = pl.ds(m * per, per), m % 2
        return [pltpu.make_async_copy(early_ref.at[at], pbuf.at[slot, 0], p_sems.at[slot, 0])] + [
            pltpu.make_async_copy(late_ref.at[n, at], pbuf.at[slot, 1 + n], p_sems.at[slot, 1 + n]) for n in range(late)]

    spread.load.start()
    for copy in weights(0):
        copy.start()
    dn_acc[...] = jnp.zeros_like(dn_acc)
    y_acc[...] = jnp.zeros_like(y_acc)
    sums[...] = jnp.zeros_like(sums)
    tiles[...] = jnp.zeros_like(tiles)
    width = hidden // 4

    def heads_step(m):
        slot = m % 2
        for copy in (*weights(m), *rows(m)):
            copy.wait()
        if m + 1 < TOKEN_STEPS:
            for copy in (*weights(m + 1), *rows(m + 1)):
                copy.start()

        def pair(i, carry):
            ds, os = [], []
            for h in range(2):
                parts = []
                for n in range(1 + late):
                    both = pbuf[slot, n, i * 2 + h]
                    parts += [both[:, :4 * head_dim], both[:, 4 * head_dim:]]
                parts = jnp.concatenate(parts, axis=0)
                ds.append(parts[:, :3 * head_dim])
                os.append(parts[:, 3 * head_dim:])
                added = jnp.sum(ds[h].astype(jnp.float32), axis=0, keepdims=True)
                for c in range(3):
                    tiles[m * per + i * 2 + h, 3 + c:4 + c, 0:head_dim] = added[:, c * head_dim:(c + 1) * head_dim]

            def columns(n, carry):
                at = pl.ds(pl.multiple_of(n * width, width), width)
                dn_acc[:, at] += dot(ds[0], wqbuf[slot, i * 2, :, at], 1, 0) + dot(ds[1], wqbuf[slot, i * 2 + 1, :, at], 1, 0)
                y_acc[:, at] += dot(os[0], wobuf[slot, i * 2, :, at], 1, 0) + dot(os[1], wobuf[slot, i * 2 + 1, :, at], 1, 0)
                return carry

            lax.fori_loop(0, 4, columns, 0)
            return carry

        lax.fori_loop(0, per // 2, pair, 0)

    def norm_step(half):
        gain = gain_ref[...].reshape(1, hidden)
        bout = bout_ref[...].reshape(1, hidden)
        count = x_ref.shape[0] // chunk

        def body(c, carry):
            at = pl.ds(pl.multiple_of(c * chunk, chunk), chunk)
            x = x_ref[at, :].astype(jnp.float32)
            dy = dy_ref[at, :].astype(jnp.float32)
            centered = x - jnp.mean(x, axis=-1, keepdims=True)
            inv_std = lax.rsqrt(jnp.mean(centered * centered, axis=-1, keepdims=True) + NORM_EPS)
            x_hat = centered * inv_std
            d_norm = dn_acc[at, :]
            d_hat = d_norm * gain
            d_mean = jnp.mean(d_hat, axis=-1, keepdims=True)
            d_proj = jnp.mean(d_hat * x_hat, axis=-1, keepdims=True)
            gx_ref[at, :] = (dy + inv_std * (d_hat - d_mean - x_hat * d_proj)).astype(jnp.bfloat16)
            y_ref[at, :] = (x + y_acc[at, :] + bout).astype(jnp.bfloat16)
            sums[0:1, :] += jnp.sum(d_norm * x_hat, axis=0, keepdims=True)
            sums[1:2, :] += jnp.sum(d_norm, axis=0, keepdims=True)
            sums[2:3, :] += jnp.sum(dy, axis=0, keepdims=True)
            return carry

        lax.fori_loop(half * count // 2, (half + 1) * count // 2, body, 0)

    greet_all(me, size)
    spread.load.wait()
    for g in range(Spread.STEPS):
        spread.step(g)
        m = g - TOKEN_AT
        if g == 1:
            for copy in trades + own_parts:
                copy.start()
        if m == 0:
            for copy in own_parts:
                copy.wait()
            for trade in trades:
                trade.wait_recv()
            for copy in rows(0):
                copy.start()
        if 0 <= m < TOKEN_STEPS:
            heads_step(m)
        elif m in (TOKEN_STEPS, TOKEN_STEPS + 1):
            norm_step(m - TOKEN_STEPS)
        elif m == TOKEN_STEPS + 2:
            for j in range(size):
                tiles[j, 0:3, 0:head_dim] = sums[0:3, j * head_dim:(j + 1) * head_dim]
            come[me] = tiles[me]
        elif m == TOKEN_STEPS + 3:
            deal.start()
        elif m == TOKEN_STEPS + 5:
            deal.wait_recv()
            total[...] = jnp.sum(come[...], axis=0)
            totals_ref[me] = total[...]
            collect.start()
    spread.close()
    for trade in trades:
        trade.wait_send()
    deal.wait_send()
    collect.wait_recv()
    collect.wait_send()


def token_side(block, parts, early, wq, wo, x, dy, gain, bout, size, collective_id):
    rows, cols = block.shape
    late = parts.shape[0] - 1
    heads, head_dim, hidden = wo.shape
    tokens = x.shape[0]
    per = heads // TOKEN_STEPS
    anywhere = pl.BlockSpec(memory_space=pl.ANY)
    vmem = pl.BlockSpec(memory_space=pltpu.VMEM)
    sem = pltpu.SemaphoreType.DMA
    bf16, f32 = jnp.bfloat16, jnp.float32
    return pl.pallas_call(
        functools.partial(token_kernel, size, head_dim, 16),
        out_shape=(
            jax.ShapeDtypeStruct((size, rows, cols), block.dtype),
            jax.ShapeDtypeStruct((late, *parts.shape[1:]), parts.dtype),
            jax.ShapeDtypeStruct((tokens, hidden), bf16),
            jax.ShapeDtypeStruct((tokens, hidden), bf16),
            jax.ShapeDtypeStruct((size, 8, LANES), f32),
        ),
        in_specs=[anywhere] * 5 + [vmem] * 4,
        out_specs=(anywhere, anywhere, vmem, vmem, vmem),
        scratch_shapes=Spread.scratch(rows, cols, block.dtype) + [
            pltpu.VMEM((2, per, 3 * head_dim, hidden), bf16),
            pltpu.VMEM((2, per, head_dim, hidden), bf16),
            pltpu.VMEM((2, 1 + late, per, *parts.shape[2:]), bf16),
            pltpu.VMEM((tokens, hidden), f32),
            pltpu.VMEM((tokens, hidden), f32),
            pltpu.VMEM((8, hidden), f32),
            pltpu.VMEM((size, 8, LANES), f32),
            pltpu.VMEM((size, 8, LANES), f32),
            pltpu.VMEM((8, LANES), f32),
            sem((late,)), sem((late,)), sem((late,)), sem((2,)), sem((2,)), sem((2, 1 + late)), sem, sem, sem, sem,
        ],
        compiler_params=pltpu.CompilerParams(collective_id=collective_id, has_side_effects=True, vmem_limit_bytes=VMEM_LIMIT),
        cost_estimate=pl.CostEstimate(flops=120_000_000_000, bytes_accessed=8 * size * rows * cols, transcendentals=0),
        name="token_side",
    )(block, parts, early, wq, wo, x, dy, gain, bout)


def hand_kernel(y_ref, gx_ref, y_out, gx_out):
    y_out[...] = y_ref[...]
    gx_out[...] = gx_ref[...]


def hand_over(y, gx):
    spec = pl.BlockSpec((y.shape[0] // 4, y.shape[1]), lambda i: (i, 0))
    return pl.pallas_call(
        hand_kernel, grid=(4,), out_shape=(jax.ShapeDtypeStruct(y.shape, y.dtype),) * 2, in_specs=[spec] * 2, out_specs=(spec,) * 2,
        cost_estimate=pl.CostEstimate(flops=1_000_000_000, bytes_accessed=8 * y.size, transcendentals=0), name="hand_over")(y, gx)


def settle_kernel(block, depth, ahead, first, src_ref, *refs):
    dst_ref, buf, read_sems, write_sems = refs[-4:]
    per = src_ref.shape[1] // block
    count = src_ref.shape[0] * per

    def slab(ref, i, start):
        return ref.at[i // per, pl.ds(pl.multiple_of(start + lax.rem(i, per) * block, 8), block)]

    def read(i):
        return pltpu.make_async_copy(slab(src_ref, i, 0), buf.at[lax.rem(i, depth)], read_sems.at[lax.rem(i, depth)])

    def write(i):
        return pltpu.make_async_copy(buf.at[lax.rem(i, depth)], slab(dst_ref, i, first), write_sems.at[lax.rem(i, depth)])

    def step(i, carry):
        @pl.when(jnp.logical_and(i >= depth, i < count))
        def _():
            write(i - depth).wait()

        @pl.when(i < count)
        def _():
            read(i).start()

        @pl.when(i >= ahead)
        def _():
            read(i - ahead).wait()
            write(i - ahead).start()

        return carry

    lax.fori_loop(0, count + ahead, step, 0)

    def drain(i, carry):
        write(i).wait()
        return carry

    lax.fori_loop(max(0, count - depth), count, drain, 0)


def settle(x, first, total, block, into=None, after=()):
    depth, ahead = 12, 6
    count, _, cols = x.shape
    sem = pltpu.SemaphoreType.DMA((depth,))
    old = [] if into is None else [into]
    return pl.pallas_call(
        functools.partial(settle_kernel, block, depth, ahead, first),
        out_shape=jax.ShapeDtypeStruct((count, total, cols), x.dtype),
        in_specs=[pl.BlockSpec(memory_space=pl.ANY)] * (1 + len(old) + len(after)),
        out_specs=pl.BlockSpec(memory_space=pl.ANY),
        scratch_shapes=[pltpu.VMEM((depth, block, cols), x.dtype), sem, sem],
        input_output_aliases={1: 0} if old else {},
        compiler_params=pltpu.CompilerParams(vmem_limit_bytes=VMEM_LIMIT),
        cost_estimate=pl.CostEstimate(flops=10_000_000_000, bytes_accessed=8 * x.size, transcendentals=0),
        name="settle",
    )(x, *old, *after)


def solution(mesh):
    size = mesh.shape["sp"]

    def block_fn(x_blk, pos_blk, keep_blk, ln_gain, ln_bias, w_qkv, b_qkv, w_out, b_out, dy_blk):
        batch, tok, hidden = x_blk.shape
        heads, head_dim = w_qkv.shape[1], w_qkv.shape[3]
        tokens = batch * tok
        wq = jnp.transpose(w_qkv, (1, 2, 3, 0)).reshape(heads, 3 * head_dim, hidden)
        wo = w_out.reshape(heads, head_dim, hidden)

        def gather(a):
            return lax.all_gather(a, "sp", axis=0, tiled=True).reshape(heads, a.shape[0], hidden)

        _, parts, early, grad_a, grad_b, grad_c, grad_d, grad_out = block_call(
            x_blk, dy_blk, ln_gain, ln_bias, pos_blk, keep_blk, wq, jnp.transpose(b_qkv, (1, 0, 2)), wo, size, 256, 0)

        all_out, _, y, grad_x, totals = token_side(
            grad_out, parts, early, wq, wo, x_blk.reshape(tokens, hidden), dy_blk.reshape(tokens, hidden), ln_gain, b_out, size, 1)
        y, grad_x = hand_over(y, grad_x)
        grad_wo = settle(all_out, 0, head_dim, head_dim, after=(y,))

        rows = 3 * head_dim
        first, second, third, own = split_rows(rows)
        grad_wq = settle(gather(grad_a), 0, rows, first, after=(grad_wo,))
        all_d = spread_rows(grad_d, grad_wq, size, 2)
        grad_wq = settle(gather(grad_b), first, rows, second, grad_wq, after=(all_d,))
        grad_wq = settle(all_d, first + second + third, rows, own, grad_wq)
        grad_wq = settle(gather(grad_c), first + second, rows, third, grad_wq)
        totals = totals[:, :, :head_dim]
        grad_wq = jnp.transpose(grad_wq.reshape(heads, 3, head_dim, hidden), (3, 0, 1, 2))
        return (y.reshape(x_blk.shape), grad_x.reshape(x_blk.shape), grad_wq, totals[:, 3:6],
                grad_wo.reshape(heads * head_dim, hidden), totals[:, 2].reshape(-1), totals[:, 0].reshape(-1), totals[:, 1].reshape(-1))

    act_spec = P("dp", "sp", None)
    tok_spec = P("dp", "sp")
    in_specs = (act_spec, tok_spec, tok_spec, P(), P(), P(), P(), P(), P(), act_spec)
    out_specs = (act_spec, act_spec, P("dp", None, None, None), P("dp", None, None), P("dp", None), P("dp"), P("dp"), P("dp"))
    return jax.shard_map(block_fn, mesh=mesh, in_specs=in_specs, out_specs=out_specs, check_vma=False)
```

```python
import functools
import math

import jax
import jax.numpy as jnp
from jax import lax
from jax.experimental import pallas as pl
from jax.experimental.pallas import tpu as pltpu
from jax.sharding import PartitionSpec as P

NORM_EPS = 1e-5
MASK_FILL = -1e30
LANES = 128
LOG2E = 1.4426950408889634
MESH = pl.DeviceIdType.MESH
VMEM_LIMIT = 61 * 1024 * 1024


def dot(a, b, ca, cb):
    return lax.dot_general(a, b, (((ca,), (cb,)), ((), ())), preferred_element_type=jnp.float32)


def greet_all(me, size, meanwhile=lambda: None):
    barrier = pltpu.get_barrier_semaphore()

    def greet(d, carry):
        pl.semaphore_signal(barrier, inc=1, device_id={"sp": lax.rem(me + d, size)}, device_id_type=MESH)
        return carry

    lax.fori_loop(1, size, greet, 0)
    meanwhile()
    pl.semaphore_wait(barrier, size - 1)


class Direct:
    def __init__(self, me, size, src, dst, whole, send_sem, recv_sem):
        self.me, self.size, self.src, self.dst, self.whole, self.send_sem, self.recv_sem = me, size, src, dst, whole, send_sem, recv_sem

    def start(self):
        def body(d, carry):
            peer = lax.rem(self.me + d, self.size)
            pltpu.make_async_remote_copy(
                src_ref=self.src(peer), dst_ref=self.dst(self.me), send_sem=self.send_sem, recv_sem=self.recv_sem,
                device_id={"sp": peer}, device_id_type=MESH).start()
            return carry

        lax.fori_loop(1, self.size, body, 0)

    def total(self):
        ref = self.whole.at[pl.ds(0, self.size - 1)]
        return pltpu.make_async_remote_copy(
            src_ref=ref, dst_ref=ref, send_sem=self.send_sem, recv_sem=self.recv_sem,
            device_id={"sp": self.me}, device_id_type=MESH)

    def wait_recv(self):
        self.total().wait_recv()

    def wait_send(self):
        self.total().wait_send()


FIRST_OF = (2, 3, 0, 1)
CYCLE = (("P", 0), ("Q", 0, 0), ("Q", 3, 2), ("P", 1), ("Q", 0, 1), ("Q", 1, 0), ("Q", 2, 0), ("P", 2), ("Q", 1, 1),
         ("Q", 2, 1), ("Q", 3, 0), ("Q", 1, 2), ("Q", 2, 2), ("Q", 3, 1), ("Q", 0, 2))
LATE = 2
LAG = 3
COLOURS = 4
READY = 6
STEP_OF = ((1, 0), (-1, 0), (0, 1), (0, -1))
PLACES = len(CYCLE)


class Torus:
    def __init__(self, size):
        self.side = math.isqrt(size // 2)
        self.me = lax.axis_index("sp")
        self.core = lax.rem(self.me, 2)
        chip = self.me // 2
        self.cx, self.cy = lax.rem(chip, self.side), chip // self.side
        self.flip = 1 - 2 * self.core
        self.sibling = self.me + self.flip

    def device_at(self, dx, dy):
        side = self.side
        return (lax.rem(self.cy + dy + side, side) * side + lax.rem(self.cx + dx + side, side)) * 2 + self.core

    def neighbour(self, link):
        return self.device_at(*STEP_OF[link])

    def chunk(self, link, place, ahead):
        what = CYCLE[place]
        if what[0] == "P":
            first, n, m = link, what[1] + ahead, 0
        else:
            first, n, m = FIRST_OF[link], what[2] + ahead, what[1]
        dx = -STEP_OF[link][0] * n - STEP_OF[first][0] * m
        dy = -STEP_OF[link][1] * n - STEP_OF[first][1] * m
        return self.device_at(dx, dy), first


def is_own(place):
    return CYCLE[place] in (("P", 0), ("Q", 0, 0))


def block_kernel(size, dims, x_ref, dy_ref, gain_ref, shift_ref, pos_ref, keep_ref, wq_ref, bias_ref, wo_ref,
                 gat_ref, parts_ref, partstok_ref, gwa_ref, gwb_ref, gwo_ref,
                 xin, stage, wbuf, wobuf, metatile, metabuf, rowbuf, sbuf, qkvb, dob, dk_acc, dv_acc, dq_all, o_all, d_all, pbuf,
                 load_sems, own_sems, piece_sems, parts_sem, ici_send, ici_recv, d2d_send, d2d_recv, own_send, own_recv,
                 meta_send, meta_recv, part_send, part_recv):
    batch, tok, head_dim, pad_dim, hidden, q_block = dims
    seq_len = size * tok
    torus = Torus(size)
    me, flip, sibling, side = torus.me, torus.flip, torus.sibling, torus.side
    places = PLACES
    scale = head_dim ** -0.5
    heads = wo_ref.shape[0]
    slope = jnp.exp2(jnp.full((1, 1), -8.0 / heads, jnp.float32) * (me + 1).astype(jnp.float32))

    def send(b, link, place):
        block, colour = torus.chunk(link, place, 0)
        dst = gat_ref.at[b, block, colour]
        return pltpu.make_async_remote_copy(
            src_ref=stage.at[b, colour] if is_own(place) else dst, dst_ref=dst,
            send_sem=ici_send.at[link], recv_sem=ici_recv.at[link, place],
            device_id={"sp": torus.neighbour(link)}, device_id_type=MESH)

    def arrival(b, link, place):
        block, colour = torus.chunk(link, place, 1)
        ref = gat_ref.at[b, block, colour]
        return pltpu.make_async_remote_copy(
            src_ref=ref, dst_ref=ref, send_sem=ici_send.at[link], recv_sem=ici_recv.at[link, place],
            device_id={"sp": me}, device_id_type=MESH)

    def share(b, link, place, shift):
        block, colour = torus.chunk(link, place, 1)
        ref = gat_ref.at[b, block + shift, colour]
        return pltpu.make_async_remote_copy(
            src_ref=ref, dst_ref=ref, send_sem=d2d_send.at[link], recv_sem=d2d_recv.at[link, place],
            device_id={"sp": sibling}, device_id_type=MESH)

    def share_own(b, block):
        return pltpu.make_async_remote_copy(
            src_ref=stage.at[b], dst_ref=gat_ref.at[b, block], send_sem=own_send.at[b], recv_sem=own_recv.at[b],
            device_id={"sp": sibling}, device_id_type=MESH)

    def keep_own(b):
        return pltpu.make_async_copy(stage.at[b], gat_ref.at[b, me], own_sems.at[b])

    load_x = pltpu.make_async_copy(x_ref, xin, load_sems.at[0])
    load_dy = pltpu.make_async_copy(dy_ref, stage.at[:, :, 0], load_sems.at[1])
    load_wq = pltpu.make_async_copy(wq_ref.at[me], wbuf, load_sems.at[2])
    load_wo = pltpu.make_async_copy(wo_ref.at[me], wobuf, load_sems.at[3])
    for load in (load_x, load_dy, load_wq, load_wo):
        load.start()
    meta = Direct(me, size, lambda j: metatile, lambda j: metabuf.at[j], metabuf, meta_send, meta_recv)
    trade = Direct(me, size, lambda j: parts_ref.at[0, j], lambda j: partstok_ref.at[j], partstok_ref, part_send, part_recv)
    own_parts = pltpu.make_async_copy(parts_ref.at[0, me], partstok_ref.at[me], load_sems.at[4])

    def prepare():
        metatile[...] = jnp.zeros_like(metatile)
        metatile[0:batch, 0:tok] = pos_ref[...]
        metatile[batch:2 * batch, 0:tok] = keep_ref[...]
        metabuf[me] = metatile[...]
        load_x.wait()

        gain, shift = gain_ref[...].reshape(1, 1, hidden), shift_ref[...].reshape(1, 1, hidden)

        def normalise(b, carry):
            x = xin[b].astype(jnp.float32)
            centered = x - jnp.mean(x, axis=-1, keepdims=True)
            inv_std = lax.rsqrt(jnp.mean(centered * centered, axis=-1, keepdims=True) + NORM_EPS)
            stage[b, :, 1] = (centered * inv_std * gain + shift).astype(jnp.bfloat16)
            return carry

        lax.fori_loop(0, batch, normalise, 0)
        load_dy.wait()

    greet_all(me, size, prepare)

    pieces = sbuf.shape[0]
    chip_rows = 2 * tok

    def chip_of(p, e):
        return torus.device_at(lax.rem(p + 1 + e, side), e) // 2

    def rows_at(p, e):
        return pl.ds(pl.multiple_of(chip_of(p, e) * chip_rows, chip_rows), chip_rows)

    def load_piece(b, p):
        return [pltpu.make_async_copy(gat_ref.at[b, pl.ds(chip_of(p, e) * 2, 2)], sbuf.at[p, e], piece_sems.at[p, e]) for e in range(side)]

    def start_piece(b, p):
        for load in load_piece(b, p):
            load.start()

    def rows_of(p, which, at=slice(None)):
        return sbuf[p, :, :, :, which, :, at].reshape(side * chip_rows, -1)

    def each(lo, hi, use):
        def body(p, carry):
            use(p)
            return carry

        lax.fori_loop(lo, hi, body, 0)

    def pad_lanes(a):
        return jnp.concatenate([a, jnp.zeros((a.shape[0], pad_dim - head_dim), a.dtype)], axis=1)

    def project(b, p):
        for load in load_piece(b, p):
            load.wait()
        bias = jnp.concatenate([bias_ref[c, pl.ds(me, 1), :] for c in range(3)], axis=1)
        r = (dot(rows_of(p, 1), wbuf[...], 1, 1) + bias).astype(jnp.bfloat16)
        d = pad_lanes(dot(rows_of(p, 0), wobuf[...], 1, 1).astype(jnp.bfloat16))
        q, k, v = (pad_lanes(r[:, c * head_dim:(c + 1) * head_dim]) for c in range(3))
        for e in range(side):
            mine = slice(e * chip_rows, (e + 1) * chip_rows)
            at = rows_at(p, e)
            for c, part in enumerate((q, k, v)):
                qkvb[at, c * pad_dim:(c + 1) * pad_dim] = part[mine]
            dob[at, :] = d[mine]

    def attend(b, i):
        span = (i + 1) * q_block
        mine = slice(i * q_block, span)
        if i == 0:
            dk_acc[...] = jnp.zeros_like(dk_acc)
            dv_acc[...] = jnp.zeros_like(dv_acc)
        q, k, v = qkvb[mine, :pad_dim], qkvb[:span, pad_dim:2 * pad_dim], qkvb[:span, 2 * pad_dim:]
        do = dob[mine, :]
        pos = rowbuf[pl.ds(b, 1), :span]
        keep = rowbuf[pl.ds(b + batch, 1), :span]
        bias = jnp.where(keep > 0, (-slope * LOG2E) * (pos[:, span - 1:] - pos).astype(jnp.float32), MASK_FILL)
        scores = dot(q, k, 1, 1) * (scale * LOG2E) + bias
        row_id = lax.broadcasted_iota(jnp.int32, (q_block, q_block), 0)
        col_id = lax.broadcasted_iota(jnp.int32, (q_block, q_block), 1)
        corner = jnp.where(col_id <= row_id, scores[:, span - q_block:], MASK_FILL)
        scores = jnp.concatenate([scores[:, :span - q_block], corner], axis=1) if i else corner
        expo = jnp.exp2(scores - jnp.max(scores, axis=-1, keepdims=True))
        prob = expo * (1.0 / jnp.sum(expo, axis=-1, keepdims=True))
        prob_lo = prob.astype(jnp.bfloat16)
        o = dot(prob_lo, v, 1, 0).astype(jnp.bfloat16)
        row_dot = jnp.sum(do.astype(jnp.float32) * o.astype(jnp.float32), axis=-1, keepdims=True)
        ds_lo = (prob * (dot(do, v, 1, 1) - row_dot)).astype(jnp.bfloat16)
        o_all[mine, :] = o
        dq_all[mine, :] = (dot(ds_lo, k, 1, 0) * scale).astype(jnp.bfloat16)
        dv_acc[:span, :] += dot(prob_lo, do, 0, 0)
        dk_acc[:span, :] += dot(ds_lo, q, 0, 0)

    def store_parts(b):
        return pltpu.make_async_copy(pbuf, parts_ref.at[b], parts_sem)

    def finish(b):
        dk = (dk_acc[...] * scale).astype(jnp.bfloat16)
        dv = dv_acc[...].astype(jnp.bfloat16)
        d_all[...] = jnp.concatenate([dq_all[:, :head_dim], dk[:, :head_dim], dv[:, :head_dim]], axis=1)
        whole = jnp.concatenate([d_all[...], o_all[:, :head_dim]], axis=1).reshape(size, tok, 4 * head_dim)
        pbuf[...] = jnp.concatenate([whole[:, :tok // 2], whole[:, tok // 2:]], axis=2)
        store_parts(b).start()

    width = min(1280, hidden)

    def gradient(p):
        d = jnp.concatenate([d_all[rows_at(p, e), :] for e in range(side)], axis=0)
        o = jnp.concatenate([o_all[rows_at(p, e), :] for e in range(side)], axis=0)[:, :head_dim]

        def columns(n, carry):
            at = pl.ds(pl.multiple_of(n * width, width), width)
            term = dot(d, rows_of(p, 1, at), 0, 0)
            row = gwa_ref.shape[0]
            gwa_ref[:, at] += term[:row]
            gwb_ref[:, at] += term[row:row + gwb_ref.shape[0]]
            gwo_ref[:head_dim, at] += dot(o, rows_of(p, 0, at), 0, 0)
            gwo_ref[head_dim:, at] += term[row + gwb_ref.shape[0]:]
            return carry

        lax.fori_loop(0, hidden // width, columns, 0)

    count = seq_len // q_block
    last = pieces - 1
    tasks = {(0, READY - 3): [lambda b: each(0, last, lambda p: start_piece(b, p))],
             (0, READY - 2): [lambda b: each(0, last - 1, lambda p: project(b, p))],
             (0, READY - 1): [lambda b: project(b, last - 1)],
             (0, READY): [lambda b: start_piece(b, last)],
             (0, READY + 1): [lambda b: project(b, last)],
             (0, READY + 7): [finish],
             (0, READY + 8): [lambda b: each(0, pieces // 2, gradient)],
             (1, 0): [lambda b: each(pieces // 2, pieces, gradient)],
             (1, 1): [lambda b: store_parts(b).wait()]}
    spot = (2, 2, 2, 3, 3, 4, 5, 6)
    for i in range(count):
        tasks.setdefault((0, READY + spot[i]), []).append(lambda b, i=i: attend(b, i))

    for ref in (gwa_ref, gwb_ref, gwo_ref):
        ref[...] = jnp.zeros_like(ref)

    def phase_of(i, place):
        return i - 1 if place == LATE else i

    def among(b):
        return jnp.logical_and(b >= 0, b < batch)

    def turn(i, carry):
        for place in range(places):
            came = (place - LAG) % places
            b_came = phase_of(i if place >= LAG else i - 1, came)

            @pl.when(among(b_came))
            def _():
                for link in range(4):
                    arrival(b_came, link, came).wait_recv()
                    share(b_came, link, came, 0).start()

            b_send = phase_of(i, place)

            @pl.when(among(b_send))
            def _():
                for link in range(4):
                    send(b_send, link, place).start()

            shared = (place - LAG - 1) % places
            b_shared = phase_of(i if place >= LAG + 1 else i - 1, shared)

            @pl.when(among(b_shared))
            def _():
                for link in range(4):
                    share(b_shared, link, shared, flip).wait_recv()

            if place == 1:
                @pl.when(i == 0)
                def _():
                    for b in range(batch):
                        share_own(b, me).start()
                        keep_own(b).start()
                    meta.start()

            if place == READY - 3:
                @pl.when(i == 1)
                def _():
                    for load in (load_wq, load_wo):
                        load.wait()
                    meta.wait_recv()
                    for j in range(size):
                        rowbuf[:, j * tok:(j + 1) * tok] = metabuf[j, :, :tok]
                    for b in range(batch):
                        share_own(b, sibling).wait_recv()
                        keep_own(b).wait()
                    meta.wait_send()
                    for b in range(batch):
                        share_own(b, me).wait_send()

            if place == READY:
                @pl.when(i == batch)
                def _():
                    own_parts.start()
                    trade.start()

            for later in (0, 1):
                if (later, place) in tasks:
                    @pl.when(among(i - 1 - later))
                    def _():
                        for task in tasks[later, place]:
                            task(i - 1 - later)
        return carry

    lax.fori_loop(0, batch + 2, turn, 0)
    own_parts.wait()
    trade.wait_recv()
    trade.wait_send()
    sent = gat_ref.at[:, pl.ds(0, places), 0]
    for link in range(4):
        for sem in (ici_send, d2d_send):
            pltpu.make_async_remote_copy(
                src_ref=sent, dst_ref=sent, send_sem=sem.at[link], recv_sem=ici_recv.at[link, 0],
                device_id={"sp": sibling}, device_id_type=MESH).wait_send()


def split_rows(rows):
    first, own = 8 * (rows * 13 // 240), 8 * (rows // 80 or 1)
    return first, rows - first - own, own


def block_call(x, dy, gain, shift, pos, keep, wq, bias, wo, size, q_block, collective_id):
    batch, tok, hidden = x.shape
    rows = tok // COLOURS
    heads, head_dim, _ = wo.shape
    pad_dim = -(-head_dim // LANES) * LANES
    seq_len = size * tok
    side = math.isqrt(size // 2)
    places = PLACES
    anywhere = pl.BlockSpec(memory_space=pl.ANY)
    vmem = pl.BlockSpec(memory_space=pltpu.VMEM)
    sem = pltpu.SemaphoreType.DMA
    bf16, f32 = jnp.bfloat16, jnp.float32
    flops = batch * (6 * seq_len * seq_len * 256 + 4 * seq_len * 4 * head_dim * hidden) + 80_000_000_000
    cut = (batch, COLOURS, rows, hidden)
    first, second, own = split_rows(3 * head_dim)
    return pl.pallas_call(
        functools.partial(block_kernel, size, (batch, tok, head_dim, pad_dim, hidden, min(q_block, seq_len))),
        out_shape=(
            jax.ShapeDtypeStruct((batch, size, COLOURS, 2, rows, hidden), bf16),
            jax.ShapeDtypeStruct((batch, size, tok // 2, 8 * head_dim), bf16),
            jax.ShapeDtypeStruct((size, tok // 2, 8 * head_dim), bf16),
            *(jax.ShapeDtypeStruct((n, hidden), f32) for n in (first, second, head_dim + own)),
        ),
        in_specs=[anywhere, anywhere, vmem, vmem, vmem, vmem, anywhere, vmem, anywhere],
        out_specs=(anywhere, anywhere, anywhere, vmem, vmem, vmem),
        scratch_shapes=[
            pltpu.VMEM(cut, bf16),
            pltpu.VMEM((batch, COLOURS, 2, rows, hidden), bf16),
            pltpu.VMEM((3 * head_dim, hidden), bf16),
            pltpu.VMEM((head_dim, hidden), bf16),
            pltpu.VMEM((8, LANES), jnp.int32),
            pltpu.VMEM((size, 8, LANES), jnp.int32),
            pltpu.VMEM((8, seq_len), jnp.int32),
            pltpu.VMEM((side, side, 2, COLOURS, 2, rows, hidden), bf16),
            pltpu.VMEM((seq_len, 3 * pad_dim), bf16),
            pltpu.VMEM((seq_len, pad_dim), bf16),
            pltpu.VMEM((seq_len, pad_dim), f32),
            pltpu.VMEM((seq_len, pad_dim), f32),
            pltpu.VMEM((seq_len, pad_dim), bf16),
            pltpu.VMEM((seq_len, pad_dim), bf16),
            pltpu.VMEM((seq_len, 3 * head_dim), bf16),
            pltpu.VMEM((size, tok // 2, 8 * head_dim), bf16),
            sem((5,)), sem((batch,)), sem((side, side)), sem,
            sem((4,)), sem((4, places)), sem((4,)), sem((4, places)), sem((batch,)), sem((batch,)), sem, sem, sem, sem,
        ],
        compiler_params=pltpu.CompilerParams(collective_id=collective_id, has_side_effects=True, vmem_limit_bytes=VMEM_LIMIT),
        cost_estimate=pl.CostEstimate(flops=flops, bytes_accessed=60_000_000, transcendentals=batch * seq_len * seq_len // 2),
        name="block",
    )(x.reshape(cut), dy.reshape(cut), gain, shift, pos, keep, wq, bias, wo)


class Spread:
    def __init__(self, size, own_ref, gat_ref, stage, sems):
        self.torus, self.size, self.gat_ref, self.stage = Torus(size), size, gat_ref, stage
        self.load_sem, self.keep_sem, self.ici_send, self.ici_recv, self.d2d_send, self.d2d_recv, self.own_send, self.own_recv = sems
        self.part = stage.shape[1] // COLOURS
        self.load = pltpu.make_async_copy(own_ref, stage, self.load_sem)
        self.keep = pltpu.make_async_copy(stage, gat_ref.at[self.torus.me], self.keep_sem)

    def columns(self, colour):
        return pl.ds(colour * self.part, self.part)

    def view(self, block, colour):
        return self.gat_ref.at[block, :, self.columns(colour)]

    def remote(self, src, dst, send_sem, recv_sem, device):
        return pltpu.make_async_remote_copy(
            src_ref=src, dst_ref=dst, send_sem=send_sem, recv_sem=recv_sem, device_id={"sp": device}, device_id_type=MESH)

    def send(self, link, place):
        block, colour = self.torus.chunk(link, place, 0)
        dst = self.view(block, colour)
        src = self.stage.at[:, self.columns(colour)] if is_own(place) else dst
        return self.remote(src, dst, self.ici_send.at[link], self.ici_recv.at[link, place], self.torus.neighbour(link))

    def arrival(self, link, place):
        ref = self.view(*self.torus.chunk(link, place, 1))
        return self.remote(ref, ref, self.ici_send.at[link], self.ici_recv.at[link, place], self.torus.me)

    def share(self, link, place, shift):
        block, colour = self.torus.chunk(link, place, 1)
        ref = self.view(block + shift, colour)
        return self.remote(ref, ref, self.d2d_send.at[link], self.d2d_recv.at[link, place], self.torus.sibling)

    def share_own(self, block):
        return self.remote(self.stage, self.gat_ref.at[block], self.own_send, self.own_recv, self.torus.sibling)

    STEPS = PLACES + LATE + LAG + 2

    def step(self, g):
        def place_of(g):
            place = g % PLACES
            return place if g >= 0 and g // PLACES == (1 if place == LATE else 0) else None

        came, now, shared = place_of(g - LAG), place_of(g), place_of(g - LAG - 1)
        for link in range(4):
            if came is not None:
                self.arrival(link, came).wait_recv()
                self.share(link, came, 0).start()
        for link in range(4):
            if now is not None:
                self.send(link, now).start()
        for link in range(4):
            if shared is not None:
                self.share(link, shared, self.torus.flip).wait_recv()
        if g == 1:
            self.share_own(self.torus.me).start()
            self.keep.start()

    def close(self):
        self.share_own(self.torus.sibling).wait_recv()
        self.keep.wait()
        self.share_own(self.torus.me).wait_send()
        sent = self.gat_ref.at[pl.ds(0, PLACES), :, pl.ds(0, self.part)]
        for link in range(4):
            for sem in (self.ici_send, self.d2d_send):
                self.remote(sent, sent, sem.at[link], self.ici_recv.at[link, 0], self.torus.sibling).wait_send()

    @staticmethod
    def scratch(rows, cols, dtype):
        sem = pltpu.SemaphoreType.DMA
        return [pltpu.VMEM((rows, cols), dtype), sem, sem, sem((4,)), sem((4, PLACES)), sem((4,)), sem((4, PLACES)), sem, sem]


TOKEN_AT = 8
TOKEN_STEPS = 8


def token_kernel(size, head_dim, chunk, own_ref, parts_ref, early_ref, wq_ref, wo_ref, x_ref, dy_ref, gain_ref, bout_ref,
                 gat_ref, late_ref, y_ref, gx_ref, totals_ref,
                 stage, load_sem, keep_sem, ici_send, ici_recv, d2d_send, d2d_recv, own_send, own_recv,
                 wqbuf, wobuf, pbuf, dn_acc, y_acc, sums, tiles, come, total,
                 part_send, part_recv, own_part_sems, wq_sems, wo_sems, p_sems, deal_send, deal_recv, collect_send, collect_recv):
    spread = Spread(size, own_ref, gat_ref, stage,
                    (load_sem, keep_sem, ici_send, ici_recv, d2d_send, d2d_recv, own_send, own_recv))
    me = spread.torus.me
    late = late_ref.shape[0]
    heads, hidden = wq_ref.shape[0], wq_ref.shape[2]
    per = heads // TOKEN_STEPS
    trades, own_parts = [], []
    for n in range(late):
        b = parts_ref.shape[0] - late + n
        trades.append(Direct(me, size, lambda j, b=b: parts_ref.at[b, j], lambda j, n=n: late_ref.at[n, j], late_ref.at[n],
                             part_send.at[n], part_recv.at[n]))
        own_parts.append(pltpu.make_async_copy(parts_ref.at[b, me], late_ref.at[n, me], own_part_sems.at[n]))
    deal = Direct(me, size, lambda j: tiles.at[j], lambda j: come.at[j], come, deal_send, deal_recv)
    collect = Direct(me, size, lambda j: total, lambda j: totals_ref.at[j], totals_ref, collect_send, collect_recv)

    def weights(m):
        at, slot = pl.ds(m * per, per), m % 2
        return (pltpu.make_async_copy(wq_ref.at[at], wqbuf.at[slot], wq_sems.at[slot]),
                pltpu.make_async_copy(wo_ref.at[at], wobuf.at[slot], wo_sems.at[slot]))

    def rows(m):
        at, slot = pl.ds(m * per, per), m % 2
        return [pltpu.make_async_copy(early_ref.at[at], pbuf.at[slot, 0], p_sems.at[slot, 0])] + [
            pltpu.make_async_copy(late_ref.at[n, at], pbuf.at[slot, 1 + n], p_sems.at[slot, 1 + n]) for n in range(late)]

    spread.load.start()
    for copy in weights(0):
        copy.start()
    dn_acc[...] = jnp.zeros_like(dn_acc)
    y_acc[...] = jnp.zeros_like(y_acc)
    sums[...] = jnp.zeros_like(sums)
    tiles[...] = jnp.zeros_like(tiles)
    width = hidden // 4

    def heads_step(m):
        slot = m % 2
        for copy in (*weights(m), *rows(m)):
            copy.wait()
        if m + 1 < TOKEN_STEPS:
            for copy in (*weights(m + 1), *rows(m + 1)):
                copy.start()

        def pair(i, carry):
            ds, os = [], []
            for h in range(2):
                parts = []
                for n in range(1 + late):
                    both = pbuf[slot, n, i * 2 + h]
                    parts += [both[:, :4 * head_dim], both[:, 4 * head_dim:]]
                parts = jnp.concatenate(parts, axis=0)
                ds.append(parts[:, :3 * head_dim])
                os.append(parts[:, 3 * head_dim:])
                added = jnp.sum(ds[h].astype(jnp.float32), axis=0, keepdims=True)
                for c in range(3):
                    tiles[m * per + i * 2 + h, 3 + c:4 + c, 0:head_dim] = added[:, c * head_dim:(c + 1) * head_dim]

            def columns(n, carry):
                at = pl.ds(pl.multiple_of(n * width, width), width)
                dn_acc[:, at] += dot(ds[0], wqbuf[slot, i * 2, :, at], 1, 0) + dot(ds[1], wqbuf[slot, i * 2 + 1, :, at], 1, 0)
                y_acc[:, at] += dot(os[0], wobuf[slot, i * 2, :, at], 1, 0) + dot(os[1], wobuf[slot, i * 2 + 1, :, at], 1, 0)
                return carry

            lax.fori_loop(0, 4, columns, 0)
            return carry

        lax.fori_loop(0, per // 2, pair, 0)

    def norm_step(half):
        gain = gain_ref[...].reshape(1, hidden)
        bout = bout_ref[...].reshape(1, hidden)
        count = x_ref.shape[0] // chunk

        def body(c, carry):
            at = pl.ds(pl.multiple_of(c * chunk, chunk), chunk)
            x = x_ref[at, :].astype(jnp.float32)
            dy = dy_ref[at, :].astype(jnp.float32)
            centered = x - jnp.mean(x, axis=-1, keepdims=True)
            inv_std = lax.rsqrt(jnp.mean(centered * centered, axis=-1, keepdims=True) + NORM_EPS)
            x_hat = centered * inv_std
            d_norm = dn_acc[at, :]
            d_hat = d_norm * gain
            d_mean = jnp.mean(d_hat, axis=-1, keepdims=True)
            d_proj = jnp.mean(d_hat * x_hat, axis=-1, keepdims=True)
            gx_ref[at, :] = (dy + inv_std * (d_hat - d_mean - x_hat * d_proj)).astype(jnp.bfloat16)
            y_ref[at, :] = (x + y_acc[at, :] + bout).astype(jnp.bfloat16)
            sums[0:1, :] += jnp.sum(d_norm * x_hat, axis=0, keepdims=True)
            sums[1:2, :] += jnp.sum(d_norm, axis=0, keepdims=True)
            sums[2:3, :] += jnp.sum(dy, axis=0, keepdims=True)
            return carry

        lax.fori_loop(half * count // 2, (half + 1) * count // 2, body, 0)

    greet_all(me, size)
    spread.load.wait()
    for g in range(Spread.STEPS):
        spread.step(g)
        m = g - TOKEN_AT
        if g == 1:
            for copy in trades + own_parts:
                copy.start()
        if m == 0:
            for copy in own_parts:
                copy.wait()
            for trade in trades:
                trade.wait_recv()
            for copy in rows(0):
                copy.start()
        if 0 <= m < TOKEN_STEPS:
            heads_step(m)
        elif m in (TOKEN_STEPS, TOKEN_STEPS + 1):
            norm_step(m - TOKEN_STEPS)
        elif m == TOKEN_STEPS + 2:
            for j in range(size):
                tiles[j, 0:3, 0:head_dim] = sums[0:3, j * head_dim:(j + 1) * head_dim]
            come[me] = tiles[me]
        elif m == TOKEN_STEPS + 3:
            deal.start()
        elif m == TOKEN_STEPS + 5:
            deal.wait_recv()
            total[...] = jnp.sum(come[...], axis=0)
            totals_ref[me] = total[...]
            collect.start()
    spread.close()
    for trade in trades:
        trade.wait_send()
    deal.wait_send()
    collect.wait_recv()
    collect.wait_send()


def token_side(block, parts, early, wq, wo, x, dy, gain, bout, size, collective_id):
    rows, cols = block.shape
    late = parts.shape[0] - 1
    heads, head_dim, hidden = wo.shape
    tokens = x.shape[0]
    per = heads // TOKEN_STEPS
    anywhere = pl.BlockSpec(memory_space=pl.ANY)
    vmem = pl.BlockSpec(memory_space=pltpu.VMEM)
    sem = pltpu.SemaphoreType.DMA
    bf16, f32 = jnp.bfloat16, jnp.float32
    return pl.pallas_call(
        functools.partial(token_kernel, size, head_dim, 16),
        out_shape=(
            jax.ShapeDtypeStruct((size, rows, cols), block.dtype),
            jax.ShapeDtypeStruct((late, *parts.shape[1:]), parts.dtype),
            jax.ShapeDtypeStruct((tokens, hidden), bf16),
            jax.ShapeDtypeStruct((tokens, hidden), bf16),
            jax.ShapeDtypeStruct((size, 8, LANES), f32),
        ),
        in_specs=[anywhere] * 5 + [vmem] * 4,
        out_specs=(anywhere, anywhere, vmem, vmem, vmem),
        scratch_shapes=Spread.scratch(rows, cols, block.dtype) + [
            pltpu.VMEM((2, per, 3 * head_dim, hidden), bf16),
            pltpu.VMEM((2, per, head_dim, hidden), bf16),
            pltpu.VMEM((2, 1 + late, per, *parts.shape[2:]), bf16),
            pltpu.VMEM((tokens, hidden), f32),
            pltpu.VMEM((tokens, hidden), f32),
            pltpu.VMEM((8, hidden), f32),
            pltpu.VMEM((size, 8, LANES), f32),
            pltpu.VMEM((size, 8, LANES), f32),
            pltpu.VMEM((8, LANES), f32),
            sem((late,)), sem((late,)), sem((late,)), sem((2,)), sem((2,)), sem((2, 1 + late)), sem, sem, sem, sem,
        ],
        compiler_params=pltpu.CompilerParams(collective_id=collective_id, has_side_effects=True, vmem_limit_bytes=VMEM_LIMIT),
        cost_estimate=pl.CostEstimate(flops=120_000_000_000, bytes_accessed=8 * size * rows * cols, transcendentals=0),
        name="token_side",
    )(block, parts, early, wq, wo, x, dy, gain, bout)


def hand_kernel(y_ref, gx_ref, y_out, gx_out):
    y_out[...] = y_ref[...]
    gx_out[...] = gx_ref[...]


def hand_over(y, gx):
    spec = pl.BlockSpec((y.shape[0] // 4, y.shape[1]), lambda i: (i, 0))
    return pl.pallas_call(
        hand_kernel, grid=(4,), out_shape=(jax.ShapeDtypeStruct(y.shape, y.dtype),) * 2, in_specs=[spec] * 2, out_specs=(spec,) * 2,
        cost_estimate=pl.CostEstimate(flops=1_000_000_000, bytes_accessed=8 * y.size, transcendentals=0), name="hand_over")(y, gx)


def settle_kernel(block, depth, ahead, per, origin, first, src_ref, *refs):
    dst_ref, buf, read_sems, write_sems = refs[-4:]
    count = src_ref.shape[0] * per

    def slab(ref, i, start):
        return ref.at[i // per, pl.ds(pl.multiple_of(start + lax.rem(i, per) * block, 8), block)]

    def read(i):
        return pltpu.make_async_copy(slab(src_ref, i, origin), buf.at[lax.rem(i, depth)], read_sems.at[lax.rem(i, depth)])

    def write(i):
        return pltpu.make_async_copy(buf.at[lax.rem(i, depth)], slab(dst_ref, i, first), write_sems.at[lax.rem(i, depth)])

    def step(i, carry):
        @pl.when(jnp.logical_and(i >= depth, i < count))
        def _():
            write(i - depth).wait()

        @pl.when(i < count)
        def _():
            read(i).start()

        @pl.when(i >= ahead)
        def _():
            read(i - ahead).wait()
            write(i - ahead).start()

        return carry

    lax.fori_loop(0, count + ahead, step, 0)

    def drain(i, carry):
        write(i).wait()
        return carry

    lax.fori_loop(max(0, count - depth), count, drain, 0)


def settle(x, origin, rows, first, total, pieces=1, into=None, after=()):
    block = rows // pieces
    depth, ahead = 12, 6
    count, _, cols = x.shape
    sem = pltpu.SemaphoreType.DMA((depth,))
    old = [] if into is None else [into]
    return pl.pallas_call(
        functools.partial(settle_kernel, block, depth, ahead, pieces, origin, first),
        out_shape=jax.ShapeDtypeStruct((count, total, cols), x.dtype),
        in_specs=[pl.BlockSpec(memory_space=pl.ANY)] * (1 + len(old) + len(after)),
        out_specs=pl.BlockSpec(memory_space=pl.ANY),
        scratch_shapes=[pltpu.VMEM((depth, block, cols), x.dtype), sem, sem],
        input_output_aliases={1: 0} if old else {},
        compiler_params=pltpu.CompilerParams(vmem_limit_bytes=VMEM_LIMIT),
        cost_estimate=pl.CostEstimate(flops=10_000_000_000, bytes_accessed=8 * x.size, transcendentals=0),
        name="settle",
    )(x, *old, *after)


def solution(mesh):
    size = mesh.shape["sp"]

    def block_fn(x_blk, pos_blk, keep_blk, ln_gain, ln_bias, w_qkv, b_qkv, w_out, b_out, dy_blk):
        batch, tok, hidden = x_blk.shape
        heads, head_dim = w_qkv.shape[1], w_qkv.shape[3]
        tokens = batch * tok
        wq = jnp.transpose(w_qkv, (1, 2, 3, 0)).reshape(heads, 3 * head_dim, hidden)
        wo = w_out.reshape(heads, head_dim, hidden)

        def gather(a):
            return lax.all_gather(a, "sp", axis=0, tiled=True).reshape(heads, a.shape[0], hidden)

        _, parts, early, grad_a, grad_b, grad_out = block_call(
            x_blk, dy_blk, ln_gain, ln_bias, pos_blk, keep_blk, wq, jnp.transpose(b_qkv, (1, 0, 2)), wo, size, 256, 0)

        all_out, _, y, grad_x, totals = token_side(
            grad_out, parts, early, wq, wo, x_blk.reshape(tokens, hidden), dy_blk.reshape(tokens, hidden), ln_gain, b_out, size, 1)
        y, grad_x = hand_over(y, grad_x)
        grad_wo = settle(all_out, 0, head_dim, 0, head_dim, after=(y,))

        rows = 3 * head_dim
        first, second, own = split_rows(rows)
        grad_wq = settle(all_out, head_dim, own, first + second, rows, after=(grad_wo,))
        grad_wq = settle(gather(grad_a), 0, first, 0, rows, into=grad_wq)
        grad_wq = settle(gather(grad_b), 0, second, first, rows, into=grad_wq)
        totals = totals[:, :, :head_dim]
        grad_wq = jnp.transpose(grad_wq.reshape(heads, 3, head_dim, hidden), (3, 0, 1, 2))
        return (y.reshape(x_blk.shape), grad_x.reshape(x_blk.shape), grad_wq, totals[:, 3:6],
                grad_wo.reshape(heads * head_dim, hidden), totals[:, 2].reshape(-1), totals[:, 0].reshape(-1), totals[:, 1].reshape(-1))

    act_spec = P("dp", "sp", None)
    tok_spec = P("dp", "sp")
    in_specs = (act_spec, tok_spec, tok_spec, P(), P(), P(), P(), P(), P(), act_spec)
    out_specs = (act_spec, act_spec, P("dp", None, None, None), P("dp", None, None), P("dp", None), P("dp"), P("dp"), P("dp"))
    return jax.shard_map(block_fn, mesh=mesh, in_specs=in_specs, out_specs=out_specs, check_vma=False)
```

```python
import functools
import math

import jax
import jax.numpy as jnp
from jax import lax
from jax.experimental import pallas as pl
from jax.experimental.pallas import tpu as pltpu
from jax.sharding import PartitionSpec as P

NORM_EPS = 1e-5
MASK_FILL = -1e30
LANES = 128
LOG2E = 1.4426950408889634
MESH = pl.DeviceIdType.MESH
VMEM_LIMIT = 61 * 1024 * 1024


def dot(a, b, ca, cb):
    return lax.dot_general(a, b, (((ca,), (cb,)), ((), ())), preferred_element_type=jnp.float32)


def greet_all(me, size, meanwhile=lambda: None):
    barrier = pltpu.get_barrier_semaphore()

    def greet(d, carry):
        pl.semaphore_signal(barrier, inc=1, device_id={"sp": lax.rem(me + d, size)}, device_id_type=MESH)
        return carry

    lax.fori_loop(1, size, greet, 0)
    meanwhile()
    pl.semaphore_wait(barrier, size - 1)


class Direct:
    def __init__(self, me, size, src, dst, whole, send_sem, recv_sem):
        self.me, self.size, self.src, self.dst, self.whole, self.send_sem, self.recv_sem = me, size, src, dst, whole, send_sem, recv_sem

    def start(self):
        def body(d, carry):
            peer = lax.rem(self.me + d, self.size)
            pltpu.make_async_remote_copy(
                src_ref=self.src(peer), dst_ref=self.dst(self.me), send_sem=self.send_sem, recv_sem=self.recv_sem,
                device_id={"sp": peer}, device_id_type=MESH).start()
            return carry

        lax.fori_loop(1, self.size, body, 0)

    def total(self):
        ref = self.whole.at[pl.ds(0, self.size - 1)]
        return pltpu.make_async_remote_copy(
            src_ref=ref, dst_ref=ref, send_sem=self.send_sem, recv_sem=self.recv_sem,
            device_id={"sp": self.me}, device_id_type=MESH)

    def wait_recv(self):
        self.total().wait_recv()

    def wait_send(self):
        self.total().wait_send()


FIRST_OF = (2, 3, 0, 1)
CYCLE = (("P", 0), ("Q", 0, 0), ("Q", 3, 2), ("P", 1), ("Q", 0, 1), ("Q", 1, 0), ("Q", 2, 0), ("P", 2), ("Q", 1, 1),
         ("Q", 2, 1), ("Q", 3, 0), ("Q", 1, 2), ("Q", 2, 2), ("Q", 3, 1), ("Q", 0, 2))
LATE = 2
LAG = 3
COLOURS = 4
READY = 6
EARLY = 2
STEP_OF = ((1, 0), (-1, 0), (0, 1), (0, -1))
PLACES = len(CYCLE)


class Torus:
    def __init__(self, size):
        self.side = math.isqrt(size // 2)
        self.me = lax.axis_index("sp")
        self.core = lax.rem(self.me, 2)
        chip = self.me // 2
        self.cx, self.cy = lax.rem(chip, self.side), chip // self.side
        self.flip = 1 - 2 * self.core
        self.sibling = self.me + self.flip

    def device_at(self, dx, dy):
        side = self.side
        return (lax.rem(self.cy + dy + side, side) * side + lax.rem(self.cx + dx + side, side)) * 2 + self.core

    def neighbour(self, link):
        return self.device_at(*STEP_OF[link])

    def chunk(self, link, place, ahead):
        what = CYCLE[place]
        if what[0] == "P":
            first, n, m = link, what[1] + ahead, 0
        else:
            first, n, m = FIRST_OF[link], what[2] + ahead, what[1]
        dx = -STEP_OF[link][0] * n - STEP_OF[first][0] * m
        dy = -STEP_OF[link][1] * n - STEP_OF[first][1] * m
        return self.device_at(dx, dy), first


def is_own(place):
    return CYCLE[place] in (("P", 0), ("Q", 0, 0))


def block_kernel(size, dims, x_ref, dy_ref, gain_ref, shift_ref, pos_ref, keep_ref, wq_ref, bias_ref, wo_ref,
                 gat_ref, parts_ref, partstok_ref, gwa_ref, gwb_ref, gwc_ref, gwo_ref,
                 xin, stage, wbuf, wobuf, metatile, metabuf, rowbuf, sbuf, qkvb, dob, dk_acc, dv_acc, dq_all, o_all, d_all, pbuf,
                 load_sems, own_sems, piece_sems, parts_sem, ici_send, ici_recv, d2d_send, d2d_recv, own_send, own_recv,
                 meta_send, meta_recv, part_send, part_recv):
    batch, tok, head_dim, pad_dim, hidden, q_block = dims
    seq_len = size * tok
    torus = Torus(size)
    me, flip, sibling, side = torus.me, torus.flip, torus.sibling, torus.side
    places = PLACES
    scale = head_dim ** -0.5
    heads = wo_ref.shape[0]
    slope = jnp.exp2(jnp.full((1, 1), -8.0 / heads, jnp.float32) * (me + 1).astype(jnp.float32))

    def send(b, link, place):
        block, colour = torus.chunk(link, place, 0)
        dst = gat_ref.at[b, block, colour]
        return pltpu.make_async_remote_copy(
            src_ref=stage.at[b, colour] if is_own(place) else dst, dst_ref=dst,
            send_sem=ici_send.at[link], recv_sem=ici_recv.at[link, place],
            device_id={"sp": torus.neighbour(link)}, device_id_type=MESH)

    def arrival(b, link, place):
        block, colour = torus.chunk(link, place, 1)
        ref = gat_ref.at[b, block, colour]
        return pltpu.make_async_remote_copy(
            src_ref=ref, dst_ref=ref, send_sem=ici_send.at[link], recv_sem=ici_recv.at[link, place],
            device_id={"sp": me}, device_id_type=MESH)

    def share(b, link, place, shift):
        block, colour = torus.chunk(link, place, 1)
        ref = gat_ref.at[b, block + shift, colour]
        return pltpu.make_async_remote_copy(
            src_ref=ref, dst_ref=ref, send_sem=d2d_send.at[link], recv_sem=d2d_recv.at[link, place],
            device_id={"sp": sibling}, device_id_type=MESH)

    def share_own(b, block):
        return pltpu.make_async_remote_copy(
            src_ref=stage.at[b], dst_ref=gat_ref.at[b, block], send_sem=own_send.at[b], recv_sem=own_recv.at[b],
            device_id={"sp": sibling}, device_id_type=MESH)

    def keep_own(b):
        return pltpu.make_async_copy(stage.at[b], gat_ref.at[b, me], own_sems.at[b])

    load_x = pltpu.make_async_copy(x_ref, xin, load_sems.at[0])
    load_dy = pltpu.make_async_copy(dy_ref, stage.at[:, :, 0], load_sems.at[1])
    load_wq = pltpu.make_async_copy(wq_ref.at[me], wbuf, load_sems.at[2])
    load_wo = pltpu.make_async_copy(wo_ref.at[me], wobuf, load_sems.at[3])
    for load in (load_x, load_dy, load_wq, load_wo):
        load.start()
    meta = Direct(me, size, lambda j: metatile, lambda j: metabuf.at[j], metabuf, meta_send, meta_recv)
    early = partstok_ref.shape[0]
    trades = [Direct(me, size, lambda j, b=b: parts_ref.at[b, j], lambda j, b=b: partstok_ref.at[b, j], partstok_ref.at[b],
                     part_send.at[b], part_recv.at[b]) for b in range(early)]
    own_parts = [pltpu.make_async_copy(parts_ref.at[b, me], partstok_ref.at[b, me], load_sems.at[4 + b]) for b in range(early)]

    def prepare():
        metatile[...] = jnp.zeros_like(metatile)
        metatile[0:batch, 0:tok] = pos_ref[...]
        metatile[batch:2 * batch, 0:tok] = keep_ref[...]
        metabuf[me] = metatile[...]
        load_x.wait()

        gain, shift = gain_ref[...].reshape(1, 1, hidden), shift_ref[...].reshape(1, 1, hidden)

        def normalise(b, carry):
            x = xin[b].astype(jnp.float32)
            centered = x - jnp.mean(x, axis=-1, keepdims=True)
            inv_std = lax.rsqrt(jnp.mean(centered * centered, axis=-1, keepdims=True) + NORM_EPS)
            stage[b, :, 1] = (centered * inv_std * gain + shift).astype(jnp.bfloat16)
            return carry

        lax.fori_loop(0, batch, normalise, 0)
        load_dy.wait()

    greet_all(me, size, prepare)

    pieces = sbuf.shape[0]
    chip_rows = 2 * tok

    def chip_of(p, e):
        return torus.device_at(lax.rem(p + 1 + e, side), e) // 2

    def rows_at(p, e):
        return pl.ds(pl.multiple_of(chip_of(p, e) * chip_rows, chip_rows), chip_rows)

    def load_piece(b, p):
        return [pltpu.make_async_copy(gat_ref.at[b, pl.ds(chip_of(p, e) * 2, 2)], sbuf.at[p, e], piece_sems.at[p, e]) for e in range(side)]

    def start_piece(b, p):
        for load in load_piece(b, p):
            load.start()

    def rows_of(p, which, at=slice(None)):
        return sbuf[p, :, :, :, which, :, at].reshape(side * chip_rows, -1)

    def each(lo, hi, use):
        def body(p, carry):
            use(p)
            return carry

        lax.fori_loop(lo, hi, body, 0)

    def pad_lanes(a):
        return jnp.concatenate([a, jnp.zeros((a.shape[0], pad_dim - head_dim), a.dtype)], axis=1)

    def project(b, p):
        for load in load_piece(b, p):
            load.wait()
        bias = jnp.concatenate([bias_ref[c, pl.ds(me, 1), :] for c in range(3)], axis=1)
        r = (dot(rows_of(p, 1), wbuf[...], 1, 1) + bias).astype(jnp.bfloat16)
        d = pad_lanes(dot(rows_of(p, 0), wobuf[...], 1, 1).astype(jnp.bfloat16))
        q, k, v = (pad_lanes(r[:, c * head_dim:(c + 1) * head_dim]) for c in range(3))
        for e in range(side):
            mine = slice(e * chip_rows, (e + 1) * chip_rows)
            at = rows_at(p, e)
            for c, part in enumerate((q, k, v)):
                qkvb[at, c * pad_dim:(c + 1) * pad_dim] = part[mine]
            dob[at, :] = d[mine]

    def attend(b, i):
        span = (i + 1) * q_block
        mine = slice(i * q_block, span)
        if i == 0:
            dk_acc[...] = jnp.zeros_like(dk_acc)
            dv_acc[...] = jnp.zeros_like(dv_acc)
        q, k, v = qkvb[mine, :pad_dim], qkvb[:span, pad_dim:2 * pad_dim], qkvb[:span, 2 * pad_dim:]
        do = dob[mine, :]
        pos = rowbuf[pl.ds(b, 1), :span]
        keep = rowbuf[pl.ds(b + batch, 1), :span]
        bias = jnp.where(keep > 0, (-slope * LOG2E) * (pos[:, span - 1:] - pos).astype(jnp.float32), MASK_FILL)
        scores = dot(q, k, 1, 1) * (scale * LOG2E) + bias
        row_id = lax.broadcasted_iota(jnp.int32, (q_block, q_block), 0)
        col_id = lax.broadcasted_iota(jnp.int32, (q_block, q_block), 1)
        corner = jnp.where(col_id <= row_id, scores[:, span - q_block:], MASK_FILL)
        scores = jnp.concatenate([scores[:, :span - q_block], corner], axis=1) if i else corner
        expo = jnp.exp2(scores - jnp.max(scores, axis=-1, keepdims=True))
        prob = expo * (1.0 / jnp.sum(expo, axis=-1, keepdims=True))
        prob_lo = prob.astype(jnp.bfloat16)
        o = dot(prob_lo, v, 1, 0).astype(jnp.bfloat16)
        row_dot = jnp.sum(do.astype(jnp.float32) * o.astype(jnp.float32), axis=-1, keepdims=True)
        ds_lo = (prob * (dot(do, v, 1, 1) - row_dot)).astype(jnp.bfloat16)
        o_all[mine, :] = o
        dq_all[mine, :] = (dot(ds_lo, k, 1, 0) * scale).astype(jnp.bfloat16)
        dv_acc[:span, :] += dot(prob_lo, do, 0, 0)
        dk_acc[:span, :] += dot(ds_lo, q, 0, 0)

    def store_parts(b):
        return pltpu.make_async_copy(pbuf, parts_ref.at[b], parts_sem)

    def finish(b):
        dk = (dk_acc[...] * scale).astype(jnp.bfloat16)
        dv = dv_acc[...].astype(jnp.bfloat16)
        d_all[...] = jnp.concatenate([dq_all[:, :head_dim], dk[:, :head_dim], dv[:, :head_dim]], axis=1)
        whole = jnp.concatenate([d_all[...], o_all[:, :head_dim]], axis=1).reshape(size, tok, 4 * head_dim)
        pbuf[...] = jnp.concatenate([whole[:, :tok // 2], whole[:, tok // 2:]], axis=2)
        store_parts(b).start()

    width = min(1280, hidden)

    def gradient(p):
        d = jnp.concatenate([d_all[rows_at(p, e), :] for e in range(side)], axis=0)
        o = jnp.concatenate([o_all[rows_at(p, e), :] for e in range(side)], axis=0)[:, :head_dim]

        def columns(n, carry):
            at = pl.ds(pl.multiple_of(n * width, width), width)
            term = dot(d, rows_of(p, 1, at), 0, 0)
            row = 0
            for ref in (gwa_ref, gwb_ref, gwc_ref):
                ref[:, at] += term[row:row + ref.shape[0]]
                row += ref.shape[0]
            gwo_ref[:head_dim, at] += dot(o, rows_of(p, 0, at), 0, 0)
            gwo_ref[head_dim:, at] += term[row:]
            return carry

        lax.fori_loop(0, hidden // width, columns, 0)

    count = seq_len // q_block
    last = pieces - 1
    tasks = {(0, READY - 3): [lambda b: each(0, last, lambda p: start_piece(b, p))],
             (0, READY - 2): [lambda b: each(0, last - 1, lambda p: project(b, p))],
             (0, READY - 1): [lambda b: project(b, last - 1)],
             (0, READY): [lambda b: start_piece(b, last)],
             (0, READY + 1): [lambda b: project(b, last)],
             (0, READY + 7): [finish],
             (0, READY + 8): [lambda b: each(0, pieces // 2, gradient)],
             (1, 0): [lambda b: each(pieces // 2, pieces, gradient)],
             (1, 1): [lambda b: store_parts(b).wait()]}
    spot = (2, 2, 2, 3, 3, 4, 5, 6)
    for i in range(count):
        tasks.setdefault((0, READY + spot[i]), []).append(lambda b, i=i: attend(b, i))

    for ref in (gwa_ref, gwb_ref, gwc_ref, gwo_ref):
        ref[...] = jnp.zeros_like(ref)

    def phase_of(i, place):
        return i - 1 if place == LATE else i

    def among(b):
        return jnp.logical_and(b >= 0, b < batch)

    def turn(i, carry):
        for place in range(places):
            came = (place - LAG) % places
            b_came = phase_of(i if place >= LAG else i - 1, came)

            @pl.when(among(b_came))
            def _():
                for link in range(4):
                    arrival(b_came, link, came).wait_recv()
                    share(b_came, link, came, 0).start()

            b_send = phase_of(i, place)

            @pl.when(among(b_send))
            def _():
                for link in range(4):
                    send(b_send, link, place).start()

            shared = (place - LAG - 1) % places
            b_shared = phase_of(i if place >= LAG + 1 else i - 1, shared)

            @pl.when(among(b_shared))
            def _():
                for link in range(4):
                    share(b_shared, link, shared, flip).wait_recv()

            if place == 1:
                @pl.when(i == 0)
                def _():
                    for b in range(batch):
                        share_own(b, me).start()
                        keep_own(b).start()
                    meta.start()

            if place == READY - 3:
                @pl.when(i == 1)
                def _():
                    for load in (load_wq, load_wo):
                        load.wait()
                    meta.wait_recv()
                    for j in range(size):
                        rowbuf[:, j * tok:(j + 1) * tok] = metabuf[j, :, :tok]
                    for b in range(batch):
                        share_own(b, sibling).wait_recv()
                        keep_own(b).wait()
                    meta.wait_send()
                    for b in range(batch):
                        share_own(b, me).wait_send()

            if place == READY:
                @pl.when(i == batch)
                def _():
                    for copy in own_parts + trades:
                        copy.start()

            for later in (0, 1):
                if (later, place) in tasks:
                    @pl.when(among(i - 1 - later))
                    def _():
                        for task in tasks[later, place]:
                            task(i - 1 - later)
        return carry

    lax.fori_loop(0, batch + 2, turn, 0)
    for copy in own_parts:
        copy.wait()
    for trade in trades:
        trade.wait_recv()
        trade.wait_send()
    sent = gat_ref.at[:, pl.ds(0, places), 0]
    for link in range(4):
        for sem in (ici_send, d2d_send):
            pltpu.make_async_remote_copy(
                src_ref=sent, dst_ref=sent, send_sem=sem.at[link], recv_sem=ici_recv.at[link, 0],
                device_id={"sp": sibling}, device_id_type=MESH).wait_send()


def split_rows(rows):
    first, short, own = 8 * (rows * 16 // 240), 8 * (rows // 80 or 1), 8 * (rows // 60 or 1)
    return first, rows - first - short - own, short, own


def block_call(x, dy, gain, shift, pos, keep, wq, bias, wo, size, q_block, collective_id):
    batch, tok, hidden = x.shape
    rows = tok // COLOURS
    heads, head_dim, _ = wo.shape
    pad_dim = -(-head_dim // LANES) * LANES
    seq_len = size * tok
    side = math.isqrt(size // 2)
    places = PLACES
    anywhere = pl.BlockSpec(memory_space=pl.ANY)
    vmem = pl.BlockSpec(memory_space=pltpu.VMEM)
    sem = pltpu.SemaphoreType.DMA
    bf16, f32 = jnp.bfloat16, jnp.float32
    flops = batch * (6 * seq_len * seq_len * 256 + 4 * seq_len * 4 * head_dim * hidden) + 80_000_000_000
    cut = (batch, COLOURS, rows, hidden)
    first, second, short, own = split_rows(3 * head_dim)
    return pl.pallas_call(
        functools.partial(block_kernel, size, (batch, tok, head_dim, pad_dim, hidden, min(q_block, seq_len))),
        out_shape=(
            jax.ShapeDtypeStruct((batch, size, COLOURS, 2, rows, hidden), bf16),
            jax.ShapeDtypeStruct((batch, size, tok // 2, 8 * head_dim), bf16),
            jax.ShapeDtypeStruct((EARLY, size, tok // 2, 8 * head_dim), bf16),
            *(jax.ShapeDtypeStruct((n, hidden), f32) for n in (first, second, short, head_dim + own)),
        ),
        in_specs=[anywhere, anywhere, vmem, vmem, vmem, vmem, anywhere, vmem, anywhere],
        out_specs=(anywhere, anywhere, anywhere, vmem, vmem, vmem, vmem),
        scratch_shapes=[
            pltpu.VMEM(cut, bf16),
            pltpu.VMEM((batch, COLOURS, 2, rows, hidden), bf16),
            pltpu.VMEM((3 * head_dim, hidden), bf16),
            pltpu.VMEM((head_dim, hidden), bf16),
            pltpu.VMEM((8, LANES), jnp.int32),
            pltpu.VMEM((size, 8, LANES), jnp.int32),
            pltpu.VMEM((8, seq_len), jnp.int32),
            pltpu.VMEM((side, side, 2, COLOURS, 2, rows, hidden), bf16),
            pltpu.VMEM((seq_len, 3 * pad_dim), bf16),
            pltpu.VMEM((seq_len, pad_dim), bf16),
            pltpu.VMEM((seq_len, pad_dim), f32),
            pltpu.VMEM((seq_len, pad_dim), f32),
            pltpu.VMEM((seq_len, pad_dim), bf16),
            pltpu.VMEM((seq_len, pad_dim), bf16),
            pltpu.VMEM((seq_len, 3 * head_dim), bf16),
            pltpu.VMEM((size, tok // 2, 8 * head_dim), bf16),
            sem((4 + EARLY,)), sem((batch,)), sem((side, side)), sem,
            sem((4,)), sem((4, places)), sem((4,)), sem((4, places)), sem((batch,)), sem((batch,)), sem, sem, sem((EARLY,)), sem((EARLY,)),
        ],
        compiler_params=pltpu.CompilerParams(collective_id=collective_id, has_side_effects=True, vmem_limit_bytes=VMEM_LIMIT),
        cost_estimate=pl.CostEstimate(flops=flops, bytes_accessed=60_000_000, transcendentals=batch * seq_len * seq_len // 2),
        name="block",
    )(x.reshape(cut), dy.reshape(cut), gain, shift, pos, keep, wq, bias, wo)


class Spread:
    def __init__(self, size, own_ref, gat_ref, stage, sems):
        self.torus, self.size, self.gat_ref, self.stage = Torus(size), size, gat_ref, stage
        self.load_sem, self.keep_sem, self.ici_send, self.ici_recv, self.d2d_send, self.d2d_recv, self.own_send, self.own_recv = sems
        self.part = stage.shape[1] // COLOURS
        self.load = pltpu.make_async_copy(own_ref, stage, self.load_sem)
        self.keep = pltpu.make_async_copy(stage, gat_ref.at[self.torus.me], self.keep_sem)

    def columns(self, colour):
        return pl.ds(colour * self.part, self.part)

    def view(self, block, colour):
        return self.gat_ref.at[block, :, self.columns(colour)]

    def remote(self, src, dst, send_sem, recv_sem, device):
        return pltpu.make_async_remote_copy(
            src_ref=src, dst_ref=dst, send_sem=send_sem, recv_sem=recv_sem, device_id={"sp": device}, device_id_type=MESH)

    def send(self, link, place):
        block, colour = self.torus.chunk(link, place, 0)
        dst = self.view(block, colour)
        src = self.stage.at[:, self.columns(colour)] if is_own(place) else dst
        return self.remote(src, dst, self.ici_send.at[link], self.ici_recv.at[link, place], self.torus.neighbour(link))

    def arrival(self, link, place):
        ref = self.view(*self.torus.chunk(link, place, 1))
        return self.remote(ref, ref, self.ici_send.at[link], self.ici_recv.at[link, place], self.torus.me)

    def share(self, link, place, shift):
        block, colour = self.torus.chunk(link, place, 1)
        ref = self.view(block + shift, colour)
        return self.remote(ref, ref, self.d2d_send.at[link], self.d2d_recv.at[link, place], self.torus.sibling)

    def share_own(self, block):
        return self.remote(self.stage, self.gat_ref.at[block], self.own_send, self.own_recv, self.torus.sibling)

    STEPS = PLACES + LATE + LAG + 2

    def step(self, g):
        def place_of(g):
            place = g % PLACES
            return place if g >= 0 and g // PLACES == (1 if place == LATE else 0) else None

        came, now, shared = place_of(g - LAG), place_of(g), place_of(g - LAG - 1)
        for link in range(4):
            if came is not None:
                self.arrival(link, came).wait_recv()
                self.share(link, came, 0).start()
        for link in range(4):
            if now is not None:
                self.send(link, now).start()
        for link in range(4):
            if shared is not None:
                self.share(link, shared, self.torus.flip).wait_recv()
        if g == 1:
            self.share_own(self.torus.me).start()
            self.keep.start()

    def close(self):
        self.share_own(self.torus.sibling).wait_recv()
        self.keep.wait()
        self.share_own(self.torus.me).wait_send()
        sent = self.gat_ref.at[pl.ds(0, PLACES), :, pl.ds(0, self.part)]
        for link in range(4):
            for sem in (self.ici_send, self.d2d_send):
                self.remote(sent, sent, sem.at[link], self.ici_recv.at[link, 0], self.torus.sibling).wait_send()

    @staticmethod
    def scratch(rows, cols, dtype):
        sem = pltpu.SemaphoreType.DMA
        return [pltpu.VMEM((rows, cols), dtype), sem, sem, sem((4,)), sem((4, PLACES)), sem((4,)), sem((4, PLACES)), sem, sem]


def spread_kernel(size, own_ref, after_ref, gat_ref, stage, *sems):
    spread = Spread(size, own_ref, gat_ref, stage, sems)
    spread.load.start()
    greet_all(spread.torus.me, size)
    spread.load.wait()
    for g in range(Spread.STEPS):
        spread.step(g)
    spread.close()


def spread_rows(block, after, size, collective_id):
    rows, cols = block.shape
    anywhere = pl.BlockSpec(memory_space=pl.ANY)
    return pl.pallas_call(
        functools.partial(spread_kernel, size),
        out_shape=jax.ShapeDtypeStruct((size, rows, cols), block.dtype),
        in_specs=[anywhere, anywhere],
        out_specs=anywhere,
        scratch_shapes=Spread.scratch(rows, cols, block.dtype),
        compiler_params=pltpu.CompilerParams(collective_id=collective_id, has_side_effects=True),
        cost_estimate=pl.CostEstimate(flops=50_000_000_000, bytes_accessed=8 * size * rows * cols, transcendentals=0),
        name="spread",
    )(block, after)


TOKEN_AT = 8
TOKEN_STEPS = 8


def token_kernel(size, head_dim, chunk, own_ref, parts_ref, early_ref, wq_ref, wo_ref, x_ref, dy_ref, gain_ref, bout_ref,
                 gat_ref, late_ref, y_ref, gx_ref, totals_ref,
                 stage, load_sem, keep_sem, ici_send, ici_recv, d2d_send, d2d_recv, own_send, own_recv,
                 wqbuf, wobuf, pbuf, dn_acc, y_acc, sums, tiles, come, total,
                 part_send, part_recv, own_part_sems, wq_sems, wo_sems, p_sems, deal_send, deal_recv, collect_send, collect_recv):
    spread = Spread(size, own_ref, gat_ref, stage,
                    (load_sem, keep_sem, ici_send, ici_recv, d2d_send, d2d_recv, own_send, own_recv))
    me = spread.torus.me
    early, late = early_ref.shape[0], late_ref.shape[0]
    heads, hidden = wq_ref.shape[0], wq_ref.shape[2]
    per = heads // TOKEN_STEPS
    trades, own_parts = [], []
    for n in range(late):
        b = parts_ref.shape[0] - late + n
        trades.append(Direct(me, size, lambda j, b=b: parts_ref.at[b, j], lambda j, n=n: late_ref.at[n, j], late_ref.at[n],
                             part_send.at[n], part_recv.at[n]))
        own_parts.append(pltpu.make_async_copy(parts_ref.at[b, me], late_ref.at[n, me], own_part_sems.at[n]))
    deal = Direct(me, size, lambda j: tiles.at[j], lambda j: come.at[j], come, deal_send, deal_recv)
    collect = Direct(me, size, lambda j: total, lambda j: totals_ref.at[j], totals_ref, collect_send, collect_recv)

    def weights(m):
        at, slot = pl.ds(m * per, per), m % 2
        return (pltpu.make_async_copy(wq_ref.at[at], wqbuf.at[slot], wq_sems.at[slot]),
                pltpu.make_async_copy(wo_ref.at[at], wobuf.at[slot], wo_sems.at[slot]))

    def rows(m):
        at, slot = pl.ds(m * per, per), m % 2
        sources = [early_ref.at[n, at] for n in range(early)] + [late_ref.at[n, at] for n in range(late)]
        return [pltpu.make_async_copy(src, pbuf.at[slot, n], p_sems.at[slot, n]) for n, src in enumerate(sources)]

    spread.load.start()
    for copy in weights(0):
        copy.start()
    dn_acc[...] = jnp.zeros_like(dn_acc)
    y_acc[...] = jnp.zeros_like(y_acc)
    sums[...] = jnp.zeros_like(sums)
    tiles[...] = jnp.zeros_like(tiles)
    width = hidden // 4

    def heads_step(m):
        slot = m % 2
        for copy in (*weights(m), *rows(m)):
            copy.wait()
        if m + 1 < TOKEN_STEPS:
            for copy in (*weights(m + 1), *rows(m + 1)):
                copy.start()

        def pair(i, carry):
            ds, os = [], []
            for h in range(2):
                parts = []
                for n in range(early + late):
                    both = pbuf[slot, n, i * 2 + h]
                    parts += [both[:, :4 * head_dim], both[:, 4 * head_dim:]]
                parts = jnp.concatenate(parts, axis=0)
                ds.append(parts[:, :3 * head_dim])
                os.append(parts[:, 3 * head_dim:])
                added = jnp.sum(ds[h].astype(jnp.float32), axis=0, keepdims=True)
                for c in range(3):
                    tiles[m * per + i * 2 + h, 3 + c:4 + c, 0:head_dim] = added[:, c * head_dim:(c + 1) * head_dim]

            def columns(n, carry):
                at = pl.ds(pl.multiple_of(n * width, width), width)
                dn_acc[:, at] += dot(ds[0], wqbuf[slot, i * 2, :, at], 1, 0) + dot(ds[1], wqbuf[slot, i * 2 + 1, :, at], 1, 0)
                y_acc[:, at] += dot(os[0], wobuf[slot, i * 2, :, at], 1, 0) + dot(os[1], wobuf[slot, i * 2 + 1, :, at], 1, 0)
                return carry

            lax.fori_loop(0, 4, columns, 0)
            return carry

        lax.fori_loop(0, per // 2, pair, 0)

    def norm_step(half):
        gain = gain_ref[...].reshape(1, hidden)
        bout = bout_ref[...].reshape(1, hidden)
        count = x_ref.shape[0] // chunk

        def body(c, carry):
            at = pl.ds(pl.multiple_of(c * chunk, chunk), chunk)
            x = x_ref[at, :].astype(jnp.float32)
            dy = dy_ref[at, :].astype(jnp.float32)
            centered = x - jnp.mean(x, axis=-1, keepdims=True)
            inv_std = lax.rsqrt(jnp.mean(centered * centered, axis=-1, keepdims=True) + NORM_EPS)
            x_hat = centered * inv_std
            d_norm = dn_acc[at, :]
            d_hat = d_norm * gain
            d_mean = jnp.mean(d_hat, axis=-1, keepdims=True)
            d_proj = jnp.mean(d_hat * x_hat, axis=-1, keepdims=True)
            gx_ref[at, :] = (dy + inv_std * (d_hat - d_mean - x_hat * d_proj)).astype(jnp.bfloat16)
            y_ref[at, :] = (x + y_acc[at, :] + bout).astype(jnp.bfloat16)
            sums[0:1, :] += jnp.sum(d_norm * x_hat, axis=0, keepdims=True)
            sums[1:2, :] += jnp.sum(d_norm, axis=0, keepdims=True)
            sums[2:3, :] += jnp.sum(dy, axis=0, keepdims=True)
            return carry

        lax.fori_loop(half * count // 2, (half + 1) * count // 2, body, 0)

    greet_all(me, size)
    spread.load.wait()
    for g in range(Spread.STEPS):
        spread.step(g)
        m = g - TOKEN_AT
        if g == 1:
            for copy in trades + own_parts:
                copy.start()
        if m == 0:
            for copy in own_parts:
                copy.wait()
            for trade in trades:
                trade.wait_recv()
            for copy in rows(0):
                copy.start()
        if 0 <= m < TOKEN_STEPS:
            heads_step(m)
        elif m in (TOKEN_STEPS, TOKEN_STEPS + 1):
            norm_step(m - TOKEN_STEPS)
        elif m == TOKEN_STEPS + 2:
            for j in range(size):
                tiles[j, 0:3, 0:head_dim] = sums[0:3, j * head_dim:(j + 1) * head_dim]
            come[me] = tiles[me]
        elif m == TOKEN_STEPS + 3:
            deal.start()
        elif m == TOKEN_STEPS + 5:
            deal.wait_recv()
            total[...] = jnp.sum(come[...], axis=0)
            totals_ref[me] = total[...]
            collect.start()
    spread.close()
    for trade in trades:
        trade.wait_send()
    deal.wait_send()
    collect.wait_recv()
    collect.wait_send()


def token_side(block, parts, early, wq, wo, x, dy, gain, bout, size, collective_id):
    rows, cols = block.shape
    late = parts.shape[0] - early.shape[0]
    heads, head_dim, hidden = wo.shape
    tokens = x.shape[0]
    per = heads // TOKEN_STEPS
    anywhere = pl.BlockSpec(memory_space=pl.ANY)
    vmem = pl.BlockSpec(memory_space=pltpu.VMEM)
    sem = pltpu.SemaphoreType.DMA
    bf16, f32 = jnp.bfloat16, jnp.float32
    return pl.pallas_call(
        functools.partial(token_kernel, size, head_dim, 16),
        out_shape=(
            jax.ShapeDtypeStruct((size, rows, cols), block.dtype),
            jax.ShapeDtypeStruct((late, *parts.shape[1:]), parts.dtype),
            jax.ShapeDtypeStruct((tokens, hidden), bf16),
            jax.ShapeDtypeStruct((tokens, hidden), bf16),
            jax.ShapeDtypeStruct((size, 8, LANES), f32),
        ),
        in_specs=[anywhere] * 5 + [vmem] * 4,
        out_specs=(anywhere, anywhere, vmem, vmem, vmem),
        scratch_shapes=Spread.scratch(rows, cols, block.dtype) + [
            pltpu.VMEM((2, per, 3 * head_dim, hidden), bf16),
            pltpu.VMEM((2, per, head_dim, hidden), bf16),
            pltpu.VMEM((2, parts.shape[0], per, *parts.shape[2:]), bf16),
            pltpu.VMEM((tokens, hidden), f32),
            pltpu.VMEM((tokens, hidden), f32),
            pltpu.VMEM((8, hidden), f32),
            pltpu.VMEM((size, 8, LANES), f32),
            pltpu.VMEM((size, 8, LANES), f32),
            pltpu.VMEM((8, LANES), f32),
            sem((late,)), sem((late,)), sem((late,)), sem((2,)), sem((2,)), sem((2, parts.shape[0])), sem, sem, sem, sem,
        ],
        compiler_params=pltpu.CompilerParams(collective_id=collective_id, has_side_effects=True, vmem_limit_bytes=VMEM_LIMIT),
        cost_estimate=pl.CostEstimate(flops=120_000_000_000, bytes_accessed=8 * size * rows * cols, transcendentals=0),
        name="token_side",
    )(block, parts, early, wq, wo, x, dy, gain, bout)


def hand_kernel(y_ref, gx_ref, y_out, gx_out):
    y_out[...] = y_ref[...]
    gx_out[...] = gx_ref[...]


def hand_over(y, gx):
    spec = pl.BlockSpec((y.shape[0] // 4, y.shape[1]), lambda i: (i, 0))
    return pl.pallas_call(
        hand_kernel, grid=(4,), out_shape=(jax.ShapeDtypeStruct(y.shape, y.dtype),) * 2, in_specs=[spec] * 2, out_specs=(spec,) * 2,
        cost_estimate=pl.CostEstimate(flops=1_000_000_000, bytes_accessed=8 * y.size, transcendentals=0), name="hand_over")(y, gx)


def settle_kernel(block, depth, ahead, per, origin, first, src_ref, *refs):
    dst_ref, buf, read_sems, write_sems = refs[-4:]
    count = src_ref.shape[0] * per

    def slab(ref, i, start):
        return ref.at[i // per, pl.ds(pl.multiple_of(start + lax.rem(i, per) * block, 8), block)]

    def read(i):
        return pltpu.make_async_copy(slab(src_ref, i, origin), buf.at[lax.rem(i, depth)], read_sems.at[lax.rem(i, depth)])

    def write(i):
        return pltpu.make_async_copy(buf.at[lax.rem(i, depth)], slab(dst_ref, i, first), write_sems.at[lax.rem(i, depth)])

    def step(i, carry):
        @pl.when(jnp.logical_and(i >= depth, i < count))
        def _():
            write(i - depth).wait()

        @pl.when(i < count)
        def _():
            read(i).start()

        @pl.when(i >= ahead)
        def _():
            read(i - ahead).wait()
            write(i - ahead).start()

        return carry

    lax.fori_loop(0, count + ahead, step, 0)

    def drain(i, carry):
        write(i).wait()
        return carry

    lax.fori_loop(max(0, count - depth), count, drain, 0)


def settle(x, origin, rows, first, total, pieces=1, into=None, after=()):
    block = rows // pieces
    depth, ahead = 12, 6
    count, _, cols = x.shape
    sem = pltpu.SemaphoreType.DMA((depth,))
    old = [] if into is None else [into]
    return pl.pallas_call(
        functools.partial(settle_kernel, block, depth, ahead, pieces, origin, first),
        out_shape=jax.ShapeDtypeStruct((count, total, cols), x.dtype),
        in_specs=[pl.BlockSpec(memory_space=pl.ANY)] * (1 + len(old) + len(after)),
        out_specs=pl.BlockSpec(memory_space=pl.ANY),
        scratch_shapes=[pltpu.VMEM((depth, block, cols), x.dtype), sem, sem],
        input_output_aliases={1: 0} if old else {},
        compiler_params=pltpu.CompilerParams(vmem_limit_bytes=VMEM_LIMIT),
        cost_estimate=pl.CostEstimate(flops=10_000_000_000, bytes_accessed=8 * x.size, transcendentals=0),
        name="settle",
    )(x, *old, *after)


def solution(mesh):
    size = mesh.shape["sp"]

    def block_fn(x_blk, pos_blk, keep_blk, ln_gain, ln_bias, w_qkv, b_qkv, w_out, b_out, dy_blk):
        batch, tok, hidden = x_blk.shape
        heads, head_dim = w_qkv.shape[1], w_qkv.shape[3]
        tokens = batch * tok
        wq = jnp.transpose(w_qkv, (1, 2, 3, 0)).reshape(heads, 3 * head_dim, hidden)
        wo = w_out.reshape(heads, head_dim, hidden)

        def gather(a):
            return lax.all_gather(a, "sp", axis=0, tiled=True).reshape(heads, a.shape[0], hidden)

        _, parts, early, grad_a, grad_b, grad_c, grad_out = block_call(
            x_blk, dy_blk, ln_gain, ln_bias, pos_blk, keep_blk, wq, jnp.transpose(b_qkv, (1, 0, 2)), wo, size, 256, 0)

        all_out, _, y, grad_x, totals = token_side(
            grad_out, parts, early, wq, wo, x_blk.reshape(tokens, hidden), dy_blk.reshape(tokens, hidden), ln_gain, b_out, size, 1)
        y, grad_x = hand_over(y, grad_x)
        grad_wo = settle(all_out, 0, head_dim, 0, head_dim, after=(y,))

        rows = 3 * head_dim
        first, second, short, own = split_rows(rows)
        grad_wq = settle(all_out, head_dim, own, first + second + short, rows, after=(grad_wo,))
        all_a = gather(grad_a)
        all_c = spread_rows(grad_c, all_a, size, 2)
        grad_wq = settle(all_a, 0, first, 0, rows, into=grad_wq, after=(all_c,))
        grad_wq = settle(all_c, 0, short, first + second, rows, into=grad_wq)
        grad_wq = settle(gather(grad_b), 0, second, first, rows, into=grad_wq)
        totals = totals[:, :, :head_dim]
        grad_wq = jnp.transpose(grad_wq.reshape(heads, 3, head_dim, hidden), (3, 0, 1, 2))
        return (y.reshape(x_blk.shape), grad_x.reshape(x_blk.shape), grad_wq, totals[:, 3:6],
                grad_wo.reshape(heads * head_dim, hidden), totals[:, 2].reshape(-1), totals[:, 0].reshape(-1), totals[:, 1].reshape(-1))

    act_spec = P("dp", "sp", None)
    tok_spec = P("dp", "sp")
    in_specs = (act_spec, tok_spec, tok_spec, P(), P(), P(), P(), P(), P(), act_spec)
    out_specs = (act_spec, act_spec, P("dp", None, None, None), P("dp", None, None), P("dp", None), P("dp"), P("dp"), P("dp"))
    return jax.shard_map(block_fn, mesh=mesh, in_specs=in_specs, out_specs=out_specs, check_vma=False)
```

```python
import functools
import math

import jax
import jax.numpy as jnp
from jax import lax
from jax.experimental import pallas as pl
from jax.experimental.pallas import tpu as pltpu
from jax.sharding import PartitionSpec as P

NORM_EPS = 1e-5
MASK_FILL = -1e30
LANES = 128
LOG2E = 1.4426950408889634
MESH = pl.DeviceIdType.MESH
VMEM_LIMIT = 61 * 1024 * 1024


def dot(a, b, ca, cb):
    return lax.dot_general(a, b, (((ca,), (cb,)), ((), ())), preferred_element_type=jnp.float32)


def greet_all(me, size, meanwhile=lambda: None):
    barrier = pltpu.get_barrier_semaphore()

    def greet(d, carry):
        pl.semaphore_signal(barrier, inc=1, device_id={"sp": lax.rem(me + d, size)}, device_id_type=MESH)
        return carry

    lax.fori_loop(1, size, greet, 0)
    meanwhile()
    pl.semaphore_wait(barrier, size - 1)


class Direct:
    def __init__(self, me, size, src, dst, whole, send_sem, recv_sem):
        self.me, self.size, self.src, self.dst, self.whole, self.send_sem, self.recv_sem = me, size, src, dst, whole, send_sem, recv_sem

    def start(self):
        def body(d, carry):
            peer = lax.rem(self.me + d, self.size)
            pltpu.make_async_remote_copy(
                src_ref=self.src(peer), dst_ref=self.dst(self.me), send_sem=self.send_sem, recv_sem=self.recv_sem,
                device_id={"sp": peer}, device_id_type=MESH).start()
            return carry

        lax.fori_loop(1, self.size, body, 0)

    def total(self):
        ref = self.whole.at[pl.ds(0, self.size - 1)]
        return pltpu.make_async_remote_copy(
            src_ref=ref, dst_ref=ref, send_sem=self.send_sem, recv_sem=self.recv_sem,
            device_id={"sp": self.me}, device_id_type=MESH)

    def wait_recv(self):
        self.total().wait_recv()

    def wait_send(self):
        self.total().wait_send()


FIRST_OF = (2, 3, 0, 1)
CYCLE = (("P", 0), ("Q", 0, 0), ("Q", 3, 2), ("P", 1), ("Q", 0, 1), ("Q", 1, 0), ("Q", 2, 0), ("P", 2), ("Q", 1, 1),
         ("Q", 2, 1), ("Q", 3, 0), ("Q", 1, 2), ("Q", 2, 2), ("Q", 3, 1), ("Q", 0, 2))
LATE = 2
LAG = 3
COLOURS = 4
READY = 6
EARLY = 1
STEP_OF = ((1, 0), (-1, 0), (0, 1), (0, -1))
PLACES = len(CYCLE)


class Torus:
    def __init__(self, size):
        self.side = math.isqrt(size // 2)
        self.me = lax.axis_index("sp")
        self.core = lax.rem(self.me, 2)
        chip = self.me // 2
        self.cx, self.cy = lax.rem(chip, self.side), chip // self.side
        self.flip = 1 - 2 * self.core
        self.sibling = self.me + self.flip

    def device_at(self, dx, dy):
        side = self.side
        return (lax.rem(self.cy + dy + side, side) * side + lax.rem(self.cx + dx + side, side)) * 2 + self.core

    def neighbour(self, link):
        return self.device_at(*STEP_OF[link])

    def chunk(self, link, place, ahead):
        what = CYCLE[place]
        if what[0] == "P":
            first, n, m = link, what[1] + ahead, 0
        else:
            first, n, m = FIRST_OF[link], what[2] + ahead, what[1]
        dx = -STEP_OF[link][0] * n - STEP_OF[first][0] * m
        dy = -STEP_OF[link][1] * n - STEP_OF[first][1] * m
        return self.device_at(dx, dy), first


def is_own(place):
    return CYCLE[place] in (("P", 0), ("Q", 0, 0))


def block_kernel(size, dims, x_ref, dy_ref, gain_ref, shift_ref, pos_ref, keep_ref, wq_ref, bias_ref, wo_ref,
                 gat_ref, parts_ref, partstok_ref, gwa_ref, gwb_ref, gwc_ref, gwo_ref,
                 xin, stage, wbuf, wobuf, metatile, metabuf, rowbuf, sbuf, qkvb, dob, dk_acc, dv_acc, dq_all, o_all, d_all, pbuf,
                 load_sems, own_sems, piece_sems, parts_sem, ici_send, ici_recv, d2d_send, d2d_recv, own_send, own_recv,
                 meta_send, meta_recv, part_send, part_recv):
    batch, tok, head_dim, pad_dim, hidden, q_block = dims
    seq_len = size * tok
    torus = Torus(size)
    me, flip, sibling, side = torus.me, torus.flip, torus.sibling, torus.side
    places = PLACES
    scale = head_dim ** -0.5
    heads = wo_ref.shape[0]
    slope = jnp.exp2(jnp.full((1, 1), -8.0 / heads, jnp.float32) * (me + 1).astype(jnp.float32))

    def send(b, link, place):
        block, colour = torus.chunk(link, place, 0)
        dst = gat_ref.at[b, block, colour]
        return pltpu.make_async_remote_copy(
            src_ref=stage.at[b, colour] if is_own(place) else dst, dst_ref=dst,
            send_sem=ici_send.at[link], recv_sem=ici_recv.at[link, place],
            device_id={"sp": torus.neighbour(link)}, device_id_type=MESH)

    def arrival(b, link, place):
        block, colour = torus.chunk(link, place, 1)
        ref = gat_ref.at[b, block, colour]
        return pltpu.make_async_remote_copy(
            src_ref=ref, dst_ref=ref, send_sem=ici_send.at[link], recv_sem=ici_recv.at[link, place],
            device_id={"sp": me}, device_id_type=MESH)

    def share(b, link, place, shift):
        block, colour = torus.chunk(link, place, 1)
        ref = gat_ref.at[b, block + shift, colour]
        return pltpu.make_async_remote_copy(
            src_ref=ref, dst_ref=ref, send_sem=d2d_send.at[link], recv_sem=d2d_recv.at[link, place],
            device_id={"sp": sibling}, device_id_type=MESH)

    def share_own(b, block):
        return pltpu.make_async_remote_copy(
            src_ref=stage.at[b], dst_ref=gat_ref.at[b, block], send_sem=own_send.at[b], recv_sem=own_recv.at[b],
            device_id={"sp": sibling}, device_id_type=MESH)

    def keep_own(b):
        return pltpu.make_async_copy(stage.at[b], gat_ref.at[b, me], own_sems.at[b])

    load_x = pltpu.make_async_copy(x_ref, xin, load_sems.at[0])
    load_dy = pltpu.make_async_copy(dy_ref, stage.at[:, :, 0], load_sems.at[1])
    load_wq = pltpu.make_async_copy(wq_ref.at[me], wbuf, load_sems.at[2])
    load_wo = pltpu.make_async_copy(wo_ref.at[me], wobuf, load_sems.at[3])
    for load in (load_x, load_dy, load_wq, load_wo):
        load.start()
    meta = Direct(me, size, lambda j: metatile, lambda j: metabuf.at[j], metabuf, meta_send, meta_recv)
    early = partstok_ref.shape[0]
    trades = [Direct(me, size, lambda j, b=b: parts_ref.at[b, j], lambda j, b=b: partstok_ref.at[b, j], partstok_ref.at[b],
                     part_send.at[b], part_recv.at[b]) for b in range(early)]
    own_parts = [pltpu.make_async_copy(parts_ref.at[b, me], partstok_ref.at[b, me], load_sems.at[4 + b]) for b in range(early)]

    def prepare():
        metatile[...] = jnp.zeros_like(metatile)
        metatile[0:batch, 0:tok] = pos_ref[...]
        metatile[batch:2 * batch, 0:tok] = keep_ref[...]
        metabuf[me] = metatile[...]
        load_x.wait()

        gain, shift = gain_ref[...].reshape(1, 1, hidden), shift_ref[...].reshape(1, 1, hidden)

        def normalise(b, carry):
            x = xin[b].astype(jnp.float32)
            centered = x - jnp.mean(x, axis=-1, keepdims=True)
            inv_std = lax.rsqrt(jnp.mean(centered * centered, axis=-1, keepdims=True) + NORM_EPS)
            stage[b, :, 1] = (centered * inv_std * gain + shift).astype(jnp.bfloat16)
            return carry

        lax.fori_loop(0, batch, normalise, 0)
        load_dy.wait()

    greet_all(me, size, prepare)

    pieces = sbuf.shape[0]
    chip_rows = 2 * tok

    def chip_of(p, e):
        return torus.device_at(lax.rem(p + 1 + e, side), e) // 2

    def rows_at(p, e):
        return pl.ds(pl.multiple_of(chip_of(p, e) * chip_rows, chip_rows), chip_rows)

    def load_piece(b, p):
        return [pltpu.make_async_copy(gat_ref.at[b, pl.ds(chip_of(p, e) * 2, 2)], sbuf.at[p, e], piece_sems.at[p, e]) for e in range(side)]

    def start_piece(b, p):
        for load in load_piece(b, p):
            load.start()

    def rows_of(p, which, at=slice(None)):
        return sbuf[p, :, :, :, which, :, at].reshape(side * chip_rows, -1)

    def each(lo, hi, use):
        def body(p, carry):
            use(p)
            return carry

        lax.fori_loop(lo, hi, body, 0)

    def pad_lanes(a):
        return jnp.concatenate([a, jnp.zeros((a.shape[0], pad_dim - head_dim), a.dtype)], axis=1)

    def project(b, p):
        for load in load_piece(b, p):
            load.wait()
        bias = jnp.concatenate([bias_ref[c, pl.ds(me, 1), :] for c in range(3)], axis=1)
        r = (dot(rows_of(p, 1), wbuf[...], 1, 1) + bias).astype(jnp.bfloat16)
        d = pad_lanes(dot(rows_of(p, 0), wobuf[...], 1, 1).astype(jnp.bfloat16))
        q, k, v = (pad_lanes(r[:, c * head_dim:(c + 1) * head_dim]) for c in range(3))
        for e in range(side):
            mine = slice(e * chip_rows, (e + 1) * chip_rows)
            at = rows_at(p, e)
            for c, part in enumerate((q, k, v)):
                qkvb[at, c * pad_dim:(c + 1) * pad_dim] = part[mine]
            dob[at, :] = d[mine]

    def attend(b, i):
        span = (i + 1) * q_block
        mine = slice(i * q_block, span)
        if i == 0:
            dk_acc[...] = jnp.zeros_like(dk_acc)
            dv_acc[...] = jnp.zeros_like(dv_acc)
        q, k, v = qkvb[mine, :pad_dim], qkvb[:span, pad_dim:2 * pad_dim], qkvb[:span, 2 * pad_dim:]
        do = dob[mine, :]
        pos = rowbuf[pl.ds(b, 1), :span]
        keep = rowbuf[pl.ds(b + batch, 1), :span]
        bias = jnp.where(keep > 0, (-slope * LOG2E) * (pos[:, span - 1:] - pos).astype(jnp.float32), MASK_FILL)
        scores = dot(q, k, 1, 1) * (scale * LOG2E) + bias
        row_id = lax.broadcasted_iota(jnp.int32, (q_block, q_block), 0)
        col_id = lax.broadcasted_iota(jnp.int32, (q_block, q_block), 1)
        corner = jnp.where(col_id <= row_id, scores[:, span - q_block:], MASK_FILL)
        scores = jnp.concatenate([scores[:, :span - q_block], corner], axis=1) if i else corner
        expo = jnp.exp2(scores - jnp.max(scores, axis=-1, keepdims=True))
        prob = expo * (1.0 / jnp.sum(expo, axis=-1, keepdims=True))
        prob_lo = prob.astype(jnp.bfloat16)
        o = dot(prob_lo, v, 1, 0).astype(jnp.bfloat16)
        row_dot = jnp.sum(do.astype(jnp.float32) * o.astype(jnp.float32), axis=-1, keepdims=True)
        ds_lo = (prob * (dot(do, v, 1, 1) - row_dot)).astype(jnp.bfloat16)
        o_all[mine, :] = o
        dq_all[mine, :] = (dot(ds_lo, k, 1, 0) * scale).astype(jnp.bfloat16)
        dv_acc[:span, :] += dot(prob_lo, do, 0, 0)
        dk_acc[:span, :] += dot(ds_lo, q, 0, 0)

    def store_parts(b):
        return pltpu.make_async_copy(pbuf, parts_ref.at[b], parts_sem)

    def finish(b):
        dk = (dk_acc[...] * scale).astype(jnp.bfloat16)
        dv = dv_acc[...].astype(jnp.bfloat16)
        d_all[...] = jnp.concatenate([dq_all[:, :head_dim], dk[:, :head_dim], dv[:, :head_dim]], axis=1)
        whole = jnp.concatenate([d_all[...], o_all[:, :head_dim]], axis=1).reshape(size, tok, 4 * head_dim)
        pbuf[...] = jnp.concatenate([whole[:, :tok // 2], whole[:, tok // 2:]], axis=2)
        store_parts(b).start()

    width = min(1280, hidden)

    def gradient(p):
        d = jnp.concatenate([d_all[rows_at(p, e), :] for e in range(side)], axis=0)
        o = jnp.concatenate([o_all[rows_at(p, e), :] for e in range(side)], axis=0)[:, :head_dim]

        def columns(n, carry):
            at = pl.ds(pl.multiple_of(n * width, width), width)
            term = dot(d, rows_of(p, 1, at), 0, 0)
            row = 0
            for ref in (gwa_ref, gwb_ref, gwc_ref):
                ref[:, at] += term[row:row + ref.shape[0]]
                row += ref.shape[0]
            gwo_ref[:, at] += dot(o, rows_of(p, 0, at), 0, 0)
            return carry

        lax.fori_loop(0, hidden // width, columns, 0)

    count = seq_len // q_block
    last = pieces - 1
    tasks = {(0, READY - 3): [lambda b: each(0, last, lambda p: start_piece(b, p))],
             (0, READY - 2): [lambda b: each(0, last - 1, lambda p: project(b, p))],
             (0, READY - 1): [lambda b: project(b, last - 1)],
             (0, READY): [lambda b: start_piece(b, last)],
             (0, READY + 1): [lambda b: project(b, last)],
             (0, READY + 7): [finish],
             (0, READY + 8): [lambda b: each(0, pieces // 2, gradient)],
             (1, 0): [lambda b: each(pieces // 2, pieces, gradient)],
             (1, 1): [lambda b: store_parts(b).wait()]}
    spot = (2, 2, 2, 3, 3, 4, 5, 6)
    for i in range(count):
        tasks.setdefault((0, READY + spot[i]), []).append(lambda b, i=i: attend(b, i))

    for ref in (gwa_ref, gwb_ref, gwc_ref, gwo_ref):
        ref[...] = jnp.zeros_like(ref)

    def phase_of(i, place):
        return i - 1 if place == LATE else i

    def among(b):
        return jnp.logical_and(b >= 0, b < batch)

    def turn(i, carry):
        for place in range(places):
            came = (place - LAG) % places
            b_came = phase_of(i if place >= LAG else i - 1, came)

            @pl.when(among(b_came))
            def _():
                for link in range(4):
                    arrival(b_came, link, came).wait_recv()
                    share(b_came, link, came, 0).start()

            b_send = phase_of(i, place)

            @pl.when(among(b_send))
            def _():
                for link in range(4):
                    send(b_send, link, place).start()

            shared = (place - LAG - 1) % places
            b_shared = phase_of(i if place >= LAG + 1 else i - 1, shared)

            @pl.when(among(b_shared))
            def _():
                for link in range(4):
                    share(b_shared, link, shared, flip).wait_recv()

            if place == 1:
                @pl.when(i == 0)
                def _():
                    for b in range(batch):
                        share_own(b, me).start()
                        keep_own(b).start()
                    meta.start()

            if place == READY - 3:
                @pl.when(i == 1)
                def _():
                    for load in (load_wq, load_wo):
                        load.wait()
                    meta.wait_recv()
                    for j in range(size):
                        rowbuf[:, j * tok:(j + 1) * tok] = metabuf[j, :, :tok]
                    for b in range(batch):
                        share_own(b, sibling).wait_recv()
                        keep_own(b).wait()
                    meta.wait_send()
                    for b in range(batch):
                        share_own(b, me).wait_send()

            if place == READY:
                @pl.when(i == batch)
                def _():
                    for copy in own_parts + trades:
                        copy.start()

            for later in (0, 1):
                if (later, place) in tasks:
                    @pl.when(among(i - 1 - later))
                    def _():
                        for task in tasks[later, place]:
                            task(i - 1 - later)
        return carry

    lax.fori_loop(0, batch + 2, turn, 0)
    for copy in own_parts:
        copy.wait()
    for trade in trades:
        trade.wait_recv()
        trade.wait_send()
    sent = gat_ref.at[:, pl.ds(0, places), 0]
    for link in range(4):
        for sem in (ici_send, d2d_send):
            pltpu.make_async_remote_copy(
                src_ref=sent, dst_ref=sent, send_sem=sem.at[link], recv_sem=ici_recv.at[link, 0],
                device_id={"sp": sibling}, device_id_type=MESH).wait_send()


def split_rows(rows):
    first, short = 8 * (rows * 20 // 240), 8 * (rows // 60 or 1)
    return first, rows - first - short, short


def block_call(x, dy, gain, shift, pos, keep, wq, bias, wo, size, q_block, collective_id):
    batch, tok, hidden = x.shape
    rows = tok // COLOURS
    heads, head_dim, _ = wo.shape
    pad_dim = -(-head_dim // LANES) * LANES
    seq_len = size * tok
    side = math.isqrt(size // 2)
    places = PLACES
    anywhere = pl.BlockSpec(memory_space=pl.ANY)
    vmem = pl.BlockSpec(memory_space=pltpu.VMEM)
    sem = pltpu.SemaphoreType.DMA
    bf16, f32 = jnp.bfloat16, jnp.float32
    flops = batch * (6 * seq_len * seq_len * 256 + 4 * seq_len * 4 * head_dim * hidden) + 80_000_000_000
    cut = (batch, COLOURS, rows, hidden)
    first, second, short = split_rows(3 * head_dim)
    return pl.pallas_call(
        functools.partial(block_kernel, size, (batch, tok, head_dim, pad_dim, hidden, min(q_block, seq_len))),
        out_shape=(
            jax.ShapeDtypeStruct((batch, size, COLOURS, 2, rows, hidden), bf16),
            jax.ShapeDtypeStruct((batch, size, tok // 2, 8 * head_dim), bf16),
            jax.ShapeDtypeStruct((EARLY, size, tok // 2, 8 * head_dim), bf16),
            *(jax.ShapeDtypeStruct((n, hidden), f32) for n in (first, second, short, head_dim)),
        ),
        in_specs=[anywhere, anywhere, vmem, vmem, vmem, vmem, anywhere, vmem, anywhere],
        out_specs=(anywhere, anywhere, anywhere, vmem, vmem, vmem, vmem),
        scratch_shapes=[
            pltpu.VMEM(cut, bf16),
            pltpu.VMEM((batch, COLOURS, 2, rows, hidden), bf16),
            pltpu.VMEM((3 * head_dim, hidden), bf16),
            pltpu.VMEM((head_dim, hidden), bf16),
            pltpu.VMEM((8, LANES), jnp.int32),
            pltpu.VMEM((size, 8, LANES), jnp.int32),
            pltpu.VMEM((8, seq_len), jnp.int32),
            pltpu.VMEM((side, side, 2, COLOURS, 2, rows, hidden), bf16),
            pltpu.VMEM((seq_len, 3 * pad_dim), bf16),
            pltpu.VMEM((seq_len, pad_dim), bf16),
            pltpu.VMEM((seq_len, pad_dim), f32),
            pltpu.VMEM((seq_len, pad_dim), f32),
            pltpu.VMEM((seq_len, pad_dim), bf16),
            pltpu.VMEM((seq_len, pad_dim), bf16),
            pltpu.VMEM((seq_len, 3 * head_dim), bf16),
            pltpu.VMEM((size, tok // 2, 8 * head_dim), bf16),
            sem((4 + EARLY,)), sem((batch,)), sem((side, side)), sem,
            sem((4,)), sem((4, places)), sem((4,)), sem((4, places)), sem((batch,)), sem((batch,)), sem, sem, sem((EARLY,)), sem((EARLY,)),
        ],
        compiler_params=pltpu.CompilerParams(collective_id=collective_id, has_side_effects=True, vmem_limit_bytes=VMEM_LIMIT),
        cost_estimate=pl.CostEstimate(flops=flops, bytes_accessed=60_000_000, transcendentals=batch * seq_len * seq_len // 2),
        name="block",
    )(x.reshape(cut), dy.reshape(cut), gain, shift, pos, keep, wq, bias, wo)


class Spread:
    def __init__(self, size, own_ref, gat_ref, stage, sems):
        self.torus, self.size, self.gat_ref, self.stage = Torus(size), size, gat_ref, stage
        self.load_sem, self.keep_sem, self.ici_send, self.ici_recv, self.d2d_send, self.d2d_recv, self.own_send, self.own_recv = sems
        self.part = stage.shape[1] // COLOURS
        self.load = pltpu.make_async_copy(own_ref, stage, self.load_sem)
        self.keep = pltpu.make_async_copy(stage, gat_ref.at[self.torus.me], self.keep_sem)

    def columns(self, colour):
        return pl.ds(colour * self.part, self.part)

    def view(self, block, colour):
        return self.gat_ref.at[block, :, self.columns(colour)]

    def remote(self, src, dst, send_sem, recv_sem, device):
        return pltpu.make_async_remote_copy(
            src_ref=src, dst_ref=dst, send_sem=send_sem, recv_sem=recv_sem, device_id={"sp": device}, device_id_type=MESH)

    def send(self, link, place):
        block, colour = self.torus.chunk(link, place, 0)
        dst = self.view(block, colour)
        src = self.stage.at[:, self.columns(colour)] if is_own(place) else dst
        return self.remote(src, dst, self.ici_send.at[link], self.ici_recv.at[link, place], self.torus.neighbour(link))

    def arrival(self, link, place):
        ref = self.view(*self.torus.chunk(link, place, 1))
        return self.remote(ref, ref, self.ici_send.at[link], self.ici_recv.at[link, place], self.torus.me)

    def share(self, link, place, shift):
        block, colour = self.torus.chunk(link, place, 1)
        ref = self.view(block + shift, colour)
        return self.remote(ref, ref, self.d2d_send.at[link], self.d2d_recv.at[link, place], self.torus.sibling)

    def share_own(self, block):
        return self.remote(self.stage, self.gat_ref.at[block], self.own_send, self.own_recv, self.torus.sibling)

    STEPS = PLACES + LATE + LAG + 2

    def step(self, g):
        def place_of(g):
            place = g % PLACES
            return place if g >= 0 and g // PLACES == (1 if place == LATE else 0) else None

        came, now, shared = place_of(g - LAG), place_of(g), place_of(g - LAG - 1)
        for link in range(4):
            if came is not None:
                self.arrival(link, came).wait_recv()
                self.share(link, came, 0).start()
        for link in range(4):
            if now is not None:
                self.send(link, now).start()
        for link in range(4):
            if shared is not None:
                self.share(link, shared, self.torus.flip).wait_recv()
        if g == 1:
            self.share_own(self.torus.me).start()
            self.keep.start()

    def close(self):
        self.share_own(self.torus.sibling).wait_recv()
        self.keep.wait()
        self.share_own(self.torus.me).wait_send()
        sent = self.gat_ref.at[pl.ds(0, PLACES), :, pl.ds(0, self.part)]
        for link in range(4):
            for sem in (self.ici_send, self.d2d_send):
                self.remote(sent, sent, sem.at[link], self.ici_recv.at[link, 0], self.torus.sibling).wait_send()

    @staticmethod
    def scratch(rows, cols, dtype):
        sem = pltpu.SemaphoreType.DMA
        return [pltpu.VMEM((rows, cols), dtype), sem, sem, sem((4,)), sem((4, PLACES)), sem((4,)), sem((4, PLACES)), sem, sem]


def spread_kernel(size, own_ref, after_ref, gat_ref, stage, *sems):
    spread = Spread(size, own_ref, gat_ref, stage, sems)
    spread.load.start()
    greet_all(spread.torus.me, size)
    spread.load.wait()
    for g in range(Spread.STEPS):
        spread.step(g)
    spread.close()


def spread_rows(block, after, size, collective_id):
    rows, cols = block.shape
    anywhere = pl.BlockSpec(memory_space=pl.ANY)
    return pl.pallas_call(
        functools.partial(spread_kernel, size),
        out_shape=jax.ShapeDtypeStruct((size, rows, cols), block.dtype),
        in_specs=[anywhere, anywhere],
        out_specs=anywhere,
        scratch_shapes=Spread.scratch(rows, cols, block.dtype),
        compiler_params=pltpu.CompilerParams(collective_id=collective_id, has_side_effects=True),
        cost_estimate=pl.CostEstimate(flops=50_000_000_000, bytes_accessed=8 * size * rows * cols, transcendentals=0),
        name="spread",
    )(block, after)


TOKEN_AT = 8
TOKEN_STEPS = 8


def token_kernel(size, head_dim, chunk, own_ref, parts_ref, early_ref, wq_ref, wo_ref, x_ref, dy_ref, gain_ref, bout_ref,
                 gat_ref, late_ref, y_ref, gx_ref, totals_ref,
                 stage, load_sem, keep_sem, ici_send, ici_recv, d2d_send, d2d_recv, own_send, own_recv,
                 wqbuf, wobuf, pbuf, dn_acc, y_acc, sums, tiles, come, total,
                 part_send, part_recv, own_part_sems, wq_sems, wo_sems, p_sems, deal_send, deal_recv, collect_send, collect_recv):
    spread = Spread(size, own_ref, gat_ref, stage,
                    (load_sem, keep_sem, ici_send, ici_recv, d2d_send, d2d_recv, own_send, own_recv))
    me = spread.torus.me
    early, late = early_ref.shape[0], late_ref.shape[0]
    heads, hidden = wq_ref.shape[0], wq_ref.shape[2]
    per = heads // TOKEN_STEPS
    trades, own_parts = [], []
    for n in range(late):
        b = parts_ref.shape[0] - late + n
        trades.append(Direct(me, size, lambda j, b=b: parts_ref.at[b, j], lambda j, n=n: late_ref.at[n, j], late_ref.at[n],
                             part_send.at[n], part_recv.at[n]))
        own_parts.append(pltpu.make_async_copy(parts_ref.at[b, me], late_ref.at[n, me], own_part_sems.at[n]))
    deal = Direct(me, size, lambda j: tiles.at[j], lambda j: come.at[j], come, deal_send, deal_recv)
    collect = Direct(me, size, lambda j: total, lambda j: totals_ref.at[j], totals_ref, collect_send, collect_recv)

    def weights(m):
        at, slot = pl.ds(m * per, per), m % 2
        return (pltpu.make_async_copy(wq_ref.at[at], wqbuf.at[slot], wq_sems.at[slot]),
                pltpu.make_async_copy(wo_ref.at[at], wobuf.at[slot], wo_sems.at[slot]))

    def rows(m):
        at, slot = pl.ds(m * per, per), m % 2
        sources = [early_ref.at[n, at] for n in range(early)] + [late_ref.at[n, at] for n in range(late)]
        return [pltpu.make_async_copy(src, pbuf.at[slot, n], p_sems.at[slot, n]) for n, src in enumerate(sources)]

    spread.load.start()
    for copy in weights(0):
        copy.start()
    dn_acc[...] = jnp.zeros_like(dn_acc)
    y_acc[...] = jnp.zeros_like(y_acc)
    sums[...] = jnp.zeros_like(sums)
    tiles[...] = jnp.zeros_like(tiles)
    width = hidden // 4

    def heads_step(m):
        slot = m % 2
        for copy in (*weights(m), *rows(m)):
            copy.wait()
        if m + 1 < TOKEN_STEPS:
            for copy in (*weights(m + 1), *rows(m + 1)):
                copy.start()

        def pair(i, carry):
            ds, os = [], []
            for h in range(2):
                parts = []
                for n in range(early + late):
                    both = pbuf[slot, n, i * 2 + h]
                    parts += [both[:, :4 * head_dim], both[:, 4 * head_dim:]]
                parts = jnp.concatenate(parts, axis=0)
                ds.append(parts[:, :3 * head_dim])
                os.append(parts[:, 3 * head_dim:])
                added = jnp.sum(ds[h].astype(jnp.float32), axis=0, keepdims=True)
                for c in range(3):
                    tiles[m * per + i * 2 + h, 3 + c:4 + c, 0:head_dim] = added[:, c * head_dim:(c + 1) * head_dim]

            def columns(n, carry):
                at = pl.ds(pl.multiple_of(n * width, width), width)
                dn_acc[:, at] += dot(ds[0], wqbuf[slot, i * 2, :, at], 1, 0) + dot(ds[1], wqbuf[slot, i * 2 + 1, :, at], 1, 0)
                y_acc[:, at] += dot(os[0], wobuf[slot, i * 2, :, at], 1, 0) + dot(os[1], wobuf[slot, i * 2 + 1, :, at], 1, 0)
                return carry

            lax.fori_loop(0, 4, columns, 0)
            return carry

        lax.fori_loop(0, per // 2, pair, 0)

    def norm_step(half):
        gain = gain_ref[...].reshape(1, hidden)
        bout = bout_ref[...].reshape(1, hidden)
        count = x_ref.shape[0] // chunk

        def body(c, carry):
            at = pl.ds(pl.multiple_of(c * chunk, chunk), chunk)
            x = x_ref[at, :].astype(jnp.float32)
            dy = dy_ref[at, :].astype(jnp.float32)
            centered = x - jnp.mean(x, axis=-1, keepdims=True)
            inv_std = lax.rsqrt(jnp.mean(centered * centered, axis=-1, keepdims=True) + NORM_EPS)
            x_hat = centered * inv_std
            d_norm = dn_acc[at, :]
            d_hat = d_norm * gain
            d_mean = jnp.mean(d_hat, axis=-1, keepdims=True)
            d_proj = jnp.mean(d_hat * x_hat, axis=-1, keepdims=True)
            gx_ref[at, :] = (dy + inv_std * (d_hat - d_mean - x_hat * d_proj)).astype(jnp.bfloat16)
            y_ref[at, :] = (x + y_acc[at, :] + bout).astype(jnp.bfloat16)
            sums[0:1, :] += jnp.sum(d_norm * x_hat, axis=0, keepdims=True)
            sums[1:2, :] += jnp.sum(d_norm, axis=0, keepdims=True)
            sums[2:3, :] += jnp.sum(dy, axis=0, keepdims=True)
            return carry

        lax.fori_loop(half * count // 2, (half + 1) * count // 2, body, 0)

    greet_all(me, size)
    spread.load.wait()
    for g in range(Spread.STEPS):
        spread.step(g)
        m = g - TOKEN_AT
        if g == 1:
            for copy in trades + own_parts:
                copy.start()
        if m == 0:
            for copy in own_parts:
                copy.wait()
            for trade in trades:
                trade.wait_recv()
            for copy in rows(0):
                copy.start()
        if 0 <= m < TOKEN_STEPS:
            heads_step(m)
        elif m in (TOKEN_STEPS, TOKEN_STEPS + 1):
            norm_step(m - TOKEN_STEPS)
        elif m == TOKEN_STEPS + 2:
            for j in range(size):
                tiles[j, 0:3, 0:head_dim] = sums[0:3, j * head_dim:(j + 1) * head_dim]
            come[me] = tiles[me]
        elif m == TOKEN_STEPS + 3:
            deal.start()
        elif m == TOKEN_STEPS + 5:
            deal.wait_recv()
            total[...] = jnp.sum(come[...], axis=0)
            totals_ref[me] = total[...]
            collect.start()
    spread.close()
    for trade in trades:
        trade.wait_send()
    deal.wait_send()
    collect.wait_recv()
    collect.wait_send()


def token_side(block, parts, early, wq, wo, x, dy, gain, bout, size, collective_id):
    rows, cols = block.shape
    late = parts.shape[0] - early.shape[0]
    heads, head_dim, hidden = wo.shape
    tokens = x.shape[0]
    per = heads // TOKEN_STEPS
    anywhere = pl.BlockSpec(memory_space=pl.ANY)
    vmem = pl.BlockSpec(memory_space=pltpu.VMEM)
    sem = pltpu.SemaphoreType.DMA
    bf16, f32 = jnp.bfloat16, jnp.float32
    return pl.pallas_call(
        functools.partial(token_kernel, size, head_dim, 16),
        out_shape=(
            jax.ShapeDtypeStruct((size, rows, cols), block.dtype),
            jax.ShapeDtypeStruct((late, *parts.shape[1:]), parts.dtype),
            jax.ShapeDtypeStruct((tokens, hidden), bf16),
            jax.ShapeDtypeStruct((tokens, hidden), bf16),
            jax.ShapeDtypeStruct((size, 8, LANES), f32),
        ),
        in_specs=[anywhere] * 5 + [vmem] * 4,
        out_specs=(anywhere, anywhere, vmem, vmem, vmem),
        scratch_shapes=Spread.scratch(rows, cols, block.dtype) + [
            pltpu.VMEM((2, per, 3 * head_dim, hidden), bf16),
            pltpu.VMEM((2, per, head_dim, hidden), bf16),
            pltpu.VMEM((2, parts.shape[0], per, *parts.shape[2:]), bf16),
            pltpu.VMEM((tokens, hidden), f32),
            pltpu.VMEM((tokens, hidden), f32),
            pltpu.VMEM((8, hidden), f32),
            pltpu.VMEM((size, 8, LANES), f32),
            pltpu.VMEM((size, 8, LANES), f32),
            pltpu.VMEM((8, LANES), f32),
            sem((late,)), sem((late,)), sem((late,)), sem((2,)), sem((2,)), sem((2, parts.shape[0])), sem, sem, sem, sem,
        ],
        compiler_params=pltpu.CompilerParams(collective_id=collective_id, has_side_effects=True, vmem_limit_bytes=VMEM_LIMIT),
        cost_estimate=pl.CostEstimate(flops=120_000_000_000, bytes_accessed=8 * size * rows * cols, transcendentals=0),
        name="token_side",
    )(block, parts, early, wq, wo, x, dy, gain, bout)


def hand_kernel(y_ref, gx_ref, y_out, gx_out):
    y_out[...] = y_ref[...]
    gx_out[...] = gx_ref[...]


def hand_over(y, gx):
    spec = pl.BlockSpec((y.shape[0] // 4, y.shape[1]), lambda i: (i, 0))
    return pl.pallas_call(
        hand_kernel, grid=(4,), out_shape=(jax.ShapeDtypeStruct(y.shape, y.dtype),) * 2, in_specs=[spec] * 2, out_specs=(spec,) * 2,
        cost_estimate=pl.CostEstimate(flops=1_000_000_000, bytes_accessed=8 * y.size, transcendentals=0), name="hand_over")(y, gx)


def settle_kernel(block, depth, ahead, per, origin, first, src_ref, *refs):
    dst_ref, buf, read_sems, write_sems = refs[-4:]
    count = src_ref.shape[0] * per

    def slab(ref, i, start):
        return ref.at[i // per, pl.ds(pl.multiple_of(start + lax.rem(i, per) * block, 8), block)]

    def read(i):
        return pltpu.make_async_copy(slab(src_ref, i, origin), buf.at[lax.rem(i, depth)], read_sems.at[lax.rem(i, depth)])

    def write(i):
        return pltpu.make_async_copy(buf.at[lax.rem(i, depth)], slab(dst_ref, i, first), write_sems.at[lax.rem(i, depth)])

    def step(i, carry):
        @pl.when(jnp.logical_and(i >= depth, i < count))
        def _():
            write(i - depth).wait()

        @pl.when(i < count)
        def _():
            read(i).start()

        @pl.when(i >= ahead)
        def _():
            read(i - ahead).wait()
            write(i - ahead).start()

        return carry

    lax.fori_loop(0, count + ahead, step, 0)

    def drain(i, carry):
        write(i).wait()
        return carry

    lax.fori_loop(max(0, count - depth), count, drain, 0)


def settle(x, origin, rows, first, total, pieces=1, into=None, after=()):
    block = rows // pieces
    depth, ahead = 12, 6
    count, _, cols = x.shape
    sem = pltpu.SemaphoreType.DMA((depth,))
    old = [] if into is None else [into]
    return pl.pallas_call(
        functools.partial(settle_kernel, block, depth, ahead, pieces, origin, first),
        out_shape=jax.ShapeDtypeStruct((count, total, cols), x.dtype),
        in_specs=[pl.BlockSpec(memory_space=pl.ANY)] * (1 + len(old) + len(after)),
        out_specs=pl.BlockSpec(memory_space=pl.ANY),
        scratch_shapes=[pltpu.VMEM((depth, block, cols), x.dtype), sem, sem],
        input_output_aliases={1: 0} if old else {},
        compiler_params=pltpu.CompilerParams(vmem_limit_bytes=VMEM_LIMIT),
        cost_estimate=pl.CostEstimate(flops=10_000_000_000, bytes_accessed=8 * x.size, transcendentals=0),
        name="settle",
    )(x, *old, *after)


def solution(mesh):
    size = mesh.shape["sp"]

    def block_fn(x_blk, pos_blk, keep_blk, ln_gain, ln_bias, w_qkv, b_qkv, w_out, b_out, dy_blk):
        batch, tok, hidden = x_blk.shape
        heads, head_dim = w_qkv.shape[1], w_qkv.shape[3]
        tokens = batch * tok
        wq = jnp.transpose(w_qkv, (1, 2, 3, 0)).reshape(heads, 3 * head_dim, hidden)
        wo = w_out.reshape(heads, head_dim, hidden)

        def gather(a):
            return lax.all_gather(a, "sp", axis=0, tiled=True).reshape(heads, a.shape[0], hidden)

        _, parts, early, grad_a, grad_b, grad_c, grad_out = block_call(
            x_blk, dy_blk, ln_gain, ln_bias, pos_blk, keep_blk, wq, jnp.transpose(b_qkv, (1, 0, 2)), wo, size, 256, 0)

        all_out, _, y, grad_x, totals = token_side(
            grad_out, parts, early, wq, wo, x_blk.reshape(tokens, hidden), dy_blk.reshape(tokens, hidden), ln_gain, b_out, size, 1)
        y, grad_x = hand_over(y, grad_x)
        grad_wo = settle(all_out, 0, head_dim, 0, head_dim, after=(y,))

        rows = 3 * head_dim
        first, second, short = split_rows(rows)
        all_c = spread_rows(grad_c, grad_wo, size, 2)
        grad_wq = settle(gather(grad_a), 0, first, 0, rows, 2, after=(all_c,))
        grad_wq = settle(all_c, 0, short, first + second, rows, into=grad_wq)
        grad_wq = settle(gather(grad_b), 0, second, first, rows, into=grad_wq)
        totals = totals[:, :, :head_dim]
        grad_wq = jnp.transpose(grad_wq.reshape(heads, 3, head_dim, hidden), (3, 0, 1, 2))
        return (y.reshape(x_blk.shape), grad_x.reshape(x_blk.shape), grad_wq, totals[:, 3:6],
                grad_wo.reshape(heads * head_dim, hidden), totals[:, 2].reshape(-1), totals[:, 0].reshape(-1), totals[:, 1].reshape(-1))

    act_spec = P("dp", "sp", None)
    tok_spec = P("dp", "sp")
    in_specs = (act_spec, tok_spec, tok_spec, P(), P(), P(), P(), P(), P(), act_spec)
    out_specs = (act_spec, act_spec, P("dp", None, None, None), P("dp", None, None), P("dp", None), P("dp"), P("dp"), P("dp"))
    return jax.shard_map(block_fn, mesh=mesh, in_specs=in_specs, out_specs=out_specs, check_vma=False)
```

```python
import functools
import math

import jax
import jax.numpy as jnp
from jax import lax
from jax.experimental import pallas as pl
from jax.experimental.pallas import tpu as pltpu
from jax.sharding import PartitionSpec as P

NORM_EPS = 1e-5
MASK_FILL = -1e30
LANES = 128
LOG2E = 1.4426950408889634
MESH = pl.DeviceIdType.MESH
VMEM_LIMIT = 61 * 1024 * 1024


def dot(a, b, ca, cb):
    return lax.dot_general(a, b, (((ca,), (cb,)), ((), ())), preferred_element_type=jnp.float32)


def greet_all(me, size, meanwhile=lambda: None):
    barrier = pltpu.get_barrier_semaphore()

    def greet(d, carry):
        pl.semaphore_signal(barrier, inc=1, device_id={"sp": lax.rem(me + d, size)}, device_id_type=MESH)
        return carry

    lax.fori_loop(1, size, greet, 0)
    meanwhile()
    pl.semaphore_wait(barrier, size - 1)


class Direct:
    def __init__(self, me, size, src, dst, whole, send_sem, recv_sem):
        self.me, self.size, self.src, self.dst, self.whole, self.send_sem, self.recv_sem = me, size, src, dst, whole, send_sem, recv_sem

    def start(self):
        def body(d, carry):
            peer = lax.rem(self.me + d, self.size)
            pltpu.make_async_remote_copy(
                src_ref=self.src(peer), dst_ref=self.dst(self.me), send_sem=self.send_sem, recv_sem=self.recv_sem,
                device_id={"sp": peer}, device_id_type=MESH).start()
            return carry

        lax.fori_loop(1, self.size, body, 0)

    def total(self):
        ref = self.whole.at[pl.ds(0, self.size - 1)]
        return pltpu.make_async_remote_copy(
            src_ref=ref, dst_ref=ref, send_sem=self.send_sem, recv_sem=self.recv_sem,
            device_id={"sp": self.me}, device_id_type=MESH)

    def wait_recv(self):
        self.total().wait_recv()

    def wait_send(self):
        self.total().wait_send()


FIRST_OF = (2, 3, 0, 1)
CYCLE = (("P", 0), ("Q", 0, 0), ("Q", 3, 2), ("P", 1), ("Q", 0, 1), ("Q", 1, 0), ("Q", 2, 0), ("P", 2), ("Q", 1, 1),
         ("Q", 2, 1), ("Q", 3, 0), ("Q", 1, 2), ("Q", 2, 2), ("Q", 3, 1), ("Q", 0, 2))
LATE = 2
LAG = 3
COLOURS = 4
READY = 6
EARLY = 1
STEP_OF = ((1, 0), (-1, 0), (0, 1), (0, -1))
PLACES = len(CYCLE)


class Torus:
    def __init__(self, size):
        self.side = math.isqrt(size // 2)
        self.me = lax.axis_index("sp")
        self.core = lax.rem(self.me, 2)
        chip = self.me // 2
        self.cx, self.cy = lax.rem(chip, self.side), chip // self.side
        self.flip = 1 - 2 * self.core
        self.sibling = self.me + self.flip

    def device_at(self, dx, dy):
        side = self.side
        return (lax.rem(self.cy + dy + side, side) * side + lax.rem(self.cx + dx + side, side)) * 2 + self.core

    def neighbour(self, link):
        return self.device_at(*STEP_OF[link])

    def chunk(self, link, place, ahead):
        what = CYCLE[place]
        if what[0] == "P":
            first, n, m = link, what[1] + ahead, 0
        else:
            first, n, m = FIRST_OF[link], what[2] + ahead, what[1]
        dx = -STEP_OF[link][0] * n - STEP_OF[first][0] * m
        dy = -STEP_OF[link][1] * n - STEP_OF[first][1] * m
        return self.device_at(dx, dy), first


def is_own(place):
    return CYCLE[place] in (("P", 0), ("Q", 0, 0))


def block_kernel(size, dims, x_ref, dy_ref, gain_ref, shift_ref, pos_ref, keep_ref, wq_ref, bias_ref, wo_ref,
                 gat_ref, parts_ref, partstok_ref, gwa_ref, gwb_ref, gwc_ref, gwo_ref,
                 xin, stage, wbuf, wobuf, metatile, metabuf, rowbuf, sbuf, qkvb, dob, dk_acc, dv_acc, dq_all, o_all, d_all, pbuf,
                 load_sems, own_sems, piece_sems, parts_sem, ici_send, ici_recv, d2d_send, d2d_recv, own_send, own_recv,
                 meta_send, meta_recv, part_send, part_recv):
    batch, tok, head_dim, pad_dim, hidden, q_block = dims
    seq_len = size * tok
    torus = Torus(size)
    me, flip, sibling, side = torus.me, torus.flip, torus.sibling, torus.side
    places = PLACES
    scale = head_dim ** -0.5
    heads = wo_ref.shape[0]
    slope = jnp.exp2(jnp.full((1, 1), -8.0 / heads, jnp.float32) * (me + 1).astype(jnp.float32))

    def send(b, link, place):
        block, colour = torus.chunk(link, place, 0)
        dst = gat_ref.at[b, block, colour]
        return pltpu.make_async_remote_copy(
            src_ref=stage.at[b, colour] if is_own(place) else dst, dst_ref=dst,
            send_sem=ici_send.at[link], recv_sem=ici_recv.at[link, place],
            device_id={"sp": torus.neighbour(link)}, device_id_type=MESH)

    def arrival(b, link, place):
        block, colour = torus.chunk(link, place, 1)
        ref = gat_ref.at[b, block, colour]
        return pltpu.make_async_remote_copy(
            src_ref=ref, dst_ref=ref, send_sem=ici_send.at[link], recv_sem=ici_recv.at[link, place],
            device_id={"sp": me}, device_id_type=MESH)

    def share(b, link, place, shift):
        block, colour = torus.chunk(link, place, 1)
        ref = gat_ref.at[b, block + shift, colour]
        return pltpu.make_async_remote_copy(
            src_ref=ref, dst_ref=ref, send_sem=d2d_send.at[link], recv_sem=d2d_recv.at[link, place],
            device_id={"sp": sibling}, device_id_type=MESH)

    def share_own(b, block):
        return pltpu.make_async_remote_copy(
            src_ref=stage.at[b], dst_ref=gat_ref.at[b, block], send_sem=own_send.at[b], recv_sem=own_recv.at[b],
            device_id={"sp": sibling}, device_id_type=MESH)

    def keep_own(b):
        return pltpu.make_async_copy(stage.at[b], gat_ref.at[b, me], own_sems.at[b])

    load_x = pltpu.make_async_copy(x_ref, xin, load_sems.at[0])
    load_dy = pltpu.make_async_copy(dy_ref, stage.at[:, :, 0], load_sems.at[1])
    load_wq = pltpu.make_async_copy(wq_ref.at[me], wbuf, load_sems.at[2])
    load_wo = pltpu.make_async_copy(wo_ref.at[me], wobuf, load_sems.at[3])
    for load in (load_x, load_dy, load_wq, load_wo):
        load.start()
    meta = Direct(me, size, lambda j: metatile, lambda j: metabuf.at[j], metabuf, meta_send, meta_recv)
    early = partstok_ref.shape[0]
    trades = [Direct(me, size, lambda j, b=b: parts_ref.at[b, j], lambda j, b=b: partstok_ref.at[b, j], partstok_ref.at[b],
                     part_send.at[b], part_recv.at[b]) for b in range(early)]
    own_parts = [pltpu.make_async_copy(parts_ref.at[b, me], partstok_ref.at[b, me], load_sems.at[4 + b]) for b in range(early)]

    def prepare():
        metatile[...] = jnp.zeros_like(metatile)
        metatile[0:batch, 0:tok] = pos_ref[...]
        metatile[batch:2 * batch, 0:tok] = keep_ref[...]
        metabuf[me] = metatile[...]
        load_x.wait()

        gain, shift = gain_ref[...].reshape(1, 1, hidden), shift_ref[...].reshape(1, 1, hidden)

        def normalise(b, carry):
            x = xin[b].astype(jnp.float32)
            centered = x - jnp.mean(x, axis=-1, keepdims=True)
            inv_std = lax.rsqrt(jnp.mean(centered * centered, axis=-1, keepdims=True) + NORM_EPS)
            stage[b, :, 1] = (centered * inv_std * gain + shift).astype(jnp.bfloat16)
            return carry

        lax.fori_loop(0, batch, normalise, 0)
        load_dy.wait()

    greet_all(me, size, prepare)

    pieces = sbuf.shape[0]
    chip_rows = 2 * tok

    def chip_of(p, e):
        return torus.device_at(lax.rem(p + 1 + e, side), e) // 2

    def rows_at(p, e):
        return pl.ds(pl.multiple_of(chip_of(p, e) * chip_rows, chip_rows), chip_rows)

    def load_piece(b, p):
        return [pltpu.make_async_copy(gat_ref.at[b, pl.ds(chip_of(p, e) * 2, 2)], sbuf.at[p, e], piece_sems.at[p, e]) for e in range(side)]

    def start_piece(b, p):
        for load in load_piece(b, p):
            load.start()

    def rows_of(p, which, at=slice(None)):
        return sbuf[p, :, :, :, which, :, at].reshape(side * chip_rows, -1)

    def each(lo, hi, use):
        def body(p, carry):
            use(p)
            return carry

        lax.fori_loop(lo, hi, body, 0)

    def pad_lanes(a):
        return jnp.concatenate([a, jnp.zeros((a.shape[0], pad_dim - head_dim), a.dtype)], axis=1)

    def project(b, p):
        for load in load_piece(b, p):
            load.wait()
        bias = jnp.concatenate([bias_ref[c, pl.ds(me, 1), :] for c in range(3)], axis=1)
        r = (dot(rows_of(p, 1), wbuf[...], 1, 1) + bias).astype(jnp.bfloat16)
        d = pad_lanes(dot(rows_of(p, 0), wobuf[...], 1, 1).astype(jnp.bfloat16))
        q, k, v = (pad_lanes(r[:, c * head_dim:(c + 1) * head_dim]) for c in range(3))
        for e in range(side):
            mine = slice(e * chip_rows, (e + 1) * chip_rows)
            at = rows_at(p, e)
            for c, part in enumerate((q, k, v)):
                qkvb[at, c * pad_dim:(c + 1) * pad_dim] = part[mine]
            dob[at, :] = d[mine]

    def attend(b, i):
        span = (i + 1) * q_block
        mine = slice(i * q_block, span)
        if i == 0:
            dk_acc[...] = jnp.zeros_like(dk_acc)
            dv_acc[...] = jnp.zeros_like(dv_acc)
        q, k, v = qkvb[mine, :pad_dim], qkvb[:span, pad_dim:2 * pad_dim], qkvb[:span, 2 * pad_dim:]
        do = dob[mine, :]
        pos = rowbuf[pl.ds(b, 1), :span]
        keep = rowbuf[pl.ds(b + batch, 1), :span]
        bias = jnp.where(keep > 0, (-slope * LOG2E) * (pos[:, span - 1:] - pos).astype(jnp.float32), MASK_FILL)
        scores = dot(q, k, 1, 1) * (scale * LOG2E) + bias
        row_id = lax.broadcasted_iota(jnp.int32, (q_block, q_block), 0)
        col_id = lax.broadcasted_iota(jnp.int32, (q_block, q_block), 1)
        corner = jnp.where(col_id <= row_id, scores[:, span - q_block:], MASK_FILL)
        scores = jnp.concatenate([scores[:, :span - q_block], corner], axis=1) if i else corner
        expo = jnp.exp2(scores - jnp.max(scores, axis=-1, keepdims=True))
        prob = expo * (1.0 / jnp.sum(expo, axis=-1, keepdims=True))
        prob_lo = prob.astype(jnp.bfloat16)
        o = dot(prob_lo, v, 1, 0).astype(jnp.bfloat16)
        row_dot = jnp.sum(do.astype(jnp.float32) * o.astype(jnp.float32), axis=-1, keepdims=True)
        ds_lo = (prob * (dot(do, v, 1, 1) - row_dot)).astype(jnp.bfloat16)
        o_all[mine, :] = o
        dq_all[mine, :] = (dot(ds_lo, k, 1, 0) * scale).astype(jnp.bfloat16)
        dv_acc[:span, :] += dot(prob_lo, do, 0, 0)
        dk_acc[:span, :] += dot(ds_lo, q, 0, 0)

    def store_parts(b):
        return pltpu.make_async_copy(pbuf, parts_ref.at[b], parts_sem)

    def finish(b):
        dk = (dk_acc[...] * scale).astype(jnp.bfloat16)
        dv = dv_acc[...].astype(jnp.bfloat16)
        d_all[...] = jnp.concatenate([dq_all[:, :head_dim], dk[:, :head_dim], dv[:, :head_dim]], axis=1)
        whole = jnp.concatenate([d_all[...], o_all[:, :head_dim]], axis=1).reshape(size, tok, 4 * head_dim)
        pbuf[...] = jnp.concatenate([whole[:, :tok // 2], whole[:, tok // 2:]], axis=2)
        store_parts(b).start()

    width = min(1280, hidden)

    def gradient(p):
        d = jnp.concatenate([d_all[rows_at(p, e), :] for e in range(side)], axis=0)
        o = jnp.concatenate([o_all[rows_at(p, e), :] for e in range(side)], axis=0)[:, :head_dim]

        def columns(n, carry):
            at = pl.ds(pl.multiple_of(n * width, width), width)
            term = dot(d, rows_of(p, 1, at), 0, 0)
            row = 0
            for ref in (gwa_ref, gwb_ref, gwc_ref):
                ref[:, at] += term[row:row + ref.shape[0]]
                row += ref.shape[0]
            gwo_ref[:, at] += dot(o, rows_of(p, 0, at), 0, 0)
            return carry

        lax.fori_loop(0, hidden // width, columns, 0)

    count = seq_len // q_block
    last = pieces - 1
    tasks = {(0, READY - 3): [lambda b: each(0, last, lambda p: start_piece(b, p))],
             (0, READY - 2): [lambda b: each(0, last - 1, lambda p: project(b, p))],
             (0, READY - 1): [lambda b: project(b, last - 1)],
             (0, READY): [lambda b: start_piece(b, last)],
             (0, READY + 1): [lambda b: project(b, last)],
             (0, READY + 7): [finish],
             (0, READY + 8): [lambda b: each(0, pieces // 2, gradient)],
             (1, 0): [lambda b: each(pieces // 2, pieces, gradient)],
             (1, 1): [lambda b: store_parts(b).wait()]}
    spot = (2, 2, 2, 3, 3, 4, 5, 6)
    for i in range(count):
        tasks.setdefault((0, READY + spot[i]), []).append(lambda b, i=i: attend(b, i))

    for ref in (gwa_ref, gwb_ref, gwc_ref, gwo_ref):
        ref[...] = jnp.zeros_like(ref)

    def phase_of(i, place):
        return i - 1 if place == LATE else i

    def among(b):
        return jnp.logical_and(b >= 0, b < batch)

    def turn(i, carry):
        for place in range(places):
            came = (place - LAG) % places
            b_came = phase_of(i if place >= LAG else i - 1, came)

            @pl.when(among(b_came))
            def _():
                for link in range(4):
                    arrival(b_came, link, came).wait_recv()
                    share(b_came, link, came, 0).start()

            b_send = phase_of(i, place)

            @pl.when(among(b_send))
            def _():
                for link in range(4):
                    send(b_send, link, place).start()

            shared = (place - LAG - 1) % places
            b_shared = phase_of(i if place >= LAG + 1 else i - 1, shared)

            @pl.when(among(b_shared))
            def _():
                for link in range(4):
                    share(b_shared, link, shared, flip).wait_recv()

            if place == 1:
                @pl.when(i == 0)
                def _():
                    for b in range(batch):
                        share_own(b, me).start()
                        keep_own(b).start()
                    meta.start()

            if place == READY - 3:
                @pl.when(i == 1)
                def _():
                    for load in (load_wq, load_wo):
                        load.wait()
                    meta.wait_recv()
                    for j in range(size):
                        rowbuf[:, j * tok:(j + 1) * tok] = metabuf[j, :, :tok]
                    for b in range(batch):
                        share_own(b, sibling).wait_recv()
                        keep_own(b).wait()
                    meta.wait_send()
                    for b in range(batch):
                        share_own(b, me).wait_send()

            if place == READY:
                @pl.when(i == batch)
                def _():
                    for copy in own_parts + trades:
                        copy.start()

            for later in (0, 1):
                if (later, place) in tasks:
                    @pl.when(among(i - 1 - later))
                    def _():
                        for task in tasks[later, place]:
                            task(i - 1 - later)
        return carry

    lax.fori_loop(0, batch + 2, turn, 0)
    for copy in own_parts:
        copy.wait()
    for trade in trades:
        trade.wait_recv()
        trade.wait_send()
    sent = gat_ref.at[:, pl.ds(0, places), 0]
    for link in range(4):
        for sem in (ici_send, d2d_send):
            pltpu.make_async_remote_copy(
                src_ref=sent, dst_ref=sent, send_sem=sem.at[link], recv_sem=ici_recv.at[link, 0],
                device_id={"sp": sibling}, device_id_type=MESH).wait_send()


def split_rows(rows):
    first, short = 8 * (rows * 17 // 240), 8 * (rows // 40)
    return first, rows - first - short, short


def block_call(x, dy, gain, shift, pos, keep, wq, bias, wo, size, q_block, collective_id):
    batch, tok, hidden = x.shape
    rows = tok // COLOURS
    heads, head_dim, _ = wo.shape
    pad_dim = -(-head_dim // LANES) * LANES
    seq_len = size * tok
    side = math.isqrt(size // 2)
    places = PLACES
    anywhere = pl.BlockSpec(memory_space=pl.ANY)
    vmem = pl.BlockSpec(memory_space=pltpu.VMEM)
    sem = pltpu.SemaphoreType.DMA
    bf16, f32 = jnp.bfloat16, jnp.float32
    flops = batch * (6 * seq_len * seq_len * 256 + 4 * seq_len * 4 * head_dim * hidden) + 80_000_000_000
    cut = (batch, COLOURS, rows, hidden)
    first, second, short = split_rows(3 * head_dim)
    return pl.pallas_call(
        functools.partial(block_kernel, size, (batch, tok, head_dim, pad_dim, hidden, min(q_block, seq_len))),
        out_shape=(
            jax.ShapeDtypeStruct((batch, size, COLOURS, 2, rows, hidden), bf16),
            jax.ShapeDtypeStruct((batch, size, tok // 2, 8 * head_dim), bf16),
            jax.ShapeDtypeStruct((EARLY, size, tok // 2, 8 * head_dim), bf16),
            *(jax.ShapeDtypeStruct((n, hidden), f32) for n in (first, second, short, head_dim)),
        ),
        in_specs=[anywhere, anywhere, vmem, vmem, vmem, vmem, anywhere, vmem, anywhere],
        out_specs=(anywhere, anywhere, anywhere, vmem, vmem, vmem, vmem),
        scratch_shapes=[
            pltpu.VMEM(cut, bf16),
            pltpu.VMEM((batch, COLOURS, 2, rows, hidden), bf16),
            pltpu.VMEM((3 * head_dim, hidden), bf16),
            pltpu.VMEM((head_dim, hidden), bf16),
            pltpu.VMEM((8, LANES), jnp.int32),
            pltpu.VMEM((size, 8, LANES), jnp.int32),
            pltpu.VMEM((8, seq_len), jnp.int32),
            pltpu.VMEM((side, side, 2, COLOURS, 2, rows, hidden), bf16),
            pltpu.VMEM((seq_len, 3 * pad_dim), bf16),
            pltpu.VMEM((seq_len, pad_dim), bf16),
            pltpu.VMEM((seq_len, pad_dim), f32),
            pltpu.VMEM((seq_len, pad_dim), f32),
            pltpu.VMEM((seq_len, pad_dim), bf16),
            pltpu.VMEM((seq_len, pad_dim), bf16),
            pltpu.VMEM((seq_len, 3 * head_dim), bf16),
            pltpu.VMEM((size, tok // 2, 8 * head_dim), bf16),
            sem((4 + EARLY,)), sem((batch,)), sem((side, side)), sem,
            sem((4,)), sem((4, places)), sem((4,)), sem((4, places)), sem((batch,)), sem((batch,)), sem, sem, sem((EARLY,)), sem((EARLY,)),
        ],
        compiler_params=pltpu.CompilerParams(collective_id=collective_id, has_side_effects=True, vmem_limit_bytes=VMEM_LIMIT),
        cost_estimate=pl.CostEstimate(flops=flops, bytes_accessed=60_000_000, transcendentals=batch * seq_len * seq_len // 2),
        name="block",
    )(x.reshape(cut), dy.reshape(cut), gain, shift, pos, keep, wq, bias, wo)


class Spread:
    def __init__(self, size, own_ref, gat_ref, stage, sems):
        self.torus, self.size, self.gat_ref, self.stage = Torus(size), size, gat_ref, stage
        self.load_sem, self.keep_sem, self.ici_send, self.ici_recv, self.d2d_send, self.d2d_recv, self.own_send, self.own_recv = sems
        self.part = stage.shape[1] // COLOURS
        self.load = pltpu.make_async_copy(own_ref, stage, self.load_sem)
        self.keep = pltpu.make_async_copy(stage, gat_ref.at[self.torus.me], self.keep_sem)

    def columns(self, colour):
        return pl.ds(colour * self.part, self.part)

    def view(self, block, colour):
        return self.gat_ref.at[block, :, self.columns(colour)]

    def remote(self, src, dst, send_sem, recv_sem, device):
        return pltpu.make_async_remote_copy(
            src_ref=src, dst_ref=dst, send_sem=send_sem, recv_sem=recv_sem, device_id={"sp": device}, device_id_type=MESH)

    def send(self, link, place):
        block, colour = self.torus.chunk(link, place, 0)
        dst = self.view(block, colour)
        src = self.stage.at[:, self.columns(colour)] if is_own(place) else dst
        return self.remote(src, dst, self.ici_send.at[link], self.ici_recv.at[link, place], self.torus.neighbour(link))

    def arrival(self, link, place):
        ref = self.view(*self.torus.chunk(link, place, 1))
        return self.remote(ref, ref, self.ici_send.at[link], self.ici_recv.at[link, place], self.torus.me)

    def share(self, link, place, shift):
        block, colour = self.torus.chunk(link, place, 1)
        ref = self.view(block + shift, colour)
        return self.remote(ref, ref, self.d2d_send.at[link], self.d2d_recv.at[link, place], self.torus.sibling)

    def share_own(self, block):
        return self.remote(self.stage, self.gat_ref.at[block], self.own_send, self.own_recv, self.torus.sibling)

    STEPS = PLACES + LATE + LAG + 2

    def step(self, g):
        def place_of(g):
            place = g % PLACES
            return place if g >= 0 and g // PLACES == (1 if place == LATE else 0) else None

        came, now, shared = place_of(g - LAG), place_of(g), place_of(g - LAG - 1)
        for link in range(4):
            if came is not None:
                self.arrival(link, came).wait_recv()
                self.share(link, came, 0).start()
        for link in range(4):
            if now is not None:
                self.send(link, now).start()
        for link in range(4):
            if shared is not None:
                self.share(link, shared, self.torus.flip).wait_recv()
        if g == 1:
            self.share_own(self.torus.me).start()
            self.keep.start()

    def close(self):
        self.share_own(self.torus.sibling).wait_recv()
        self.keep.wait()
        self.share_own(self.torus.me).wait_send()
        sent = self.gat_ref.at[pl.ds(0, PLACES), :, pl.ds(0, self.part)]
        for link in range(4):
            for sem in (self.ici_send, self.d2d_send):
                self.remote(sent, sent, sem.at[link], self.ici_recv.at[link, 0], self.torus.sibling).wait_send()

    @staticmethod
    def scratch(rows, cols, dtype):
        sem = pltpu.SemaphoreType.DMA
        return [pltpu.VMEM((rows, cols), dtype), sem, sem, sem((4,)), sem((4, PLACES)), sem((4,)), sem((4, PLACES)), sem, sem]


def spread_kernel(size, own_ref, after_ref, gat_ref, stage, *sems):
    spread = Spread(size, own_ref, gat_ref, stage, sems)
    spread.load.start()
    greet_all(spread.torus.me, size)
    spread.load.wait()
    for g in range(Spread.STEPS):
        spread.step(g)
    spread.close()


def spread_rows(block, after, size, collective_id):
    rows, cols = block.shape
    anywhere = pl.BlockSpec(memory_space=pl.ANY)
    return pl.pallas_call(
        functools.partial(spread_kernel, size),
        out_shape=jax.ShapeDtypeStruct((size, rows, cols), block.dtype),
        in_specs=[anywhere, anywhere],
        out_specs=anywhere,
        scratch_shapes=Spread.scratch(rows, cols, block.dtype),
        compiler_params=pltpu.CompilerParams(collective_id=collective_id, has_side_effects=True),
        cost_estimate=pl.CostEstimate(flops=50_000_000_000, bytes_accessed=8 * size * rows * cols, transcendentals=0),
        name="spread",
    )(block, after)


TOKEN_AT = 8
TOKEN_STEPS = 8


def token_kernel(size, head_dim, chunk, own_ref, parts_ref, early_ref, wq_ref, wo_ref, x_ref, dy_ref, gain_ref, bout_ref,
                 gat_ref, late_ref, y_ref, gx_ref, totals_ref,
                 stage, load_sem, keep_sem, ici_send, ici_recv, d2d_send, d2d_recv, own_send, own_recv,
                 wqbuf, wobuf, pbuf, dn_acc, y_acc, sums, tiles, come, total,
                 part_send, part_recv, own_part_sems, wq_sems, wo_sems, p_sems, deal_send, deal_recv, collect_send, collect_recv):
    spread = Spread(size, own_ref, gat_ref, stage,
                    (load_sem, keep_sem, ici_send, ici_recv, d2d_send, d2d_recv, own_send, own_recv))
    me = spread.torus.me
    early, late = early_ref.shape[0], late_ref.shape[0]
    heads, hidden = wq_ref.shape[0], wq_ref.shape[2]
    per = heads // TOKEN_STEPS
    trades, own_parts = [], []
    for n in range(late):
        b = parts_ref.shape[0] - late + n
        trades.append(Direct(me, size, lambda j, b=b: parts_ref.at[b, j], lambda j, n=n: late_ref.at[n, j], late_ref.at[n],
                             part_send.at[n], part_recv.at[n]))
        own_parts.append(pltpu.make_async_copy(parts_ref.at[b, me], late_ref.at[n, me], own_part_sems.at[n]))
    deal = Direct(me, size, lambda j: tiles.at[j], lambda j: come.at[j], come, deal_send, deal_recv)
    collect = Direct(me, size, lambda j: total, lambda j: totals_ref.at[j], totals_ref, collect_send, collect_recv)

    def weights(m):
        at, slot = pl.ds(m * per, per), m % 2
        return (pltpu.make_async_copy(wq_ref.at[at], wqbuf.at[slot], wq_sems.at[slot]),
                pltpu.make_async_copy(wo_ref.at[at], wobuf.at[slot], wo_sems.at[slot]))

    def rows(m):
        at, slot = pl.ds(m * per, per), m % 2
        sources = [early_ref.at[n, at] for n in range(early)] + [late_ref.at[n, at] for n in range(late)]
        return [pltpu.make_async_copy(src, pbuf.at[slot, n], p_sems.at[slot, n]) for n, src in enumerate(sources)]

    spread.load.start()
    for copy in weights(0):
        copy.start()
    dn_acc[...] = jnp.zeros_like(dn_acc)
    y_acc[...] = jnp.zeros_like(y_acc)
    sums[...] = jnp.zeros_like(sums)
    tiles[...] = jnp.zeros_like(tiles)
    width = hidden // 4

    def heads_step(m):
        slot = m % 2
        for copy in (*weights(m), *rows(m)):
            copy.wait()
        if m + 1 < TOKEN_STEPS:
            for copy in (*weights(m + 1), *rows(m + 1)):
                copy.start()

        def pair(i, carry):
            ds, os = [], []
            for h in range(2):
                parts = []
                for n in range(early + late):
                    both = pbuf[slot, n, i * 2 + h]
                    parts += [both[:, :4 * head_dim], both[:, 4 * head_dim:]]
                parts = jnp.concatenate(parts, axis=0)
                ds.append(parts[:, :3 * head_dim])
                os.append(parts[:, 3 * head_dim:])
                added = jnp.sum(ds[h].astype(jnp.float32), axis=0, keepdims=True)
                for c in range(3):
                    tiles[m * per + i * 2 + h, 3 + c:4 + c, 0:head_dim] = added[:, c * head_dim:(c + 1) * head_dim]

            def columns(n, carry):
                at = pl.ds(pl.multiple_of(n * width, width), width)
                dn_acc[:, at] += dot(ds[0], wqbuf[slot, i * 2, :, at], 1, 0) + dot(ds[1], wqbuf[slot, i * 2 + 1, :, at], 1, 0)
                y_acc[:, at] += dot(os[0], wobuf[slot, i * 2, :, at], 1, 0) + dot(os[1], wobuf[slot, i * 2 + 1, :, at], 1, 0)
                return carry

            lax.fori_loop(0, 4, columns, 0)
            return carry

        lax.fori_loop(0, per // 2, pair, 0)

    def norm_step(half):
        gain = gain_ref[...].reshape(1, hidden)
        bout = bout_ref[...].reshape(1, hidden)
        count = x_ref.shape[0] // chunk

        def body(c, carry):
            at = pl.ds(pl.multiple_of(c * chunk, chunk), chunk)
            x = x_ref[at, :].astype(jnp.float32)
            dy = dy_ref[at, :].astype(jnp.float32)
            centered = x - jnp.mean(x, axis=-1, keepdims=True)
            inv_std = lax.rsqrt(jnp.mean(centered * centered, axis=-1, keepdims=True) + NORM_EPS)
            x_hat = centered * inv_std
            d_norm = dn_acc[at, :]
            d_hat = d_norm * gain
            d_mean = jnp.mean(d_hat, axis=-1, keepdims=True)
            d_proj = jnp.mean(d_hat * x_hat, axis=-1, keepdims=True)
            gx_ref[at, :] = (dy + inv_std * (d_hat - d_mean - x_hat * d_proj)).astype(jnp.bfloat16)
            y_ref[at, :] = (x + y_acc[at, :] + bout).astype(jnp.bfloat16)
            sums[0:1, :] += jnp.sum(d_norm * x_hat, axis=0, keepdims=True)
            sums[1:2, :] += jnp.sum(d_norm, axis=0, keepdims=True)
            sums[2:3, :] += jnp.sum(dy, axis=0, keepdims=True)
            return carry

        lax.fori_loop(half * count // 2, (half + 1) * count // 2, body, 0)

    greet_all(me, size)
    spread.load.wait()
    for g in range(Spread.STEPS):
        spread.step(g)
        m = g - TOKEN_AT
        if g == 1:
            for copy in trades + own_parts:
                copy.start()
        if m == 0:
            for copy in own_parts:
                copy.wait()
            for trade in trades:
                trade.wait_recv()
            for copy in rows(0):
                copy.start()
        if 0 <= m < TOKEN_STEPS:
            heads_step(m)
        elif m in (TOKEN_STEPS, TOKEN_STEPS + 1):
            norm_step(m - TOKEN_STEPS)
        elif m == TOKEN_STEPS + 2:
            for j in range(size):
                tiles[j, 0:3, 0:head_dim] = sums[0:3, j * head_dim:(j + 1) * head_dim]
            come[me] = tiles[me]
        elif m == TOKEN_STEPS + 3:
            deal.start()
        elif m == TOKEN_STEPS + 5:
            deal.wait_recv()
            total[...] = jnp.sum(come[...], axis=0)
            totals_ref[me] = total[...]
            collect.start()
    spread.close()
    for trade in trades:
        trade.wait_send()
    deal.wait_send()
    collect.wait_recv()
    collect.wait_send()


def token_side(block, parts, early, wq, wo, x, dy, gain, bout, size, collective_id):
    rows, cols = block.shape
    late = parts.shape[0] - early.shape[0]
    heads, head_dim, hidden = wo.shape
    tokens = x.shape[0]
    per = heads // TOKEN_STEPS
    anywhere = pl.BlockSpec(memory_space=pl.ANY)
    vmem = pl.BlockSpec(memory_space=pltpu.VMEM)
    sem = pltpu.SemaphoreType.DMA
    bf16, f32 = jnp.bfloat16, jnp.float32
    return pl.pallas_call(
        functools.partial(token_kernel, size, head_dim, 16),
        out_shape=(
            jax.ShapeDtypeStruct((size, rows, cols), block.dtype),
            jax.ShapeDtypeStruct((late, *parts.shape[1:]), parts.dtype),
            jax.ShapeDtypeStruct((tokens, hidden), bf16),
            jax.ShapeDtypeStruct((tokens, hidden), bf16),
            jax.ShapeDtypeStruct((size, 8, LANES), f32),
        ),
        in_specs=[anywhere] * 5 + [vmem] * 4,
        out_specs=(anywhere, anywhere, vmem, vmem, vmem),
        scratch_shapes=Spread.scratch(rows, cols, block.dtype) + [
            pltpu.VMEM((2, per, 3 * head_dim, hidden), bf16),
            pltpu.VMEM((2, per, head_dim, hidden), bf16),
            pltpu.VMEM((2, parts.shape[0], per, *parts.shape[2:]), bf16),
            pltpu.VMEM((tokens, hidden), f32),
            pltpu.VMEM((tokens, hidden), f32),
            pltpu.VMEM((8, hidden), f32),
            pltpu.VMEM((size, 8, LANES), f32),
            pltpu.VMEM((size, 8, LANES), f32),
            pltpu.VMEM((8, LANES), f32),
            sem((late,)), sem((late,)), sem((late,)), sem((2,)), sem((2,)), sem((2, parts.shape[0])), sem, sem, sem, sem,
        ],
        compiler_params=pltpu.CompilerParams(collective_id=collective_id, has_side_effects=True, vmem_limit_bytes=VMEM_LIMIT),
        cost_estimate=pl.CostEstimate(flops=120_000_000_000, bytes_accessed=8 * size * rows * cols, transcendentals=0),
        name="token_side",
    )(block, parts, early, wq, wo, x, dy, gain, bout)


def hand_kernel(y_ref, gx_ref, y_out, gx_out):
    y_out[...] = y_ref[...]
    gx_out[...] = gx_ref[...]


def hand_over(y, gx):
    spec = pl.BlockSpec((y.shape[0] // 4, y.shape[1]), lambda i: (i, 0))
    return pl.pallas_call(
        hand_kernel, grid=(4,), out_shape=(jax.ShapeDtypeStruct(y.shape, y.dtype),) * 2, in_specs=[spec] * 2, out_specs=(spec,) * 2,
        cost_estimate=pl.CostEstimate(flops=1_000_000_000, bytes_accessed=8 * y.size, transcendentals=0), name="hand_over")(y, gx)


def settle_kernel(block, depth, ahead, per, origin, first, src_ref, *refs):
    dst_ref, buf, read_sems, write_sems = refs[-4:]
    count = src_ref.shape[0] * per

    def slab(ref, i, start):
        return ref.at[i // per, pl.ds(pl.multiple_of(start + lax.rem(i, per) * block, 8), block)]

    def read(i):
        return pltpu.make_async_copy(slab(src_ref, i, origin), buf.at[lax.rem(i, depth)], read_sems.at[lax.rem(i, depth)])

    def write(i):
        return pltpu.make_async_copy(buf.at[lax.rem(i, depth)], slab(dst_ref, i, first), write_sems.at[lax.rem(i, depth)])

    def step(i, carry):
        @pl.when(jnp.logical_and(i >= depth, i < count))
        def _():
            write(i - depth).wait()

        @pl.when(i < count)
        def _():
            read(i).start()

        @pl.when(i >= ahead)
        def _():
            read(i - ahead).wait()
            write(i - ahead).start()

        return carry

    lax.fori_loop(0, count + ahead, step, 0)

    def drain(i, carry):
        write(i).wait()
        return carry

    lax.fori_loop(max(0, count - depth), count, drain, 0)


def settle(x, origin, rows, first, total, pieces=1, into=None, after=()):
    block = rows // pieces
    depth, ahead = 12, 6
    count, _, cols = x.shape
    sem = pltpu.SemaphoreType.DMA((depth,))
    old = [] if into is None else [into]
    return pl.pallas_call(
        functools.partial(settle_kernel, block, depth, ahead, pieces, origin, first),
        out_shape=jax.ShapeDtypeStruct((count, total, cols), x.dtype),
        in_specs=[pl.BlockSpec(memory_space=pl.ANY)] * (1 + len(old) + len(after)),
        out_specs=pl.BlockSpec(memory_space=pl.ANY),
        scratch_shapes=[pltpu.VMEM((depth, block, cols), x.dtype), sem, sem],
        input_output_aliases={1: 0} if old else {},
        compiler_params=pltpu.CompilerParams(vmem_limit_bytes=VMEM_LIMIT),
        cost_estimate=pl.CostEstimate(flops=10_000_000_000, bytes_accessed=8 * x.size, transcendentals=0),
        name="settle",
    )(x, *old, *after)


def solution(mesh):
    size = mesh.shape["sp"]

    def block_fn(x_blk, pos_blk, keep_blk, ln_gain, ln_bias, w_qkv, b_qkv, w_out, b_out, dy_blk):
        batch, tok, hidden = x_blk.shape
        heads, head_dim = w_qkv.shape[1], w_qkv.shape[3]
        tokens = batch * tok
        wq = jnp.transpose(w_qkv, (1, 2, 3, 0)).reshape(heads, 3 * head_dim, hidden)
        wo = w_out.reshape(heads, head_dim, hidden)

        def gather(a):
            return lax.all_gather(a, "sp", axis=0, tiled=True).reshape(heads, a.shape[0], hidden)

        _, parts, early, grad_a, grad_b, grad_c, grad_out = block_call(
            x_blk, dy_blk, ln_gain, ln_bias, pos_blk, keep_blk, wq, jnp.transpose(b_qkv, (1, 0, 2)), wo, size, 256, 0)

        all_out, _, y, grad_x, totals = token_side(
            grad_out, parts, early, wq, wo, x_blk.reshape(tokens, hidden), dy_blk.reshape(tokens, hidden), ln_gain, b_out, size, 1)
        y, grad_x = hand_over(y, grad_x)
        grad_wo = settle(all_out, 0, head_dim, 0, head_dim, after=(y,))

        rows = 3 * head_dim
        first, second, short = split_rows(rows)
        all_c = spread_rows(grad_c, grad_wo, size, 2)
        grad_wq = settle(gather(grad_a), 0, first, 0, rows, after=(all_c,))
        grad_wq = settle(all_c, 0, short, first + second, rows, into=grad_wq)
        grad_wq = settle(gather(grad_b), 0, second, first, rows, into=grad_wq)
        totals = totals[:, :, :head_dim]
        grad_wq = jnp.transpose(grad_wq.reshape(heads, 3, head_dim, hidden), (3, 0, 1, 2))
        return (y.reshape(x_blk.shape), grad_x.reshape(x_blk.shape), grad_wq, totals[:, 3:6],
                grad_wo.reshape(heads * head_dim, hidden), totals[:, 2].reshape(-1), totals[:, 0].reshape(-1), totals[:, 1].reshape(-1))

    act_spec = P("dp", "sp", None)
    tok_spec = P("dp", "sp")
    in_specs = (act_spec, tok_spec, tok_spec, P(), P(), P(), P(), P(), P(), act_spec)
    out_specs = (act_spec, act_spec, P("dp", None, None, None), P("dp", None, None), P("dp", None), P("dp"), P("dp"), P("dp"))
    return jax.shard_map(block_fn, mesh=mesh, in_specs=in_specs, out_specs=out_specs, check_vma=False)
```

```python
import functools
import math

import jax
import jax.numpy as jnp
from jax import lax
from jax.experimental import pallas as pl
from jax.experimental.pallas import tpu as pltpu
from jax.sharding import PartitionSpec as P

NORM_EPS = 1e-5
MASK_FILL = -1e30
LANES = 128
LOG2E = 1.4426950408889634
MESH = pl.DeviceIdType.MESH
VMEM_LIMIT = 61 * 1024 * 1024


def dot(a, b, ca, cb):
    return lax.dot_general(a, b, (((ca,), (cb,)), ((), ())), preferred_element_type=jnp.float32)


def greet_all(me, size, meanwhile=lambda: None):
    barrier = pltpu.get_barrier_semaphore()

    def greet(d, carry):
        pl.semaphore_signal(barrier, inc=1, device_id={"sp": lax.rem(me + d, size)}, device_id_type=MESH)
        return carry

    lax.fori_loop(1, size, greet, 0)
    meanwhile()
    pl.semaphore_wait(barrier, size - 1)


class Direct:
    def __init__(self, me, size, src, dst, whole, send_sem, recv_sem):
        self.me, self.size, self.src, self.dst, self.whole, self.send_sem, self.recv_sem = me, size, src, dst, whole, send_sem, recv_sem

    def start(self):
        def body(d, carry):
            peer = lax.rem(self.me + d, self.size)
            pltpu.make_async_remote_copy(
                src_ref=self.src(peer), dst_ref=self.dst(self.me), send_sem=self.send_sem, recv_sem=self.recv_sem,
                device_id={"sp": peer}, device_id_type=MESH).start()
            return carry

        lax.fori_loop(1, self.size, body, 0)

    def total(self):
        ref = self.whole.at[pl.ds(0, self.size - 1)]
        return pltpu.make_async_remote_copy(
            src_ref=ref, dst_ref=ref, send_sem=self.send_sem, recv_sem=self.recv_sem,
            device_id={"sp": self.me}, device_id_type=MESH)

    def wait_recv(self):
        self.total().wait_recv()

    def wait_send(self):
        self.total().wait_send()


FIRST_OF = (2, 3, 0, 1)
CYCLE = (("P", 0), ("Q", 0, 0), ("Q", 3, 2), ("P", 1), ("Q", 0, 1), ("Q", 1, 0), ("Q", 2, 0), ("P", 2), ("Q", 1, 1),
         ("Q", 2, 1), ("Q", 3, 0), ("Q", 1, 2), ("Q", 2, 2), ("Q", 3, 1), ("Q", 0, 2))
LATE = 2
LAG = 3
COLOURS = 4
READY = 6
EARLY = 1
STEP_OF = ((1, 0), (-1, 0), (0, 1), (0, -1))
PLACES = len(CYCLE)


class Torus:
    def __init__(self, size):
        self.side = math.isqrt(size // 2)
        self.me = lax.axis_index("sp")
        self.core = lax.rem(self.me, 2)
        chip = self.me // 2
        self.cx, self.cy = lax.rem(chip, self.side), chip // self.side
        self.flip = 1 - 2 * self.core
        self.sibling = self.me + self.flip

    def device_at(self, dx, dy):
        side = self.side
        return (lax.rem(self.cy + dy + side, side) * side + lax.rem(self.cx + dx + side, side)) * 2 + self.core

    def neighbour(self, link):
        return self.device_at(*STEP_OF[link])

    def chunk(self, link, place, ahead):
        what = CYCLE[place]
        if what[0] == "P":
            first, n, m = link, what[1] + ahead, 0
        else:
            first, n, m = FIRST_OF[link], what[2] + ahead, what[1]
        dx = -STEP_OF[link][0] * n - STEP_OF[first][0] * m
        dy = -STEP_OF[link][1] * n - STEP_OF[first][1] * m
        return self.device_at(dx, dy), first


def is_own(place):
    return CYCLE[place] in (("P", 0), ("Q", 0, 0))


def block_kernel(size, dims, x_ref, dy_ref, gain_ref, shift_ref, pos_ref, keep_ref, wq_ref, bias_ref, wo_ref,
                 gat_ref, parts_ref, partstok_ref, gwa_ref, gwb_ref, gwc_ref, gwo_ref,
                 xin, stage, wbuf, wobuf, metatile, metabuf, rowbuf, sbuf, qkvb, dob, dk_acc, dv_acc, dq_all, o_all, d_all, pbuf,
                 load_sems, own_sems, piece_sems, parts_sem, ici_send, ici_recv, d2d_send, d2d_recv, own_send, own_recv,
                 meta_send, meta_recv, part_send, part_recv):
    batch, tok, head_dim, pad_dim, hidden, q_block = dims
    seq_len = size * tok
    torus = Torus(size)
    me, flip, sibling, side = torus.me, torus.flip, torus.sibling, torus.side
    places = PLACES
    scale = head_dim ** -0.5
    heads = wo_ref.shape[0]
    slope = jnp.exp2(jnp.full((1, 1), -8.0 / heads, jnp.float32) * (me + 1).astype(jnp.float32))

    def send(b, link, place):
        block, colour = torus.chunk(link, place, 0)
        dst = gat_ref.at[b, block, colour]
        return pltpu.make_async_remote_copy(
            src_ref=stage.at[b, colour] if is_own(place) else dst, dst_ref=dst,
            send_sem=ici_send.at[link], recv_sem=ici_recv.at[link, place],
            device_id={"sp": torus.neighbour(link)}, device_id_type=MESH)

    def arrival(b, link, place):
        block, colour = torus.chunk(link, place, 1)
        ref = gat_ref.at[b, block, colour]
        return pltpu.make_async_remote_copy(
            src_ref=ref, dst_ref=ref, send_sem=ici_send.at[link], recv_sem=ici_recv.at[link, place],
            device_id={"sp": me}, device_id_type=MESH)

    def share(b, link, place, shift):
        block, colour = torus.chunk(link, place, 1)
        ref = gat_ref.at[b, block + shift, colour]
        return pltpu.make_async_remote_copy(
            src_ref=ref, dst_ref=ref, send_sem=d2d_send.at[link], recv_sem=d2d_recv.at[link, place],
            device_id={"sp": sibling}, device_id_type=MESH)

    def share_own(b, block):
        return pltpu.make_async_remote_copy(
            src_ref=stage.at[b], dst_ref=gat_ref.at[b, block], send_sem=own_send.at[b], recv_sem=own_recv.at[b],
            device_id={"sp": sibling}, device_id_type=MESH)

    def keep_own(b):
        return pltpu.make_async_copy(stage.at[b], gat_ref.at[b, me], own_sems.at[b])

    load_x = pltpu.make_async_copy(x_ref, xin, load_sems.at[0])
    load_dy = pltpu.make_async_copy(dy_ref, stage.at[:, :, 0], load_sems.at[1])
    load_wq = pltpu.make_async_copy(wq_ref.at[me], wbuf, load_sems.at[2])
    load_wo = pltpu.make_async_copy(wo_ref.at[me], wobuf, load_sems.at[3])
    for load in (load_x, load_dy, load_wq, load_wo):
        load.start()
    meta = Direct(me, size, lambda j: metatile, lambda j: metabuf.at[j], metabuf, meta_send, meta_recv)
    early = partstok_ref.shape[0]
    trades = [Direct(me, size, lambda j, b=b: parts_ref.at[b, j], lambda j, b=b: partstok_ref.at[b, j], partstok_ref.at[b],
                     part_send.at[b], part_recv.at[b]) for b in range(early)]
    own_parts = [pltpu.make_async_copy(parts_ref.at[b, me], partstok_ref.at[b, me], load_sems.at[4 + b]) for b in range(early)]

    def prepare():
        metatile[...] = jnp.zeros_like(metatile)
        metatile[0:batch, 0:tok] = pos_ref[...]
        metatile[batch:2 * batch, 0:tok] = keep_ref[...]
        metabuf[me] = metatile[...]
        load_x.wait()

        gain, shift = gain_ref[...].reshape(1, 1, hidden), shift_ref[...].reshape(1, 1, hidden)

        def normalise(b, carry):
            x = xin[b].astype(jnp.float32)
            centered = x - jnp.mean(x, axis=-1, keepdims=True)
            inv_std = lax.rsqrt(jnp.mean(centered * centered, axis=-1, keepdims=True) + NORM_EPS)
            stage[b, :, 1] = (centered * inv_std * gain + shift).astype(jnp.bfloat16)
            return carry

        lax.fori_loop(0, batch, normalise, 0)
        load_dy.wait()

    greet_all(me, size, prepare)

    pieces = sbuf.shape[0]
    chip_rows = 2 * tok

    def chip_of(p, e):
        return torus.device_at(lax.rem(p + 1 + e, side), e) // 2

    def rows_at(p, e):
        return pl.ds(pl.multiple_of(chip_of(p, e) * chip_rows, chip_rows), chip_rows)

    def load_piece(b, p):
        return [pltpu.make_async_copy(gat_ref.at[b, pl.ds(chip_of(p, e) * 2, 2)], sbuf.at[p, e], piece_sems.at[p, e]) for e in range(side)]

    def start_piece(b, p):
        for load in load_piece(b, p):
            load.start()

    def rows_of(p, which, at=slice(None)):
        return sbuf[p, :, :, :, which, :, at].reshape(side * chip_rows, -1)

    def each(lo, hi, use):
        def body(p, carry):
            use(p)
            return carry

        lax.fori_loop(lo, hi, body, 0)

    def pad_lanes(a):
        return jnp.concatenate([a, jnp.zeros((a.shape[0], pad_dim - head_dim), a.dtype)], axis=1)

    def project(b, p):
        for load in load_piece(b, p):
            load.wait()
        bias = jnp.concatenate([bias_ref[c, pl.ds(me, 1), :] for c in range(3)], axis=1)
        r = (dot(rows_of(p, 1), wbuf[...], 1, 1) + bias).astype(jnp.bfloat16)
        d = pad_lanes(dot(rows_of(p, 0), wobuf[...], 1, 1).astype(jnp.bfloat16))
        q, k, v = (pad_lanes(r[:, c * head_dim:(c + 1) * head_dim]) for c in range(3))
        for e in range(side):
            mine = slice(e * chip_rows, (e + 1) * chip_rows)
            at = rows_at(p, e)
            for c, part in enumerate((q, k, v)):
                qkvb[at, c * pad_dim:(c + 1) * pad_dim] = part[mine]
            dob[at, :] = d[mine]

    def attend(b, i):
        span = (i + 1) * q_block
        mine = slice(i * q_block, span)
        if i == 0:
            dk_acc[...] = jnp.zeros_like(dk_acc)
            dv_acc[...] = jnp.zeros_like(dv_acc)
        q, k, v = qkvb[mine, :pad_dim], qkvb[:span, pad_dim:2 * pad_dim], qkvb[:span, 2 * pad_dim:]
        do = dob[mine, :]
        pos = rowbuf[pl.ds(b, 1), :span]
        keep = rowbuf[pl.ds(b + batch, 1), :span]
        bias = jnp.where(keep > 0, (-slope * LOG2E) * (pos[:, span - 1:] - pos).astype(jnp.float32), MASK_FILL)
        scores = dot(q, k, 1, 1) * (scale * LOG2E) + bias
        row_id = lax.broadcasted_iota(jnp.int32, (q_block, q_block), 0)
        col_id = lax.broadcasted_iota(jnp.int32, (q_block, q_block), 1)
        corner = jnp.where(col_id <= row_id, scores[:, span - q_block:], MASK_FILL)
        scores = jnp.concatenate([scores[:, :span - q_block], corner], axis=1) if i else corner
        expo = jnp.exp2(scores - jnp.max(scores, axis=-1, keepdims=True))
        prob = expo * (1.0 / jnp.sum(expo, axis=-1, keepdims=True))
        prob_lo = prob.astype(jnp.bfloat16)
        o = dot(prob_lo, v, 1, 0).astype(jnp.bfloat16)
        row_dot = jnp.sum(do.astype(jnp.float32) * o.astype(jnp.float32), axis=-1, keepdims=True)
        ds_lo = (prob * (dot(do, v, 1, 1) - row_dot)).astype(jnp.bfloat16)
        o_all[mine, :] = o
        dq_all[mine, :] = (dot(ds_lo, k, 1, 0) * scale).astype(jnp.bfloat16)
        dv_acc[:span, :] += dot(prob_lo, do, 0, 0)
        dk_acc[:span, :] += dot(ds_lo, q, 0, 0)

    def store_parts(b):
        return pltpu.make_async_copy(pbuf, parts_ref.at[b], parts_sem)

    def finish(b):
        dk = (dk_acc[...] * scale).astype(jnp.bfloat16)
        dv = dv_acc[...].astype(jnp.bfloat16)
        d_all[...] = jnp.concatenate([dq_all[:, :head_dim], dk[:, :head_dim], dv[:, :head_dim]], axis=1)
        whole = jnp.concatenate([d_all[...], o_all[:, :head_dim]], axis=1).reshape(size, tok, 4 * head_dim)
        pbuf[...] = jnp.concatenate([whole[:, :tok // 2], whole[:, tok // 2:]], axis=2)
        store_parts(b).start()

    width = min(1280, hidden)

    def gradient(p):
        d = jnp.concatenate([d_all[rows_at(p, e), :] for e in range(side)], axis=0)
        o = jnp.concatenate([o_all[rows_at(p, e), :] for e in range(side)], axis=0)[:, :head_dim]

        def columns(n, carry):
            at = pl.ds(pl.multiple_of(n * width, width), width)
            term = dot(d, rows_of(p, 1, at), 0, 0)
            row = 0
            for ref in (gwa_ref, gwb_ref, gwc_ref):
                ref[:, at] += term[row:row + ref.shape[0]]
                row += ref.shape[0]
            gwo_ref[:, at] += dot(o, rows_of(p, 0, at), 0, 0)
            return carry

        lax.fori_loop(0, hidden // width, columns, 0)

    count = seq_len // q_block
    last = pieces - 1
    tasks = {(0, READY - 3): [lambda b: each(0, last, lambda p: start_piece(b, p))],
             (0, READY - 2): [lambda b: each(0, last - 1, lambda p: project(b, p))],
             (0, READY - 1): [lambda b: project(b, last - 1)],
             (0, READY): [lambda b: start_piece(b, last)],
             (0, READY + 1): [lambda b: project(b, last)],
             (0, READY + 7): [finish],
             (0, READY + 8): [lambda b: each(0, pieces // 2, gradient)],
             (1, 0): [lambda b: each(pieces // 2, pieces, gradient)],
             (1, 1): [lambda b: store_parts(b).wait()]}
    spot = (2, 2, 2, 3, 3, 4, 5, 6)
    for i in range(count):
        tasks.setdefault((0, READY + spot[i]), []).append(lambda b, i=i: attend(b, i))

    for ref in (gwa_ref, gwb_ref, gwc_ref, gwo_ref):
        ref[...] = jnp.zeros_like(ref)

    def phase_of(i, place):
        return i - 1 if place == LATE else i

    def among(b):
        return jnp.logical_and(b >= 0, b < batch)

    def turn(i, carry):
        for place in range(places):
            came = (place - LAG) % places
            b_came = phase_of(i if place >= LAG else i - 1, came)

            @pl.when(among(b_came))
            def _():
                for link in range(4):
                    arrival(b_came, link, came).wait_recv()
                    share(b_came, link, came, 0).start()

            b_send = phase_of(i, place)

            @pl.when(among(b_send))
            def _():
                for link in range(4):
                    send(b_send, link, place).start()

            shared = (place - LAG - 1) % places
            b_shared = phase_of(i if place >= LAG + 1 else i - 1, shared)

            @pl.when(among(b_shared))
            def _():
                for link in range(4):
                    share(b_shared, link, shared, flip).wait_recv()

            if place == 1:
                @pl.when(i == 0)
                def _():
                    for b in range(batch):
                        share_own(b, me).start()
                        keep_own(b).start()
                    meta.start()

            if place == READY - 3:
                @pl.when(i == 1)
                def _():
                    for load in (load_wq, load_wo):
                        load.wait()
                    meta.wait_recv()
                    for j in range(size):
                        rowbuf[:, j * tok:(j + 1) * tok] = metabuf[j, :, :tok]
                    for b in range(batch):
                        share_own(b, sibling).wait_recv()
                        keep_own(b).wait()
                    meta.wait_send()
                    for b in range(batch):
                        share_own(b, me).wait_send()

            if place == READY:
                @pl.when(i == batch)
                def _():
                    for copy in own_parts + trades:
                        copy.start()

            for later in (0, 1):
                if (later, place) in tasks:
                    @pl.when(among(i - 1 - later))
                    def _():
                        for task in tasks[later, place]:
                            task(i - 1 - later)
        return carry

    lax.fori_loop(0, batch + 2, turn, 0)
    for copy in own_parts:
        copy.wait()
    for trade in trades:
        trade.wait_recv()
        trade.wait_send()
    sent = gat_ref.at[:, pl.ds(0, places), 0]
    for link in range(4):
        for sem in (ici_send, d2d_send):
            pltpu.make_async_remote_copy(
                src_ref=sent, dst_ref=sent, send_sem=sem.at[link], recv_sem=ici_recv.at[link, 0],
                device_id={"sp": sibling}, device_id_type=MESH).wait_send()


def split_rows(rows):
    first, short = 8 * (rows * 17 // 240), 8 * (rows // 40)
    return first, rows - first - short, short


def block_call(x, dy, gain, shift, pos, keep, wq, bias, wo, size, q_block, collective_id):
    batch, tok, hidden = x.shape
    rows = tok // COLOURS
    heads, head_dim, _ = wo.shape
    pad_dim = -(-head_dim // LANES) * LANES
    seq_len = size * tok
    side = math.isqrt(size // 2)
    places = PLACES
    anywhere = pl.BlockSpec(memory_space=pl.ANY)
    vmem = pl.BlockSpec(memory_space=pltpu.VMEM)
    sem = pltpu.SemaphoreType.DMA
    bf16, f32 = jnp.bfloat16, jnp.float32
    flops = batch * (6 * seq_len * seq_len * 256 + 4 * seq_len * 4 * head_dim * hidden) + 80_000_000_000
    cut = (batch, COLOURS, rows, hidden)
    first, second, short = split_rows(3 * head_dim)
    return pl.pallas_call(
        functools.partial(block_kernel, size, (batch, tok, head_dim, pad_dim, hidden, min(q_block, seq_len))),
        out_shape=(
            jax.ShapeDtypeStruct((batch, size, COLOURS, 2, rows, hidden), bf16),
            jax.ShapeDtypeStruct((batch, size, tok // 2, 8 * head_dim), bf16),
            jax.ShapeDtypeStruct((EARLY, size, tok // 2, 8 * head_dim), bf16),
            *(jax.ShapeDtypeStruct((n, hidden), f32) for n in (first, second, short, head_dim)),
        ),
        in_specs=[anywhere, anywhere, vmem, vmem, vmem, vmem, anywhere, vmem, anywhere],
        out_specs=(anywhere, anywhere, anywhere, vmem, vmem, vmem, vmem),
        scratch_shapes=[
            pltpu.VMEM(cut, bf16),
            pltpu.VMEM((batch, COLOURS, 2, rows, hidden), bf16),
            pltpu.VMEM((3 * head_dim, hidden), bf16),
            pltpu.VMEM((head_dim, hidden), bf16),
            pltpu.VMEM((8, LANES), jnp.int32),
            pltpu.VMEM((size, 8, LANES), jnp.int32),
            pltpu.VMEM((8, seq_len), jnp.int32),
            pltpu.VMEM((side, side, 2, COLOURS, 2, rows, hidden), bf16),
            pltpu.VMEM((seq_len, 3 * pad_dim), bf16),
            pltpu.VMEM((seq_len, pad_dim), bf16),
            pltpu.VMEM((seq_len, pad_dim), f32),
            pltpu.VMEM((seq_len, pad_dim), f32),
            pltpu.VMEM((seq_len, pad_dim), bf16),
            pltpu.VMEM((seq_len, pad_dim), bf16),
            pltpu.VMEM((seq_len, 3 * head_dim), bf16),
            pltpu.VMEM((size, tok // 2, 8 * head_dim), bf16),
            sem((4 + EARLY,)), sem((batch,)), sem((side, side)), sem,
            sem((4,)), sem((4, places)), sem((4,)), sem((4, places)), sem((batch,)), sem((batch,)), sem, sem, sem((EARLY,)), sem((EARLY,)),
        ],
        compiler_params=pltpu.CompilerParams(collective_id=collective_id, has_side_effects=True, vmem_limit_bytes=VMEM_LIMIT),
        cost_estimate=pl.CostEstimate(flops=flops, bytes_accessed=60_000_000, transcendentals=batch * seq_len * seq_len // 2),
        name="block",
    )(x.reshape(cut), dy.reshape(cut), gain, shift, pos, keep, wq, bias, wo)


class Spread:
    def __init__(self, size, own_ref, gat_ref, stage, sems):
        self.torus, self.size, self.gat_ref, self.stage = Torus(size), size, gat_ref, stage
        self.load_sem, self.keep_sem, self.ici_send, self.ici_recv, self.d2d_send, self.d2d_recv, self.own_send, self.own_recv = sems
        self.part = stage.shape[1] // COLOURS
        self.load = pltpu.make_async_copy(own_ref, stage, self.load_sem)
        self.keep = pltpu.make_async_copy(stage, gat_ref.at[self.torus.me], self.keep_sem)

    def columns(self, colour):
        return pl.ds(colour * self.part, self.part)

    def view(self, block, colour):
        return self.gat_ref.at[block, :, self.columns(colour)]

    def remote(self, src, dst, send_sem, recv_sem, device):
        return pltpu.make_async_remote_copy(
            src_ref=src, dst_ref=dst, send_sem=send_sem, recv_sem=recv_sem, device_id={"sp": device}, device_id_type=MESH)

    def send(self, link, place):
        block, colour = self.torus.chunk(link, place, 0)
        dst = self.view(block, colour)
        src = self.stage.at[:, self.columns(colour)] if is_own(place) else dst
        return self.remote(src, dst, self.ici_send.at[link], self.ici_recv.at[link, place], self.torus.neighbour(link))

    def arrival(self, link, place):
        ref = self.view(*self.torus.chunk(link, place, 1))
        return self.remote(ref, ref, self.ici_send.at[link], self.ici_recv.at[link, place], self.torus.me)

    def share(self, link, place, shift):
        block, colour = self.torus.chunk(link, place, 1)
        ref = self.view(block + shift, colour)
        return self.remote(ref, ref, self.d2d_send.at[link], self.d2d_recv.at[link, place], self.torus.sibling)

    def share_own(self, block):
        return self.remote(self.stage, self.gat_ref.at[block], self.own_send, self.own_recv, self.torus.sibling)

    STEPS = PLACES + LATE + LAG + 2

    def step(self, g):
        def place_of(g):
            place = g % PLACES
            return place if g >= 0 and g // PLACES == (1 if place == LATE else 0) else None

        came, now, shared = place_of(g - LAG), place_of(g), place_of(g - LAG - 1)
        for link in range(4):
            if came is not None:
                self.arrival(link, came).wait_recv()
                self.share(link, came, 0).start()
        for link in range(4):
            if now is not None:
                self.send(link, now).start()
        for link in range(4):
            if shared is not None:
                self.share(link, shared, self.torus.flip).wait_recv()
        if g == 1:
            self.share_own(self.torus.me).start()
            self.keep.start()

    def close(self):
        self.share_own(self.torus.sibling).wait_recv()
        self.keep.wait()
        self.share_own(self.torus.me).wait_send()
        sent = self.gat_ref.at[pl.ds(0, PLACES), :, pl.ds(0, self.part)]
        for link in range(4):
            for sem in (self.ici_send, self.d2d_send):
                self.remote(sent, sent, sem.at[link], self.ici_recv.at[link, 0], self.torus.sibling).wait_send()

    @staticmethod
    def scratch(rows, cols, dtype):
        sem = pltpu.SemaphoreType.DMA
        return [pltpu.VMEM((rows, cols), dtype), sem, sem, sem((4,)), sem((4, PLACES)), sem((4,)), sem((4, PLACES)), sem, sem]


def spread_kernel(size, own_ref, after_ref, gat_ref, stage, *sems):
    spread = Spread(size, own_ref, gat_ref, stage, sems)
    spread.load.start()
    barrier = pltpu.get_barrier_semaphore()
    friends = [spread.torus.neighbour(link) for link in range(4)] + [spread.torus.sibling]
    for friend in friends:
        pl.semaphore_signal(barrier, inc=1, device_id={"sp": friend}, device_id_type=MESH)
    pl.semaphore_wait(barrier, len(friends))
    spread.load.wait()
    for g in range(Spread.STEPS):
        spread.step(g)
    spread.close()


def spread_rows(block, after, size, collective_id):
    rows, cols = block.shape
    anywhere = pl.BlockSpec(memory_space=pl.ANY)
    return pl.pallas_call(
        functools.partial(spread_kernel, size),
        out_shape=jax.ShapeDtypeStruct((size, rows, cols), block.dtype),
        in_specs=[anywhere, anywhere],
        out_specs=anywhere,
        scratch_shapes=Spread.scratch(rows, cols, block.dtype),
        compiler_params=pltpu.CompilerParams(collective_id=collective_id, has_side_effects=True),
        cost_estimate=pl.CostEstimate(flops=50_000_000_000, bytes_accessed=8 * size * rows * cols, transcendentals=0),
        name="spread",
    )(block, after)


TOKEN_AT = 8
TOKEN_STEPS = 8


def token_kernel(size, head_dim, chunk, own_ref, parts_ref, early_ref, wq_ref, wo_ref, x_ref, dy_ref, gain_ref, bout_ref,
                 gat_ref, late_ref, y_ref, gx_ref, totals_ref,
                 stage, load_sem, keep_sem, ici_send, ici_recv, d2d_send, d2d_recv, own_send, own_recv,
                 wqbuf, wobuf, pbuf, dn_acc, y_acc, sums, tiles, come, total,
                 part_send, part_recv, own_part_sems, wq_sems, wo_sems, p_sems, deal_send, deal_recv, collect_send, collect_recv):
    spread = Spread(size, own_ref, gat_ref, stage,
                    (load_sem, keep_sem, ici_send, ici_recv, d2d_send, d2d_recv, own_send, own_recv))
    me = spread.torus.me
    early, late = early_ref.shape[0], late_ref.shape[0]
    heads, hidden = wq_ref.shape[0], wq_ref.shape[2]
    per = heads // TOKEN_STEPS
    trades, own_parts = [], []
    for n in range(late):
        b = parts_ref.shape[0] - late + n
        trades.append(Direct(me, size, lambda j, b=b: parts_ref.at[b, j], lambda j, n=n: late_ref.at[n, j], late_ref.at[n],
                             part_send.at[n], part_recv.at[n]))
        own_parts.append(pltpu.make_async_copy(parts_ref.at[b, me], late_ref.at[n, me], own_part_sems.at[n]))
    deal = Direct(me, size, lambda j: tiles.at[j], lambda j: come.at[j], come, deal_send, deal_recv)
    collect = Direct(me, size, lambda j: total, lambda j: totals_ref.at[j], totals_ref, collect_send, collect_recv)

    def weights(m):
        at, slot = pl.ds(m * per, per), m % 2
        return (pltpu.make_async_copy(wq_ref.at[at], wqbuf.at[slot], wq_sems.at[slot]),
                pltpu.make_async_copy(wo_ref.at[at], wobuf.at[slot], wo_sems.at[slot]))

    def rows(m):
        at, slot = pl.ds(m * per, per), m % 2
        sources = [early_ref.at[n, at] for n in range(early)] + [late_ref.at[n, at] for n in range(late)]
        return [pltpu.make_async_copy(src, pbuf.at[slot, n], p_sems.at[slot, n]) for n, src in enumerate(sources)]

    spread.load.start()
    for copy in weights(0):
        copy.start()
    dn_acc[...] = jnp.zeros_like(dn_acc)
    y_acc[...] = jnp.zeros_like(y_acc)
    sums[...] = jnp.zeros_like(sums)
    tiles[...] = jnp.zeros_like(tiles)
    width = hidden // 4

    def heads_step(m):
        slot = m % 2
        for copy in (*weights(m), *rows(m)):
            copy.wait()
        if m + 1 < TOKEN_STEPS:
            for copy in (*weights(m + 1), *rows(m + 1)):
                copy.start()

        def pair(i, carry):
            ds, os = [], []
            for h in range(2):
                parts = []
                for n in range(early + late):
                    both = pbuf[slot, n, i * 2 + h]
                    parts += [both[:, :4 * head_dim], both[:, 4 * head_dim:]]
                parts = jnp.concatenate(parts, axis=0)
                ds.append(parts[:, :3 * head_dim])
                os.append(parts[:, 3 * head_dim:])
                added = jnp.sum(ds[h].astype(jnp.float32), axis=0, keepdims=True)
                for c in range(3):
                    tiles[m * per + i * 2 + h, 3 + c:4 + c, 0:head_dim] = added[:, c * head_dim:(c + 1) * head_dim]

            def columns(n, carry):
                at = pl.ds(pl.multiple_of(n * width, width), width)
                dn_acc[:, at] += dot(ds[0], wqbuf[slot, i * 2, :, at], 1, 0) + dot(ds[1], wqbuf[slot, i * 2 + 1, :, at], 1, 0)
                y_acc[:, at] += dot(os[0], wobuf[slot, i * 2, :, at], 1, 0) + dot(os[1], wobuf[slot, i * 2 + 1, :, at], 1, 0)
                return carry

            lax.fori_loop(0, 4, columns, 0)
            return carry

        lax.fori_loop(0, per // 2, pair, 0)

    def norm_step(half):
        gain = gain_ref[...].reshape(1, hidden)
        bout = bout_ref[...].reshape(1, hidden)
        count = x_ref.shape[0] // chunk

        def body(c, carry):
            at = pl.ds(pl.multiple_of(c * chunk, chunk), chunk)
            x = x_ref[at, :].astype(jnp.float32)
            dy = dy_ref[at, :].astype(jnp.float32)
            centered = x - jnp.mean(x, axis=-1, keepdims=True)
            inv_std = lax.rsqrt(jnp.mean(centered * centered, axis=-1, keepdims=True) + NORM_EPS)
            x_hat = centered * inv_std
            d_norm = dn_acc[at, :]
            d_hat = d_norm * gain
            d_mean = jnp.mean(d_hat, axis=-1, keepdims=True)
            d_proj = jnp.mean(d_hat * x_hat, axis=-1, keepdims=True)
            gx_ref[at, :] = (dy + inv_std * (d_hat - d_mean - x_hat * d_proj)).astype(jnp.bfloat16)
            y_ref[at, :] = (x + y_acc[at, :] + bout).astype(jnp.bfloat16)
            sums[0:1, :] += jnp.sum(d_norm * x_hat, axis=0, keepdims=True)
            sums[1:2, :] += jnp.sum(d_norm, axis=0, keepdims=True)
            sums[2:3, :] += jnp.sum(dy, axis=0, keepdims=True)
            return carry

        lax.fori_loop(half * count // 2, (half + 1) * count // 2, body, 0)

    greet_all(me, size)
    spread.load.wait()
    for g in range(Spread.STEPS):
        spread.step(g)
        m = g - TOKEN_AT
        if g == 1:
            for copy in trades + own_parts:
                copy.start()
        if m == 0:
            for copy in own_parts:
                copy.wait()
            for trade in trades:
                trade.wait_recv()
            for copy in rows(0):
                copy.start()
        if 0 <= m < TOKEN_STEPS:
            heads_step(m)
        elif m in (TOKEN_STEPS, TOKEN_STEPS + 1):
            norm_step(m - TOKEN_STEPS)
        elif m == TOKEN_STEPS + 2:
            for j in range(size):
                tiles[j, 0:3, 0:head_dim] = sums[0:3, j * head_dim:(j + 1) * head_dim]
            come[me] = tiles[me]
        elif m == TOKEN_STEPS + 3:
            deal.start()
        elif m == TOKEN_STEPS + 5:
            deal.wait_recv()
            total[...] = jnp.sum(come[...], axis=0)
            totals_ref[me] = total[...]
            collect.start()
    spread.close()
    for trade in trades:
        trade.wait_send()
    deal.wait_send()
    collect.wait_recv()
    collect.wait_send()


def token_side(block, parts, early, wq, wo, x, dy, gain, bout, size, collective_id):
    rows, cols = block.shape
    late = parts.shape[0] - early.shape[0]
    heads, head_dim, hidden = wo.shape
    tokens = x.shape[0]
    per = heads // TOKEN_STEPS
    anywhere = pl.BlockSpec(memory_space=pl.ANY)
    vmem = pl.BlockSpec(memory_space=pltpu.VMEM)
    sem = pltpu.SemaphoreType.DMA
    bf16, f32 = jnp.bfloat16, jnp.float32
    return pl.pallas_call(
        functools.partial(token_kernel, size, head_dim, 16),
        out_shape=(
            jax.ShapeDtypeStruct((size, rows, cols), block.dtype),
            jax.ShapeDtypeStruct((late, *parts.shape[1:]), parts.dtype),
            jax.ShapeDtypeStruct((tokens, hidden), bf16),
            jax.ShapeDtypeStruct((tokens, hidden), bf16),
            jax.ShapeDtypeStruct((size, 8, LANES), f32),
        ),
        in_specs=[anywhere] * 5 + [vmem] * 4,
        out_specs=(anywhere, anywhere, vmem, vmem, vmem),
        scratch_shapes=Spread.scratch(rows, cols, block.dtype) + [
            pltpu.VMEM((2, per, 3 * head_dim, hidden), bf16),
            pltpu.VMEM((2, per, head_dim, hidden), bf16),
            pltpu.VMEM((2, parts.shape[0], per, *parts.shape[2:]), bf16),
            pltpu.VMEM((tokens, hidden), f32),
            pltpu.VMEM((tokens, hidden), f32),
            pltpu.VMEM((8, hidden), f32),
            pltpu.VMEM((size, 8, LANES), f32),
            pltpu.VMEM((size, 8, LANES), f32),
            pltpu.VMEM((8, LANES), f32),
            sem((late,)), sem((late,)), sem((late,)), sem((2,)), sem((2,)), sem((2, parts.shape[0])), sem, sem, sem, sem,
        ],
        compiler_params=pltpu.CompilerParams(collective_id=collective_id, has_side_effects=True, vmem_limit_bytes=VMEM_LIMIT),
        cost_estimate=pl.CostEstimate(flops=120_000_000_000, bytes_accessed=8 * size * rows * cols, transcendentals=0),
        name="token_side",
    )(block, parts, early, wq, wo, x, dy, gain, bout)


def hand_kernel(y_ref, gx_ref, y_out, gx_out, buf, sems):
    reads = [pltpu.make_async_copy(ref, buf.at[n], sems.at[0, n]) for n, ref in enumerate((y_ref, gx_ref))]
    writes = [pltpu.make_async_copy(buf.at[n], ref, sems.at[1, n]) for n, ref in enumerate((y_out, gx_out))]
    for read in reads:
        read.start()
    for read, write in zip(reads, writes):
        read.wait()
        write.start()
    for write in writes:
        write.wait()


def hand_over(y, gx):
    spec = pl.BlockSpec(memory_space=pl.ANY)
    return pl.pallas_call(
        hand_kernel, out_shape=(jax.ShapeDtypeStruct(y.shape, y.dtype),) * 2, in_specs=[spec] * 2, out_specs=(spec,) * 2,
        scratch_shapes=[pltpu.VMEM((2, *y.shape), y.dtype), pltpu.SemaphoreType.DMA((2, 2))],
        cost_estimate=pl.CostEstimate(flops=1_000_000_000, bytes_accessed=8 * y.size, transcendentals=0), name="hand_over")(y, gx)


def settle_kernel(block, depth, ahead, per, origin, first, src_ref, *refs):
    dst_ref, buf, read_sems, write_sems = refs[-4:]
    count = src_ref.shape[0] * per

    def slab(ref, i, start):
        return ref.at[i // per, pl.ds(pl.multiple_of(start + lax.rem(i, per) * block, 8), block)]

    def read(i):
        return pltpu.make_async_copy(slab(src_ref, i, origin), buf.at[lax.rem(i, depth)], read_sems.at[lax.rem(i, depth)])

    def write(i):
        return pltpu.make_async_copy(buf.at[lax.rem(i, depth)], slab(dst_ref, i, first), write_sems.at[lax.rem(i, depth)])

    def step(i, carry):
        @pl.when(jnp.logical_and(i >= depth, i < count))
        def _():
            write(i - depth).wait()

        @pl.when(i < count)
        def _():
            read(i).start()

        @pl.when(i >= ahead)
        def _():
            read(i - ahead).wait()
            write(i - ahead).start()

        return carry

    lax.fori_loop(0, count + ahead, step, 0)

    def drain(i, carry):
        write(i).wait()
        return carry

    lax.fori_loop(max(0, count - depth), count, drain, 0)


def settle(x, origin, rows, first, total, pieces=1, into=None, after=()):
    block = rows // pieces
    depth, ahead = 12, 6
    count, _, cols = x.shape
    sem = pltpu.SemaphoreType.DMA((depth,))
    old = [] if into is None else [into]
    return pl.pallas_call(
        functools.partial(settle_kernel, block, depth, ahead, pieces, origin, first),
        out_shape=jax.ShapeDtypeStruct((count, total, cols), x.dtype),
        in_specs=[pl.BlockSpec(memory_space=pl.ANY)] * (1 + len(old) + len(after)),
        out_specs=pl.BlockSpec(memory_space=pl.ANY),
        scratch_shapes=[pltpu.VMEM((depth, block, cols), x.dtype), sem, sem],
        input_output_aliases={1: 0} if old else {},
        compiler_params=pltpu.CompilerParams(vmem_limit_bytes=VMEM_LIMIT),
        cost_estimate=pl.CostEstimate(flops=10_000_000_000, bytes_accessed=8 * x.size, transcendentals=0),
        name="settle",
    )(x, *old, *after)


def solution(mesh):
    size = mesh.shape["sp"]

    def block_fn(x_blk, pos_blk, keep_blk, ln_gain, ln_bias, w_qkv, b_qkv, w_out, b_out, dy_blk):
        batch, tok, hidden = x_blk.shape
        heads, head_dim = w_qkv.shape[1], w_qkv.shape[3]
        tokens = batch * tok
        wq = jnp.transpose(w_qkv, (1, 2, 3, 0)).reshape(heads, 3 * head_dim, hidden)
        wo = w_out.reshape(heads, head_dim, hidden)

        def gather(a):
            return lax.all_gather(a, "sp", axis=0, tiled=True).reshape(heads, a.shape[0], hidden)

        _, parts, early, grad_a, grad_b, grad_c, grad_out = block_call(
            x_blk, dy_blk, ln_gain, ln_bias, pos_blk, keep_blk, wq, jnp.transpose(b_qkv, (1, 0, 2)), wo, size, 256, 0)

        all_out, _, y, grad_x, totals = token_side(
            grad_out, parts, early, wq, wo, x_blk.reshape(tokens, hidden), dy_blk.reshape(tokens, hidden), ln_gain, b_out, size, 1)
        y, grad_x = hand_over(y, grad_x)
        grad_wo = settle(all_out, 0, head_dim, 0, head_dim, after=(y,))

        rows = 3 * head_dim
        first, second, short = split_rows(rows)
        all_c = spread_rows(grad_c, grad_wo, size, 2)
        grad_wq = settle(gather(grad_a), 0, first, 0, rows, after=(all_c,))
        grad_wq = settle(all_c, 0, short, first + second, rows, into=grad_wq)
        grad_wq = settle(gather(grad_b), 0, second, first, rows, into=grad_wq)
        totals = totals[:, :, :head_dim]
        grad_wq = jnp.transpose(grad_wq.reshape(heads, 3, head_dim, hidden), (3, 0, 1, 2))
        return (y.reshape(x_blk.shape), grad_x.reshape(x_blk.shape), grad_wq, totals[:, 3:6],
                grad_wo.reshape(heads * head_dim, hidden), totals[:, 2].reshape(-1), totals[:, 0].reshape(-1), totals[:, 1].reshape(-1))

    act_spec = P("dp", "sp", None)
    tok_spec = P("dp", "sp")
    in_specs = (act_spec, tok_spec, tok_spec, P(), P(), P(), P(), P(), P(), act_spec)
    out_specs = (act_spec, act_spec, P("dp", None, None, None), P("dp", None, None), P("dp", None), P("dp"), P("dp"), P("dp"))
    return jax.shard_map(block_fn, mesh=mesh, in_specs=in_specs, out_specs=out_specs, check_vma=False)
```
